32 devices in a mesh: tp: 4 (over z), cp: 2 (over y), fsdp: 4 (over x, core).
Axes of the slice: x: 2, y: 2, z: 4, core: 2. Of those that a mesh axis runs over, the one named last changes fastest.
Arguments:
- hidden: bfloat16 [4, 2048, 4096], P('fsdp', 'cp')
- cotangent: bfloat16 [4, 2048, 4096], P('fsdp', 'cp')
- positions: int32 [2048], P('cp')
- gain: bfloat16 [4096], P('fsdp')
- w_query: bfloat16 [4096, 32, 128], P('fsdp', 'tp')
- w_key: bfloat16 [4096, 8, 128], P('fsdp', 'tp')
- w_value: bfloat16 [4096, 8, 128], P('fsdp', 'tp')
- w_out: bfloat16 [32, 128, 4096], P('tp', None, 'fsdp')
Outputs:
- output 1: bfloat16 [4, 2048, 4096], P('fsdp', 'cp')
- output 2: bfloat16 [4, 2048, 4096], P('fsdp', 'cp')
- output 3: float32 [4096], P('fsdp')
- output 4: float32 [4096, 32, 128], P('fsdp', 'tp')
- output 5: float32 [4096, 8, 128], P('fsdp', 'tp')
- output 6: float32 [4096, 8, 128], P('fsdp', 'tp')
- output 7: float32 [32, 128, 4096], P('tp', None, 'fsdp')
All inputs are finite; a program needn't handle non-finite values.
Results may differ from the reference program's by a relative error of at most 0.0138206.
Values are sent between devices in bfloat16 or wider.
A program may use at most 1 GiB of HBM per device.

```python
import math
import jax
import jax.numpy as jnp
from jax import lax

BATCH_ROWS = 4
SEQ_LEN = 2048
MODEL_DIM = 4096
NUM_HEADS = 32
NUM_KV = 8
HEAD_DIM = 128
WINDOW_LEN = 4096

ROPE_BASE = 10000.0
NORM_EPS = 1e-5
NEG_BIG = -1e30
GROUP_SIZE = NUM_HEADS // NUM_KV
Q_BLOCK = math.gcd(SEQ_LEN, 512)
KEY_SPAN = min(Q_BLOCK + WINDOW_LEN, SEQ_LEN)


def setup_inputs(seed: int = 0) -> dict:
    key_list = jax.random.split(jax.random.key(seed), 9)
    act_shape = (BATCH_ROWS, SEQ_LEN, MODEL_DIM)
    hidden = jax.random.normal(key_list[0], act_shape, jnp.float32)
    cotangent = jax.random.normal(key_list[1], act_shape, jnp.float32)
    step_key, start_key = jax.random.split(key_list[2])
    pos_steps = jax.random.randint(step_key, (SEQ_LEN,), 1, 3)
    pos_start = jax.random.randint(start_key, (), 0, 64)
    positions = (pos_start + jnp.cumsum(pos_steps) - pos_steps[0]).astype(jnp.int32)
    gain = 1.0 + 0.5 * jax.random.normal(key_list[3], (MODEL_DIM,), jnp.float32)
    in_scale = MODEL_DIM ** -0.5
    out_scale = (NUM_HEADS * HEAD_DIM) ** -0.5
    w_query = jax.random.normal(key_list[4], (MODEL_DIM, NUM_HEADS, HEAD_DIM), jnp.float32) * in_scale
    w_key = jax.random.normal(key_list[5], (MODEL_DIM, NUM_KV, HEAD_DIM), jnp.float32) * in_scale
    w_value = jax.random.normal(key_list[6], (MODEL_DIM, NUM_KV, HEAD_DIM), jnp.float32) * in_scale
    w_out = jax.random.normal(key_list[7], (NUM_HEADS, HEAD_DIM, MODEL_DIM), jnp.float32) * out_scale
    return {"hidden": hidden.astype(jnp.bfloat16), "cotangent": cotangent.astype(jnp.bfloat16), "positions": positions, "gain": gain.astype(jnp.bfloat16), "w_query": w_query.astype(jnp.bfloat16), "w_key": w_key.astype(jnp.bfloat16), "w_value": w_value.astype(jnp.bfloat16), "w_out": w_out.astype(jnp.bfloat16)}


def to_bf16(vals_in):
    return vals_in + lax.stop_gradient(vals_in.astype(jnp.bfloat16).astype(jnp.float32) - vals_in)


def rope_tables(positions):
    inv_freq = ROPE_BASE ** (-jnp.arange(0, HEAD_DIM, 2).astype(jnp.float32) / HEAD_DIM)
    angles = positions.astype(jnp.float32)[:, None] * inv_freq[None, :]
    return jnp.cos(angles), jnp.sin(angles)


def rope_apply(head_vals, cosines, sines):
    half_dim = HEAD_DIM // 2
    first_half = head_vals[..., :half_dim]
    second_half = head_vals[..., half_dim:]
    cos_b = cosines[:, None, :]
    sin_b = sines[:, None, :]
    return jnp.concatenate([first_half * cos_b - second_half * sin_b, second_half * cos_b + first_half * sin_b], axis=-1)


def row_forward(x_row, param_set, cosines, sines):
    gain, w_query, w_key, w_value, w_out = param_set
    inv_rms = lax.rsqrt(jnp.mean(x_row * x_row, axis=-1, keepdims=True) + NORM_EPS)
    normed = to_bf16(x_row * inv_rms * gain)
    q_rot = to_bf16(rope_apply(jnp.einsum("sm,mhd->shd", normed, w_query), cosines, sines))
    k_rot = to_bf16(rope_apply(jnp.einsum("sm,mhd->shd", normed, w_key), cosines, sines))
    v_val = to_bf16(jnp.einsum("sm,mhd->shd", normed, w_value))
    q_grp = q_rot.reshape(SEQ_LEN, NUM_KV, GROUP_SIZE, HEAD_DIM)
    score_scale = HEAD_DIM ** -0.5

    def attend_block(blk_idx):
        q_start = blk_idx * Q_BLOCK
        k_start = jnp.clip(q_start + Q_BLOCK - KEY_SPAN, 0, SEQ_LEN - KEY_SPAN)
        q_blk = lax.dynamic_slice_in_dim(q_grp, q_start, Q_BLOCK, 0)
        k_blk = lax.dynamic_slice_in_dim(k_rot, k_start, KEY_SPAN, 0)
        v_blk = lax.dynamic_slice_in_dim(v_val, k_start, KEY_SPAN, 0)
        q_idx = q_start + jnp.arange(Q_BLOCK)
        k_idx = k_start + jnp.arange(KEY_SPAN)
        allowed = (k_idx[None, :] <= q_idx[:, None]) & (k_idx[None, :] > q_idx[:, None] - WINDOW_LEN)
        scores = jnp.einsum("qkgd,skd->kgqs", q_blk, k_blk) * score_scale
        scores = jnp.where(allowed, scores, NEG_BIG)
        prob_vals = to_bf16(jax.nn.softmax(scores, axis=-1))
        return to_bf16(jnp.einsum("kgqs,skd->qkgd", prob_vals, v_blk))

    attn_out = lax.map(jax.checkpoint(attend_block), jnp.arange(SEQ_LEN // Q_BLOCK))
    attn_out = attn_out.reshape(SEQ_LEN, NUM_HEADS, HEAD_DIM)
    return x_row + jnp.einsum("shd,hdm->sm", attn_out, w_out)


def reference(hidden, cotangent, positions, gain, w_query, w_key, w_value, w_out):
    cosines, sines = rope_tables(positions)
    params = tuple(weight.astype(jnp.float32) for weight in (gain, w_query, w_key, w_value, w_out))

    def row_step(grad_acc, row_pair):
        x_row, ct_row = row_pair
        out_row, pullback = jax.vjp(lambda x_in, param_set: row_forward(x_in, param_set, cosines, sines), x_row.astype(jnp.float32), params)
        dx_row, grad_parts = pullback(ct_row.astype(jnp.float32))
        grad_acc = tuple(grad_sum + grad_part for grad_sum, grad_part in zip(grad_acc, grad_parts))
        return grad_acc, (out_row.astype(jnp.bfloat16), dx_row.astype(jnp.bfloat16))

    zero_grads = tuple(jnp.zeros_like(weight) for weight in params)
    grad_tuple, row_outs = lax.scan(row_step, zero_grads, (hidden, cotangent))
    return (row_outs[0], row_outs[1], grad_tuple[0], grad_tuple[1], grad_tuple[2], grad_tuple[3], grad_tuple[4])
```

```python
import functools
import math

import jax
import jax.numpy as jnp
from jax import lax
from jax.experimental import pallas as pl
from jax.experimental.pallas import tpu as pltpu
from jax.sharding import PartitionSpec as P

WINDOW_LEN = 4096
ROPE_BASE = 10000.0
NORM_EPS = 1e-5
NEG_BIG = -1e30
LOG2E = math.log2(math.e)
TILES = 4
CHUNKS = 16

MESH = pl.DeviceIdType.MESH


NT = (((1,), (1,)), ((), ()))
NN = (((1,), (0,)), ((), ()))


def dot(a, b, dims):
    return lax.dot_general(a, b, dims, preferred_element_type=jnp.float32)


def rope_tables(positions, head_dim):
    inv_freq = ROPE_BASE ** (-jnp.arange(0, head_dim, 2).astype(jnp.float32) / head_dim)
    angles = positions.astype(jnp.float32)[:, None] * inv_freq[None, :]
    cosines, sines = jnp.cos(angles), jnp.sin(angles)
    return jnp.concatenate([cosines, cosines], axis=1), jnp.concatenate([-sines, sines], axis=1)


def rope_rows(vals, cosines, sines, heads):
    rows, width = vals.shape
    head_dim = width // heads
    parts = vals.reshape(rows, heads, 2, head_dim // 2)
    swapped = jnp.concatenate([parts[:, :, 1:], parts[:, :, :1]], axis=2).reshape(rows, heads, head_dim)
    out = vals.reshape(rows, heads, head_dim) * cosines[:, None, :] + swapped * sines[:, None, :]
    return out.reshape(rows, width)


def fwd_kernel(group, tq, flag_ref, q_ref, cos_ref, sin_ref, kl_ref, vl_ref, kp_ref, vp_ref, o_ref, qr_ref, lse_ref, qs_ref, vt_ref, m_ref, l_ref, acc_ref):
    tile = pl.program_id(1)
    head_dim = kl_ref.shape[1]
    half = head_dim // 2
    kv_len = kl_ref.shape[0]
    wide = group * tq
    scale = head_dim ** -0.5 * LOG2E

    @pl.when(tile == 0)
    def _():
        vt_ref[0] = vl_ref[...].T
        vt_ref[1] = vp_ref[...].T

    for h in range(group):
        q_h = q_ref[:, h * head_dim:(h + 1) * head_dim]
        q_h = (q_h * cos_ref[...] + pltpu.roll(q_h, half, 1) * sin_ref[...]).astype(jnp.bfloat16)
        qr_ref[:, h * head_dim:(h + 1) * head_dim] = q_h
        qs_ref[h * tq:(h + 1) * tq, :] = q_h
    m_ref[...] = jnp.full_like(m_ref, NEG_BIG)
    l_ref[...] = jnp.zeros_like(l_ref)
    acc_ref[...] = jnp.zeros_like(acc_ref)

    def piece(k_ref, side, start, masked):
        scores = dot(k_ref[pl.ds(start, tq), :], qs_ref[...], NT)
        if masked:
            key_idx = lax.broadcasted_iota(jnp.int32, (tq, wide), 0)
            q_idx = lax.rem(lax.broadcasted_iota(jnp.int32, (tq, wide), 1), tq)
            scores = jnp.where(key_idx <= q_idx, scores, NEG_BIG)
        m_old = m_ref[...]
        m_new = jnp.maximum(m_old, jnp.max(scores, axis=0, keepdims=True))
        probs = jnp.exp2((scores - m_new) * scale)
        fade = jnp.exp2((m_old - m_new) * scale)
        m_ref[...] = m_new
        l_ref[...] = l_ref[...] * fade + jnp.sum(probs, axis=0, keepdims=True)
        acc_ref[...] = acc_ref[...] * fade + dot(vt_ref[side, :, pl.ds(start, tq)], probs.astype(jnp.bfloat16), NN)

    piece(kl_ref, 0, pl.multiple_of(tile * tq, tq), True)

    @pl.loop(0, tile)
    def _(i):
        piece(kl_ref, 0, pl.multiple_of(i * tq, tq), False)

    @pl.loop(0, flag_ref[0] * (kv_len // tq))
    def _(i):
        piece(kp_ref, 1, pl.multiple_of(i * tq, tq), False)

    total = l_ref[...]
    lse_ref[0] = m_ref[...] * scale + jnp.log2(total)
    out_t = acc_ref[...] / total
    for h in range(group):
        o_ref[:, h * head_dim:(h + 1) * head_dim] = out_t[:, h * tq:(h + 1) * tq].T.astype(jnp.bfloat16)


def bwd_kernel(group, tq, flag_ref, q_ref, o_ref, do_ref, lse_ref, cos_ref, sin_ref, kl_ref, vl_ref, kp_ref, vp_ref, dq_ref, dkl_ref, dvl_ref, dkp_ref, dvp_ref, qs_ref, dos_ref, delta_ref, kt_ref, dqt_ref):
    tile = pl.program_id(1)
    head_dim = kl_ref.shape[1]
    half = head_dim // 2
    kv_len = kl_ref.shape[0]
    wide = group * tq
    score_scale = head_dim ** -0.5

    @pl.when(tile == 0)
    def _():
        kt_ref[0] = kl_ref[...].T
        kt_ref[1] = kp_ref[...].T
        for ref in (dkl_ref, dvl_ref, dkp_ref, dvp_ref):
            ref[...] = jnp.zeros_like(ref)

    for h in range(group):
        cols = slice(h * head_dim, (h + 1) * head_dim)
        rows = slice(h * tq, (h + 1) * tq)
        qs_ref[rows, :] = q_ref[:, cols]
        d_h = do_ref[:, cols]
        dos_ref[rows, :] = d_h
        prod = d_h.astype(jnp.float32) * o_ref[:, cols].astype(jnp.float32)
        delta_ref[:, rows] = jnp.sum(prod.T, axis=0, keepdims=True)
    dqt_ref[...] = jnp.zeros_like(dqt_ref)

    def piece(k_ref, v_ref, dk_ref, dv_ref, side, start, masked):
        span = pl.ds(start, tq)
        scores = dot(k_ref[span, :], qs_ref[...], NT)
        if masked:
            key_idx = lax.broadcasted_iota(jnp.int32, (tq, wide), 0)
            q_idx = lax.rem(lax.broadcasted_iota(jnp.int32, (tq, wide), 1), tq)
            scores = jnp.where(key_idx <= q_idx, scores, NEG_BIG)
        probs = jnp.exp2(scores * (score_scale * LOG2E) - lse_ref[0])
        d_probs = dot(v_ref[span, :], dos_ref[...], NT)
        d_scores = (probs * (d_probs - delta_ref[...]) * score_scale).astype(jnp.bfloat16)
        dv_ref[span, :] += dot(probs.astype(jnp.bfloat16), dos_ref[...], NN)
        dk_ref[span, :] += dot(d_scores, qs_ref[...], NN)
        dqt_ref[...] += dot(kt_ref[side, :, span], d_scores, NN)

    piece(kl_ref, vl_ref, dkl_ref, dvl_ref, 0, pl.multiple_of(tile * tq, tq), True)

    @pl.loop(0, tile)
    def _(i):
        piece(kl_ref, vl_ref, dkl_ref, dvl_ref, 0, pl.multiple_of(i * tq, tq), False)

    @pl.loop(0, flag_ref[0] * (kv_len // tq))
    def _(i):
        piece(kp_ref, vp_ref, dkp_ref, dvp_ref, 1, pl.multiple_of(i * tq, tq), False)

    for h in range(group):
        dq_h = dqt_ref[:, h * tq:(h + 1) * tq].T
        dq_h = dq_h * cos_ref[...] - pltpu.roll(dq_h, half, 1) * sin_ref[...]
        dq_ref[:, h * head_dim:(h + 1) * head_dim] = dq_h.astype(jnp.bfloat16)


def attn_specs(q_len, head_dim, group, tq):
    q_spec = pl.BlockSpec((tq, group * head_dim), lambda g, i: (i, g))
    kv_spec = pl.BlockSpec((q_len, head_dim), lambda g, i: (0, g))
    row_spec = pl.BlockSpec((tq, head_dim), lambda g, i: (i, 0))
    lse_spec = pl.BlockSpec((1, 1, group * tq), lambda g, i: (g * TILES + i, 0, 0))
    flag_spec = pl.BlockSpec(memory_space=pltpu.SMEM)
    return flag_spec, q_spec, kv_spec, row_spec, lse_spec


def attn_forward(flag, q_lin, cosines, sines, k_loc, v_loc, k_prev, v_prev, group, head_dim):
    q_len, width = q_lin.shape
    kv_heads = width // (group * head_dim)
    tq = q_len // TILES
    wide = group * tq
    flag_spec, q_spec, kv_spec, row_spec, lse_spec = attn_specs(q_len, head_dim, group, tq)
    return pl.pallas_call(
        functools.partial(fwd_kernel, group, tq),
        grid=(kv_heads, TILES),
        in_specs=[flag_spec, q_spec, row_spec, row_spec, kv_spec, kv_spec, kv_spec, kv_spec],
        out_specs=[q_spec, q_spec, lse_spec],
        out_shape=[jax.ShapeDtypeStruct((q_len, width), jnp.bfloat16), jax.ShapeDtypeStruct((q_len, width), jnp.bfloat16), jax.ShapeDtypeStruct((kv_heads * TILES, 1, wide), jnp.float32)],
        scratch_shapes=[pltpu.VMEM((wide, head_dim), jnp.bfloat16), pltpu.VMEM((2, head_dim, q_len), jnp.bfloat16), pltpu.VMEM((1, wide), jnp.float32), pltpu.VMEM((1, wide), jnp.float32), pltpu.VMEM((head_dim, wide), jnp.float32)],
        compiler_params=pltpu.CompilerParams(dimension_semantics=("arbitrary", "arbitrary")),
        cost_estimate=pl.CostEstimate(flops=4 * 12 * q_len * q_len // 8 * width, bytes_accessed=10 * q_len * width, transcendentals=12 * q_len * q_len),
        name="attn_fwd",
    )(flag, q_lin, cosines, sines, k_loc, v_loc, k_prev, v_prev)


def attn_backward(flag, q_rot, attn_out, d_attn, lse, cosines, sines, k_loc, v_loc, k_prev, v_prev, group, head_dim):
    q_len, width = q_rot.shape
    kv_heads = width // (group * head_dim)
    tq = q_len // TILES
    wide = group * tq
    flag_spec, q_spec, kv_spec, row_spec, lse_spec = attn_specs(q_len, head_dim, group, tq)
    kv_shape = jax.ShapeDtypeStruct((q_len, kv_heads * head_dim), jnp.float32)
    return pl.pallas_call(
        functools.partial(bwd_kernel, group, tq),
        grid=(kv_heads, TILES),
        in_specs=[flag_spec, q_spec, q_spec, q_spec, lse_spec, row_spec, row_spec, kv_spec, kv_spec, kv_spec, kv_spec],
        out_specs=[q_spec, kv_spec, kv_spec, kv_spec, kv_spec],
        out_shape=[jax.ShapeDtypeStruct((q_len, width), jnp.bfloat16), kv_shape, kv_shape, kv_shape, kv_shape],
        scratch_shapes=[pltpu.VMEM((wide, head_dim), jnp.bfloat16), pltpu.VMEM((wide, head_dim), jnp.bfloat16), pltpu.VMEM((1, wide), jnp.float32), pltpu.VMEM((2, head_dim, q_len), jnp.bfloat16), pltpu.VMEM((head_dim, wide), jnp.float32)],
        compiler_params=pltpu.CompilerParams(dimension_semantics=("arbitrary", "arbitrary")),
        cost_estimate=pl.CostEstimate(flops=10 * 12 * q_len * q_len // 8 * width, bytes_accessed=20 * q_len * width, transcendentals=12 * q_len * q_len),
        name="attn_bwd",
    )(flag, q_rot, attn_out, d_attn, lse, cosines, sines, k_loc, v_loc, k_prev, v_prev)


def line_barrier(z, last):
    barrier = pltpu.get_barrier_semaphore()

    @pl.when(z > 0)
    def _():
        pl.semaphore_signal(barrier, inc=1, device_id={"tp": z - 1}, device_id_type=MESH)

    @pl.when(z < last)
    def _():
        pl.semaphore_signal(barrier, inc=1, device_id={"tp": z + 1}, device_id_type=MESH)

    pl.semaphore_wait(barrier, jnp.where(z > 0, 1, 0) + jnp.where(z < last, 1, 0))


def rs_kernel(n_line, dims, x_ref, w_ref, gain_ref, hid_ref, ct_ref, own_ref, gg_ref, buf_ref, pbuf_ref, hbuf_ref, cbuf_ref, send_sem, recv_sem, load_sem):
    last = n_line - 1
    z = lax.axis_index("tp")
    chunks, rows = buf_ref.shape[1], buf_ref.shape[2]
    block = pbuf_ref.shape[1]
    per_block = block // rows
    half = chunks * rows
    is_grad = ct_ref is not None
    own_side = jnp.where(z == last, 1, 0)
    own_rows = pl.ds(pl.multiple_of(own_side * half, half), half)
    loads = [pltpu.make_async_copy(hid_ref.at[own_rows], hbuf_ref, load_sem.at[0])]
    if is_grad:
        loads.append(pltpu.make_async_copy(ct_ref.at[own_rows], cbuf_ref, load_sem.at[1]))
        gg_ref[...] = jnp.zeros_like(gg_ref)
    for load in loads:
        load.start()
    line_barrier(z, last)
    for load in loads:
        load.wait()

    def copy(side, chunk):
        target = jnp.clip(z - 1 if side == 0 else z + 1, 0, last)
        return pltpu.make_async_remote_copy(src_ref=buf_ref.at[side, chunk], dst_ref=buf_ref.at[side, chunk], send_sem=send_sem.at[side, chunk], recv_sem=recv_sem.at[side, chunk], device_id={"tp": target}, device_id_type=MESH)

    def finish(chunk, total):
        span = pl.ds(pl.multiple_of(chunk * rows, rows), rows)
        x_in = hbuf_ref[span, :].astype(jnp.float32)
        if not is_grad:
            own_ref[span, :] = (x_in + total).astype(jnp.bfloat16)
            return
        inv = lax.rsqrt(jnp.mean(x_in * x_in, axis=1, keepdims=True) + NORM_EPS)
        x_hat = x_in * inv
        gg_ref[...] += jnp.sum(total * x_hat, axis=0, keepdims=True)
        scaled = total * gain_ref[...]
        inner = jnp.mean(scaled * x_hat, axis=1, keepdims=True)
        own_ref[span, :] = (cbuf_ref[span, :].astype(jnp.float32) + inv * (scaled - x_hat * inner)).astype(jnp.bfloat16)

    def dist(side):
        return last - z if side == 0 else z

    @pl.loop(0, chunks + last)
    def _(step):
        for side in range(2):
            chunk = step - dist(side)

            @pl.when((chunk >= 0) & (chunk < chunks) & (lax.rem(chunk, per_block) == 0))
            def _():
                start = pl.multiple_of(side * half + chunk * rows, block)
                pbuf_ref[side] = dot(x_ref[pl.ds(start, block), :], w_ref[...], dims)

        for side in range(2):
            chunk = step - dist(side)
            part = pl.ds(pl.multiple_of(lax.rem(jnp.maximum(chunk, 0), per_block) * rows, rows), rows)

            @pl.when((chunk >= 0) & (chunk < chunks))
            def _():
                @pl.when(dist(side) == 0)
                def _():
                    buf_ref[side, chunk] = pbuf_ref[side, part, :]
                    copy(side, chunk).start()

                @pl.when(dist(side) > 0)
                def _():
                    copy(side, chunk).wait_recv()

                @pl.when((dist(side) > 0) & (dist(side) < last))
                def _():
                    buf_ref[side, chunk] += pbuf_ref[side, part, :]
                    copy(side, chunk).start()

                @pl.when(dist(side) == last)
                def _():
                    finish(chunk, buf_ref[side, chunk] + pbuf_ref[side, part, :])

    for side in range(2):
        @pl.when(dist(side) < last)
        def _():
            @pl.loop(0, chunks)
            def _(chunk):
                copy(side, chunk).wait_send()


def line_reduce(x, w, dims, hidden, cotangent, gain, n_line, cid):
    q_len, model_dim = hidden.shape
    half = q_len // 2
    rows = half // CHUNKS
    block = min(128, half)
    anyspec, vspec = pl.BlockSpec(memory_space=pl.ANY), pl.BlockSpec(memory_space=pltpu.VMEM)
    is_grad = cotangent is not None
    out_shape = [jax.ShapeDtypeStruct((half, model_dim), jnp.bfloat16)] + ([jax.ShapeDtypeStruct((1, model_dim), jnp.float32)] if is_grad else [])
    scratch = [
        pltpu.VMEM((2, CHUNKS, rows, model_dim), jnp.float32),
        pltpu.VMEM((2, block, model_dim), jnp.float32),
        pltpu.VMEM((half, model_dim), jnp.bfloat16),
    ]
    sems = [pltpu.SemaphoreType.DMA((2, CHUNKS)), pltpu.SemaphoreType.DMA((2, CHUNKS)), pltpu.SemaphoreType.DMA((2,))]
    if is_grad:
        body = functools.partial(rs_kernel, n_line, dims)
        args = (x, w, gain, hidden, cotangent)
        in_specs = [vspec, vspec, vspec, anyspec, anyspec]
        scratch.append(pltpu.VMEM((half, model_dim), jnp.bfloat16))
    else:
        def body(x_ref, w_ref, hid_ref, own_ref, buf_ref, pbuf_ref, hbuf_ref, *sem):
            rs_kernel(n_line, dims, x_ref, w_ref, None, hid_ref, None, own_ref, None, buf_ref, pbuf_ref, hbuf_ref, None, *sem)

        args = (x, w, hidden)
        in_specs = [vspec, vspec, anyspec]
    return pl.pallas_call(
        body,
        in_specs=in_specs,
        out_specs=[vspec] * len(out_shape),
        out_shape=out_shape,
        scratch_shapes=scratch + sems,
        compiler_params=pltpu.CompilerParams(collective_id=cid, has_side_effects=True, vmem_limit_bytes=63 * 2**20),
        cost_estimate=pl.CostEstimate(flops=2 * 10**11, bytes_accessed=2**25, transcendentals=0),
        name="line_reduce",
    )(*args)


def ag_kernel(n_line, chunks, own_a_ref, own_b_ref, out_a_ref, out_b_ref, local_sem, send_sem, recv_sem):
    last = n_line - 1
    z = lax.axis_index("tp")
    half = own_a_ref.shape[0]
    rows = half // chunks
    pairs = ((own_a_ref, out_a_ref), (own_b_ref, out_b_ref))
    line_barrier(z, last)

    def dist(side):
        return last - z if side == 0 else z

    def span(side, chunk):
        return pl.ds(pl.multiple_of(side * half + chunk * rows, rows), rows)

    def forward(which, side, chunk, src):
        target = jnp.clip(z + 1 if side == 0 else z - 1, 0, last)
        slot = which * chunks + chunk
        return pltpu.make_async_remote_copy(src_ref=src, dst_ref=pairs[which][1].at[span(side, chunk)], send_sem=send_sem.at[side, slot], recv_sem=recv_sem.at[side, slot], device_id={"tp": target}, device_id_type=MESH)

    def local(which, side):
        own, out = pairs[which]
        return pltpu.make_async_copy(own, out.at[pl.ds(side * half, half)], local_sem.at[which])

    for side in range(2):
        @pl.when(dist(side) == last)
        def _():
            for which in range(2):
                @pl.loop(0, chunks)
                def _(chunk):
                    piece = pl.ds(pl.multiple_of(chunk * rows, rows), rows)
                    forward(which, side, chunk, pairs[which][0].at[piece]).start()
            for which in range(2):
                local(which, side).start()

    for which in range(2):
        @pl.loop(0, chunks + last - 1)
        def _(step):
            for side in range(2):
                chunk = step - (last - 1 - dist(side))

                @pl.when((dist(side) < last) & (chunk >= 0) & (chunk < chunks))
                def _():
                    src = pairs[which][1].at[span(side, jnp.clip(chunk, 0, chunks - 1))]
                    hop = forward(which, side, jnp.clip(chunk, 0, chunks - 1), src)
                    hop.wait_recv()

                    @pl.when(dist(side) > 0)
                    def _():
                        hop.start()

    for side in range(2):
        for which in range(2):
            @pl.when(dist(side) == last)
            def _():
                local(which, side).wait()

            @pl.when(dist(side) > 0)
            def _():
                @pl.loop(0, chunks)
                def _(chunk):
                    forward(which, side, chunk, pairs[which][1].at[span(side, chunk)]).wait_send()


def line_spread(own_a, own_b, n_line, cid):
    half, model_dim = own_a.shape
    anyspec, vspec = pl.BlockSpec(memory_space=pl.ANY), pl.BlockSpec(memory_space=pltpu.VMEM)
    out = jax.ShapeDtypeStruct((2 * half, model_dim), jnp.bfloat16)
    return pl.pallas_call(
        functools.partial(ag_kernel, n_line, CHUNKS),
        in_specs=[vspec, vspec],
        out_specs=[anyspec, anyspec],
        out_shape=[out, out],
        scratch_shapes=[pltpu.SemaphoreType.DMA((2,)), pltpu.SemaphoreType.DMA((2, 2 * CHUNKS)), pltpu.SemaphoreType.DMA((2, 2 * CHUNKS))],
        compiler_params=pltpu.CompilerParams(collective_id=cid, has_side_effects=True),
        cost_estimate=pl.CostEstimate(flops=2 * 10**11, bytes_accessed=2**25, transcendentals=0),
        name="line_spread",
    )(own_a, own_b)


def solution(mesh):
    act_spec = P("fsdp", "cp", None)
    proj_spec = P("fsdp", "tp", None)
    wout_spec = P("tp", None, "fsdp")
    n_line = mesh.shape["tp"]

    def reduce_grad(full_grad, dim):
        part = lax.psum_scatter(full_grad, "fsdp", scatter_dimension=dim, tiled=True)
        return part + lax.ppermute(part, "cp", [(0, 1), (1, 0)])

    def device_step(hidden, cotangent, positions, gain, w_query, w_key, w_value, w_out):
        hidden = hidden[0]
        cotangent = cotangent[0]
        q_len, model_dim = hidden.shape
        feat, q_heads, head_dim = w_query.shape
        kv_heads = w_key.shape[1]
        group = q_heads // kv_heads
        q_width, kv_width = q_heads * head_dim, kv_heads * head_dim
        flag = lax.axis_index("cp").astype(jnp.int32).reshape(1)

        gain_full = lax.all_gather(gain, "fsdp", axis=0, tiled=True).astype(jnp.float32)
        w_kv = jnp.concatenate([w_key.reshape(feat, kv_width), w_value.reshape(feat, kv_width)], axis=1)
        wkv_full = lax.all_gather(w_kv, "fsdp", axis=0, tiled=True)
        wq_full = lax.all_gather(w_query.reshape(feat, q_width), "fsdp", axis=0, tiled=True)
        wo_full = lax.all_gather(w_out.reshape(q_width, feat), "fsdp", axis=1, tiled=True)
        cosines, sines = rope_tables(positions, head_dim)

        hidden_f = hidden.astype(jnp.float32)
        inv_rms = lax.rsqrt(jnp.mean(hidden_f * hidden_f, axis=-1, keepdims=True) + NORM_EPS)
        normed = (hidden_f * inv_rms * gain_full).astype(jnp.bfloat16)

        kv_lin = dot(normed, wkv_full, NN)
        k_loc = rope_rows(kv_lin[:, :kv_width], cosines, sines, kv_heads).astype(jnp.bfloat16)
        v_loc = kv_lin[:, kv_width:].astype(jnp.bfloat16)
        k_prev = lax.ppermute(k_loc, "cp", [(0, 1)])
        v_prev = lax.ppermute(v_loc, "cp", [(0, 1)])
        q_lin = dot(normed, wq_full, NN)
        attn_out, q_rot, lse = attn_forward(flag, q_lin, cosines, sines, k_loc, v_loc, k_prev, v_prev, group, head_dim)

        own_out, = line_reduce(attn_out, wo_full, NN, hidden, None, None, n_line, 0)

        d_attn = dot(cotangent, wo_full, NT).astype(jnp.bfloat16)
        grad_wout = dot(attn_out, cotangent, (((0,), (0,)), ((), ())))
        dq_lin, dk_loc, dv_loc, dk_prev, dv_prev = attn_backward(flag, q_rot, attn_out, d_attn, lse, cosines, sines, k_loc, v_loc, k_prev, v_prev, group, head_dim)
        dk_rot = dk_loc + lax.ppermute(dk_prev, "cp", [(1, 0)])
        dv_lin = (dv_loc + lax.ppermute(dv_prev, "cp", [(1, 0)])).astype(jnp.bfloat16)
        dk_lin = rope_rows(dk_rot, cosines, -sines, kv_heads).astype(jnp.bfloat16)
        dkv_lin = jnp.concatenate([dk_lin, dv_lin], axis=1)
        TN = (((0,), (0,)), ((), ()))
        grad_query = dot(normed, dq_lin, TN)
        grad_kv = dot(normed, dkv_lin, TN)
        w_all = jnp.concatenate([wq_full, wkv_full], axis=1)
        d_all = jnp.concatenate([dq_lin, dkv_lin], axis=1)
        own_hid, gain_part = line_reduce(d_all, w_all, NT, hidden, cotangent, gain_full[None], n_line, 1)
        block_out, grad_hidden = line_spread(own_out, own_hid, n_line, 2)
        gain_sum = lax.psum(gain_part[0], ("tp", "cp", "fsdp"))
        grad_gain = lax.dynamic_slice_in_dim(gain_sum, lax.axis_index("fsdp") * feat, feat, 0)
        g_kv = reduce_grad(grad_kv, 0)
        g_out = reduce_grad(grad_wout, 1)
        g_q = reduce_grad(grad_query, 0)
        return (
            block_out[None],
            grad_hidden[None],
            grad_gain,
            g_q.reshape(feat, q_heads, head_dim),
            g_kv[:, :kv_width].reshape(feat, kv_heads, head_dim),
            g_kv[:, kv_width:].reshape(feat, kv_heads, head_dim),
            g_out.reshape(q_heads, head_dim, feat),
        )

    return jax.shard_map(device_step, mesh=mesh, in_specs=(act_spec, act_spec, P("cp"), P("fsdp"), proj_spec, proj_spec, proj_spec, wout_spec), out_specs=(act_spec, act_spec, P("fsdp"), proj_spec, proj_spec, proj_spec, wout_spec), check_vma=False)
```

```python
import functools
import math

import jax
import jax.numpy as jnp
from jax import lax
from jax.experimental import pallas as pl
from jax.experimental.pallas import tpu as pltpu
from jax.sharding import PartitionSpec as P

WINDOW_LEN = 4096
ROPE_BASE = 10000.0
NORM_EPS = 1e-5
NEG_BIG = -1e30
LOG2E = math.log2(math.e)
TILES = 4
CHUNKS = 16

MESH = pl.DeviceIdType.MESH


NT = (((1,), (1,)), ((), ()))
NN = (((1,), (0,)), ((), ()))


def dot(a, b, dims):
    return lax.dot_general(a, b, dims, preferred_element_type=jnp.float32)


def rope_tables(positions, head_dim):
    inv_freq = ROPE_BASE ** (-jnp.arange(0, head_dim, 2).astype(jnp.float32) / head_dim)
    angles = positions.astype(jnp.float32)[:, None] * inv_freq[None, :]
    cosines, sines = jnp.cos(angles), jnp.sin(angles)
    return jnp.concatenate([cosines, cosines], axis=1), jnp.concatenate([-sines, sines], axis=1)


def rope_rows(vals, cosines, sines, heads):
    rows, width = vals.shape
    head_dim = width // heads
    parts = vals.reshape(rows, heads, 2, head_dim // 2)
    swapped = jnp.concatenate([parts[:, :, 1:], parts[:, :, :1]], axis=2).reshape(rows, heads, head_dim)
    out = vals.reshape(rows, heads, head_dim) * cosines[:, None, :] + swapped * sines[:, None, :]
    return out.reshape(rows, width)


def fwd_kernel(group, tq, flag_ref, q_ref, cos_ref, sin_ref, kl_ref, vl_ref, kp_ref, vp_ref, o_ref, qr_ref, lse_ref, qs_ref, vt_ref, m_ref, l_ref, acc_ref):
    tile = pl.program_id(1)
    head_dim = kl_ref.shape[1]
    half = head_dim // 2
    kv_len = kl_ref.shape[0]
    wide = group * tq
    scale = head_dim ** -0.5 * LOG2E

    @pl.when(tile == 0)
    def _():
        vt_ref[0] = vl_ref[...].T
        vt_ref[1] = vp_ref[...].T

    for h in range(group):
        q_h = q_ref[:, h * head_dim:(h + 1) * head_dim]
        q_h = (q_h * cos_ref[...] + pltpu.roll(q_h, half, 1) * sin_ref[...]).astype(jnp.bfloat16)
        qr_ref[:, h * head_dim:(h + 1) * head_dim] = q_h
        qs_ref[h * tq:(h + 1) * tq, :] = q_h
    m_ref[...] = jnp.full_like(m_ref, NEG_BIG)
    l_ref[...] = jnp.zeros_like(l_ref)
    acc_ref[...] = jnp.zeros_like(acc_ref)

    def piece(k_ref, side, start, masked):
        scores = dot(k_ref[pl.ds(start, tq), :], qs_ref[...], NT)
        if masked:
            key_idx = lax.broadcasted_iota(jnp.int32, (tq, wide), 0)
            q_idx = lax.rem(lax.broadcasted_iota(jnp.int32, (tq, wide), 1), tq)
            scores = jnp.where(key_idx <= q_idx, scores, NEG_BIG)
        m_old = m_ref[...]
        m_new = jnp.maximum(m_old, jnp.max(scores, axis=0, keepdims=True))
        probs = jnp.exp2((scores - m_new) * scale)
        fade = jnp.exp2((m_old - m_new) * scale)
        m_ref[...] = m_new
        l_ref[...] = l_ref[...] * fade + jnp.sum(probs, axis=0, keepdims=True)
        acc_ref[...] = acc_ref[...] * fade + dot(vt_ref[side, :, pl.ds(start, tq)], probs.astype(jnp.bfloat16), NN)

    piece(kl_ref, 0, pl.multiple_of(tile * tq, tq), True)

    @pl.loop(0, tile)
    def _(i):
        piece(kl_ref, 0, pl.multiple_of(i * tq, tq), False)

    @pl.loop(0, flag_ref[0] * (kv_len // tq))
    def _(i):
        piece(kp_ref, 1, pl.multiple_of(i * tq, tq), False)

    total = l_ref[...]
    lse_ref[0] = m_ref[...] * scale + jnp.log2(total)
    out_t = acc_ref[...] / total
    for h in range(group):
        o_ref[:, h * head_dim:(h + 1) * head_dim] = out_t[:, h * tq:(h + 1) * tq].T.astype(jnp.bfloat16)


def attn_specs(q_len, head_dim, group, tq):
    q_spec = pl.BlockSpec((tq, group * head_dim), lambda g, i: (i, g))
    kv_spec = pl.BlockSpec((q_len, head_dim), lambda g, i: (0, g))
    row_spec = pl.BlockSpec((tq, head_dim), lambda g, i: (i, 0))
    lse_spec = pl.BlockSpec((1, 1, group * tq), lambda g, i: (g * TILES + i, 0, 0))
    flag_spec = pl.BlockSpec(memory_space=pltpu.SMEM)
    return flag_spec, q_spec, kv_spec, row_spec, lse_spec


def attn_forward(flag, q_lin, cosines, sines, k_loc, v_loc, k_prev, v_prev, group, head_dim):
    q_len, width = q_lin.shape
    kv_heads = width // (group * head_dim)
    tq = q_len // TILES
    wide = group * tq
    flag_spec, q_spec, kv_spec, row_spec, lse_spec = attn_specs(q_len, head_dim, group, tq)
    return pl.pallas_call(
        functools.partial(fwd_kernel, group, tq),
        grid=(kv_heads, TILES),
        in_specs=[flag_spec, q_spec, row_spec, row_spec, kv_spec, kv_spec, kv_spec, kv_spec],
        out_specs=[q_spec, q_spec, lse_spec],
        out_shape=[jax.ShapeDtypeStruct((q_len, width), jnp.bfloat16), jax.ShapeDtypeStruct((q_len, width), jnp.bfloat16), jax.ShapeDtypeStruct((kv_heads * TILES, 1, wide), jnp.float32)],
        scratch_shapes=[pltpu.VMEM((wide, head_dim), jnp.bfloat16), pltpu.VMEM((2, head_dim, q_len), jnp.bfloat16), pltpu.VMEM((1, wide), jnp.float32), pltpu.VMEM((1, wide), jnp.float32), pltpu.VMEM((head_dim, wide), jnp.float32)],
        compiler_params=pltpu.CompilerParams(dimension_semantics=("arbitrary", "arbitrary")),
        cost_estimate=pl.CostEstimate(flops=4 * 12 * q_len * q_len // 8 * width, bytes_accessed=10 * q_len * width, transcendentals=12 * q_len * q_len),
        name="attn_fwd",
    )(flag, q_lin, cosines, sines, k_loc, v_loc, k_prev, v_prev)


def neighbor_barrier(z, last, other):
    barrier = pltpu.get_barrier_semaphore()

    @pl.when(z > 0)
    def _():
        pl.semaphore_signal(barrier, inc=1, device_id={"tp": z - 1}, device_id_type=MESH)

    @pl.when(z < last)
    def _():
        pl.semaphore_signal(barrier, inc=1, device_id={"tp": z + 1}, device_id_type=MESH)

    if other is not None:
        pl.semaphore_signal(barrier, inc=1, device_id={"cp": other}, device_id_type=MESH)
    extra = 0 if other is None else 1
    pl.semaphore_wait(barrier, jnp.where(z > 0, 1, 0) + jnp.where(z < last, 1, 0) + extra)


class Line:
    def __init__(self, n_line, buf_ref, pbuf_ref, send_sem, recv_sem, block_dot, finish):
        self.last = n_line - 1
        self.z = lax.axis_index("tp")
        self.buf, self.pbuf, self.send_sem, self.recv_sem = buf_ref, pbuf_ref, send_sem, recv_sem
        self.chunks, self.rows = buf_ref.shape[1], buf_ref.shape[2]
        self.block = pbuf_ref.shape[1]
        self.per_block = self.block // self.rows
        self.half = self.chunks * self.rows
        self.block_dot, self.finish = block_dot, finish
        self.steps = self.chunks + self.last

    def dist(self, side):
        return self.last - self.z if side == 0 else self.z

    def copy(self, side, chunk):
        target = jnp.clip(self.z - 1 if side == 0 else self.z + 1, 0, self.last)
        return pltpu.make_async_remote_copy(src_ref=self.buf.at[side, chunk], dst_ref=self.buf.at[side, chunk], send_sem=self.send_sem.at[side, chunk], recv_sem=self.recv_sem.at[side, chunk], device_id={"tp": target}, device_id_type=MESH)

    def tick(self, step):
        for side in range(2):
            chunk = step - self.dist(side)

            @pl.when((chunk >= 0) & (chunk < self.chunks) & (lax.rem(chunk, self.per_block) == 0))
            def _():
                start = pl.multiple_of(side * self.half + chunk * self.rows, self.block)
                self.pbuf[side] = self.block_dot(pl.ds(start, self.block))

        for side in range(2):
            chunk = step - self.dist(side)
            dist = self.dist(side)
            part = pl.ds(pl.multiple_of(lax.rem(jnp.maximum(chunk, 0), self.per_block) * self.rows, self.rows), self.rows)

            @pl.when((chunk >= 0) & (chunk < self.chunks))
            def _():
                @pl.when(dist == 0)
                def _():
                    self.buf[side, chunk] = self.pbuf[side, part, :]
                    self.copy(side, chunk).start()

                @pl.when(dist > 0)
                def _():
                    self.copy(side, chunk).wait_recv()

                @pl.when((dist > 0) & (dist < self.last))
                def _():
                    self.buf[side, chunk] += self.pbuf[side, part, :]
                    self.copy(side, chunk).start()

                @pl.when(dist == self.last)
                def _():
                    span = pl.ds(pl.multiple_of(chunk * self.rows, self.rows), self.rows)
                    self.finish(span, self.buf[side, chunk] + self.pbuf[side, part, :])

    def drain(self):
        for side in range(2):
            @pl.when(self.dist(side) < self.last)
            def _():
                @pl.loop(0, self.chunks)
                def _(chunk):
                    self.copy(side, chunk).wait_send()


def mid_kernel(n_line, group, o_ref, w_ref, q_ref, lse_ref, cos_ref, sin_ref, kl_ref, vl_ref, kp_ref, vp_ref, hid_ref, ct_ref, _after_ref, own_ref, dq_ref, dkv_ref, buf_ref, pbuf_ref, hbuf_ref, ctb_ref, do_ref, dkl_ref, dvl_ref, dkp_ref, dvp_ref, qs_ref, dos_ref, delta_ref, kt_ref, dqt_ref, send_sem, recv_sem, load_sem, ct_sem, xs_sem, xr_sem):
    last = n_line - 1
    z, flag = lax.axis_index("tp"), lax.axis_index("cp")
    q_len, width = o_ref.shape
    head_dim = cos_ref.shape[1]
    half_dim = head_dim // 2
    kv_width = kl_ref.shape[1]
    kv_heads = kv_width // head_dim
    tq = q_len // TILES
    wide = group * tq
    score_scale = head_dim ** -0.5
    half = q_len // 2
    own_rows = pl.ds(pl.multiple_of(jnp.where(z == last, half, 0), half), half)
    load = pltpu.make_async_copy(hid_ref.at[own_rows], hbuf_ref, load_sem.at[0])
    load.start()

    def ct_load(tile):
        slot = lax.rem(tile, 2)
        return pltpu.make_async_copy(ct_ref.at[pl.ds(pl.multiple_of(tile * tq, tq), tq)], ctb_ref.at[slot], ct_sem.at[slot])

    ct_load(0).start()
    ct_load(1).start()
    for ref in (dkl_ref, dvl_ref):
        ref[...] = jnp.zeros_like(ref)

    @pl.when(flag == 1)
    def _():
        for ref in (dkp_ref, dvp_ref):
            ref[...] = jnp.zeros_like(ref)

    neighbor_barrier(z, last, 1 - flag)
    load.wait()

    def finish(span, total):
        own_ref[span, :] = (hbuf_ref[span, :].astype(jnp.float32) + total).astype(jnp.bfloat16)

    line = Line(n_line, buf_ref, pbuf_ref, send_sem, recv_sem, lambda rows: dot(o_ref[rows, :], w_ref[...], NN), finish)

    def do_tile(tile):
        ct_load(tile).wait()
        rows = pl.ds(pl.multiple_of(tile * tq, tq), tq)
        do_ref[rows, :] = dot(ctb_ref[lax.rem(tile, 2)], w_ref[...], NT).astype(jnp.bfloat16)

        @pl.when(tile + 2 < TILES)
        def _():
            ct_load(tile + 2).start()

    def bwd_item(item):
        g, tile = item // TILES, lax.rem(item, TILES)
        kv_cols = pl.ds(pl.multiple_of(g * head_dim, head_dim), head_dim)
        rows = pl.ds(pl.multiple_of(tile * tq, tq), tq)

        @pl.when(tile == 0)
        def _():
            kt_ref[0] = kl_ref[:, kv_cols].T
            kt_ref[1] = kp_ref[:, kv_cols].T

        for h in range(group):
            cols = pl.ds(pl.multiple_of((g * group + h) * head_dim, head_dim), head_dim)
            stack = slice(h * tq, (h + 1) * tq)
            qs_ref[stack, :] = q_ref[rows, cols]
            d_h = do_ref[rows, cols]
            dos_ref[stack, :] = d_h
            prod = d_h.astype(jnp.float32) * o_ref[rows, cols].astype(jnp.float32)
            delta_ref[:, stack] = jnp.sum(prod.T, axis=0, keepdims=True)
        dqt_ref[...] = jnp.zeros_like(dqt_ref)

        def piece(k_ref, v_ref, dk_ref, dv_ref, side, start, masked):
            span = pl.ds(start, tq)
            scores = dot(k_ref[span, kv_cols], qs_ref[...], NT)
            if masked:
                key_idx = lax.broadcasted_iota(jnp.int32, (tq, wide), 0)
                q_idx = lax.rem(lax.broadcasted_iota(jnp.int32, (tq, wide), 1), tq)
                scores = jnp.where(key_idx <= q_idx, scores, NEG_BIG)
            probs = jnp.exp2(scores * (score_scale * LOG2E) - lse_ref[item])
            d_probs = dot(v_ref[span, kv_cols], dos_ref[...], NT)
            d_scores = (probs * (d_probs - delta_ref[...]) * score_scale).astype(jnp.bfloat16)
            dv_ref[g, span, :] += dot(probs.astype(jnp.bfloat16), dos_ref[...], NN)
            dk_ref[g, span, :] += dot(d_scores, qs_ref[...], NN)
            dqt_ref[...] += dot(kt_ref[side, :, span], d_scores, NN)

        piece(kl_ref, vl_ref, dkl_ref, dvl_ref, 0, pl.multiple_of(tile * tq, tq), True)

        @pl.loop(0, tile)
        def _(i):
            piece(kl_ref, vl_ref, dkl_ref, dvl_ref, 0, pl.multiple_of(i * tq, tq), False)

        @pl.loop(0, flag * (q_len // tq))
        def _(i):
            piece(kp_ref, vp_ref, dkp_ref, dvp_ref, 1, pl.multiple_of(i * tq, tq), False)

        for h in range(group):
            dq_h = dqt_ref[:, h * tq:(h + 1) * tq].T
            dq_h = dq_h * cos_ref[rows, :] - pltpu.roll(dq_h, half_dim, 1) * sin_ref[rows, :]
            dq_ref[rows, pl.ds(pl.multiple_of((g * group + h) * head_dim, head_dim), head_dim)] = dq_h.astype(jnp.bfloat16)

        @pl.when((tile == TILES - 1) & (flag == 1))
        def _():
            for copy in back(g):
                copy.start()

    def back(g):
        return [pltpu.make_async_remote_copy(src_ref=ref.at[g], dst_ref=ref.at[g], send_sem=xs_sem.at[k, g], recv_sem=xr_sem.at[k, g], device_id={"cp": 0}, device_id_type=MESH) for k, ref in enumerate((dkp_ref, dvp_ref))]

    def kv_done(g):
        @pl.when(flag == 0)
        def _():
            for copy in back(g):
                copy.wait_recv()
            dkl_ref[g] += dkp_ref[g]
            dvl_ref[g] += dvp_ref[g]

        dk = dkl_ref[g]
        dk = dk * cos_ref[...] - pltpu.roll(dk, half_dim, 1) * sin_ref[...]
        dkv_ref[:, g * head_dim:(g + 1) * head_dim] = dk.astype(jnp.bfloat16)
        dkv_ref[:, kv_width + g * head_dim:kv_width + (g + 1) * head_dim] = dvl_ref[g].astype(jnp.bfloat16)

        @pl.when(flag == 1)
        def _():
            for copy in back(g):
                copy.wait_send()

    items = TILES * kv_heads

    @pl.loop(0, line.steps)
    def _(step):
        line.tick(step)

        @pl.when(step < TILES)
        def _():
            do_tile(step)

        @pl.when((step >= TILES) & (step < TILES + items))
        def _():
            bwd_item(step - TILES)

        for g in range(kv_heads):
            @pl.when(step == min(TILES * (g + 2) + 4, line.steps - 1))
            def _():
                kv_done(g)

    line.drain()


def line_middle(attn_out, wo_full, q_rot, lse, cosines, sines, k_loc, v_loc, k_prev, v_prev, hidden, cotangent, after, n_line, group, cid):
    q_len, model_dim = hidden.shape
    width = attn_out.shape[1]
    head_dim = cosines.shape[1]
    kv_width = k_loc.shape[1]
    kv_heads = kv_width // head_dim
    half = q_len // 2
    tq = q_len // TILES
    wide = group * tq
    block = min(128, half)
    anyspec, vspec = pl.BlockSpec(memory_space=pl.ANY), pl.BlockSpec(memory_space=pltpu.VMEM)
    bf, f32 = jnp.bfloat16, jnp.float32
    acc = pltpu.VMEM((kv_heads, q_len, head_dim), f32)
    return pl.pallas_call(
        functools.partial(mid_kernel, n_line, group),
        in_specs=[vspec] * 10 + [anyspec] * 3,
        out_specs=[vspec] * 3,
        out_shape=[jax.ShapeDtypeStruct((half, model_dim), bf), jax.ShapeDtypeStruct((q_len, width), bf), jax.ShapeDtypeStruct((q_len, 2 * kv_width), bf)],
        scratch_shapes=[
            pltpu.VMEM((2, CHUNKS, half // CHUNKS, model_dim), f32),
            pltpu.VMEM((2, block, model_dim), f32),
            pltpu.VMEM((half, model_dim), bf),
            pltpu.VMEM((2, tq, model_dim), bf),
            pltpu.VMEM((q_len, width), bf),
            acc, acc, acc, acc,
            pltpu.VMEM((wide, head_dim), bf),
            pltpu.VMEM((wide, head_dim), bf),
            pltpu.VMEM((1, wide), f32),
            pltpu.VMEM((2, head_dim, q_len), bf),
            pltpu.VMEM((head_dim, wide), f32),
            pltpu.SemaphoreType.DMA((2, CHUNKS)),
            pltpu.SemaphoreType.DMA((2, CHUNKS)),
            pltpu.SemaphoreType.DMA((1,)),
            pltpu.SemaphoreType.DMA((2,)),
            pltpu.SemaphoreType.DMA((2, kv_heads)),
            pltpu.SemaphoreType.DMA((2, kv_heads)),
        ],
        compiler_params=pltpu.CompilerParams(collective_id=cid, has_side_effects=True, vmem_limit_bytes=67043328),
        cost_estimate=pl.CostEstimate(flops=2 * 10**11, bytes_accessed=2**25, transcendentals=0),
        name="line_middle",
    )(attn_out, wo_full, q_rot, lse, cosines, sines, k_loc, v_loc, k_prev, v_prev, hidden, cotangent, after)


def in_kernel(n_line, dq_ref, dkv_ref, wq_ref, wkv_ref, gain_ref, hid_ref, ct_ref, own_ref, gg_ref, buf_ref, pbuf_ref, hbuf_ref, cbuf_ref, send_sem, recv_sem, load_sem):
    last = n_line - 1
    z = lax.axis_index("tp")
    half = hbuf_ref.shape[0]
    own_rows = pl.ds(pl.multiple_of(jnp.where(z == last, half, 0), half), half)
    loads = [pltpu.make_async_copy(src.at[own_rows], dst, load_sem.at[k]) for k, (src, dst) in enumerate(((hid_ref, hbuf_ref), (ct_ref, cbuf_ref)))]
    for load in loads:
        load.start()
    gg_ref[...] = jnp.zeros_like(gg_ref)
    neighbor_barrier(z, last, None)
    for load in loads:
        load.wait()

    def finish(span, total):
        x_in = hbuf_ref[span, :].astype(jnp.float32)
        inv = lax.rsqrt(jnp.mean(x_in * x_in, axis=1, keepdims=True) + NORM_EPS)
        x_hat = x_in * inv
        gg_ref[...] += jnp.sum(total * x_hat, axis=0, keepdims=True)
        scaled = total * gain_ref[...]
        inner = jnp.mean(scaled * x_hat, axis=1, keepdims=True)
        own_ref[span, :] = (cbuf_ref[span, :].astype(jnp.float32) + inv * (scaled - x_hat * inner)).astype(jnp.bfloat16)

    def block_dot(rows):
        return dot(dq_ref[rows, :], wq_ref[...], NT) + dot(dkv_ref[rows, :], wkv_ref[...], NT)

    line = Line(n_line, buf_ref, pbuf_ref, send_sem, recv_sem, block_dot, finish)

    @pl.loop(0, line.steps)
    def _(step):
        line.tick(step)

    line.drain()


def line_input(dq_lin, dkv_lin, wq_full, wkv_full, gain, hidden, cotangent, n_line, cid):
    q_len, model_dim = hidden.shape
    half = q_len // 2
    block = min(128, half)
    anyspec, vspec = pl.BlockSpec(memory_space=pl.ANY), pl.BlockSpec(memory_space=pltpu.VMEM)
    return pl.pallas_call(
        functools.partial(in_kernel, n_line),
        in_specs=[vspec] * 5 + [anyspec] * 2,
        out_specs=[vspec] * 2,
        out_shape=[jax.ShapeDtypeStruct((half, model_dim), jnp.bfloat16), jax.ShapeDtypeStruct((1, model_dim), jnp.float32)],
        scratch_shapes=[
            pltpu.VMEM((2, CHUNKS, half // CHUNKS, model_dim), jnp.float32),
            pltpu.VMEM((2, block, model_dim), jnp.float32),
            pltpu.VMEM((half, model_dim), jnp.bfloat16),
            pltpu.VMEM((half, model_dim), jnp.bfloat16),
            pltpu.SemaphoreType.DMA((2, CHUNKS)),
            pltpu.SemaphoreType.DMA((2, CHUNKS)),
            pltpu.SemaphoreType.DMA((2,)),
        ],
        compiler_params=pltpu.CompilerParams(collective_id=cid, has_side_effects=True, vmem_limit_bytes=67043328),
        cost_estimate=pl.CostEstimate(flops=2 * 10**11, bytes_accessed=2**25, transcendentals=0),
        name="line_input",
    )(dq_lin, dkv_lin, wq_full, wkv_full, gain, hidden, cotangent)


def ag_kernel(n_line, chunks, own_a_ref, own_b_ref, out_a_ref, out_b_ref, local_sem, send_sem, recv_sem):
    last = n_line - 1
    z = lax.axis_index("tp")
    half = own_a_ref.shape[0]
    rows = half // chunks
    pairs = ((own_a_ref, out_a_ref), (own_b_ref, out_b_ref))
    neighbor_barrier(z, last, None)

    def dist(side):
        return last - z if side == 0 else z

    def span(side, chunk):
        return pl.ds(pl.multiple_of(side * half + chunk * rows, rows), rows)

    def forward(which, side, chunk, src):
        target = jnp.clip(z + 1 if side == 0 else z - 1, 0, last)
        slot = which * chunks + chunk
        return pltpu.make_async_remote_copy(src_ref=src, dst_ref=pairs[which][1].at[span(side, chunk)], send_sem=send_sem.at[side, slot], recv_sem=recv_sem.at[side, slot], device_id={"tp": target}, device_id_type=MESH)

    def local(which, side):
        own, out = pairs[which]
        return pltpu.make_async_copy(own, out.at[pl.ds(side * half, half)], local_sem.at[which])

    for side in range(2):
        @pl.when(dist(side) == last)
        def _():
            for which in range(2):
                @pl.loop(0, chunks)
                def _(chunk):
                    piece = pl.ds(pl.multiple_of(chunk * rows, rows), rows)
                    forward(which, side, chunk, pairs[which][0].at[piece]).start()
            for which in range(2):
                local(which, side).start()

    for which in range(2):
        @pl.loop(0, chunks + last - 1)
        def _(step):
            for side in range(2):
                chunk = step - (last - 1 - dist(side))

                @pl.when((dist(side) < last) & (chunk >= 0) & (chunk < chunks))
                def _():
                    src = pairs[which][1].at[span(side, jnp.clip(chunk, 0, chunks - 1))]
                    hop = forward(which, side, jnp.clip(chunk, 0, chunks - 1), src)
                    hop.wait_recv()

                    @pl.when(dist(side) > 0)
                    def _():
                        hop.start()

    for side in range(2):
        for which in range(2):
            @pl.when(dist(side) == last)
            def _():
                local(which, side).wait()

            @pl.when(dist(side) > 0)
            def _():
                @pl.loop(0, chunks)
                def _(chunk):
                    forward(which, side, chunk, pairs[which][1].at[span(side, chunk)]).wait_send()


def line_spread(own_a, own_b, n_line, cid):
    half, model_dim = own_a.shape
    anyspec, vspec = pl.BlockSpec(memory_space=pl.ANY), pl.BlockSpec(memory_space=pltpu.VMEM)
    out = jax.ShapeDtypeStruct((2 * half, model_dim), jnp.bfloat16)
    return pl.pallas_call(
        functools.partial(ag_kernel, n_line, CHUNKS),
        in_specs=[vspec, vspec],
        out_specs=[anyspec, anyspec],
        out_shape=[out, out],
        scratch_shapes=[pltpu.SemaphoreType.DMA((2,)), pltpu.SemaphoreType.DMA((2, 2 * CHUNKS)), pltpu.SemaphoreType.DMA((2, 2 * CHUNKS))],
        compiler_params=pltpu.CompilerParams(collective_id=cid, has_side_effects=True),
        cost_estimate=pl.CostEstimate(flops=2 * 10**11, bytes_accessed=2**25, transcendentals=0),
        name="line_spread",
    )(own_a, own_b)


def solution(mesh):
    act_spec = P("fsdp", "cp", None)
    proj_spec = P("fsdp", "tp", None)
    wout_spec = P("tp", None, "fsdp")
    n_line = mesh.shape["tp"]

    def scatter(full_grad, dim):
        return lax.psum_scatter(full_grad, "fsdp", scatter_dimension=dim, tiled=True)

    def other_half(part):
        return lax.ppermute(part, "cp", [(0, 1), (1, 0)])

    def device_step(hidden, cotangent, positions, gain, w_query, w_key, w_value, w_out):
        hidden = hidden[0]
        cotangent = cotangent[0]
        q_len, model_dim = hidden.shape
        feat, q_heads, head_dim = w_query.shape
        kv_heads = w_key.shape[1]
        group = q_heads // kv_heads
        q_width, kv_width = q_heads * head_dim, kv_heads * head_dim
        flag = lax.axis_index("cp").astype(jnp.int32).reshape(1)

        gain_full = lax.all_gather(gain, "fsdp", axis=0, tiled=True).astype(jnp.float32)
        w_kv = jnp.concatenate([w_key.reshape(feat, kv_width), w_value.reshape(feat, kv_width)], axis=1)
        wkv_full = lax.all_gather(w_kv, "fsdp", axis=0, tiled=True)
        wq_full = lax.all_gather(w_query.reshape(feat, q_width), "fsdp", axis=0, tiled=True)
        wo_full = lax.all_gather(w_out.reshape(q_width, feat), "fsdp", axis=1, tiled=True)
        cosines, sines = rope_tables(positions, head_dim)

        hidden_f = hidden.astype(jnp.float32)
        inv_rms = lax.rsqrt(jnp.mean(hidden_f * hidden_f, axis=-1, keepdims=True) + NORM_EPS)
        normed = (hidden_f * inv_rms * gain_full).astype(jnp.bfloat16)

        kv_lin = dot(normed, wkv_full, NN)
        k_loc = rope_rows(kv_lin[:, :kv_width], cosines, sines, kv_heads).astype(jnp.bfloat16)
        v_loc = kv_lin[:, kv_width:].astype(jnp.bfloat16)
        k_prev = lax.ppermute(k_loc, "cp", [(0, 1)])
        v_prev = lax.ppermute(v_loc, "cp", [(0, 1)])
        q_lin = dot(normed, wq_full, NN)
        attn_out, q_rot, lse = attn_forward(flag, q_lin, cosines, sines, k_loc, v_loc, k_prev, v_prev, group, head_dim)

        TN = (((0,), (0,)), ((), ()))
        grad_wout = dot(attn_out, cotangent, TN)
        own_out, dq_lin, dkv_lin = line_middle(attn_out, wo_full, q_rot, lse, cosines, sines, k_loc, v_loc, k_prev, v_prev, hidden, cotangent, grad_wout, n_line, group, 0)
        part_out = scatter(grad_wout, 1)
        normed, part_out = lax.optimization_barrier((normed, part_out))
        far_out = other_half(part_out)
        part_kv = scatter(dot(normed, dkv_lin, TN), 0)
        part_q = scatter(dot(normed, dq_lin, TN), 0)
        own_hid, gain_part = line_input(dq_lin, dkv_lin, wq_full, wkv_full, gain_full[None], hidden, cotangent, n_line, 1)
        own_hid, far_out = lax.optimization_barrier((own_hid, far_out))
        block_out, grad_hidden = line_spread(own_out, own_hid, n_line, 2)
        gain_sum = lax.psum(gain_part[0], ("tp", "cp", "fsdp"))
        grad_gain = lax.dynamic_slice_in_dim(gain_sum, lax.axis_index("fsdp") * feat, feat, 0)
        g_kv, g_out, g_q = part_kv + other_half(part_kv), part_out + far_out, part_q + other_half(part_q)
        return (
            block_out[None],
            grad_hidden[None],
            grad_gain,
            g_q.reshape(feat, q_heads, head_dim),
            g_kv[:, :kv_width].reshape(feat, kv_heads, head_dim),
            g_kv[:, kv_width:].reshape(feat, kv_heads, head_dim),
            g_out.reshape(q_heads, head_dim, feat),
        )

    return jax.shard_map(device_step, mesh=mesh, in_specs=(act_spec, act_spec, P("cp"), P("fsdp"), proj_spec, proj_spec, proj_spec, wout_spec), out_specs=(act_spec, act_spec, P("fsdp"), proj_spec, proj_spec, proj_spec, wout_spec), check_vma=False)
```

```python
import functools
import math

import jax
import jax.numpy as jnp
from jax import lax
from jax.experimental import pallas as pl
from jax.experimental.pallas import tpu as pltpu
from jax.sharding import PartitionSpec as P

WINDOW_LEN = 4096
ROPE_BASE = 10000.0
NORM_EPS = 1e-5
NEG_BIG = -1e30
LOG2E = math.log2(math.e)
TILES = 4
CHUNKS = 16
PIECES = 4
O_PIECES = 2

MESH = pl.DeviceIdType.MESH


NT = (((1,), (1,)), ((), ()))
NN = (((1,), (0,)), ((), ()))


def dot(a, b, dims):
    return lax.dot_general(a, b, dims, preferred_element_type=jnp.float32)


def rope_tables(positions, head_dim):
    inv_freq = ROPE_BASE ** (-jnp.arange(0, head_dim, 2).astype(jnp.float32) / head_dim)
    angles = positions.astype(jnp.float32)[:, None] * inv_freq[None, :]
    cosines, sines = jnp.cos(angles), jnp.sin(angles)
    return jnp.concatenate([cosines, cosines], axis=1), jnp.concatenate([-sines, sines], axis=1)


def front_kernel(group, hid_ref, gain_ref, w_ref, wo_ref, cos_ref, sin_ref, o_ref, qr_ref, lse_ref, kl_ref, vl_ref, kp_ref, vp_ref, gfull_ref, n_out, w_out, wo_out, wbuf, nbuf, acc, hbuf, gbuf, qs, vt, m_all, l_all, acc_all, h_sem, g_send, g_recv, own_send, own_recv, x_send, x_recv, y_send, y_recv, d_send, d_recv, kv_send, kv_recv, ox_send, ox_recv, oy_send, oy_recv, od_send, od_recv, out_sem):
    q_len, feat = hid_ref.shape[0], w_ref.shape[0]
    head_dim = cos_ref.shape[1]
    half_dim = head_dim // 2
    kv_width = kl_ref.shape[1]
    kv_heads = kv_width // head_dim
    q_width = qr_ref.shape[1]
    tq = q_len // TILES
    wide = group * tq
    scale = head_dim ** -0.5 * LOG2E
    half = feat // 2
    piece = half // PIECES
    o_rows = wo_ref.shape[0]
    o_half = o_rows // 2
    o_piece = o_half // O_PIECES
    flag, f = lax.axis_index("cp"), lax.axis_index("fsdp")
    x, core = f // 2, lax.rem(f, 2)
    f_core = 2 * x + 1 - core
    f_x = 2 * (1 - x) + core
    f_diag = 2 * (1 - x) + 1 - core

    def remote(src, dst, send, recv, where):
        return pltpu.make_async_remote_copy(src_ref=src, dst_ref=dst, send_sem=send, recv_sem=recv, device_id=where, device_id_type=MESH)

    to_core, to_x, to_diag, to_y = {"fsdp": f_core}, {"fsdp": f_x}, {"fsdp": f_diag}, {"cp": 1 - flag}

    def h_load(tile):
        slot = lax.rem(tile, 2)
        return pltpu.make_async_copy(hid_ref.at[pl.ds(pl.multiple_of(tile * tq, tq), tq)], hbuf.at[slot], h_sem.at[slot])

    h_load(0).start()
    h_load(1).start()
    barrier = pltpu.get_barrier_semaphore()
    for where in (to_core, to_x, to_diag, to_y):
        pl.semaphore_signal(barrier, inc=1, device_id=where, device_id_type=MESH)
    pl.semaphore_wait(barrier, 4)

    def span(side, j):
        return pl.ds(pl.multiple_of(side * half + j * piece, piece), piece)

    def x_copy(j):
        return remote(w_ref.at[span(flag, j)], wbuf.at[f, span(flag, j)], x_send.at[j], x_recv.at[j], to_x)

    def x_in(j):
        return remote(w_ref.at[span(flag, j)], wbuf.at[f_x, span(flag, j)], x_send.at[j], x_recv.at[j], to_x)

    def y_copy(j, side):
        return remote(wbuf.at[f_x, span(side, j)], wbuf.at[f_x, span(side, j)], y_send.at[j], y_recv.at[j], to_y)

    def d_copy(j, side, slot):
        where = pl.ds(pl.multiple_of(side * half + j * piece, piece), piece)
        return remote(wbuf.at[slot, where], wbuf.at[slot, where], d_send.at[side, j], d_recv.at[side, j], to_core)

    def g_copy(k, where, slot):
        return remote(gain_ref, gbuf.at[slot], g_send.at[k], g_recv.at[k], where)

    def own_copy(slot):
        return remote(w_ref, wbuf.at[slot], own_send.at[0], own_recv.at[0], to_core)

    def o_span(side, j):
        return pl.ds(pl.multiple_of(side * o_half + j * o_piece, o_piece), o_piece)

    def ox_copy(j, slot):
        return remote(wo_ref.at[o_span(flag, j)], wo_out.at[slot, o_span(flag, j)], ox_send.at[j], ox_recv.at[j], to_x)

    def oy_copy(j, side):
        return remote(wo_out.at[f_x, o_span(side, j)], wo_out.at[f_x, o_span(side, j)], oy_send.at[j], oy_recv.at[j], to_y)

    def od_copy(k, src, slot, where):
        return remote(src, wo_out.at[slot, where], od_send.at[k], od_recv.at[k], to_core)

    gains = ((0, to_core, f_core), (1, to_x, f_x), (2, to_diag, f_diag))
    for k, where, _ in gains:
        g_copy(k, where, f).start()
    for j in range(PIECES):
        x_copy(j).start()
    own_copy(f).start()
    for j in range(O_PIECES):
        ox_copy(j, f).start()
    all_rows = pl.ds(0, o_rows)
    od_copy(0, wo_ref, f, all_rows).start()
    local_w = pltpu.make_async_copy(w_ref, wbuf.at[f], out_sem.at[0])
    local_w.start()
    local_o = pltpu.make_async_copy(wo_ref, wo_out.at[f], out_sem.at[1])
    local_o.start()
    gbuf[f] = gain_ref[...]
    for k, where, slot in gains:
        g_copy(k, where, slot).wait_recv()
    for k in range(4):
        gfull_ref[:, k * feat:(k + 1) * feat] = gbuf[k]

    for tile in range(TILES):
        h_load(tile).wait()
        strip = min(32, tq)

        @pl.loop(0, tq // strip)
        def _(i):
            vals = hbuf[tile % 2, pl.ds(pl.multiple_of(i * strip, strip), strip), :].astype(jnp.float32)
            inv = lax.rsqrt(jnp.mean(vals * vals, axis=1, keepdims=True) + NORM_EPS)
            nbuf[pl.ds(pl.multiple_of(tile * tq + i * strip, strip), strip), :] = (vals * inv * gfull_ref[...]).astype(jnp.bfloat16)

        if tile + 2 < TILES:
            h_load(tile + 2).start()
    put_n = pltpu.make_async_copy(nbuf, n_out, out_sem.at[2])
    put_n.start()

    def project(slot, start, rows, first=False):
        cols = pl.ds(pl.multiple_of(slot * feat + start, 128), rows)

        @pl.loop(0, TILES)
        def _(tile):
            here = pl.ds(pl.multiple_of(tile * tq, tq), tq)
            part = dot(nbuf[here, cols], wbuf[slot, pl.ds(start, rows), :], NN)
            acc[here, :] = part if first else acc[here, :] + part

    def x_tick(j):
        x_in(j).wait_recv()
        y_copy(j, flag).start()
        d_copy(j, flag, f_x).start()

    def y_tick(j):
        y_copy(j, 1 - flag).wait_recv()
        d_copy(j, 1 - flag, f_x).start()

    local_w.wait()
    project(f, 0, feat, first=True)
    x_tick(0)
    own_copy(f_core).wait_recv()
    project(f_core, 0, feat)
    x_tick(1)
    y_tick(0)
    x_tick(2)
    y_tick(1)
    x_tick(3)
    for j in range(PIECES):
        d_copy(j, flag, f_diag).wait_recv()
    first_half = pl.multiple_of(flag * half, half)
    project(f_x, first_half, half)
    y_tick(2)
    project(f_diag, first_half, half)
    y_tick(3)
    for j in range(PIECES):
        d_copy(j, 1 - flag, f_diag).wait_recv()
    second_half = pl.multiple_of((1 - flag) * half, half)
    project(f_x, second_half, half)
    project(f_diag, second_half, half)
    put_w = pltpu.make_async_copy(wbuf, w_out, out_sem.at[3])
    put_w.start()

    @pl.loop(0, TILES)
    def _(tile):
        here = pl.ds(pl.multiple_of(tile * tq, tq), tq)
        cos, sin = cos_ref[here, :], sin_ref[here, :]
        for h in range(kv_heads):
            cols = slice(h * head_dim, (h + 1) * head_dim)
            val = acc[here, q_width + h * head_dim:q_width + (h + 1) * head_dim]
            kl_ref[here, cols] = (val * cos + pltpu.roll(val, half_dim, 1) * sin).astype(jnp.bfloat16)
            vl_ref[here, cols] = acc[here, q_width + kv_width + h * head_dim:q_width + kv_width + (h + 1) * head_dim].astype(jnp.bfloat16)

    kv_pairs = ((kl_ref, kp_ref), (vl_ref, vp_ref))

    def kv_copy(k):
        return remote(kv_pairs[k][0], kv_pairs[k][1], kv_send.at[k], kv_recv.at[k], {"cp": 1})

    @pl.loop(0, TILES)
    def _(tile):
        here = pl.ds(pl.multiple_of(tile * tq, tq), tq)
        cos, sin = cos_ref[here, :], sin_ref[here, :]
        for h in range(group * kv_heads):
            cols = slice(h * head_dim, (h + 1) * head_dim)
            val = acc[here, cols]
            qr_ref[here, cols] = (val * cos + pltpu.roll(val, half_dim, 1) * sin).astype(jnp.bfloat16)

    @pl.when(flag == 0)
    def _():
        kp_ref[...] = jnp.zeros_like(kp_ref)
        vp_ref[...] = jnp.zeros_like(vp_ref)
        for k in range(2):
            kv_copy(k).start()

    def load_q(item):
        g, tile = item // TILES, lax.rem(item, TILES)
        rows = pl.ds(pl.multiple_of(tile * tq, tq), tq)
        for h in range(group):
            qs[h * tq:(h + 1) * tq, :] = qr_ref[rows, pl.ds(pl.multiple_of((g * group + h) * head_dim, head_dim), head_dim)]

    def key_piece(item, k_ref, side, start, masked):
        g = item // TILES
        scores = dot(k_ref[pl.ds(start, tq), pl.ds(pl.multiple_of(g * head_dim, head_dim), head_dim)], qs[...], NT)
        if masked:
            key_idx = lax.broadcasted_iota(jnp.int32, (tq, wide), 0)
            q_idx = lax.rem(lax.broadcasted_iota(jnp.int32, (tq, wide), 1), tq)
            scores = jnp.where(key_idx <= q_idx, scores, NEG_BIG)
        m_old = m_all[item]
        m_new = jnp.maximum(m_old, jnp.max(scores, axis=0, keepdims=True))
        probs = jnp.exp2((scores - m_new) * scale)
        fade = jnp.exp2((m_old - m_new) * scale)
        m_all[item] = m_new
        l_all[item] = l_all[item] * fade + jnp.sum(probs, axis=0, keepdims=True)
        acc_all[item] = acc_all[item] * fade + dot(vt[g, side, :, pl.ds(start, tq)], probs.astype(jnp.bfloat16), NN)

    for g in range(kv_heads):
        vt[g, 0] = vl_ref[:, g * head_dim:(g + 1) * head_dim].T

    @pl.loop(0, kv_heads * TILES)
    def _(item):
        tile = lax.rem(item, TILES)
        load_q(item)
        m_all[item] = jnp.full(m_all.shape[1:], NEG_BIG, jnp.float32)
        l_all[item] = jnp.zeros(l_all.shape[1:], jnp.float32)
        acc_all[item] = jnp.zeros(acc_all.shape[1:], jnp.float32)
        key_piece(item, kl_ref, 0, pl.multiple_of(tile * tq, tq), True)

        @pl.loop(0, tile)
        def _(i):
            key_piece(item, kl_ref, 0, pl.multiple_of(i * tq, tq), False)

    for j in range(O_PIECES):
        ox_copy(j, f_x).wait_recv()
        oy_copy(j, flag).start()
        od_copy(1 + j, wo_out.at[f_x, o_span(flag, j)], f_x, o_span(flag, j)).start()

    @pl.when(flag == 1)
    def _():
        for k in range(2):
            kv_copy(k).wait_recv()
        for g in range(kv_heads):
            vt[g, 1] = vp_ref[:, g * head_dim:(g + 1) * head_dim].T

    @pl.loop(0, kv_heads * TILES)
    def _(item):
        g, tile = item // TILES, lax.rem(item, TILES)
        rows = pl.ds(pl.multiple_of(tile * tq, tq), tq)

        @pl.when(flag == 1)
        def _():
            load_q(item)

        @pl.loop(0, flag * TILES)
        def _(i):
            key_piece(item, kp_ref, 1, pl.multiple_of(i * tq, tq), False)

        total = l_all[item]
        lse_ref[item] = m_all[item] * scale + jnp.log2(total)
        out_t = acc_all[item] / total
        for h in range(group):
            o_ref[rows, pl.ds(pl.multiple_of((g * group + h) * head_dim, head_dim), head_dim)] = out_t[:, h * tq:(h + 1) * tq].T.astype(jnp.bfloat16)

        for j in range(O_PIECES):
            @pl.when(item == (j + 1) * kv_heads * TILES // O_PIECES - 1)
            def _():
                oy_copy(j, 1 - flag).wait_recv()
                od_copy(1 + O_PIECES + j, wo_out.at[f_x, o_span(1 - flag, j)], f_x, o_span(1 - flag, j)).start()

    od_copy(0, wo_ref, f_core, all_rows).wait_recv()
    for j in range(O_PIECES):
        od_copy(1 + j, wo_out.at[f_x, o_span(flag, j)], f_diag, o_span(flag, j)).wait_recv()
        od_copy(1 + O_PIECES + j, wo_out.at[f_x, o_span(1 - flag, j)], f_diag, o_span(1 - flag, j)).wait_recv()

    for k, where, _ in gains:
        g_copy(k, where, f).wait_send()
    own_copy(f).wait_send()
    od_copy(0, wo_ref, f, all_rows).wait_send()
    for j in range(PIECES):
        x_copy(j).wait_send()
        y_copy(j, flag).wait_send()
        d_copy(j, flag, f_x).wait_send()
        d_copy(j, 1 - flag, f_x).wait_send()
    for j in range(O_PIECES):
        ox_copy(j, f).wait_send()
        oy_copy(j, flag).wait_send()
        od_copy(1 + j, wo_out.at[f_x, o_span(flag, j)], f_x, o_span(flag, j)).wait_send()
        od_copy(1 + O_PIECES + j, wo_out.at[f_x, o_span(1 - flag, j)], f_x, o_span(1 - flag, j)).wait_send()

    @pl.when(flag == 0)
    def _():
        for k in range(2):
            kv_copy(k).wait_send()

    for local in (local_o, put_n, put_w):
        local.wait()


def front(hidden, gain, w_qkv, w_out, cosines, sines, group, kv_width, cid):
    q_len, model_dim = hidden.shape
    feat, width = w_qkv.shape
    head_dim = cosines.shape[1]
    q_width = width - 2 * kv_width
    kv_heads = kv_width // head_dim
    o_rows, o_cols = w_out.shape
    n_fsdp = model_dim // feat
    tq = q_len // TILES
    wide = group * tq
    items = kv_heads * TILES
    anyspec, vspec = pl.BlockSpec(memory_space=pl.ANY), pl.BlockSpec(memory_space=pltpu.VMEM)
    bf, f32 = jnp.bfloat16, jnp.float32
    dma = pltpu.SemaphoreType.DMA

    def sds(shape, dtype):
        return jax.ShapeDtypeStruct(shape, dtype)

    kv = sds((q_len, kv_width), bf)
    return pl.pallas_call(
        functools.partial(front_kernel, group),
        in_specs=[anyspec] + [vspec] * 5,
        out_specs=[vspec] * 8 + [anyspec] * 3,
        out_shape=[sds((q_len, q_width), bf), sds((q_len, q_width), bf), sds((items, 1, wide), f32), kv, kv, kv, kv, sds((1, model_dim), f32), sds((q_len, model_dim), bf), sds((n_fsdp, feat, width), bf), sds((n_fsdp, o_rows, o_cols), bf)],
        scratch_shapes=[
            pltpu.VMEM((n_fsdp, feat, width), bf),
            pltpu.VMEM((q_len, model_dim), bf),
            pltpu.VMEM((q_len, width), f32),
            pltpu.VMEM((2, tq, model_dim), bf),
            pltpu.VMEM((n_fsdp, 1, feat), f32),
            pltpu.VMEM((wide, head_dim), bf),
            pltpu.VMEM((kv_heads, 2, head_dim, q_len), bf),
            pltpu.VMEM((items, 1, wide), f32),
            pltpu.VMEM((items, 1, wide), f32),
            pltpu.VMEM((items, head_dim, wide), f32),
            dma((2,)), dma((3,)), dma((3,)), dma((1,)), dma((1,)),
            dma((PIECES,)), dma((PIECES,)), dma((PIECES,)), dma((PIECES,)), dma((2, PIECES)), dma((2, PIECES)),
            dma((2,)), dma((2,)),
            dma((O_PIECES,)), dma((O_PIECES,)), dma((O_PIECES,)), dma((O_PIECES,)), dma((1 + 2 * O_PIECES,)), dma((1 + 2 * O_PIECES,)),
            dma((4,)),
        ],
        compiler_params=pltpu.CompilerParams(collective_id=cid, has_side_effects=True, vmem_limit_bytes=67043328),
        cost_estimate=pl.CostEstimate(flops=10**11, bytes_accessed=2**26, transcendentals=0),
        name="front",
    )(hidden, gain, w_qkv, w_out, cosines, sines)


def neighbor_barrier(z, last, other):
    barrier = pltpu.get_barrier_semaphore()

    @pl.when(z > 0)
    def _():
        pl.semaphore_signal(barrier, inc=1, device_id={"tp": z - 1}, device_id_type=MESH)

    @pl.when(z < last)
    def _():
        pl.semaphore_signal(barrier, inc=1, device_id={"tp": z + 1}, device_id_type=MESH)

    if other is not None:
        pl.semaphore_signal(barrier, inc=1, device_id={"cp": other}, device_id_type=MESH)
    extra = 0 if other is None else 1
    pl.semaphore_wait(barrier, jnp.where(z > 0, 1, 0) + jnp.where(z < last, 1, 0) + extra)


class Line:
    def __init__(self, n_line, buf_ref, pbuf_ref, send_sem, recv_sem, fill, finish):
        self.last = n_line - 1
        self.z = lax.axis_index("tp")
        self.buf, self.pbuf, self.send_sem, self.recv_sem = buf_ref, pbuf_ref, send_sem, recv_sem
        self.chunks, self.rows = buf_ref.shape[1], buf_ref.shape[2]
        self.block = pbuf_ref.shape[1]
        self.per_block = self.block // self.rows
        self.half = self.chunks * self.rows
        self.fill, self.finish = fill, finish
        self.steps = self.chunks + self.last

    def dist(self, side):
        return self.last - self.z if side == 0 else self.z

    def copy(self, side, chunk):
        target = jnp.clip(self.z - 1 if side == 0 else self.z + 1, 0, self.last)
        return pltpu.make_async_remote_copy(src_ref=self.buf.at[side, chunk], dst_ref=self.buf.at[side, chunk], send_sem=self.send_sem.at[side, chunk], recv_sem=self.recv_sem.at[side, chunk], device_id={"tp": target}, device_id_type=MESH)

    def tick(self, step):
        for side in range(2):
            chunk = step - self.dist(side)

            @pl.when((chunk >= 0) & (chunk < self.chunks) & (lax.rem(chunk, self.per_block) == 0))
            def _():
                start = pl.multiple_of(side * self.half + chunk * self.rows, self.block)
                self.fill(self.pbuf.at[side], pl.ds(start, self.block))

        for side in range(2):
            chunk = step - self.dist(side)
            dist = self.dist(side)
            part = pl.ds(pl.multiple_of(lax.rem(jnp.maximum(chunk, 0), self.per_block) * self.rows, self.rows), self.rows)

            @pl.when((chunk >= 0) & (chunk < self.chunks))
            def _():
                @pl.when(dist == 0)
                def _():
                    self.buf[side, chunk] = self.pbuf[side, part, :]
                    self.copy(side, chunk).start()

                @pl.when(dist > 0)
                def _():
                    self.copy(side, chunk).wait_recv()

                @pl.when((dist > 0) & (dist < self.last))
                def _():
                    self.buf[side, chunk] += self.pbuf[side, part, :]
                    self.copy(side, chunk).start()

                @pl.when(dist == self.last)
                def _():
                    span = pl.ds(pl.multiple_of(chunk * self.rows, self.rows), self.rows)
                    self.finish(span, self.buf[side, chunk] + self.pbuf[side, part, :])

    def drain(self):
        for side in range(2):
            @pl.when(self.dist(side) < self.last)
            def _():
                @pl.loop(0, self.chunks)
                def _(chunk):
                    self.copy(side, chunk).wait_send()


def mid_kernel(n_line, group, o_ref, w_ref, q_ref, lse_ref, cos_ref, sin_ref, kl_ref, vl_ref, kp_ref, vp_ref, hid_ref, ct_ref, _after_ref, own_ref, dq_ref, buf_ref, pbuf_ref, hbuf_ref, ctb_ref, do_ref, dkl_ref, dvl_ref, dkp_ref, dvp_ref, qs_ref, dos_ref, delta_ref, kt_ref, dqt_ref, send_sem, recv_sem, load_sem, ct_sem, xs_sem, xr_sem):
    last = n_line - 1
    z, flag = lax.axis_index("tp"), lax.axis_index("cp")
    q_len, width = o_ref.shape
    head_dim = cos_ref.shape[1]
    half_dim = head_dim // 2
    kv_width = kl_ref.shape[1]
    kv_heads = kv_width // head_dim
    tq = q_len // TILES
    wide = group * tq
    score_scale = head_dim ** -0.5
    half = q_len // 2
    own_rows = pl.ds(pl.multiple_of(jnp.where(z == last, half, 0), half), half)
    load = pltpu.make_async_copy(hid_ref.at[own_rows], hbuf_ref, load_sem.at[0])
    load.start()

    def ct_load(tile):
        slot = lax.rem(tile, 2)
        return pltpu.make_async_copy(ct_ref.at[pl.ds(pl.multiple_of(tile * tq, tq), tq)], ctb_ref.at[slot], ct_sem.at[slot])

    ct_load(0).start()
    ct_load(1).start()
    for ref in (dkl_ref, dvl_ref):
        ref[...] = jnp.zeros_like(ref)

    @pl.when(flag == 1)
    def _():
        for ref in (dkp_ref, dvp_ref):
            ref[...] = jnp.zeros_like(ref)

    neighbor_barrier(z, last, 1 - flag)
    load.wait()

    def finish(span, total):
        own_ref[span, :] = (hbuf_ref[span, :].astype(jnp.float32) + total).astype(jnp.bfloat16)

    n_parts, _, part = w_ref.shape

    def fill(dst, rows):
        for k in range(n_parts):
            dst[:, k * part:(k + 1) * part] = dot(o_ref[rows, :], w_ref[k], NN)

    line = Line(n_line, buf_ref, pbuf_ref, send_sem, recv_sem, fill, finish)

    def do_tile(tile):
        ct_load(tile).wait()
        rows = pl.ds(pl.multiple_of(tile * tq, tq), tq)
        slot = lax.rem(tile, 2)
        total = dot(ctb_ref[slot, :, :part], w_ref[0], NT)
        for k in range(1, n_parts):
            total = total + dot(ctb_ref[slot, :, k * part:(k + 1) * part], w_ref[k], NT)
        do_ref[rows, :] = total.astype(jnp.bfloat16)

        @pl.when(tile + 2 < TILES)
        def _():
            ct_load(tile + 2).start()

    def bwd_item(item):
        g, tile = item // TILES, lax.rem(item, TILES)
        kv_cols = pl.ds(pl.multiple_of(g * head_dim, head_dim), head_dim)
        rows = pl.ds(pl.multiple_of(tile * tq, tq), tq)

        @pl.when(tile == 0)
        def _():
            kt_ref[0] = kl_ref[:, kv_cols].T
            kt_ref[1] = kp_ref[:, kv_cols].T

        for h in range(group):
            cols = pl.ds(pl.multiple_of((g * group + h) * head_dim, head_dim), head_dim)
            stack = slice(h * tq, (h + 1) * tq)
            qs_ref[stack, :] = q_ref[rows, cols]
            d_h = do_ref[rows, cols]
            dos_ref[stack, :] = d_h
            prod = d_h.astype(jnp.float32) * o_ref[rows, cols].astype(jnp.float32)
            delta_ref[:, stack] = jnp.sum(prod.T, axis=0, keepdims=True)
        dqt_ref[...] = jnp.zeros_like(dqt_ref)

        def piece(k_ref, v_ref, dk_ref, dv_ref, side, start, masked):
            span = pl.ds(start, tq)
            scores = dot(k_ref[span, kv_cols], qs_ref[...], NT)
            if masked:
                key_idx = lax.broadcasted_iota(jnp.int32, (tq, wide), 0)
                q_idx = lax.rem(lax.broadcasted_iota(jnp.int32, (tq, wide), 1), tq)
                scores = jnp.where(key_idx <= q_idx, scores, NEG_BIG)
            probs = jnp.exp2(scores * (score_scale * LOG2E) - lse_ref[item])
            d_probs = dot(v_ref[span, kv_cols], dos_ref[...], NT)
            d_scores = (probs * (d_probs - delta_ref[...]) * score_scale).astype(jnp.bfloat16)
            dv_ref[g, span, :] += dot(probs.astype(jnp.bfloat16), dos_ref[...], NN)
            dk_ref[g, span, :] += dot(d_scores, qs_ref[...], NN)
            dqt_ref[...] += dot(kt_ref[side, :, span], d_scores, NN)

        piece(kl_ref, vl_ref, dkl_ref, dvl_ref, 0, pl.multiple_of(tile * tq, tq), True)

        @pl.loop(0, tile)
        def _(i):
            piece(kl_ref, vl_ref, dkl_ref, dvl_ref, 0, pl.multiple_of(i * tq, tq), False)

        @pl.loop(0, flag * (q_len // tq))
        def _(i):
            piece(kp_ref, vp_ref, dkp_ref, dvp_ref, 1, pl.multiple_of(i * tq, tq), False)

        for h in range(group):
            dq_h = dqt_ref[:, h * tq:(h + 1) * tq].T
            dq_h = dq_h * cos_ref[rows, :] - pltpu.roll(dq_h, half_dim, 1) * sin_ref[rows, :]
            dq_ref[rows, pl.ds(pl.multiple_of((g * group + h) * head_dim, head_dim), head_dim)] = dq_h.astype(jnp.bfloat16)

        @pl.when((tile == TILES - 1) & (flag == 1))
        def _():
            for copy in back(g):
                copy.start()

    def back(g):
        return [pltpu.make_async_remote_copy(src_ref=ref.at[g], dst_ref=ref.at[g], send_sem=xs_sem.at[k, g], recv_sem=xr_sem.at[k, g], device_id={"cp": 0}, device_id_type=MESH) for k, ref in enumerate((dkp_ref, dvp_ref))]

    def kv_done(g):
        @pl.when(flag == 0)
        def _():
            for copy in back(g):
                copy.wait_recv()
            dkl_ref[g] += dkp_ref[g]
            dvl_ref[g] += dvp_ref[g]

        dk = dkl_ref[g]
        dk = dk * cos_ref[...] - pltpu.roll(dk, half_dim, 1) * sin_ref[...]
        dq_ref[:, width + g * head_dim:width + (g + 1) * head_dim] = dk.astype(jnp.bfloat16)
        dq_ref[:, width + kv_width + g * head_dim:width + kv_width + (g + 1) * head_dim] = dvl_ref[g].astype(jnp.bfloat16)

        @pl.when(flag == 1)
        def _():
            for copy in back(g):
                copy.wait_send()

    items = TILES * kv_heads

    @pl.loop(0, line.steps)
    def _(step):
        line.tick(step)

        @pl.when(step < TILES)
        def _():
            do_tile(step)

        @pl.when((step >= TILES) & (step < TILES + items))
        def _():
            bwd_item(step - TILES)

        for g in range(kv_heads):
            @pl.when(step == min(TILES * (g + 2) + 4, line.steps - 1))
            def _():
                kv_done(g)

    line.drain()


def line_middle(attn_out, wo_full, q_rot, lse, cosines, sines, k_loc, v_loc, k_prev, v_prev, hidden, cotangent, after, n_line, group, cid):
    q_len, model_dim = hidden.shape
    width = attn_out.shape[1]
    head_dim = cosines.shape[1]
    kv_width = k_loc.shape[1]
    kv_heads = kv_width // head_dim
    half = q_len // 2
    tq = q_len // TILES
    wide = group * tq
    block = min(128, half)
    anyspec, vspec = pl.BlockSpec(memory_space=pl.ANY), pl.BlockSpec(memory_space=pltpu.VMEM)
    bf, f32 = jnp.bfloat16, jnp.float32
    acc = pltpu.VMEM((kv_heads, q_len, head_dim), f32)
    return pl.pallas_call(
        functools.partial(mid_kernel, n_line, group),
        in_specs=[vspec] * 10 + [anyspec] * 3,
        out_specs=[vspec] * 2,
        out_shape=[jax.ShapeDtypeStruct((half, model_dim), bf), jax.ShapeDtypeStruct((q_len, width + 2 * kv_width), bf)],
        scratch_shapes=[
            pltpu.VMEM((2, CHUNKS, half // CHUNKS, model_dim), f32),
            pltpu.VMEM((2, block, model_dim), f32),
            pltpu.VMEM((half, model_dim), bf),
            pltpu.VMEM((2, tq, model_dim), bf),
            pltpu.VMEM((q_len, width), bf),
            acc, acc, acc, acc,
            pltpu.VMEM((wide, head_dim), bf),
            pltpu.VMEM((wide, head_dim), bf),
            pltpu.VMEM((1, wide), f32),
            pltpu.VMEM((2, head_dim, q_len), bf),
            pltpu.VMEM((head_dim, wide), f32),
            pltpu.SemaphoreType.DMA((2, CHUNKS)),
            pltpu.SemaphoreType.DMA((2, CHUNKS)),
            pltpu.SemaphoreType.DMA((1,)),
            pltpu.SemaphoreType.DMA((2,)),
            pltpu.SemaphoreType.DMA((2, kv_heads)),
            pltpu.SemaphoreType.DMA((2, kv_heads)),
        ],
        compiler_params=pltpu.CompilerParams(collective_id=cid, has_side_effects=True, vmem_limit_bytes=67043328),
        cost_estimate=pl.CostEstimate(flops=2 * 10**11, bytes_accessed=2**25, transcendentals=0),
        name="line_middle",
    )(attn_out, wo_full, q_rot, lse, cosines, sines, k_loc, v_loc, k_prev, v_prev, hidden, cotangent, after)


def in_kernel(n_line, d_ref, w_ref, gain_ref, hid_ref, ct_ref, own_ref, gg_ref, buf_ref, pbuf_ref, hbuf_ref, cbuf_ref, send_sem, recv_sem, load_sem):
    last = n_line - 1
    z = lax.axis_index("tp")
    half = hbuf_ref.shape[0]
    own_rows = pl.ds(pl.multiple_of(jnp.where(z == last, half, 0), half), half)
    loads = [pltpu.make_async_copy(src.at[own_rows], dst, load_sem.at[k]) for k, (src, dst) in enumerate(((hid_ref, hbuf_ref), (ct_ref, cbuf_ref)))]
    for load in loads:
        load.start()
    gg_ref[...] = jnp.zeros_like(gg_ref)
    neighbor_barrier(z, last, None)
    for load in loads:
        load.wait()

    def finish(span, total):
        x_in = hbuf_ref[span, :].astype(jnp.float32)
        inv = lax.rsqrt(jnp.mean(x_in * x_in, axis=1, keepdims=True) + NORM_EPS)
        x_hat = x_in * inv
        gg_ref[...] += jnp.sum(total * x_hat, axis=0, keepdims=True)
        scaled = total * gain_ref[...]
        inner = jnp.mean(scaled * x_hat, axis=1, keepdims=True)
        own_ref[span, :] = (cbuf_ref[span, :].astype(jnp.float32) + inv * (scaled - x_hat * inner)).astype(jnp.bfloat16)

    n_parts, part, _ = w_ref.shape

    def fill(dst, rows):
        for k in range(n_parts):
            dst[:, k * part:(k + 1) * part] = dot(d_ref[rows, :], w_ref[k], NT)

    line = Line(n_line, buf_ref, pbuf_ref, send_sem, recv_sem, fill, finish)

    @pl.loop(0, line.steps)
    def _(step):
        line.tick(step)

    line.drain()


def line_input(d_lin, w_full, gain, hidden, cotangent, n_line, cid):
    q_len, model_dim = hidden.shape
    half = q_len // 2
    block = min(128, half)
    anyspec, vspec = pl.BlockSpec(memory_space=pl.ANY), pl.BlockSpec(memory_space=pltpu.VMEM)
    return pl.pallas_call(
        functools.partial(in_kernel, n_line),
        in_specs=[vspec] * 3 + [anyspec] * 2,
        out_specs=[vspec] * 2,
        out_shape=[jax.ShapeDtypeStruct((half, model_dim), jnp.bfloat16), jax.ShapeDtypeStruct((1, model_dim), jnp.float32)],
        scratch_shapes=[
            pltpu.VMEM((2, CHUNKS, half // CHUNKS, model_dim), jnp.float32),
            pltpu.VMEM((2, block, model_dim), jnp.float32),
            pltpu.VMEM((half, model_dim), jnp.bfloat16),
            pltpu.VMEM((half, model_dim), jnp.bfloat16),
            pltpu.SemaphoreType.DMA((2, CHUNKS)),
            pltpu.SemaphoreType.DMA((2, CHUNKS)),
            pltpu.SemaphoreType.DMA((2,)),
        ],
        compiler_params=pltpu.CompilerParams(collective_id=cid, has_side_effects=True, vmem_limit_bytes=67043328),
        cost_estimate=pl.CostEstimate(flops=2 * 10**11, bytes_accessed=2**25, transcendentals=0),
        name="line_input",
    )(d_lin, w_full, gain, hidden, cotangent)


def ag_kernel(n_line, n_fsdp, chunks, own_a_ref, own_b_ref, gp_ref, out_a_ref, out_b_ref, gg_ref, ga, gs, gb, gt, gc, local_sem, send_sem, recv_sem, ga_send, ga_recv, gb_sem, gc_send, gc_recv):
    last = n_line - 1
    z = lax.axis_index("tp")
    half = own_a_ref.shape[0]
    rows = half // chunks
    pairs = ((own_a_ref, out_a_ref), (own_b_ref, out_b_ref))
    flag, f = lax.axis_index("cp"), lax.axis_index("fsdp")
    feat = gg_ref.shape[1]
    barrier = pltpu.get_barrier_semaphore()
    others = [{"tp": lax.rem(z + k, n_line)} for k in range(1, n_line)] + [{"cp": 1 - flag}] + [{"fsdp": lax.rem(f + k, n_fsdp)} for k in range(1, n_fsdp)]
    for where in others:
        pl.semaphore_signal(barrier, inc=1, device_id=where, device_id_type=MESH)
    pl.semaphore_wait(barrier, len(others))

    def ga_copy(end, k):
        where = {"tp": 1 + k if end == 0 else k}
        return pltpu.make_async_remote_copy(src_ref=gp_ref, dst_ref=ga.at[end], send_sem=ga_send.at[k], recv_sem=ga_recv.at[end], device_id=where, device_id_type=MESH)

    def gb_copy():
        return pltpu.make_async_remote_copy(src_ref=gs, dst_ref=gb, send_sem=gb_sem.at[0], recv_sem=gb_sem.at[1], device_id={"cp": 1 - flag}, device_id_type=MESH)

    def gc_copy(k, slot):
        to = lax.rem(f + k, n_fsdp)
        return pltpu.make_async_remote_copy(src_ref=gt.at[to], dst_ref=gc.at[slot], send_sem=gc_send.at[k - 1], recv_sem=gc_recv.at[k - 1], device_id={"fsdp": to}, device_id_type=MESH)

    for end in range(2):
        at_end = z == (0 if end == 0 else last)

        @pl.when(at_end)
        def _():
            ga[end] = gp_ref[...]
            for k in range(last):
                ga_copy(end, k).start()

    def dist(side):
        return last - z if side == 0 else z

    def span(side, chunk):
        return pl.ds(pl.multiple_of(side * half + chunk * rows, rows), rows)

    def forward(which, side, chunk, src):
        target = jnp.clip(z + 1 if side == 0 else z - 1, 0, last)
        slot = which * chunks + chunk
        return pltpu.make_async_remote_copy(src_ref=src, dst_ref=pairs[which][1].at[span(side, chunk)], send_sem=send_sem.at[side, slot], recv_sem=recv_sem.at[side, slot], device_id={"tp": target}, device_id_type=MESH)

    def local(which, side):
        own, out = pairs[which]
        return pltpu.make_async_copy(own, out.at[pl.ds(side * half, half)], local_sem.at[which])

    for side in range(2):
        @pl.when(dist(side) == last)
        def _():
            for which in range(2):
                @pl.loop(0, chunks)
                def _(chunk):
                    piece = pl.ds(pl.multiple_of(chunk * rows, rows), rows)
                    forward(which, side, chunk, pairs[which][0].at[piece]).start()
            for which in range(2):
                local(which, side).start()

    for end in range(2):
        @pl.when(z != (0 if end == 0 else last))
        def _():
            ga_copy(end, 0).wait_recv()
    gs[...] = ga[0] + ga[1]

    for which in range(2):
        if which == 1:
            gb_copy().start()

        @pl.loop(0, chunks + last - 1)
        def _(step):
            for side in range(2):
                chunk = step - (last - 1 - dist(side))

                @pl.when((dist(side) < last) & (chunk >= 0) & (chunk < chunks))
                def _():
                    src = pairs[which][1].at[span(side, jnp.clip(chunk, 0, chunks - 1))]
                    hop = forward(which, side, jnp.clip(chunk, 0, chunks - 1), src)
                    hop.wait_recv()

                    @pl.when(dist(side) > 0)
                    def _():
                        hop.start()

    gb_copy().wait()
    for k in range(n_fsdp):
        gt[k] = gs[:, k * feat:(k + 1) * feat] + gb[:, k * feat:(k + 1) * feat]
    gc[f] = gt[f]

    for side in range(2):
        for which in range(2):
            @pl.when(dist(side) == last)
            def _():
                local(which, side).wait()

            @pl.when(dist(side) > 0)
            def _():
                @pl.loop(0, chunks)
                def _(chunk):
                    forward(which, side, chunk, pairs[which][1].at[span(side, chunk)]).wait_send()

    for k in range(1, n_fsdp):
        gc_copy(k, f).start()
    for k in range(1, n_fsdp):
        gc_copy(k, lax.rem(f + n_fsdp - k, n_fsdp)).wait_recv()
    total = gc[0]
    for k in range(1, n_fsdp):
        total = total + gc[k]
    gg_ref[...] = total
    for k in range(1, n_fsdp):
        gc_copy(k, f).wait_send()
    for end in range(2):
        @pl.when(z == (0 if end == 0 else last))
        def _():
            for k in range(last):
                ga_copy(end, k).wait_send()


def line_spread(own_a, own_b, gain_part, n_line, n_fsdp, cid):
    half, model_dim = own_a.shape
    feat = model_dim // n_fsdp
    f32, dma = jnp.float32, pltpu.SemaphoreType.DMA
    anyspec, vspec = pl.BlockSpec(memory_space=pl.ANY), pl.BlockSpec(memory_space=pltpu.VMEM)
    out = jax.ShapeDtypeStruct((2 * half, model_dim), jnp.bfloat16)
    return pl.pallas_call(
        functools.partial(ag_kernel, n_line, n_fsdp, CHUNKS),
        in_specs=[vspec] * 3,
        out_specs=[anyspec, anyspec, vspec],
        out_shape=[out, out, jax.ShapeDtypeStruct((1, feat), f32)],
        scratch_shapes=[
            pltpu.VMEM((2, 1, model_dim), f32),
            pltpu.VMEM((1, model_dim), f32),
            pltpu.VMEM((1, model_dim), f32),
            pltpu.VMEM((n_fsdp, 1, feat), f32),
            pltpu.VMEM((n_fsdp, 1, feat), f32),
            dma((2,)), dma((2, 2 * CHUNKS)), dma((2, 2 * CHUNKS)),
            dma((n_line - 1,)), dma((2,)), dma((2,)), dma((n_fsdp - 1,)), dma((n_fsdp - 1,)),
        ],
        compiler_params=pltpu.CompilerParams(collective_id=cid, has_side_effects=True),
        cost_estimate=pl.CostEstimate(flops=2 * 10**11, bytes_accessed=2**25, transcendentals=0),
        name="line_spread",
    )(own_a, own_b, gain_part)


def solution(mesh):
    act_spec = P("fsdp", "cp", None)
    proj_spec = P("fsdp", "tp", None)
    wout_spec = P("tp", None, "fsdp")
    n_line, n_fsdp = mesh.shape["tp"], mesh.shape["fsdp"]

    def scatter(full_grad, dim):
        return lax.psum_scatter(full_grad, "fsdp", scatter_dimension=dim, tiled=True)

    def other_half(part):
        return lax.ppermute(part, "cp", [(0, 1), (1, 0)])

    def device_step(hidden, cotangent, positions, gain, w_query, w_key, w_value, w_out):
        hidden = hidden[0]
        cotangent = cotangent[0]
        q_len, model_dim = hidden.shape
        feat, q_heads, head_dim = w_query.shape
        kv_heads = w_key.shape[1]
        group = q_heads // kv_heads
        q_width, kv_width = q_heads * head_dim, kv_heads * head_dim
        w_qkv = jnp.concatenate([w_query.reshape(feat, q_width), w_key.reshape(feat, kv_width), w_value.reshape(feat, kv_width)], axis=1)
        cosines, sines = rope_tables(positions, head_dim)
        attn_out, q_rot, lse, k_loc, v_loc, k_prev, v_prev, gain_full, normed, w_full, wo_full = front(hidden, gain.astype(jnp.float32)[None], w_qkv, w_out.reshape(q_width, feat), cosines, sines, group, kv_width, 3)
        TN = (((0,), (0,)), ((), ()))
        grad_wout = dot(attn_out, cotangent, TN)
        own_out, d_lin = line_middle(attn_out, wo_full, q_rot, lse, cosines, sines, k_loc, v_loc, k_prev, v_prev, hidden, cotangent, grad_wout, n_line, group, 0)
        part_out = scatter(grad_wout, 1)
        normed, part_out = lax.optimization_barrier((normed, part_out))
        far_out = other_half(part_out)
        part_in = scatter(dot(normed, d_lin, TN), 0)
        own_hid, gain_part = line_input(d_lin, w_full, gain_full, hidden, cotangent, n_line, 1)
        own_hid, far_out = lax.optimization_barrier((own_hid, far_out))
        block_out, grad_hidden, grad_gain = line_spread(own_out, own_hid, gain_part, n_line, n_fsdp, 2)
        g_in, g_out = part_in + other_half(part_in), part_out + far_out
        return (
            block_out[None],
            grad_hidden[None],
            grad_gain[0],
            g_in[:, :q_width].reshape(feat, q_heads, head_dim),
            g_in[:, q_width:q_width + kv_width].reshape(feat, kv_heads, head_dim),
            g_in[:, q_width + kv_width:].reshape(feat, kv_heads, head_dim),
            g_out.reshape(q_heads, head_dim, feat),
        )

    return jax.shard_map(device_step, mesh=mesh, in_specs=(act_spec, act_spec, P("cp"), P("fsdp"), proj_spec, proj_spec, proj_spec, wout_spec), out_specs=(act_spec, act_spec, P("fsdp"), proj_spec, proj_spec, proj_spec, wout_spec), check_vma=False)
```

```python
import functools
import math

import jax
import jax.numpy as jnp
from jax import lax
from jax.experimental import pallas as pl
from jax.experimental.pallas import tpu as pltpu
from jax.sharding import PartitionSpec as P

WINDOW_LEN = 4096
ROPE_BASE = 10000.0
NORM_EPS = 1e-5
NEG_BIG = -1e30
LOG2E = math.log2(math.e)
TILES = 4
CHUNKS = 16
PIECES = 4
O_PIECES = 2
GRAD_CHUNKS = 8
FIRST_X = 5
EARLY = 6
VMEM_BYTES = 67043328

MESH = pl.DeviceIdType.MESH
ANY = pl.BlockSpec(memory_space=pl.ANY)
VMEM = pl.BlockSpec(memory_space=pltpu.VMEM)
DMA = pltpu.SemaphoreType.DMA
BF, F32 = jnp.bfloat16, jnp.float32

NT = (((1,), (1,)), ((), ()))
NN = (((1,), (0,)), ((), ()))
TN = (((0,), (0,)), ((), ()))


def dot(a, b, dims):
    return lax.dot_general(a, b, dims, preferred_element_type=F32)


def blk(k, n):
    return pl.ds(k * n if isinstance(k, int) else pl.multiple_of(k * n, n), n)


def lane_mean(vals):
    return jnp.mean(vals, axis=1, keepdims=True)


def row_sum(vals):
    return jnp.sum(vals, axis=0, keepdims=True)


def zero(ref):
    ref[...] = jnp.zeros_like(ref)


def remote(src, dst, send, recv, where):
    return pltpu.make_async_remote_copy(src_ref=src, dst_ref=dst, send_sem=send, recv_sem=recv, device_id=where, device_id_type=MESH)


def meet(peers):
    barrier = pltpu.get_barrier_semaphore()
    for where in peers:
        pl.semaphore_signal(barrier, inc=1, device_id=where, device_id_type=MESH)
    pl.semaphore_wait(barrier, len(peers))


def fsdp_peers(f):
    core = lax.rem(f, 2)
    other = f + 1 - 2 * core
    far = lax.rem(f + 2, 4)
    return other, far, lax.rem(other + 2, 4)


def others(axis, index, count):
    return [{axis: lax.rem(index + k, count)} for k in range(1, count)]


def rope(vals, cos, sin, half_dim):
    return vals * cos + pltpu.roll(vals, half_dim, 1) * sin


def causal(scores, tq):
    key_idx = lax.broadcasted_iota(jnp.int32, scores.shape, 0)
    q_idx = lax.rem(lax.broadcasted_iota(jnp.int32, scores.shape, 1), tq)
    return jnp.where(key_idx <= q_idx, scores, NEG_BIG)


def params(cid):
    return pltpu.CompilerParams(collective_id=cid, has_side_effects=True, vmem_limit_bytes=VMEM_BYTES)


def rope_tables(positions, head_dim):
    inv_freq = ROPE_BASE ** (-jnp.arange(0, head_dim, 2).astype(F32) / head_dim)
    angles = positions.astype(F32)[:, None] * inv_freq[None, :]
    cosines, sines = jnp.cos(angles), jnp.sin(angles)
    return jnp.concatenate([cosines, cosines], axis=1), jnp.concatenate([-sines, sines], axis=1)


def front_kernel(group, n_line, hid_ref, gain_ref, w_ref, wo_ref, cos_ref, sin_ref, o_ref, qr_ref, lse_ref, kl_ref, vl_ref, kp_ref, vp_ref, gfull_ref, n_out, w_out, wo_all, wbuf, nbuf, acc, hbuf, gbuf, qs, vt, m_all, l_all, acc_all, h_sem, g_send, g_recv, own_send, own_recv, x_send, x_recv, y_send, y_recv, d_send, d_recv, kv_send, kv_recv, ox_send, ox_recv, oy_send, oy_recv, od_send, od_recv, zw_send, zw_recv, out_sem):
    q_len, feat = hid_ref.shape[0], w_ref.shape[0]
    head_dim = cos_ref.shape[1]
    half_dim = head_dim // 2
    kv_width = kl_ref.shape[1]
    kv_heads = kv_width // head_dim
    q_width = qr_ref.shape[1]
    tq = q_len // TILES
    wide = group * tq
    scale = head_dim ** -0.5 * LOG2E
    half = feat // 2
    piece = half // PIECES
    o_rows = wo_ref.shape[0]
    o_half = o_rows // 2
    o_piece = o_half // O_PIECES
    flag, f, z = lax.axis_index("cp"), lax.axis_index("fsdp"), lax.axis_index("tp")
    wo_out = wo_all.at[z]
    far = 1 - flag
    f_core, f_x, f_diag = fsdp_peers(f)
    to_core, to_x, to_diag, to_y = {"fsdp": f_core}, {"fsdp": f_x}, {"fsdp": f_diag}, {"cp": far}

    def h_load(tile):
        slot = lax.rem(tile, 2)
        return pltpu.make_async_copy(hid_ref.at[blk(tile, tq)], hbuf.at[slot], h_sem.at[slot])

    h_load(0).start()
    h_load(1).start()
    meet([to_core, to_x, to_diag, to_y] + others("tp", z, n_line))

    def span(side, j):
        return blk(side * PIECES + j, piece)

    def x_copy(j):
        return remote(w_ref.at[span(flag, j)], wbuf.at[f, span(flag, j)], x_send.at[j], x_recv.at[j], to_x)

    def x_in(j):
        return remote(w_ref.at[span(flag, j)], wbuf.at[f_x, span(flag, j)], x_send.at[j], x_recv.at[j], to_x)

    def y_copy(j, side):
        return remote(wbuf.at[f_x, span(side, j)], wbuf.at[f_x, span(side, j)], y_send.at[j], y_recv.at[j], to_y)

    def d_copy(j, side, slot):
        return remote(wbuf.at[slot, span(side, j)], wbuf.at[slot, span(side, j)], d_send.at[side, j], d_recv.at[side, j], to_core)

    def g_copy(k, where, slot):
        return remote(gain_ref, gbuf.at[slot], g_send.at[k], g_recv.at[k], where)

    def own_copy(slot):
        return remote(w_ref, wbuf.at[slot], own_send, own_recv, to_core)

    def o_span(side, j):
        return blk(side * O_PIECES + j, o_piece)

    def ox_copy(j, slot):
        return remote(wo_ref.at[o_span(flag, j)], wo_out.at[slot, o_span(flag, j)], ox_send.at[j], ox_recv.at[j], to_x)

    def oy_copy(j, side):
        return remote(wo_out.at[f_x, o_span(side, j)], wo_out.at[f_x, o_span(side, j)], oy_send.at[j], oy_recv.at[j], to_y)

    def od_copy(k, src, slot, where):
        return remote(src, wo_out.at[slot, where], od_send.at[k], od_recv.at[k], to_core)

    def zw_copy(k, owner):
        mine = blk(flag, o_half)
        return remote(wo_ref.at[mine], wo_all.at[owner, f, mine], zw_send.at[k - 1], zw_recv.at[k - 1], {"tp": lax.rem(z + k, n_line)})

    for k in range(1, n_line):
        zw_copy(k, z).start()
    gains = [(k, where, where["fsdp"]) for k, where in enumerate((to_core, to_x, to_diag))]
    for k, where, _ in gains:
        g_copy(k, where, f).start()
    for j in range(PIECES):
        x_copy(j).start()
    own_copy(f).start()
    for j in range(O_PIECES):
        ox_copy(j, f).start()
    all_rows = pl.ds(0, o_rows)
    od_copy(0, wo_ref, f, all_rows).start()
    local_w = pltpu.make_async_copy(w_ref, wbuf.at[f], out_sem.at[0])
    local_w.start()
    local_o = pltpu.make_async_copy(wo_ref, wo_out.at[f], out_sem.at[1])
    local_o.start()
    gbuf[f] = gain_ref[...]
    for k, where, slot in gains:
        g_copy(k, where, slot).wait_recv()
    for k in range(gbuf.shape[0]):
        gfull_ref[:, blk(k, feat)] = gbuf[k]

    for tile in range(TILES):
        h_load(tile).wait()
        strip = min(32, tq)

        @pl.loop(0, tq // strip)
        def _(i):
            vals = hbuf[tile % 2, blk(i, strip), :].astype(F32)
            inv = lax.rsqrt(lane_mean(vals * vals) + NORM_EPS)
            nbuf[pl.ds(pl.multiple_of(tile * tq + i * strip, strip), strip), :] = (vals * inv * gfull_ref[...]).astype(BF)

        if tile + 2 < TILES:
            h_load(tile + 2).start()
    put_n = pltpu.make_async_copy(nbuf, n_out, out_sem.at[2])
    put_n.start()

    def project(slot, start, rows, first=False):
        cols = pl.ds(pl.multiple_of(slot * feat + start, 128), rows)

        @pl.loop(0, TILES)
        def _(tile):
            here = blk(tile, tq)
            part = dot(nbuf[here, cols], wbuf[slot, pl.ds(start, rows), :], NN)
            acc[here, :] = part if first else acc[here, :] + part

    def x_tick(j):
        x_in(j).wait_recv()
        y_copy(j, flag).start()
        d_copy(j, flag, f_x).start()

    def y_tick(j):
        y_copy(j, far).wait_recv()
        d_copy(j, 1 - flag, f_x).start()

    local_w.wait()
    project(f, 0, feat, first=True)
    x_tick(0)
    own_copy(f_core).wait_recv()
    project(f_core, 0, feat)
    x_tick(1)
    y_tick(0)
    x_tick(2)
    y_tick(1)
    x_tick(3)
    for j in range(PIECES):
        d_copy(j, flag, f_diag).wait_recv()
    first_half = pl.multiple_of(flag * half, half)
    project(f_x, first_half, half)
    y_tick(2)
    project(f_diag, first_half, half)
    y_tick(3)
    for j in range(PIECES):
        d_copy(j, 1 - flag, f_diag).wait_recv()
    second_half = pl.multiple_of((far) * half, half)
    project(f_x, second_half, half)
    project(f_diag, second_half, half)
    put_w = pltpu.make_async_copy(wbuf, w_out, out_sem.at[3])
    put_w.start()

    @pl.loop(0, TILES)
    def _(tile):
        here = blk(tile, tq)
        cos, sin = cos_ref[here, :], sin_ref[here, :]
        for h in range(kv_heads):
            k_at = q_width // head_dim + h
            kl_ref[here, blk(h, head_dim)] = rope(acc[here, blk(k_at, head_dim)], cos, sin, half_dim).astype(BF)
            vl_ref[here, blk(h, head_dim)] = acc[here, blk(k_at + kv_heads, head_dim)].astype(BF)

    kv_pairs = ((kl_ref, kp_ref), (vl_ref, vp_ref))

    def kv_copy(k):
        return remote(kv_pairs[k][0], kv_pairs[k][1], kv_send.at[k], kv_recv.at[k], {"cp": 1})

    @pl.loop(0, TILES)
    def _(tile):
        here = blk(tile, tq)
        cos, sin = cos_ref[here, :], sin_ref[here, :]
        for h in range(group * kv_heads):
            cols = blk(h, head_dim)
            qr_ref[here, cols] = rope(acc[here, cols], cos, sin, half_dim).astype(BF)

    @pl.when(flag == 0)
    def _():
        zero(kp_ref)
        zero(vp_ref)
        for k in range(len(kv_pairs)):
            kv_copy(k).start()

    def load_q(item):
        g, tile = item // TILES, lax.rem(item, TILES)
        rows = blk(tile, tq)
        for h in range(group):
            qs[blk(h, tq), :] = qr_ref[rows, blk(g * group + h, head_dim)]

    def key_piece(item, k_ref, side, start, masked):
        g = item // TILES
        scores = dot(k_ref[start, blk(g, head_dim)], qs[...], NT)
        if masked:
            scores = causal(scores, tq)
        m_old = m_all[item]
        m_new = jnp.maximum(m_old, jnp.max(scores, axis=0, keepdims=True))
        probs = jnp.exp2((scores - m_new) * scale)
        fade = jnp.exp2((m_old - m_new) * scale)
        m_all[item] = m_new
        l_all[item] = l_all[item] * fade + row_sum(probs)
        acc_all[item] = acc_all[item] * fade + dot(vt[g, side, :, start], probs.astype(BF), NN)

    for g in range(kv_heads):
        vt[g, 0] = vl_ref[:, blk(g, head_dim)].T

    @pl.loop(0, kv_heads * TILES)
    def _(item):
        tile = lax.rem(item, TILES)
        load_q(item)
        m_all[item] = jnp.full_like(m_all[item], NEG_BIG)
        l_all[item] = jnp.zeros_like(l_all[item])
        acc_all[item] = jnp.zeros_like(acc_all[item])
        key_piece(item, kl_ref, 0, blk(tile, tq), True)

        @pl.loop(0, tile)
        def _(i):
            key_piece(item, kl_ref, 0, blk(i, tq), False)

    for j in range(O_PIECES):
        ox_copy(j, f_x).wait_recv()
        oy_copy(j, flag).start()
        od_copy(1 + j, wo_out.at[f_x, o_span(flag, j)], f_x, o_span(flag, j)).start()

    @pl.when(flag == 1)
    def _():
        for k in range(len(kv_pairs)):
            kv_copy(k).wait_recv()
        for g in range(kv_heads):
            vt[g, 1] = vp_ref[:, blk(g, head_dim)].T

    @pl.loop(0, kv_heads * TILES)
    def _(item):
        g, tile = item // TILES, lax.rem(item, TILES)
        rows = blk(tile, tq)

        @pl.when(flag == 1)
        def _():
            load_q(item)

        @pl.loop(0, flag * TILES)
        def _(i):
            key_piece(item, kp_ref, 1, blk(i, tq), False)

        total = l_all[item]
        lse_ref[item] = m_all[item] * scale + jnp.log2(total)
        out_t = acc_all[item] / total
        for h in range(group):
            o_ref[rows, blk(g * group + h, head_dim)] = out_t[:, h * tq:h * tq + tq].T.astype(BF)

        for j in range(O_PIECES):
            @pl.when(item == (j + 1) * kv_heads * TILES // O_PIECES - 1)
            def _():
                oy_copy(j, far).wait_recv()
                od_copy(1 + O_PIECES + j, wo_out.at[f_x, o_span(1 - flag, j)], f_x, o_span(1 - flag, j)).start()

    od_copy(0, wo_ref, f_core, all_rows).wait_recv()
    for j in range(O_PIECES):
        od_copy(1 + j, wo_out.at[f_x, o_span(flag, j)], f_diag, o_span(flag, j)).wait_recv()
        od_copy(1 + O_PIECES + j, wo_out.at[f_x, o_span(1 - flag, j)], f_diag, o_span(1 - flag, j)).wait_recv()

    for k in range(1, n_line):
        zw_copy(k, lax.rem(z + n_line - k, n_line)).wait_recv()
        zw_copy(k, z).wait_send()
    for k, where, _ in gains:
        g_copy(k, where, f).wait_send()
    own_copy(f).wait_send()
    od_copy(0, wo_ref, f, all_rows).wait_send()
    for j in range(PIECES):
        x_copy(j).wait_send()
        y_copy(j, flag).wait_send()
        d_copy(j, flag, f_x).wait_send()
        d_copy(j, 1 - flag, f_x).wait_send()
    for j in range(O_PIECES):
        ox_copy(j, f).wait_send()
        oy_copy(j, flag).wait_send()
        od_copy(1 + j, wo_out.at[f_x, o_span(flag, j)], f_x, o_span(flag, j)).wait_send()
        od_copy(1 + O_PIECES + j, wo_out.at[f_x, o_span(1 - flag, j)], f_x, o_span(1 - flag, j)).wait_send()

    @pl.when(flag == 0)
    def _():
        for k in range(len(kv_pairs)):
            kv_copy(k).wait_send()

    for local in (local_o, put_n, put_w):
        local.wait()


def front(hidden, gain, w_qkv, w_out, cosines, sines, group, kv_width, n_line, cid):
    q_len, model_dim = hidden.shape
    feat, width = w_qkv.shape
    head_dim = cosines.shape[1]
    q_width = width - 2 * kv_width
    kv_heads = kv_width // head_dim
    o_rows, o_cols = w_out.shape
    n_fsdp = model_dim // feat
    tq = q_len // TILES
    wide = group * tq
    items = kv_heads * TILES
    sds = jax.ShapeDtypeStruct
    kv = sds((q_len, kv_width), BF)
    q_like = sds((q_len, q_width), BF)
    line = pltpu.VMEM((items, 1, wide), F32)
    own, pair, trio = DMA(()), DMA((2,)), DMA((n_fsdp - 1,))
    w_link, w_side, o_link, o_core, z_link = DMA((PIECES,)), DMA((2, PIECES)), DMA((O_PIECES,)), DMA((1 + 2 * O_PIECES,)), DMA((n_line - 1,))
    return pl.pallas_call(
        functools.partial(front_kernel, group, n_line),
        in_specs=[ANY] + [VMEM] * 5,
        out_specs=[VMEM] * 8 + [ANY] * 3,
        out_shape=[q_like, q_like, sds((items, 1, wide), F32), kv, kv, kv, kv, sds((1, model_dim), F32), sds((q_len, model_dim), BF), sds((n_fsdp, feat, width), BF), sds((n_line, n_fsdp, o_rows, o_cols), BF)],
        scratch_shapes=[
            pltpu.VMEM((n_fsdp, feat, width), BF),
            pltpu.VMEM((q_len, model_dim), BF),
            pltpu.VMEM((q_len, width), F32),
            pltpu.VMEM((2, tq, model_dim), BF),
            pltpu.VMEM((n_fsdp, 1, feat), F32),
            pltpu.VMEM((wide, head_dim), BF),
            pltpu.VMEM((kv_heads, 2, head_dim, q_len), BF),
            line,
            line,
            pltpu.VMEM((items, head_dim, wide), F32),
        ] + [pair, trio, trio, own, own, w_link, w_link, w_link, w_link, w_side, w_side, pair, pair, o_link, o_link, o_link, o_link, o_core, o_core, z_link, z_link, DMA((4,))],
        compiler_params=params(cid),
        name="front",
    )(hidden, gain, w_qkv, w_out, cosines, sines)


def back_kernel(n_line, group, o_ref, q_ref, lse_ref, cos_ref, sin_ref, kl_ref, vl_ref, kp_ref, vp_ref, _wo_in, ct_ref, d_ref, o_all, wo_all, w_ref, ctb_ref, do_ref, dkl_ref, dvl_ref, dkp_ref, dvp_ref, qs_ref, dos_ref, delta_ref, kt_ref, dqt_ref, load_sem, keep_sem, ct_sem, od_send, ou_send, o_recv, y_send, y_recv, x_send, x_recv, c_send, c_recv, cx_send, cx_recv, kv_send, kv_recv):
    last = n_line - 1
    z, flag, f = lax.axis_index("tp"), lax.axis_index("cp"), lax.axis_index("fsdp")
    far = 1 - flag
    f_core, f_x, f_diag = fsdp_peers(f)
    q_len, width = o_ref.shape
    head_dim = cos_ref.shape[1]
    half_dim = head_dim // 2
    kv_width = kl_ref.shape[1]
    kv_heads = kv_width // head_dim
    tq = q_len // TILES
    wide = group * tq
    score_scale = head_dim ** -0.5
    n_parts, o_rows, part = w_ref.shape
    o_half = o_rows // 2
    load = pltpu.make_async_copy(wo_all.at[z], w_ref, load_sem)
    load.start()
    keep = pltpu.make_async_copy(o_ref, o_all.at[z], keep_sem)
    keep.start()

    def ct_load(tile):
        slot = lax.rem(tile, 2)
        return pltpu.make_async_copy(ct_ref.at[blk(tile, tq)], ctb_ref.at[slot], ct_sem.at[slot])

    ct_load(0).start()
    ct_load(1).start()

    to_core, to_x, to_y = {"fsdp": f_core}, {"fsdp": f_x}, {"cp": far}
    meet([to_core, to_x, to_y] + others("tp", z, n_line))

    def tile_rows(j):
        return blk(j, tq)

    def o_down(t, j, src):
        return remote(src, o_all.at[t, tile_rows(j)], od_send.at[t, j], o_recv.at[t, j], {"tp": jnp.maximum(z - 1, 0)})

    def o_up(t, j, src):
        return remote(src, o_all.at[t, tile_rows(j)], ou_send.at[t, j], o_recv.at[t, j], {"tp": jnp.minimum(z + 1, last)})

    def wo_half(r, slot, side):
        return wo_all.at[lax.rem(z + r, n_line), slot, blk(side, o_half)]

    def y_copy(r, side):
        return remote(wo_half(r, f, side), wo_half(r, f, side), y_send.at[r - 1], y_recv.at[r - 1], to_y)

    def x_copy(r, side, slot):
        return remote(wo_half(r, slot, side), wo_half(r, slot, side), x_send.at[side, r - 1], x_recv.at[side, r - 1], to_x)

    def c_copy(r, side, slot):
        return remote(wo_half(r, slot, side), wo_half(r, slot, side), c_send.at[side, r - 1], c_recv.at[side, r - 1], to_core)

    def cx_copy(r, side, slot):
        return remote(wo_half(r, slot, side), wo_half(r, slot, side), cx_send.at[side, r - 1], cx_recv.at[side, r - 1], to_core)

    for j in range(TILES):
        @pl.when(z > 0)
        def _():
            o_down(z, j, o_ref.at[tile_rows(j)]).start()

        @pl.when(z < last)
        def _():
            o_up(z, j, o_ref.at[tile_rows(j)]).start()

    for r in range(1, n_line):
        y_copy(r, flag).start()
        x_copy(r, flag, f).start()
        c_copy(r, flag, f).start()

    def o_tick(k):
        r, j = k // TILES + 1, lax.rem(k, TILES)

        @pl.when(z + r <= last)
        def _():
            t = jnp.minimum(z + r, last)
            o_down(t, j, o_all.at[t, tile_rows(j)]).wait_recv()

            @pl.when(z > 0)
            def _():
                o_down(t, j, o_all.at[t, tile_rows(j)]).start()

        @pl.when(z - r >= 0)
        def _():
            t = jnp.maximum(z - r, 0)
            o_up(t, j, o_all.at[t, tile_rows(j)]).wait_recv()

            @pl.when(z < last)
            def _():
                o_up(t, j, o_all.at[t, tile_rows(j)]).start()

    def y_tick(r):
        y_copy(r, far).wait_recv()
        x_copy(r, far, f).start()
        c_copy(r, far, f).start()

    def x_tick(q):
        r, side = q % (n_line - 1) + 1, flag if q < n_line - 1 else far
        x_copy(r, side, f_x).wait_recv()
        cx_copy(r, side, f_x).start()

    zero(dkl_ref)
    zero(dvl_ref)

    @pl.when(flag == 1)
    def _():
        zero(dkp_ref)
        zero(dvp_ref)

    load.wait()

    def do_tile(tile):
        ct_load(tile).wait()
        slot = lax.rem(tile, 2)
        total = sum(dot(ctb_ref[slot, :, blk(k, part)], w_ref[k], NT) for k in range(n_parts))
        do_ref[tile_rows(tile), :] = total.astype(BF)

        @pl.when(tile + 2 < TILES)
        def _():
            ct_load(tile + 2).start()

    def bwd_item(item):
        g, tile = item // TILES, lax.rem(item, TILES)
        kv_cols = blk(g, head_dim)
        rows = blk(tile, tq)

        @pl.when(tile == 0)
        def _():
            kt_ref[0] = kl_ref[:, kv_cols].T
            kt_ref[1] = kp_ref[:, kv_cols].T

        for h in range(group):
            cols = blk(g * group + h, head_dim)
            stack = blk(h, tq)
            qs_ref[stack, :] = q_ref[rows, cols]
            d_h = do_ref[rows, cols]
            dos_ref[stack, :] = d_h
            prod = d_h.astype(F32) * o_ref[rows, cols].astype(F32)
            delta_ref[:, stack] = row_sum(prod.T)
        zero(dqt_ref)

        def piece(k_ref, v_ref, dk_ref, dv_ref, side, span, masked):
            scores = dot(k_ref[span, kv_cols], qs_ref[...], NT)
            if masked:
                scores = causal(scores, tq)
            probs = jnp.exp2(scores * (score_scale * LOG2E) - lse_ref[item])
            d_probs = dot(v_ref[span, kv_cols], dos_ref[...], NT)
            d_scores = (probs * (d_probs - delta_ref[...]) * score_scale).astype(BF)
            dv_ref[g, span, :] += dot(probs.astype(BF), dos_ref[...], NN)
            dk_ref[g, span, :] += dot(d_scores, qs_ref[...], NN)
            dqt_ref[...] += dot(kt_ref[side, :, span], d_scores, NN)

        piece(kl_ref, vl_ref, dkl_ref, dvl_ref, 0, blk(tile, tq), True)

        @pl.loop(0, tile)
        def _(i):
            piece(kl_ref, vl_ref, dkl_ref, dvl_ref, 0, blk(i, tq), False)

        @pl.loop(0, flag * (q_len // tq))
        def _(i):
            piece(kp_ref, vp_ref, dkp_ref, dvp_ref, 1, blk(i, tq), False)

        for h in range(group):
            dq_h = dqt_ref[:, h * tq:h * tq + tq].T
            d_ref[rows, blk(g * group + h, head_dim)] = rope(dq_h, cos_ref[rows, :], -sin_ref[rows, :], half_dim).astype(BF)

        @pl.when((tile == TILES - 1) & (flag == 1))
        def _():
            for copy in back(g):
                copy.start()

    def back(g):
        return [remote(ref.at[g], ref.at[g], kv_send.at[k, g], kv_recv.at[k, g], {"cp": 0}) for k, ref in enumerate((dkp_ref, dvp_ref))]

    def kv_done(g):
        @pl.when(flag == 0)
        def _():
            for copy in back(g):
                copy.wait_recv()
            dkl_ref[g] += dkp_ref[g]
            dvl_ref[g] += dvp_ref[g]

        dk = rope(dkl_ref[g], cos_ref[...], -sin_ref[...], half_dim)
        k_at = width // head_dim + g
        d_ref[:, blk(k_at, head_dim)] = dk.astype(BF)
        d_ref[:, blk(k_at + kv_heads, head_dim)] = dvl_ref[g].astype(BF)

        @pl.when(flag == 1)
        def _():
            for copy in back(g):
                copy.wait_send()

    items = TILES * (kv_heads + 1)
    o_ticks, x_ticks = TILES * last, 2 * last
    y_at = {4 + 3 * (r - 1): r for r in range(1, n_line)}
    x_at = {5: 0, 9: 1, 11: 2}

    @pl.loop(0, items)
    def _(item):
        @pl.when(item < TILES)
        def _():
            do_tile(item)

        @pl.when(item >= TILES)
        def _():
            bwd_item(item - TILES)

        @pl.when(lax.rem(item, 2) == 1)
        def _():
            o_tick(item // 2)

        for at, r in y_at.items():
            @pl.when(item == at)
            def _():
                y_tick(r)

        for at, q in x_at.items():
            @pl.when(item == at)
            def _():
                x_tick(q)

    done = items // 2
    tail = [("x", q) for q in range(len(x_at), x_ticks)] + [("kv", g) for g in range(kv_heads)]
    for k in range(done, o_ticks):
        o_tick(jnp.int32(k))
        if (k - done) % 2 == 1 and tail:
            kind, arg = tail.pop(0)
            x_tick(arg) if kind == "x" else kv_done(arg)
            later = [t for t in tail if t[0] == "kv"]
            if later:
                tail.remove(later[0])
                kv_done(later[0][1])
    for kind, arg in tail:
        x_tick(arg) if kind == "x" else kv_done(arg)

    for r in range(1, n_line):
        for side in (flag, far):
            c_copy(r, side, f_core).wait_recv()
            cx_copy(r, side, f_diag).wait_recv()
            x_copy(r, side, f).wait_send()
            c_copy(r, side, f).wait_send()
            cx_copy(r, side, f_x).wait_send()
        y_copy(r, flag).wait_send()

    @pl.loop(0, n_line)
    def _(t):
        @pl.when((t >= z) & (z > 0))
        def _():
            for j in range(TILES):
                o_down(t, j, o_all.at[t, tile_rows(j)]).wait_send()

        @pl.when((t <= z) & (z < last))
        def _():
            for j in range(TILES):
                o_up(t, j, o_all.at[t, tile_rows(j)]).wait_send()

    keep.wait()


def attn_back(attn_out, q_rot, lse, cosines, sines, k_loc, v_loc, k_prev, v_prev, wo_all, cotangent, n_line, group, cid):
    q_len, width = attn_out.shape
    head_dim = cosines.shape[1]
    kv_width = k_loc.shape[1]
    kv_heads = kv_width // head_dim
    _, n_fsdp, o_rows, o_cols = wo_all.shape
    tq = q_len // TILES
    wide = group * tq
    acc = pltpu.VMEM((kv_heads, q_len, head_dim), F32)
    stack = pltpu.VMEM((wide, head_dim), BF)
    own, pair, tiles, hop, side, kv = DMA(()), DMA((2,)), DMA((n_line, TILES)), DMA((n_line - 1,)), DMA((2, n_line - 1)), DMA((2, kv_heads))
    return pl.pallas_call(
        functools.partial(back_kernel, n_line, group),
        in_specs=[VMEM] * 9 + [ANY] * 2,
        out_specs=[VMEM, ANY, ANY],
        out_shape=[jax.ShapeDtypeStruct((q_len, width + 2 * kv_width), BF), jax.ShapeDtypeStruct((n_line, q_len, width), BF), jax.ShapeDtypeStruct(wo_all.shape, BF)],
        input_output_aliases={9: 2},
        scratch_shapes=[
            pltpu.VMEM((n_fsdp, o_rows, o_cols), BF),
            pltpu.VMEM((2, tq, cotangent.shape[1]), BF),
            pltpu.VMEM((q_len, width), BF),
            acc, acc, acc, acc,
            stack,
            stack,
            pltpu.VMEM((1, wide), F32),
            pltpu.VMEM((2, head_dim, q_len), BF),
            pltpu.VMEM((head_dim, wide), F32),
        ] + [own, own, pair, tiles, tiles, tiles, hop, hop, side, side, side, side, side, side, kv, kv],
        compiler_params=params(cid),
        name="attn_back",
    )(attn_out, q_rot, lse, cosines, sines, k_loc, v_loc, k_prev, v_prev, wo_all, cotangent)


class Line:
    def __init__(self, n_line, buf_ref, pbuf_ref, send_sem, recv_sem, fill, finish):
        self.last = n_line - 1
        self.z = lax.axis_index("tp")
        self.buf, self.pbuf, self.send_sem, self.recv_sem = buf_ref, pbuf_ref, send_sem, recv_sem
        self.chunks, self.rows = buf_ref.shape[1], buf_ref.shape[2]
        self.block = pbuf_ref.shape[1]
        self.per_block = self.block // self.rows
        self.fill, self.finish = fill, finish
        self.steps = self.chunks + self.last

    def dist(self, side):
        return self.z if side else self.last - self.z

    def toward(self, side, back=False):
        up = bool(side) != back
        return {"tp": jnp.clip(self.z + 1 if up else self.z - 1, 0, self.last)}

    def copy(self, side, chunk):
        spot = self.buf.at[side, chunk]
        return remote(spot, spot, self.send_sem.at[side, chunk], self.recv_sem.at[side, chunk], self.toward(side))

    def live(self, side, step):
        chunk = step - self.dist(side)
        return chunk, (chunk >= 0) & (chunk < self.chunks)

    def tick(self, step):
        for side in range(2):
            chunk, ok = self.live(side, step)

            @pl.when(ok & (lax.rem(chunk, self.per_block) == 0))
            def _():
                self.fill(self.pbuf.at[side], blk((side * self.chunks + chunk) // self.per_block, self.block))

        for side in range(2):
            chunk, ok = self.live(side, step)
            dist = self.dist(side)
            part = blk(lax.rem(jnp.maximum(chunk, 0), self.per_block), self.rows)

            @pl.when(ok & (dist == 0))
            def _():
                self.buf[side, chunk] = self.pbuf[side, part, :]

            @pl.when(ok & (dist > 0))
            def _():
                self.copy(side, chunk).wait_recv()
                self.buf[side, chunk] += self.pbuf[side, part, :]

            @pl.when(ok & (dist < self.last))
            def _():
                self.copy(side, chunk).start()

            @pl.when(ok & (dist == self.last))
            def _():
                self.finish(chunk, self.buf[side, chunk])

    def drain(self):
        for side in range(2):
            @pl.when(self.dist(side) < self.last)
            def _():
                @pl.loop(0, self.chunks)
                def _(chunk):
                    self.copy(side, chunk).wait_send()


def close_kernel(n_line, n_fsdp, d_ref, o_ref, gain_ref, hid_ref, ct_ref, n_ref, w_all, o_all, wo_all, out_ref, blk_ref, gg_ref, ts, yr, dl, xs, ks, xr, buf, gp, ga, gs, gb, gt, gc, ebuf, fb_in, fb_ct, fb_out, send_sem, recv_sem, w_sem, f_sem, ct_sem, fo_sem, lhs_sem, a_send, a_recv, ld_sem, st_sem, x_send, x_recv, e_sem, es_sem, y_send, y_recv, out_send, out_recv, o_sem, wl_sem, h_sem, r_sem, ga_send, ga_recv, gb_send, gb_recv, gc_send, gc_recv):
    last = n_line - 1
    z, flag, f = lax.axis_index("tp"), lax.axis_index("cp"), lax.axis_index("fsdp")
    far = 1 - flag
    f_core, f_x, f_diag = fsdp_peers(f)
    to_core, to_x, to_y = {"fsdp": f_core}, {"fsdp": f_x}, {"cp": far}
    _, feat, width = w_all.shape
    chunks, rows = buf.shape[1], buf.shape[2]
    half = chunks * rows
    g_rows = feat // GRAD_CHUNKS
    owner = (z == 0) | (z == last)
    own_base = jnp.where(z == last, chunks, 0)
    copy = pltpu.make_async_copy

    def own_span(chunk):
        return blk(own_base + chunk, rows)

    def f_loads(chunk):
        slot = lax.rem(chunk, 2)
        return copy(hid_ref.at[own_span(chunk)], fb_in.at[slot], f_sem.at[slot]), copy(ct_ref.at[own_span(chunk)], fb_ct.at[slot], ct_sem.at[slot])

    def f_store(chunk):
        slot = lax.rem(chunk, 2)
        return copy(fb_out.at[slot], out_ref.at[own_span(chunk)], fo_sem.at[slot])

    @pl.when(owner)
    def _():
        for chunk in range(2):
            for load in f_loads(chunk):
                load.start()

    zero(gp)
    meet([to_core, to_x, to_y] + others("tp", z, n_line) + [{"fsdp": f_diag}])

    def finish(chunk, total):
        slot = lax.rem(chunk, 2)
        for load in f_loads(chunk):
            load.wait()

        @pl.when(chunk > 1)
        def _():
            f_store(chunk - 2).wait()

        x_in = fb_in[slot].astype(F32)
        inv = lax.rsqrt(lane_mean(x_in * x_in) + NORM_EPS)
        x_hat = x_in * inv
        gp[...] += row_sum(total * x_hat)
        scaled = total * gain_ref[...]
        fb_out[slot] = (fb_ct[slot].astype(F32) + inv * (scaled - x_hat * lane_mean(scaled * x_hat))).astype(BF)
        f_store(chunk).start()

        @pl.when(chunk + 2 < chunks)
        def _():
            for load in f_loads(chunk + 2):
                load.start()

    kinds = range(2)

    def g_at(ref, j):
        return ref.at[blk(j, g_rows)]

    def x_copy(j):
        return remote(g_at(xs, j), g_at(xr, j), x_send.at[j], x_recv.at[j], to_x)

    def y_copy(j):
        return remote(g_at(ts, j), g_at(yr, j), y_send.at[j], y_recv.at[j], to_y)

    def e_store(j):
        return copy(ebuf.at[0], g_at(ts, j), es_sem)

    def meet_x(j):
        x_copy(j).wait_recv()
        loads = [copy(g_at(src, j), ebuf.at[k], e_sem.at[k]) for k, src in enumerate((ks, xr))]
        for load in loads:
            load.start()
        for load in loads:
            load.wait()
        ebuf[0] += ebuf[1]
        e_store(j).start()

    def send_y(j):
        e_store(j).wait()
        y_copy(j).start()

    def sum_phase(wbuf, pbuf, abuf, bbuf, lbuf, lhs):
        w_load = copy(w_all, wbuf, w_sem)
        w_load.start()

        def fill(dst, span):
            for k in range(n_fsdp):
                dst[:, blk(k, feat)] = dot(d_ref[span, :], wbuf[k], NT)

        line = Line(n_line, buf, pbuf, send_sem, recv_sem, fill, finish)
        slots = (f_diag, f_core, f_x, f)

        def lhs_loads(j):
            return [copy(src.at[:, blk(slot * GRAD_CHUNKS + j, g_rows)], lhs.at[m, k], lhs_sem.at[m, k]) for m, src in enumerate((n_ref, ct_ref)) for k, slot in enumerate(slots)]

        def a_copy(kind, j):
            return remote(abuf.at[kind], dl.at[kind, blk(j, g_rows)], a_send.at[kind], a_recv.at[kind, j], to_core)

        def b_stores(j):
            return [copy(bbuf.at[k], g_at(dst, j), st_sem.at[k]) for k, dst in enumerate((xs, ks))]

        def send_x(j):
            for kind in kinds:
                a_copy(kind, j).wait_send()
            for store in b_stores(j):
                store.wait()
            x_copy(j).start()

        def make(j):
            for load in lhs_loads(j):
                load.wait()
            for k in range(len(slots)):
                dst = (abuf, bbuf)[k // 2].at[k % 2]
                dst[:, :width] = dot(lhs[0, k], d_ref[...], TN)
                dst[:, width:] = dot(lhs[1, k], o_ref[...], TN)
            for kind in kinds:
                a_copy(kind, j).start()

            @pl.when(j + 1 < GRAD_CHUNKS)
            def _():
                for load in lhs_loads(j + 1):
                    load.start()

        def meet_core(j):
            loads = [copy(dl.at[kind, blk(j, g_rows)], lbuf.at[kind], ld_sem.at[kind]) for kind in kinds]
            for kind in kinds:
                a_copy(kind, j).wait_recv()
                loads[kind].start()
            for kind in kinds:
                loads[kind].wait()
                bbuf[kind] += lbuf[kind]
            for store in b_stores(j):
                store.start()

        for load in lhs_loads(0):
            load.start()
        w_load.wait()

        @pl.loop(0, line.steps)
        def _(step):
            line.tick(step)
            j, odd = step // 2, lax.rem(step, 2)

            @pl.when((odd == 0) & (j > 0) & (j <= GRAD_CHUNKS))
            def _():
                send_x(j - 1)

            @pl.when((odd == 0) & (j < GRAD_CHUNKS))
            def _():
                make(j)

            @pl.when((odd == 1) & (j < GRAD_CHUNKS))
            def _():
                meet_core(j)

            for late in range(2):
                k = (step - FIRST_X - late) * 2 // 5

                @pl.when((k >= 0) & (k < EARLY) & (step - late == FIRST_X + (5 * k + 1) // 2))
                def _():
                    send_y(k) if late else meet_x(k)

        line.drain()

    pl.run_scoped(
        sum_phase,
        pltpu.VMEM(w_all.shape, BF),
        pltpu.VMEM((2, min(128, half), buf.shape[3]), F32),
        pltpu.VMEM((2, g_rows, ts.shape[1]), F32),
        pltpu.VMEM((2, g_rows, ts.shape[1]), F32),
        pltpu.VMEM((2, g_rows, ts.shape[1]), F32),
        pltpu.VMEM((2, n_fsdp, d_ref.shape[0], g_rows), BF),
    )
    steps = chunks + last - 1

    def dist(side):
        return z if side else last - z

    def hop(side, chunk):
        span = blk(side * chunks + chunk, rows)
        up = z - 1 if side else z + 1
        return remote(out_ref.at[span], out_ref.at[span], out_send.at[side, chunk], out_recv.at[side, chunk], {"tp": jnp.clip(up, 0, last)})

    def ga_copy(end, k):
        return remote(gp, ga.at[end], ga_send.at[k], ga_recv.at[end], {"tp": k if end else 1 + k})

    def gb_copy():
        return remote(gs, gb, gb_send, gb_recv, to_y)

    def gc_copy(k, slot):
        to = lax.rem(f + k, n_fsdp)
        return remote(gt.at[to], gc.at[slot], gc_send.at[k - 1], gc_recv.at[k - 1], {"fsdp": to})

    ends = [(end, z == (last if end else 0)) for end in range(2)]

    def spread_phase(obuf, wbuf, hbuf, rbuf):
        o_load = copy(o_all, obuf, o_sem)
        o_load.start()
        q_len, n_cols = hbuf.shape[1], hbuf.shape[2]
        per_part = wo_all.shape[3] // n_cols
        items = per_part * n_fsdp

        def item_loads(item):
            slot = lax.rem(item, 2)
            return copy(wo_all.at[:, item // per_part, :, blk(lax.rem(item, per_part), n_cols)], wbuf.at[slot], wl_sem.at[slot]), copy(hid_ref.at[:, blk(item, n_cols)], hbuf.at[slot], h_sem.at[slot])

        def item_store(item):
            slot = lax.rem(item, 2)
            return copy(rbuf.at[slot], blk_ref.at[:, blk(item, n_cols)], r_sem.at[slot])

        for item in range(2):
            for load in item_loads(item):
                load.start()

        for end, here in ends:
            @pl.when(here)
            def _():
                ga[end] = gp[...]
                for k in range(last):
                    ga_copy(end, k).start()

                for chunk in range(chunks - 2, chunks):
                    f_store(chunk).wait()

                @pl.loop(0, chunks)
                def _(chunk):
                    hop(end, chunk).start()

        def project(item):
            slot = lax.rem(item, 2)
            for load in item_loads(item):
                load.wait()

            @pl.when(item > 1)
            def _():
                item_store(item - 2).wait()

            @pl.loop(0, TILES)
            def _(tile):
                span = blk(tile, q_len // TILES)
                total = sum(dot(obuf[t, span, :], wbuf[slot, t], NN) for t in range(n_line))
                rbuf[slot, span, :] = (hbuf[slot, span, :].astype(F32) + total).astype(BF)

            item_store(item).start()

            @pl.when(item + 2 < items)
            def _():
                for load in item_loads(item + 2):
                    load.start()

        for end, here in ends:
            @pl.when(jnp.logical_not(here))
            def _():
                ga_copy(end, 0).wait_recv()
        gs[...] = ga[0] + ga[1]
        o_load.wait()
        gb_copy().start()

        @pl.loop(0, steps)
        def _(step):
            for side in range(2):
                chunk = step - (last - 1 - dist(side))

                @pl.when((dist(side) < last) & (chunk >= 0) & (chunk < chunks))
                def _():
                    hop(side, chunk).wait_recv()

                    @pl.when(dist(side) > 0)
                    def _():
                        hop(side, chunk).start()

            @pl.when((lax.rem(step, 2) == 0) & (step // 2 < items))
            def _():
                project(step // 2)

            for k in range(EARLY, GRAD_CHUNKS):
                @pl.when(step == 1 + 5 * (k - EARLY))
                def _():
                    meet_x(k)

            for k in range(EARLY - 1, GRAD_CHUNKS):
                @pl.when(step == 2 + 5 * (k - EARLY) if k >= EARLY else step == 0)
                def _():
                    send_y(k)

        for item in range(items - 2, items):
            item_store(item).wait()

    pl.run_scoped(
        spread_phase,
        pltpu.VMEM(o_all.shape, BF),
        pltpu.VMEM((2, n_line, wo_all.shape[2], min(512, feat)), BF),
        pltpu.VMEM((2, d_ref.shape[0], min(512, feat)), BF),
        pltpu.VMEM((2, d_ref.shape[0], min(512, feat)), BF),
    )

    gb_copy().wait()
    for k in range(n_fsdp):
        gt[k] = gs[:, blk(k, feat)] + gb[:, blk(k, feat)]
    gc[f] = gt[f]
    for side in range(2):
        @pl.when(dist(side) > 0)
        def _():
            @pl.loop(0, chunks)
            def _(chunk):
                hop(side, chunk).wait_send()

    @pl.loop(0, GRAD_CHUNKS)
    def _(j):
        x_copy(j).wait_send()

    for k in range(1, n_fsdp):
        gc_copy(k, f).start()
    for k in range(1, n_fsdp):
        gc_copy(k, lax.rem(f + n_fsdp - k, n_fsdp)).wait_recv()
    gg_ref[...] = sum(gc[k] for k in range(n_fsdp))
    for k in range(1, n_fsdp):
        gc_copy(k, f).wait_send()
    for end, here in ends:
        @pl.when(here)
        def _():
            for k in range(last):
                ga_copy(end, k).wait_send()

    @pl.loop(0, GRAD_CHUNKS)
    def _(j):
        y_copy(j).wait()


def close(d_lin, attn_out, gain, hidden, cotangent, normed, w_full, o_all, wo_all, cid):
    q_len, model_dim = hidden.shape
    n_line, n_fsdp = wo_all.shape[:2]
    _, feat, width = w_full.shape
    g_width = width + attn_out.shape[1]
    half = q_len // 2
    rows = half // CHUNKS
    sds = jax.ShapeDtypeStruct
    row = pltpu.VMEM((1, model_dim), F32)
    slices = pltpu.VMEM((n_fsdp, 1, feat), F32)
    strip = pltpu.VMEM((2, rows, model_dim), BF)
    own, pair, line, grad, grads = DMA(()), DMA((2,)), DMA((2, CHUNKS)), DMA((GRAD_CHUNKS,)), DMA((2, GRAD_CHUNKS))
    z_trio, f_trio = DMA((n_line - 1,)), DMA((n_fsdp - 1,))
    act, g_part = sds((q_len, model_dim), BF), sds((feat, g_width), F32)
    return pl.pallas_call(
        functools.partial(close_kernel, n_line, n_fsdp),
        in_specs=[VMEM] * 3 + [ANY] * 6,
        out_specs=[ANY, ANY, VMEM] + [ANY] * 6,
        out_shape=[act, act, sds((1, feat), F32), g_part, g_part, sds((2, feat, g_width), F32), g_part, g_part, g_part],
        scratch_shapes=[
            pltpu.VMEM((2, CHUNKS, rows, model_dim), F32),
            row,
            pltpu.VMEM((2, 1, model_dim), F32),
            row,
            row,
            slices,
            slices,
            pltpu.VMEM((2, feat // GRAD_CHUNKS, g_width), F32),
            strip,
            strip,
            strip,
        ] + [line, line, own, pair, pair, pair, DMA((2, n_fsdp)), pair, grads, pair, pair, grad, grad, pair, own, grad, grad, line, line, own, pair, pair, pair, z_trio, pair, own, own, f_trio, f_trio],
        compiler_params=params(cid),
        name="close",
    )(d_lin, attn_out, gain, hidden, cotangent, normed, w_full, o_all, wo_all)


def solution(mesh):
    act_spec = P("fsdp", "cp", None)
    proj_spec = P("fsdp", "tp", None)
    wout_spec = P("tp", None, "fsdp")
    n_line = mesh.shape["tp"]

    def device_step(hidden, cotangent, positions, gain, w_query, w_key, w_value, w_out):
        hidden, cotangent = hidden[0], cotangent[0]
        assert hidden.shape[0] * mesh.shape["cp"] <= WINDOW_LEN
        feat, q_heads, head_dim = w_query.shape
        kv_heads = w_key.shape[1]
        group = q_heads // kv_heads
        q_width, kv_width = q_heads * head_dim, kv_heads * head_dim
        w_qkv = jnp.concatenate([w_query.reshape(feat, q_width), w_key.reshape(feat, kv_width), w_value.reshape(feat, kv_width)], axis=1)
        cosines, sines = rope_tables(positions, head_dim)
        attn_out, q_rot, lse, k_loc, v_loc, k_prev, v_prev, gain_full, normed, w_full, wo_all = front(hidden, gain.astype(F32)[None], w_qkv, w_out.reshape(q_width, feat), cosines, sines, group, kv_width, n_line, 0)
        d_lin, o_all, wo_all = attn_back(attn_out, q_rot, lse, cosines, sines, k_loc, v_loc, k_prev, v_prev, wo_all, cotangent, n_line, group, 1)
        grad_hidden, block_out, grad_gain, mine, theirs = close(d_lin, attn_out, gain_full, hidden, cotangent, normed, w_full, o_all, wo_all, 2)[:5]
        cuts = [q_width, q_width + kv_width, q_width + 2 * kv_width]
        g_query, g_key, g_value, g_out = [one + two for one, two in zip(jnp.split(mine, cuts, axis=1), jnp.split(theirs, cuts, axis=1))]
        return (
            block_out[None],
            grad_hidden[None],
            grad_gain[0],
            g_query.reshape(w_query.shape),
            g_key.reshape(w_key.shape),
            g_value.reshape(w_value.shape),
            g_out.T.reshape(w_out.shape),
        )

    specs = (act_spec, act_spec, P("fsdp"), proj_spec, proj_spec, proj_spec, wout_spec)
    return jax.shard_map(device_step, mesh=mesh, in_specs=specs[:2] + (P("cp"),) + specs[2:], out_specs=specs, check_vma=False)
```

```python
import functools
import math

import jax
import jax.numpy as jnp
from jax import lax
from jax.experimental import pallas as pl
from jax.experimental.pallas import tpu as pltpu
from jax.sharding import PartitionSpec as P

WINDOW_LEN = 4096
ROPE_BASE = 10000.0
NORM_EPS = 1e-5
NEG_BIG = -1e30
LOG2E = math.log2(math.e)
TILES = 4
CHUNKS = 32
PER_STEP = 2
PIECES = 4
O_PIECES = 2
O_EARLY = 2
GRAD_CHUNKS = 8
FIRST_X = 5
EARLY = 5
LATE = ((5, 1), (6, 10), (7, 20))
VMEM_BYTES = 67043328

MESH = pl.DeviceIdType.MESH
ANY = pl.BlockSpec(memory_space=pl.ANY)
VMEM = pl.BlockSpec(memory_space=pltpu.VMEM)
DMA = pltpu.SemaphoreType.DMA
BF, F32 = jnp.bfloat16, jnp.float32

NT = (((1,), (1,)), ((), ()))
NN = (((1,), (0,)), ((), ()))
TN = (((0,), (0,)), ((), ()))


def dot(a, b, dims):
    return lax.dot_general(a, b, dims, preferred_element_type=F32)


def blk(k, n):
    return pl.ds(k * n if isinstance(k, int) else pl.multiple_of(k * n, n), n)


def lane_mean(vals):
    return jnp.mean(vals, axis=1, keepdims=True)


def row_sum(vals):
    return jnp.sum(vals, axis=0, keepdims=True)


def zero(ref):
    ref[...] = jnp.zeros_like(ref)


def remote(src, dst, send, recv, where):
    return pltpu.make_async_remote_copy(src_ref=src, dst_ref=dst, send_sem=send, recv_sem=recv, device_id=where, device_id_type=MESH)


def meet(peers):
    barrier = pltpu.get_barrier_semaphore()
    for where in peers:
        pl.semaphore_signal(barrier, inc=1, device_id=where, device_id_type=MESH)
    pl.semaphore_wait(barrier, len(peers))


def fsdp_peers(f):
    core = lax.rem(f, 2)
    other = f + 1 - 2 * core
    far = lax.rem(f + 2, 4)
    return other, far, lax.rem(other + 2, 4)


def others(axis, index, count):
    return [{axis: lax.rem(index + k, count)} for k in range(1, count)]


def nearest(z, last):
    near = jnp.where(z > 0, last, 1)
    second = jnp.where(z == 0, 2, jnp.where(z == last, last - 1, 1))
    return near, second


def rope(vals, cos, sin, half_dim):
    return vals * cos + pltpu.roll(vals, half_dim, 1) * sin


def causal(scores, tq):
    key_idx = lax.broadcasted_iota(jnp.int32, scores.shape, 0)
    q_idx = lax.rem(lax.broadcasted_iota(jnp.int32, scores.shape, 1), tq)
    return jnp.where(key_idx <= q_idx, scores, NEG_BIG)


def params(cid):
    return pltpu.CompilerParams(collective_id=cid, has_side_effects=True, vmem_limit_bytes=VMEM_BYTES)


def rope_tables(positions, head_dim):
    inv_freq = ROPE_BASE ** (-jnp.arange(0, head_dim, 2).astype(F32) / head_dim)
    angles = positions.astype(F32)[:, None] * inv_freq[None, :]
    cosines, sines = jnp.cos(angles), jnp.sin(angles)
    return jnp.concatenate([cosines, cosines], axis=1), jnp.concatenate([-sines, sines], axis=1)


def front_kernel(group, n_line, hid_ref, gain_ref, w_ref, wo_ref, cos_ref, sin_ref, o_ref, qr_ref, lse_ref, kl_ref, vl_ref, kp_ref, vp_ref, gfull_ref, n_out, w_out, wo_all, o_all, wbuf, nbuf, acc, hbuf, gbuf, qs, vt, m_all, l_all, acc_all, h_sem, g_send, g_recv, own_send, own_recv, x_send, x_recv, y_send, y_recv, d_send, d_recv, kv_send, kv_recv, ox_send, ox_recv, oy_send, oy_recv, od_send, od_recv, zw_send, zw_recv, wx_send, wx_recv, ot_send, ot_recv, out_sem):
    q_len, feat = hid_ref.shape[0], w_ref.shape[0]
    head_dim = cos_ref.shape[1]
    half_dim = head_dim // 2
    kv_width = kl_ref.shape[1]
    kv_heads = kv_width // head_dim
    q_width = qr_ref.shape[1]
    tq = q_len // TILES
    wide = group * tq
    scale = head_dim ** -0.5 * LOG2E
    half = feat // 2
    piece = half // PIECES
    o_rows = wo_ref.shape[0]
    o_half = o_rows // 2
    o_piece = o_half // O_PIECES
    flag, f, z = lax.axis_index("cp"), lax.axis_index("fsdp"), lax.axis_index("tp")
    wo_out = wo_all.at[z]
    far = 1 - flag
    f_core, f_x, f_diag = fsdp_peers(f)
    to_core, to_x, to_diag, to_y = {"fsdp": f_core}, {"fsdp": f_x}, {"fsdp": f_diag}, {"cp": far}

    def h_load(tile):
        slot = lax.rem(tile, 2)
        return pltpu.make_async_copy(hid_ref.at[blk(tile, tq)], hbuf.at[slot], h_sem.at[slot])

    h_load(0).start()
    h_load(1).start()
    meet([to_core, to_x, to_diag, to_y] + others("tp", z, n_line))

    def span(side, j):
        return blk(side * PIECES + j, piece)

    def x_copy(j):
        return remote(w_ref.at[span(flag, j)], wbuf.at[f, span(flag, j)], x_send.at[j], x_recv.at[j], to_x)

    def x_in(j):
        return remote(w_ref.at[span(flag, j)], wbuf.at[f_x, span(flag, j)], x_send.at[j], x_recv.at[j], to_x)

    def y_copy(j, side):
        return remote(wbuf.at[f_x, span(side, j)], wbuf.at[f_x, span(side, j)], y_send.at[j], y_recv.at[j], to_y)

    def d_copy(j, side, slot):
        return remote(wbuf.at[slot, span(side, j)], wbuf.at[slot, span(side, j)], d_send.at[side, j], d_recv.at[side, j], to_core)

    def g_copy(k, where, slot):
        return remote(gain_ref, gbuf.at[slot], g_send.at[k], g_recv.at[k], where)

    def own_copy(slot):
        return remote(w_ref, wbuf.at[slot], own_send, own_recv, to_core)

    def o_span(side, j):
        return blk(side * O_PIECES + j, o_piece)

    def ox_copy(j, slot):
        return remote(wo_ref.at[o_span(flag, j)], wo_out.at[slot, o_span(flag, j)], ox_send.at[j], ox_recv.at[j], to_x)

    def oy_copy(j, side):
        return remote(wo_out.at[f_x, o_span(side, j)], wo_out.at[f_x, o_span(side, j)], oy_send.at[j], oy_recv.at[j], to_y)

    def od_copy(k, src, slot, where):
        return remote(src, wo_out.at[slot, where], od_send.at[k], od_recv.at[k], to_core)

    def zw_copy(k, owner):
        mine = blk(flag, o_half)
        return remote(wo_ref.at[mine], wo_all.at[owner, f, mine], zw_send.at[k - 1], zw_recv.at[k - 1], {"tp": lax.rem(z + k, n_line)})

    def wx_copy(k, r, slot):
        spot = wo_all.at[lax.rem(z + r, n_line), slot, blk(flag, o_half)]
        return remote(spot, spot, wx_send.at[k], wx_recv.at[k], to_x)

    def wx_start(k, r):
        zw_copy(n_line - r, lax.rem(z + r, n_line)).wait_recv()
        wx_copy(k, r, f).start()

    def ot_copy(up, j, owner):
        src = o_ref.at[blk(j, tq)]
        where = jnp.minimum(z + 1, last) if up else jnp.maximum(z - 1, 0)
        return remote(src, o_all.at[owner, blk(j, tq)], ot_send.at[up, j], ot_recv.at[up, j], {"tp": where})

    last = n_line - 1
    steps_x = nearest(z, last)
    for k in range(1, n_line):
        zw_copy(k, z).start()
    gains = [(k, where, where["fsdp"]) for k, where in enumerate((to_core, to_x, to_diag))]
    for k, where, _ in gains:
        g_copy(k, where, f).start()
    for j in range(PIECES):
        x_copy(j).start()
    own_copy(f).start()
    for j in range(O_PIECES):
        ox_copy(j, f).start()
    all_rows = pl.ds(0, o_rows)
    od_copy(0, wo_ref, f, all_rows).start()
    local_w = pltpu.make_async_copy(w_ref, wbuf.at[f], out_sem.at[0])
    local_w.start()
    local_o = pltpu.make_async_copy(wo_ref, wo_out.at[f], out_sem.at[1])
    local_o.start()
    gbuf[f] = gain_ref[...]
    for k, where, slot in gains:
        g_copy(k, where, slot).wait_recv()
    for k in range(gbuf.shape[0]):
        gfull_ref[:, blk(k, feat)] = gbuf[k]

    for tile in range(TILES):
        h_load(tile).wait()
        strip = min(32, tq)

        @pl.loop(0, tq // strip)
        def _(i):
            vals = hbuf[tile % 2, blk(i, strip), :].astype(F32)
            inv = lax.rsqrt(lane_mean(vals * vals) + NORM_EPS)
            nbuf[pl.ds(pl.multiple_of(tile * tq + i * strip, strip), strip), :] = (vals * inv * gfull_ref[...]).astype(BF)

        if tile + 2 < TILES:
            h_load(tile + 2).start()
    put_n = pltpu.make_async_copy(nbuf, n_out, out_sem.at[2])
    put_n.start()

    def project(slot, start, rows, first=False):
        cols = pl.ds(pl.multiple_of(slot * feat + start, 128), rows)

        @pl.loop(0, TILES)
        def _(tile):
            here = blk(tile, tq)
            part = dot(nbuf[here, cols], wbuf[slot, pl.ds(start, rows), :], NN)
            acc[here, :] = part if first else acc[here, :] + part

    def x_tick(j):
        x_in(j).wait_recv()
        y_copy(j, flag).start()
        d_copy(j, flag, f_x).start()

    def y_tick(j):
        y_copy(j, far).wait_recv()
        d_copy(j, 1 - flag, f_x).start()

    local_w.wait()
    project(f, 0, feat, first=True)
    x_tick(0)
    own_copy(f_core).wait_recv()
    project(f_core, 0, feat)
    x_tick(1)
    y_tick(0)
    x_tick(2)
    y_tick(1)
    x_tick(3)
    for j in range(PIECES):
        d_copy(j, flag, f_diag).wait_recv()
    first_half = pl.multiple_of(flag * half, half)
    project(f_x, first_half, half)
    y_tick(2)
    project(f_diag, first_half, half)
    y_tick(3)
    for j in range(PIECES):
        d_copy(j, 1 - flag, f_diag).wait_recv()
    second_half = pl.multiple_of((far) * half, half)
    project(f_x, second_half, half)
    project(f_diag, second_half, half)
    put_w = pltpu.make_async_copy(wbuf, w_out, out_sem.at[3])
    put_w.start()

    @pl.loop(0, TILES)
    def _(tile):
        here = blk(tile, tq)
        cos, sin = cos_ref[here, :], sin_ref[here, :]
        for h in range(kv_heads):
            k_at = q_width // head_dim + h
            kl_ref[here, blk(h, head_dim)] = rope(acc[here, blk(k_at, head_dim)], cos, sin, half_dim).astype(BF)
            vl_ref[here, blk(h, head_dim)] = acc[here, blk(k_at + kv_heads, head_dim)].astype(BF)

    kv_pairs = ((kl_ref, kp_ref), (vl_ref, vp_ref))

    def kv_copy(k):
        return remote(kv_pairs[k][0], kv_pairs[k][1], kv_send.at[k], kv_recv.at[k], {"cp": 1})

    @pl.loop(0, TILES)
    def _(tile):
        here = blk(tile, tq)
        cos, sin = cos_ref[here, :], sin_ref[here, :]
        for h in range(group * kv_heads):
            cols = blk(h, head_dim)
            qr_ref[here, cols] = rope(acc[here, cols], cos, sin, half_dim).astype(BF)

    @pl.when(flag == 0)
    def _():
        zero(kp_ref)
        zero(vp_ref)
        for k in range(len(kv_pairs)):
            kv_copy(k).start()

    def load_q(item):
        g, tile = lax.rem(item, kv_heads), item // kv_heads
        rows = blk(tile, tq)
        for h in range(group):
            qs[:, blk(h, tq)] = qr_ref[rows, blk(g * group + h, head_dim)].T

    def key_piece(item, k_ref, side, start, masked):
        g = lax.rem(item, kv_heads)
        scores = dot(k_ref[start, blk(g, head_dim)], qs[...], NN)
        if masked:
            scores = causal(scores, tq)
        m_old = m_all[item]
        m_new = jnp.maximum(m_old, jnp.max(scores, axis=0, keepdims=True))
        probs = jnp.exp2((scores - m_new) * scale)
        fade = jnp.exp2((m_old - m_new) * scale)
        m_all[item] = m_new
        l_all[item] = l_all[item] * fade + row_sum(probs)
        acc_all[item] = acc_all[item] * fade + dot(vt[g, side, :, start], probs.astype(BF), NN)

    for g in range(kv_heads):
        vt[g, 0] = vl_ref[:, blk(g, head_dim)].T

    wx_start(0, steps_x[0])

    @pl.loop(0, kv_heads * TILES)
    def _(item):
        tile = item // kv_heads
        load_q(item)
        m_all[item] = jnp.full_like(m_all[item], NEG_BIG)
        l_all[item] = jnp.zeros_like(l_all[item])
        acc_all[item] = jnp.zeros_like(acc_all[item])
        key_piece(item, kl_ref, 0, blk(tile, tq), True)

        @pl.loop(0, tile // 2)
        def _(i):
            key_piece(item, kl_ref, 0, blk(i, 2 * tq), False)

        @pl.when(lax.rem(tile, 2) == 1)
        def _():
            key_piece(item, kl_ref, 0, blk(tile - 1, tq), False)

    for j in range(O_PIECES):
        ox_copy(j, f_x).wait_recv()
        oy_copy(j, flag).start()
        od_copy(1 + j, wo_out.at[f_x, o_span(flag, j)], f_x, o_span(flag, j)).start()
    wx_start(1, steps_x[1])

    @pl.when(flag == 1)
    def _():
        for k in range(len(kv_pairs)):
            kv_copy(k).wait_recv()
        for g in range(kv_heads):
            vt[g, 1] = vp_ref[:, blk(g, head_dim)].T

    @pl.loop(0, kv_heads * TILES)
    def _(item):
        g, tile = lax.rem(item, kv_heads), item // kv_heads
        rows = blk(tile, tq)

        @pl.when(flag == 1)
        def _():
            load_q(item)

        @pl.loop(0, flag * TILES // 2)
        def _(i):
            key_piece(item, kp_ref, 1, blk(i, 2 * tq), False)

        total = l_all[item]
        lse_ref[g * TILES + tile] = m_all[item] * scale + jnp.log2(total)
        out_t = acc_all[item] / total
        for h in range(group):
            o_ref[rows, blk(g * group + h, head_dim)] = out_t[:, h * tq:h * tq + tq].T.astype(BF)

        for j in range(O_EARLY):
            @pl.when((item == (j + 1) * kv_heads) & (z > 0))
            def _():
                ot_copy(0, j, z).start()

            @pl.when((item == (j + 1) * kv_heads) & (z < last))
            def _():
                ot_copy(1, j, z).start()

        for j in range(O_PIECES):
            @pl.when(item == (j + 1) * kv_heads * TILES // O_PIECES - 1)
            def _():
                oy_copy(j, far).wait_recv()
                od_copy(1 + O_PIECES + j, wo_out.at[f_x, o_span(1 - flag, j)], f_x, o_span(1 - flag, j)).start()

    od_copy(0, wo_ref, f_core, all_rows).wait_recv()
    for j in range(O_PIECES):
        od_copy(1 + j, wo_out.at[f_x, o_span(flag, j)], f_diag, o_span(flag, j)).wait_recv()
        od_copy(1 + O_PIECES + j, wo_out.at[f_x, o_span(1 - flag, j)], f_diag, o_span(1 - flag, j)).wait_recv()

    third = n_line * last // 2 - sum(steps_x)
    zw_copy(n_line - third, lax.rem(z + third, n_line)).wait_recv()
    for k in range(1, n_line):
        zw_copy(k, z).wait_send()
    for k, r in enumerate(steps_x):
        wx_copy(k, r, f_x).wait_recv()
        wx_copy(k, r, f).wait_send()
    for j in range(O_EARLY):
        for up in range(2):
            @pl.when(z < last if up else z > 0)
            def _():
                ot_copy(up, j, z).wait_send()
                ot_copy(1 - up, j, z + 1 if up else z - 1).wait_recv()

    for k, where, _ in gains:
        g_copy(k, where, f).wait_send()
    own_copy(f).wait_send()
    od_copy(0, wo_ref, f, all_rows).wait_send()
    for j in range(PIECES):
        x_copy(j).wait_send()
        y_copy(j, flag).wait_send()
        d_copy(j, flag, f_x).wait_send()
        d_copy(j, 1 - flag, f_x).wait_send()
    for j in range(O_PIECES):
        ox_copy(j, f).wait_send()
        oy_copy(j, flag).wait_send()
        od_copy(1 + j, wo_out.at[f_x, o_span(flag, j)], f_x, o_span(flag, j)).wait_send()
        od_copy(1 + O_PIECES + j, wo_out.at[f_x, o_span(1 - flag, j)], f_x, o_span(1 - flag, j)).wait_send()

    @pl.when(flag == 0)
    def _():
        for k in range(len(kv_pairs)):
            kv_copy(k).wait_send()

    for local in (local_o, put_n, put_w):
        local.wait()


def front(hidden, gain, w_qkv, w_out, cosines, sines, group, kv_width, n_line, cid):
    q_len, model_dim = hidden.shape
    feat, width = w_qkv.shape
    head_dim = cosines.shape[1]
    q_width = width - 2 * kv_width
    kv_heads = kv_width // head_dim
    o_rows, o_cols = w_out.shape
    n_fsdp = model_dim // feat
    tq = q_len // TILES
    wide = group * tq
    items = kv_heads * TILES
    sds = jax.ShapeDtypeStruct
    kv = sds((q_len, kv_width), BF)
    q_like = sds((q_len, q_width), BF)
    line = pltpu.VMEM((items, 1, wide), F32)
    own, pair, trio = DMA(()), DMA((2,)), DMA((n_fsdp - 1,))
    early = DMA((2, O_EARLY))
    w_link, w_side, o_link, o_core, z_link = DMA((PIECES,)), DMA((2, PIECES)), DMA((O_PIECES,)), DMA((1 + 2 * O_PIECES,)), DMA((n_line - 1,))
    return pl.pallas_call(
        functools.partial(front_kernel, group, n_line),
        in_specs=[ANY] + [VMEM] * 5,
        out_specs=[VMEM] * 8 + [ANY] * 4,
        out_shape=[q_like, q_like, sds((items, 1, wide), F32), kv, kv, kv, kv, sds((1, model_dim), F32), sds((q_len, model_dim), BF), sds((n_fsdp, feat, width), BF), sds((n_line, n_fsdp, o_rows, o_cols), BF), sds((n_line, q_len, q_width), BF)],
        scratch_shapes=[
            pltpu.VMEM((n_fsdp, feat, width), BF),
            pltpu.VMEM((q_len, model_dim), BF),
            pltpu.VMEM((q_len, width), F32),
            pltpu.VMEM((2, tq, model_dim), BF),
            pltpu.VMEM((n_fsdp, 1, feat), F32),
            pltpu.VMEM((head_dim, wide), BF),
            pltpu.VMEM((kv_heads, 2, head_dim, q_len), BF),
            line,
            line,
            pltpu.VMEM((items, head_dim, wide), F32),
        ] + [pair, trio, trio, own, own, w_link, w_link, w_link, w_link, w_side, w_side, pair, pair, o_link, o_link, o_link, o_link, o_core, o_core, z_link, z_link, pair, pair, early, early, DMA((4,))],
        compiler_params=params(cid),
        name="front",
    )(hidden, gain, w_qkv, w_out, cosines, sines)


def back_kernel(n_line, group, o_ref, q_ref, lse_ref, cos_ref, sin_ref, kl_ref, vl_ref, kp_ref, vp_ref, _wo_in, _o_in, ct_ref, d_ref, o_all, wo_all, w_ref, ctb_ref, do_ref, dkl_ref, dvl_ref, dkp_ref, dvp_ref, qs_ref, dos_ref, delta_ref, kt_ref, dqt_ref, load_sem, keep_sem, ct_sem, od_send, ou_send, o_recv, y_send, y_recv, x_send, x_recv, c_send, c_recv, cx_send, cx_recv, kv_send, kv_recv):
    last = n_line - 1
    z, flag, f = lax.axis_index("tp"), lax.axis_index("cp"), lax.axis_index("fsdp")
    far = 1 - flag
    f_core, f_x, f_diag = fsdp_peers(f)
    q_len, width = o_ref.shape
    head_dim = cos_ref.shape[1]
    half_dim = head_dim // 2
    kv_width = kl_ref.shape[1]
    kv_heads = kv_width // head_dim
    tq = q_len // TILES
    wide = group * tq
    score_scale = head_dim ** -0.5
    n_parts, o_rows, part = w_ref.shape
    o_half = o_rows // 2
    load = pltpu.make_async_copy(wo_all.at[z], w_ref, load_sem)
    load.start()
    keep = pltpu.make_async_copy(o_ref, o_all.at[z], keep_sem)
    keep.start()

    def ct_load(tile):
        slot = lax.rem(tile, 2)
        return pltpu.make_async_copy(ct_ref.at[blk(tile, tq)], ctb_ref.at[slot], ct_sem.at[slot])

    ct_load(0).start()
    ct_load(1).start()

    to_core, to_x, to_y = {"fsdp": f_core}, {"fsdp": f_x}, {"cp": far}
    meet([to_core, to_x, to_y] + others("tp", z, n_line))

    def tile_rows(j):
        return blk(j, tq)

    def o_down(t, j, src):
        return remote(src, o_all.at[t, tile_rows(j)], od_send.at[t, j], o_recv.at[t, j], {"tp": jnp.maximum(z - 1, 0)})

    def o_up(t, j, src):
        return remote(src, o_all.at[t, tile_rows(j)], ou_send.at[t, j], o_recv.at[t, j], {"tp": jnp.minimum(z + 1, last)})

    def wo_half(r, slot, side):
        return wo_all.at[lax.rem(z + r, n_line), slot, blk(side, o_half)]

    def y_copy(r, side):
        return remote(wo_half(r, f, side), wo_half(r, f, side), y_send.at[r - 1], y_recv.at[r - 1], to_y)

    def x_copy(r, side, slot):
        return remote(wo_half(r, slot, side), wo_half(r, slot, side), x_send.at[side, r - 1], x_recv.at[side, r - 1], to_x)

    def c_copy(r, side, slot):
        return remote(wo_half(r, slot, side), wo_half(r, slot, side), c_send.at[side, r - 1], c_recv.at[side, r - 1], to_core)

    def cx_copy(r, side, slot):
        return remote(wo_half(r, slot, side), wo_half(r, slot, side), cx_send.at[side, r - 1], cx_recv.at[side, r - 1], to_core)

    for j in range(O_EARLY, TILES):
        @pl.when(z > 0)
        def _():
            o_down(z, j, o_ref.at[tile_rows(j)]).start()

        @pl.when(z < last)
        def _():
            o_up(z, j, o_ref.at[tile_rows(j)]).start()

    for j in range(O_EARLY):
        @pl.when((z > 0) & (z < last))
        def _():
            o_down(z + 1, j, o_all.at[z + 1, tile_rows(j)]).start()
            o_up(z - 1, j, o_all.at[z - 1, tile_rows(j)]).start()

    steps_x = nearest(z, last)
    third = n_line * last // 2 - sum(steps_x)
    x_copy(third, flag, f).start()
    for r in steps_x:
        cx_copy(r, flag, f_x).start()
    for r in range(1, n_line):
        y_copy(r, flag).start()
        c_copy(r, flag, f).start()

    def o_tick(k):
        r, j = k // TILES + 1, lax.rem(k, TILES)

        @pl.when(z + r <= last)
        def _():
            t = jnp.minimum(z + r, last)
            o_down(t, j, o_all.at[t, tile_rows(j)]).wait_recv()

            @pl.when(z > 0)
            def _():
                o_down(t, j, o_all.at[t, tile_rows(j)]).start()

        @pl.when(z - r >= 0)
        def _():
            t = jnp.maximum(z - r, 0)
            o_up(t, j, o_all.at[t, tile_rows(j)]).wait_recv()

            @pl.when(z < last)
            def _():
                o_up(t, j, o_all.at[t, tile_rows(j)]).start()

    def y_tick(r):
        y_copy(r, far).wait_recv()
        x_copy(r, far, f).start()
        c_copy(r, far, f).start()

    def x_tick(q):
        r, side = (q, far) if q else (third, flag)
        x_copy(r, side, f_x).wait_recv()
        cx_copy(r, side, f_x).start()

    zero(dkl_ref)
    zero(dvl_ref)

    @pl.when(flag == 1)
    def _():
        zero(dkp_ref)
        zero(dvp_ref)

    load.wait()

    def do_tile(tile):
        ct_load(tile).wait()
        slot = lax.rem(tile, 2)
        total = sum(dot(ctb_ref[slot, :, blk(k, part)], w_ref[k], NT) for k in range(n_parts))
        do_ref[tile_rows(tile), :] = total.astype(BF)

        @pl.when(tile + 2 < TILES)
        def _():
            ct_load(tile + 2).start()

    def bwd_item(item):
        g, tile = item // TILES, lax.rem(item, TILES)
        kv_cols = blk(g, head_dim)
        rows = blk(tile, tq)

        @pl.when(tile == 0)
        def _():
            kt_ref[0] = kl_ref[:, kv_cols].T
            kt_ref[1] = kp_ref[:, kv_cols].T

        for h in range(group):
            cols = blk(g * group + h, head_dim)
            stack = blk(h, tq)
            qs_ref[stack, :] = q_ref[rows, cols]
            d_h = do_ref[rows, cols]
            dos_ref[stack, :] = d_h
            prod = d_h.astype(F32) * o_ref[rows, cols].astype(F32)
            delta_ref[:, stack] = row_sum(prod.T)
        zero(dqt_ref)

        def piece(k_ref, v_ref, dk_ref, dv_ref, side, span, masked):
            scores = dot(k_ref[span, kv_cols], qs_ref[...], NT)
            if masked:
                scores = causal(scores, tq)
            probs = jnp.exp2(scores * (score_scale * LOG2E) - lse_ref[item])
            d_probs = dot(v_ref[span, kv_cols], dos_ref[...], NT)
            d_scores = (probs * (d_probs - delta_ref[...])).astype(BF)
            dv_ref[g, span, :] += dot(probs.astype(BF), dos_ref[...], NN)
            dk_ref[g, span, :] += dot(d_scores, qs_ref[...], NN)
            dqt_ref[...] += dot(kt_ref[side, :, span], d_scores, NN)

        piece(kl_ref, vl_ref, dkl_ref, dvl_ref, 0, blk(tile, tq), True)

        @pl.loop(0, tile // 2)
        def _(i):
            piece(kl_ref, vl_ref, dkl_ref, dvl_ref, 0, blk(i, 2 * tq), False)

        @pl.when(lax.rem(tile, 2) == 1)
        def _():
            piece(kl_ref, vl_ref, dkl_ref, dvl_ref, 0, blk(tile - 1, tq), False)

        @pl.loop(0, flag * TILES // 2)
        def _(i):
            piece(kp_ref, vp_ref, dkp_ref, dvp_ref, 1, blk(i, 2 * tq), False)

        for h in range(group):
            dq_h = dqt_ref[:, blk(h, tq)].T * score_scale
            d_ref[rows, blk(g * group + h, head_dim)] = rope(dq_h, cos_ref[rows, :], -sin_ref[rows, :], half_dim).astype(BF)

        @pl.when((tile == TILES - 1) & (flag == 1))
        def _():
            for copy in back(g):
                copy.start()

    def back(g):
        return [remote(ref.at[g], ref.at[g], kv_send.at[k, g], kv_recv.at[k, g], {"cp": 0}) for k, ref in enumerate((dkp_ref, dvp_ref))]

    def kv_done(g):
        @pl.when(flag == 0)
        def _():
            for copy in back(g):
                copy.wait_recv()
            dkl_ref[g] += dkp_ref[g]
            dvl_ref[g] += dvp_ref[g]

        dk = rope(dkl_ref[g] * score_scale, cos_ref[...], -sin_ref[...], half_dim)
        k_at = width // head_dim + g
        d_ref[:, blk(k_at, head_dim)] = dk.astype(BF)
        d_ref[:, blk(k_at + kv_heads, head_dim)] = dvl_ref[g].astype(BF)

        @pl.when(flag == 1)
        def _():
            for copy in back(g):
                copy.wait_send()

    items = TILES * (kv_heads + 1)
    o_ticks = TILES * last
    x_at = {5: 0, 8: 1, 11: 2}

    @pl.loop(0, items)
    def _(item):
        @pl.when(item < TILES)
        def _():
            do_tile(item)

        @pl.when(item >= TILES)
        def _():
            bwd_item(item - TILES)

        @pl.when((lax.rem(item, 2) == 1) & (item > 1))
        def _():
            o_tick(item // 2 - 1 + O_EARLY)

        for r in range(1, n_line):
            @pl.when(item == 3 * r + 1)
            def _():
                y_tick(r)

        for at, q in x_at.items():
            @pl.when(item == at)
            def _():
                x_tick(q)

    done = items // 2 - 1 + O_EARLY
    tail = [("x", q) for q in range(len(x_at), n_line)] + [("kv", g) for g in range(kv_heads)]
    for k in range(done, o_ticks):
        o_tick(jnp.int32(k))
        if (k - done) % 2 == 1 and tail:
            kind, arg = tail.pop(0)
            x_tick(arg) if kind == "x" else kv_done(arg)
            later = [t for t in tail if t[0] == "kv"]
            if later:
                tail.remove(later[0])
                kv_done(later[0][1])
    for kind, arg in tail:
        x_tick(arg) if kind == "x" else kv_done(arg)

    for r in range(1, n_line):
        for side in (flag, far):
            c_copy(r, side, f_core).wait_recv()
            cx_copy(r, side, f_diag).wait_recv()
            c_copy(r, side, f).wait_send()
            cx_copy(r, side, f_x).wait_send()
        x_copy(r, far, f).wait_send()
        y_copy(r, flag).wait_send()
    x_copy(third, flag, f).wait_send()

    @pl.loop(0, n_line)
    def _(t):
        @pl.when((t >= z) & (z > 0))
        def _():
            @pl.loop(jnp.where(t == z, O_EARLY, 0), TILES)
            def _(j):
                o_down(t, j, o_all.at[t, tile_rows(j)]).wait_send()

        @pl.when((t <= z) & (z < last))
        def _():
            @pl.loop(jnp.where(t == z, O_EARLY, 0), TILES)
            def _(j):
                o_up(t, j, o_all.at[t, tile_rows(j)]).wait_send()

    keep.wait()


def attn_back(attn_out, q_rot, lse, cosines, sines, k_loc, v_loc, k_prev, v_prev, wo_all, o_all, cotangent, n_line, group, cid):
    q_len, width = attn_out.shape
    head_dim = cosines.shape[1]
    kv_width = k_loc.shape[1]
    kv_heads = kv_width // head_dim
    _, n_fsdp, o_rows, o_cols = wo_all.shape
    tq = q_len // TILES
    wide = group * tq
    acc = pltpu.VMEM((kv_heads, q_len, head_dim), F32)
    stack = pltpu.VMEM((wide, head_dim), BF)
    own, pair, tiles, hop, side, kv = DMA(()), DMA((2,)), DMA((n_line, TILES)), DMA((n_line - 1,)), DMA((2, n_line - 1)), DMA((2, kv_heads))
    return pl.pallas_call(
        functools.partial(back_kernel, n_line, group),
        in_specs=[VMEM] * 9 + [ANY] * 3,
        out_specs=[VMEM, ANY, ANY],
        out_shape=[jax.ShapeDtypeStruct((q_len, width + 2 * kv_width), BF), jax.ShapeDtypeStruct((n_line, q_len, width), BF), jax.ShapeDtypeStruct(wo_all.shape, BF)],
        input_output_aliases={9: 2, 10: 1},
        scratch_shapes=[
            pltpu.VMEM((n_fsdp, o_rows, o_cols), BF),
            pltpu.VMEM((2, tq, cotangent.shape[1]), BF),
            pltpu.VMEM((q_len, width), BF),
            acc, acc, acc, acc,
            stack,
            stack,
            pltpu.VMEM((1, wide), F32),
            pltpu.VMEM((2, head_dim, q_len), BF),
            pltpu.VMEM((head_dim, wide), F32),
        ] + [own, own, pair, tiles, tiles, tiles, hop, hop, side, side, side, side, side, side, kv, kv],
        compiler_params=params(cid),
        name="attn_back",
    )(attn_out, q_rot, lse, cosines, sines, k_loc, v_loc, k_prev, v_prev, wo_all, o_all, cotangent)


class Line:
    def __init__(self, n_line, buf_ref, pbuf_ref, send_sem, recv_sem, fill, finish):
        self.last = n_line - 1
        self.z = lax.axis_index("tp")
        self.buf, self.pbuf, self.send_sem, self.recv_sem = buf_ref, pbuf_ref, send_sem, recv_sem
        self.chunks, self.rows = buf_ref.shape[1], buf_ref.shape[2]
        self.block = pbuf_ref.shape[1]
        self.per_block = self.block // self.rows
        self.fill, self.finish = fill, finish
        self.steps = self.chunks + self.last

    def dist(self, side):
        return self.z if side else self.last - self.z

    def toward(self, side, back=False):
        up = bool(side) != back
        return {"tp": jnp.clip(self.z + 1 if up else self.z - 1, 0, self.last)}

    def copy(self, side, chunk):
        spot = self.buf.at[side, chunk]
        return remote(spot, spot, self.send_sem.at[side, chunk], self.recv_sem.at[side, chunk], self.toward(side))

    def live(self, side, step):
        chunk = step - self.dist(side)
        return chunk, (chunk >= 0) & (chunk < self.chunks)

    def tick(self, step):
        for side in range(2):
            chunk, ok = self.live(side, step)

            @pl.when(ok & (lax.rem(chunk, self.per_block) == 0))
            def _():
                self.fill(self.pbuf.at[side], blk((side * self.chunks + chunk) // self.per_block, self.block))

        for side in range(2):
            chunk, ok = self.live(side, step)
            dist = self.dist(side)
            part = blk(lax.rem(jnp.maximum(chunk, 0), self.per_block), self.rows)

            @pl.when(ok & (dist == 0))
            def _():
                self.buf[side, chunk] = self.pbuf[side, part, :]

            @pl.when(ok & (dist > 0))
            def _():
                self.copy(side, chunk).wait_recv()
                self.buf[side, chunk] += self.pbuf[side, part, :]

            @pl.when(ok & (dist < self.last))
            def _():
                self.copy(side, chunk).start()

            @pl.when(ok & (dist == self.last))
            def _():
                self.finish(chunk, self.buf[side, chunk])

    def drain(self):
        for side in range(2):
            @pl.when(self.dist(side) < self.last)
            def _():
                @pl.loop(0, self.chunks)
                def _(chunk):
                    self.copy(side, chunk).wait_send()


def close_kernel(n_line, n_fsdp, d_ref, o_ref, gain_ref, hid_ref, ct_ref, n_ref, w_all, o_all, wo_all, out_ref, blk_ref, gg_ref, ts, yr, dl, xs, ks, xr, buf, gp, ga, gs, gb, gt, gc, ebuf, fb_in, fb_ct, fb_out, send_sem, recv_sem, w_sem, f_sem, ct_sem, fo_sem, lhs_sem, a_send, a_recv, ld_sem, st_sem, x_send, x_recv, e_sem, es_sem, y_send, y_recv, out_send, out_recv, o_sem, wl_sem, h_sem, r_sem, ga_send, ga_recv, gb_send, gb_recv, gc_send, gc_recv):
    last = n_line - 1
    z, flag, f = lax.axis_index("tp"), lax.axis_index("cp"), lax.axis_index("fsdp")
    far = 1 - flag
    f_core, f_x, f_diag = fsdp_peers(f)
    to_core, to_x, to_y = {"fsdp": f_core}, {"fsdp": f_x}, {"cp": far}
    _, feat, width = w_all.shape
    chunks, rows = buf.shape[1], buf.shape[2]
    half = chunks * rows
    g_rows = feat // GRAD_CHUNKS
    owner = (z == 0) | (z == last)
    own_base = jnp.where(z == last, chunks, 0)
    copy = pltpu.make_async_copy

    def own_span(chunk):
        return blk(own_base + chunk, rows)

    def f_loads(chunk):
        slot = lax.rem(chunk, 2)
        return copy(hid_ref.at[own_span(chunk)], fb_in.at[slot], f_sem.at[slot]), copy(ct_ref.at[own_span(chunk)], fb_ct.at[slot], ct_sem.at[slot])

    def f_store(chunk):
        slot = lax.rem(chunk, 2)
        return copy(fb_out.at[slot], out_ref.at[own_span(chunk)], fo_sem.at[slot])

    @pl.when(owner)
    def _():
        for chunk in range(2):
            for load in f_loads(chunk):
                load.start()

    zero(gp)
    meet([to_core, to_x, to_y] + others("tp", z, n_line) + [{"fsdp": f_diag}])

    def finish(chunk, total):
        slot = lax.rem(chunk, 2)
        for load in f_loads(chunk):
            load.wait()

        @pl.when(chunk > 1)
        def _():
            f_store(chunk - 2).wait()

        x_in = fb_in[slot].astype(F32)
        inv = lax.rsqrt(lane_mean(x_in * x_in) + NORM_EPS)
        x_hat = x_in * inv
        gp[...] += row_sum(total * x_hat)
        scaled = total * gain_ref[...]
        fb_out[slot] = (fb_ct[slot].astype(F32) + inv * (scaled - x_hat * lane_mean(scaled * x_hat))).astype(BF)
        f_store(chunk).start()

        @pl.when(chunk + 2 < chunks)
        def _():
            for load in f_loads(chunk + 2):
                load.start()

    kinds = range(2)

    def g_at(ref, j):
        return ref.at[blk(j, g_rows)]

    def x_copy(j):
        return remote(g_at(xs, j), g_at(xr, j), x_send.at[j], x_recv.at[j], to_x)

    def y_copy(j):
        return remote(g_at(ts, j), g_at(yr, j), y_send.at[j], y_recv.at[j], to_y)

    def e_store(j):
        return copy(ebuf.at[0], g_at(ts, j), es_sem)

    def meet_x(j):
        x_copy(j).wait_recv()
        loads = [copy(g_at(src, j), ebuf.at[k], e_sem.at[k]) for k, src in enumerate((ks, xr))]
        for load in loads:
            load.start()
        for load in loads:
            load.wait()
        ebuf[0] += ebuf[1]
        e_store(j).start()

    def send_y(j):
        e_store(j).wait()
        y_copy(j).start()

    steps = chunks + last - 1

    def dist(side):
        return z if side else last - z

    def hop(side, chunk):
        span = blk(side * chunks + chunk, rows)
        up = z - 1 if side else z + 1
        return remote(out_ref.at[span], out_ref.at[span], out_send.at[side, chunk], out_recv.at[side, chunk], {"tp": jnp.clip(up, 0, last)})

    ends = [(end, z == (last if end else 0)) for end in range(2)]

    def owner_send(first, stop):
        for end, here in ends:
            @pl.when(here)
            def _():
                @pl.loop(first, stop)
                def _(c):
                    hop(end, c).start()

    def pass_on(step):
        for side in range(2):
            chunk = step - (last - 1 - dist(side))

            @pl.when((dist(side) < last) & (chunk >= 0) & (chunk < chunks))
            def _():
                hop(side, chunk).wait_recv()

                @pl.when(dist(side) > 0)
                def _():
                    hop(side, chunk).start()

    def sum_phase(wbuf, pbuf, abuf, bbuf, lbuf, lhs):
        w_load = copy(w_all, wbuf, w_sem)
        w_load.start()

        def fill(dst, span):
            for k in range(n_fsdp):
                dst[:, blk(k, feat)] = dot(d_ref[span, :], wbuf[k], NT)

        line = Line(n_line, buf, pbuf, send_sem, recv_sem, fill, finish)
        slots = (f_diag, f_core, f_x, f)

        def lhs_loads(j):
            return [copy(src.at[:, blk(slot * GRAD_CHUNKS + j, g_rows)], lhs.at[m, k], lhs_sem.at[m, k]) for m, src in enumerate((n_ref, ct_ref)) for k, slot in enumerate(slots)]

        def a_copy(kind, j):
            return remote(abuf.at[kind], dl.at[kind, blk(j, g_rows)], a_send.at[kind], a_recv.at[kind, j], to_core)

        def b_stores(j):
            return [copy(bbuf.at[k], g_at(dst, j), st_sem.at[k]) for k, dst in enumerate((xs, ks))]

        def send_x(j):
            for kind in kinds:
                a_copy(kind, j).wait_send()
            for store in b_stores(j):
                store.wait()
            x_copy(j).start()

        def make(j):
            for load in lhs_loads(j):
                load.wait()
            for k in range(len(slots)):
                dst = (abuf, bbuf)[k // 2].at[k % 2]
                dst[:, :width] = dot(lhs[0, k], d_ref[...], TN)
                dst[:, width:] = dot(lhs[1, k], o_ref[...], TN)
            for kind in kinds:
                a_copy(kind, j).start()

            @pl.when(j + 1 < GRAD_CHUNKS)
            def _():
                for load in lhs_loads(j + 1):
                    load.start()

        def meet_core(j):
            loads = [copy(dl.at[kind, blk(j, g_rows)], lbuf.at[kind], ld_sem.at[kind]) for kind in kinds]
            for kind in kinds:
                a_copy(kind, j).wait_recv()
                loads[kind].start()
            for kind in kinds:
                loads[kind].wait()
                bbuf[kind] += lbuf[kind]
            for store in b_stores(j):
                store.start()

        for load in lhs_loads(0):
            load.start()
        w_load.wait()

        @pl.loop(0, line.steps)
        def _(fine):
            line.tick(fine)
            step = fine // PER_STEP
            whole = lax.rem(fine, PER_STEP) == 0
            j, odd = step // 2, lax.rem(step, 2)

            @pl.when(whole & (odd == 0) & (j > 0) & (j <= GRAD_CHUNKS))
            def _():
                send_x(j - 1)

            @pl.when(whole & (odd == 0) & (j < GRAD_CHUNKS))
            def _():
                make(j)

            @pl.when(whole & (odd == 1) & (j < GRAD_CHUNKS))
            def _():
                meet_core(j)

            for late in range(2):
                k = (step - FIRST_X - late) * 2 // 5

                @pl.when(whole & (k >= 0) & (k < EARLY) & (step - late == FIRST_X + (5 * k + 1) // 2))
                def _():
                    send_y(k) if late else meet_x(k)

            @pl.when(fine >= chunks)
            def _():
                ready = fine - last - 1
                owner_send(jnp.where(fine == chunks, 0, ready - 1), ready)

            @pl.when(fine > chunks)
            def _():
                for k in range(PER_STEP):
                    pass_on((fine - chunks - 1) * PER_STEP + k)

        @pl.when(owner)
        def _():
            for chunk in range(chunks - 2, chunks):
                f_store(chunk).wait()

        owner_send(chunks - 2, chunks)
        line.drain()

    pl.run_scoped(
        sum_phase,
        pltpu.VMEM(w_all.shape, BF),
        pltpu.VMEM((2, min(128, half), buf.shape[3]), F32),
        pltpu.VMEM((2, g_rows, ts.shape[1]), F32),
        pltpu.VMEM((2, g_rows, ts.shape[1]), F32),
        pltpu.VMEM((2, g_rows, ts.shape[1]), F32),
        pltpu.VMEM((2, n_fsdp, d_ref.shape[0], g_rows), BF),
    )
    def ga_copy(end, k):
        return remote(gp, ga.at[end], ga_send.at[k], ga_recv.at[end], {"tp": k if end else 1 + k})

    def gb_copy():
        return remote(gs, gb, gb_send, gb_recv, to_y)

    def gc_copy(k, slot):
        to = lax.rem(f + k, n_fsdp)
        return remote(gt.at[to], gc.at[slot], gc_send.at[k - 1], gc_recv.at[k - 1], {"fsdp": to})

    def spread_phase(obuf, wbuf, hbuf, rbuf):
        o_load = copy(o_all, obuf, o_sem)
        o_load.start()
        q_len, n_cols = hbuf.shape[1], hbuf.shape[2]
        per_part = wo_all.shape[3] // n_cols
        items = per_part * n_fsdp

        def item_loads(item):
            slot = lax.rem(item, 2)
            return copy(wo_all.at[:, item // per_part, :, blk(lax.rem(item, per_part), n_cols)], wbuf.at[slot], wl_sem.at[slot]), copy(hid_ref.at[:, blk(item, n_cols)], hbuf.at[slot], h_sem.at[slot])

        def item_store(item):
            slot = lax.rem(item, 2)
            return copy(rbuf.at[slot], blk_ref.at[:, blk(item, n_cols)], r_sem.at[slot])

        for item in range(2):
            for load in item_loads(item):
                load.start()

        for end, here in ends:
            @pl.when(here)
            def _():
                ga[end] = gp[...]
                for k in range(last):
                    ga_copy(end, k).start()


        def project(item):
            slot = lax.rem(item, 2)
            for load in item_loads(item):
                load.wait()

            @pl.when(item > 1)
            def _():
                item_store(item - 2).wait()

            @pl.loop(0, TILES)
            def _(tile):
                span = blk(tile, q_len // TILES)
                total = sum(dot(obuf[t, span, :], wbuf[slot, t], NN) for t in range(n_line))
                rbuf[slot, span, :] = (hbuf[slot, span, :].astype(F32) + total).astype(BF)

            item_store(item).start()

            @pl.when(item + 2 < items)
            def _():
                for load in item_loads(item + 2):
                    load.start()

        for end, here in ends:
            @pl.when(jnp.logical_not(here))
            def _():
                ga_copy(end, 0).wait_recv()
        gs[...] = ga[0] + ga[1]
        o_load.wait()
        gb_copy().start()

        early = (last - 1) * PER_STEP

        @pl.loop(0, steps - early)
        def _(step):
            pass_on(step + early)

            @pl.when((lax.rem(step, 3) == 0) & (step // 3 < items))
            def _():
                project(step // 3)

            for k, at in LATE:
                @pl.when(step == at)
                def _():
                    meet_x(k)

            for k, at in LATE:
                @pl.when(step == at + 1)
                def _():
                    send_y(k)

        for item in range(items - 2, items):
            item_store(item).wait()

    pl.run_scoped(
        spread_phase,
        pltpu.VMEM(o_all.shape, BF),
        pltpu.VMEM((2, n_line, wo_all.shape[2], min(512, feat)), BF),
        pltpu.VMEM((2, d_ref.shape[0], min(512, feat)), BF),
        pltpu.VMEM((2, d_ref.shape[0], min(512, feat)), BF),
    )

    gb_copy().wait()
    for k in range(n_fsdp):
        gt[k] = gs[:, blk(k, feat)] + gb[:, blk(k, feat)]
    gc[f] = gt[f]
    for side in range(2):
        @pl.when(dist(side) > 0)
        def _():
            @pl.loop(0, chunks)
            def _(chunk):
                hop(side, chunk).wait_send()

    @pl.loop(0, GRAD_CHUNKS)
    def _(j):
        x_copy(j).wait_send()

    for k in range(1, n_fsdp):
        gc_copy(k, f).start()
    for k in range(1, n_fsdp):
        gc_copy(k, lax.rem(f + n_fsdp - k, n_fsdp)).wait_recv()
    gg_ref[...] = sum(gc[k] for k in range(n_fsdp))
    for k in range(1, n_fsdp):
        gc_copy(k, f).wait_send()
    for end, here in ends:
        @pl.when(here)
        def _():
            for k in range(last):
                ga_copy(end, k).wait_send()

    @pl.loop(0, GRAD_CHUNKS)
    def _(j):
        y_copy(j).wait()


def close(d_lin, attn_out, gain, hidden, cotangent, normed, w_full, o_all, wo_all, cid):
    q_len, model_dim = hidden.shape
    n_line, n_fsdp = wo_all.shape[:2]
    _, feat, width = w_full.shape
    g_width = width + attn_out.shape[1]
    half = q_len // 2
    rows = half // CHUNKS
    sds = jax.ShapeDtypeStruct
    row = pltpu.VMEM((1, model_dim), F32)
    slices = pltpu.VMEM((n_fsdp, 1, feat), F32)
    strip = pltpu.VMEM((2, rows, model_dim), BF)
    own, pair, line, grad, grads = DMA(()), DMA((2,)), DMA((2, CHUNKS)), DMA((GRAD_CHUNKS,)), DMA((2, GRAD_CHUNKS))
    z_trio, f_trio = DMA((n_line - 1,)), DMA((n_fsdp - 1,))
    act, g_part = sds((q_len, model_dim), BF), sds((feat, g_width), F32)
    return pl.pallas_call(
        functools.partial(close_kernel, n_line, n_fsdp),
        in_specs=[VMEM] * 3 + [ANY] * 6,
        out_specs=[ANY, ANY, VMEM] + [ANY] * 6,
        out_shape=[act, act, sds((1, feat), F32), g_part, g_part, sds((2, feat, g_width), F32), g_part, g_part, g_part],
        scratch_shapes=[
            pltpu.VMEM((2, CHUNKS, rows, model_dim), F32),
            row,
            pltpu.VMEM((2, 1, model_dim), F32),
            row,
            row,
            slices,
            slices,
            pltpu.VMEM((2, feat // GRAD_CHUNKS, g_width), F32),
            strip,
            strip,
            strip,
        ] + [line, line, own, pair, pair, pair, DMA((2, n_fsdp)), pair, grads, pair, pair, grad, grad, pair, own, grad, grad, line, line, own, pair, pair, pair, z_trio, pair, own, own, f_trio, f_trio],
        compiler_params=params(cid),
        name="close",
    )(d_lin, attn_out, gain, hidden, cotangent, normed, w_full, o_all, wo_all)


def tail_kernel(head_dim, blk_ref, hid_ref, mine_ref, theirs_ref, blk_out, hid_out, q_out, k_out, v_out, o_out):
    blk_out[...] = blk_ref[...]
    hid_out[...] = hid_ref[...]
    at = 0
    for ref in (q_out, k_out, v_out):
        for h in range(ref.shape[1]):
            cols = blk(at, head_dim)
            ref[:, h, :] = mine_ref[:, cols] + theirs_ref[:, cols]
            at += 1
    rest = slice(at * head_dim, None)
    o_out[...] = (mine_ref[:, rest] + theirs_ref[:, rest]).T


def tail(block_out, grad_hidden, mine, theirs, q_heads, kv_heads, head_dim):
    q_len, model_dim = block_out.shape
    feat = mine.shape[0]
    sds = jax.ShapeDtypeStruct
    act = pl.BlockSpec((q_len // GRAD_CHUNKS, model_dim), lambda i: (i, 0))
    part = pl.BlockSpec((feat // GRAD_CHUNKS, mine.shape[1]), lambda i: (i, 0))

    def heads(n):
        return pl.BlockSpec((feat // GRAD_CHUNKS, n, head_dim), lambda i: (i, 0, 0))

    def like(n):
        return sds((feat, n, head_dim), F32)

    o_rows = q_heads * head_dim
    return pl.pallas_call(
        functools.partial(tail_kernel, head_dim),
        grid=(GRAD_CHUNKS,),
        in_specs=[act, act, part, part],
        out_specs=[act, act, heads(q_heads), heads(kv_heads), heads(kv_heads), pl.BlockSpec((o_rows, feat // GRAD_CHUNKS), lambda i: (0, i))],
        out_shape=[sds(block_out.shape, BF), sds(block_out.shape, BF), like(q_heads), like(kv_heads), like(kv_heads), sds((o_rows, feat), F32)],
        compiler_params=pltpu.CompilerParams(vmem_limit_bytes=VMEM_BYTES),
        name="tail",
    )(block_out, grad_hidden, mine, theirs)


def solution(mesh):
    act_spec = P("fsdp", "cp", None)
    proj_spec = P("fsdp", "tp", None)
    wout_spec = P("tp", None, "fsdp")
    n_line = mesh.shape["tp"]

    def device_step(hidden, cotangent, positions, gain, w_query, w_key, w_value, w_out):
        hidden, cotangent = hidden[0], cotangent[0]
        assert hidden.shape[0] * mesh.shape["cp"] <= WINDOW_LEN
        feat, q_heads, head_dim = w_query.shape
        kv_heads = w_key.shape[1]
        group = q_heads // kv_heads
        q_width, kv_width = q_heads * head_dim, kv_heads * head_dim
        w_qkv = jnp.concatenate([w_query.reshape(feat, q_width), w_key.reshape(feat, kv_width), w_value.reshape(feat, kv_width)], axis=1)
        cosines, sines = rope_tables(positions, head_dim)
        attn_out, q_rot, lse, k_loc, v_loc, k_prev, v_prev, gain_full, normed, w_full, wo_all, o_all = front(hidden, gain.astype(F32)[None], w_qkv, w_out.reshape(q_width, feat), cosines, sines, group, kv_width, n_line, 0)
        d_lin, o_all, wo_all = attn_back(attn_out, q_rot, lse, cosines, sines, k_loc, v_loc, k_prev, v_prev, wo_all, o_all, cotangent, n_line, group, 1)
        grad_hidden, block_out, grad_gain, mine, theirs = close(d_lin, attn_out, gain_full, hidden, cotangent, normed, w_full, o_all, wo_all, 2)[:5]
        block_out, grad_hidden, g_query, g_key, g_value, g_out = tail(block_out, grad_hidden, mine, theirs, q_heads, kv_heads, head_dim)
        return block_out[None], grad_hidden[None], grad_gain[0], g_query, g_key, g_value, g_out.reshape(w_out.shape)

    specs = (act_spec, act_spec, P("fsdp"), proj_spec, proj_spec, proj_spec, wout_spec)
    return jax.shard_map(device_step, mesh=mesh, in_specs=specs[:2] + (P("cp"),) + specs[2:], out_specs=specs, check_vma=False)
```

```python
import functools
import math

import jax
import jax.numpy as jnp
from jax import lax
from jax.experimental import pallas as pl
from jax.experimental.pallas import tpu as pltpu
from jax.sharding import PartitionSpec as P

WINDOW_LEN = 4096
ROPE_BASE = 10000.0
NORM_EPS = 1e-5
NEG_BIG = -1e30
LOG2E = math.log2(math.e)
TILES = 4
CHUNKS = 16
PER_STEP = 1
PIECES = 4
O_PIECES = 2
O_EARLY = 2
GRAD_CHUNKS = 8
FIRST_X = 5
EARLY = 6
LATE = ((6, 2), (7, 7))
VMEM_BYTES = 67043328
SIDES = range(2)

MESH = pl.DeviceIdType.MESH
ANY = pl.BlockSpec(memory_space=pl.ANY)
VMEM = pl.BlockSpec(memory_space=pltpu.VMEM)
DMA = pltpu.SemaphoreType.DMA
BF, F32 = jnp.bfloat16, jnp.float32

NT = (((1,), (1,)), ((), ()))
NN = (((1,), (0,)), ((), ()))
TN = (((0,), (0,)), ((), ()))


def dot(a, b, dims):
    return lax.dot_general(a, b, dims, preferred_element_type=F32)


def parity(k):
    return lax.rem(k, 2)


def blk(k, n):
    return pl.ds(k * n if isinstance(k, int) else pl.multiple_of(k * n, n), n)


def lane_mean(vals):
    return jnp.mean(vals, axis=1, keepdims=True)


def row_sum(vals):
    return jnp.sum(vals, axis=0, keepdims=True)


def zero(ref):
    ref[...] = jnp.zeros_like(ref)


def remote(src, dst, send, recv, where):
    return pltpu.make_async_remote_copy(src_ref=src, dst_ref=dst, send_sem=send, recv_sem=recv, device_id=where, device_id_type=MESH)


def meet(peers):
    barrier = pltpu.get_barrier_semaphore()
    for where in peers:
        pl.semaphore_signal(barrier, inc=1, device_id=where, device_id_type=MESH)
    pl.semaphore_wait(barrier, len(peers))


def fsdp_peers(f):
    core = parity(f)
    other = f + 1 - 2 * core
    far = lax.rem(f + 2, 4)
    return other, far, lax.rem(other + 2, 4)


def others(axis, index, count):
    return [{axis: lax.rem(index + k, count)} for k in range(1, count)]


def nearest(z, last):
    near = jnp.where(z > 0, last, 1)
    second = jnp.where(z == 0, 2, jnp.where(z == last, last - 1, 1))
    return near, second


def rope(vals, cos, sin, half_dim):
    return vals * cos + pltpu.roll(vals, half_dim, 1) * sin


def causal(scores, tq):
    key_idx = lax.broadcasted_iota(jnp.int32, scores.shape, 0)
    q_idx = lax.rem(lax.broadcasted_iota(jnp.int32, scores.shape, 1), tq)
    return jnp.where(key_idx <= q_idx, scores, NEG_BIG)


def params(cid):
    return pltpu.CompilerParams(collective_id=cid, has_side_effects=True, vmem_limit_bytes=VMEM_BYTES)


def rope_tables(positions, head_dim):
    inv_freq = ROPE_BASE ** (-jnp.arange(0, head_dim, 2).astype(F32) / head_dim)
    angles = positions.astype(F32)[:, None] * inv_freq[None, :]
    cosines, sines = jnp.cos(angles), jnp.sin(angles)
    return jnp.concatenate([cosines, cosines], axis=1), jnp.concatenate([-sines, sines], axis=1)


def front_kernel(group, n_line, hid_ref, gain_ref, w_ref, wo_ref, cos_ref, sin_ref, o_ref, qr_ref, lse_ref, kl_ref, vl_ref, kp_ref, vp_ref, gfull_ref, n_out, w_out, wo_all, o_all, wbuf, nbuf, acc, hbuf, gbuf, qs, vt, m_all, l_all, acc_all, h_sem, g_send, g_recv, own_send, own_recv, x_send, x_recv, y_send, y_recv, d_send, d_recv, kv_send, kv_recv, ox_send, ox_recv, oy_send, oy_recv, od_send, od_recv, zw_send, zw_recv, wx_send, wx_recv, ot_send, ot_recv, out_sem):
    q_len, feat = hid_ref.shape[0], w_ref.shape[0]
    head_dim = cos_ref.shape[1]
    half_dim = head_dim // 2
    kv_width = kl_ref.shape[1]
    kv_heads = kv_width // head_dim
    q_width = qr_ref.shape[1]
    tq = q_len // TILES
    wide = group * tq
    scale = head_dim ** -0.5 * LOG2E
    half = feat // 2
    piece = half // PIECES
    o_rows = wo_ref.shape[0]
    o_half = o_rows // 2
    o_piece = o_half // O_PIECES
    flag, f, z = lax.axis_index("cp"), lax.axis_index("fsdp"), lax.axis_index("tp")
    wo_out = wo_all.at[z]
    last = n_line - 1
    far = 1 - flag
    f_core, f_x, f_diag = fsdp_peers(f)
    to_core, to_x, to_diag, to_y = {"fsdp": f_core}, {"fsdp": f_x}, {"fsdp": f_diag}, {"cp": far}

    def h_load(tile):
        slot = parity(tile)
        return pltpu.make_async_copy(hid_ref.at[blk(tile, tq)], hbuf.at[slot], h_sem.at[slot])

    h_load(0).start()
    h_load(1).start()
    meet([to_core, to_x, to_diag, to_y] + others("tp", z, n_line))

    def span(side, j):
        return blk(side * PIECES + j, piece)

    def x_copy(j):
        return remote(w_ref.at[span(flag, j)], wbuf.at[f, span(flag, j)], x_send.at[j], x_recv.at[j], to_x)

    def x_in(j):
        return remote(w_ref.at[span(flag, j)], wbuf.at[f_x, span(flag, j)], x_send.at[j], x_recv.at[j], to_x)

    def y_copy(j, side):
        return remote(wbuf.at[f_x, span(side, j)], wbuf.at[f_x, span(side, j)], y_send.at[j], y_recv.at[j], to_y)

    def d_copy(j, side, slot):
        return remote(wbuf.at[slot, span(side, j)], wbuf.at[slot, span(side, j)], d_send.at[side, j], d_recv.at[side, j], to_core)

    def g_copy(k, where, slot):
        return remote(gain_ref, gbuf.at[slot], g_send.at[k], g_recv.at[k], where)

    def own_copy(slot):
        return remote(w_ref, wbuf.at[slot], own_send, own_recv, to_core)

    def o_span(side, j):
        return blk(side * O_PIECES + j, o_piece)

    def ox_copy(j, slot):
        return remote(wo_ref.at[o_span(flag, j)], wo_out.at[slot, o_span(flag, j)], ox_send.at[j], ox_recv.at[j], to_x)

    def oy_copy(j, side):
        return remote(wo_out.at[f_x, o_span(side, j)], wo_out.at[f_x, o_span(side, j)], oy_send.at[j], oy_recv.at[j], to_y)

    def od_copy(k, src, slot, where):
        return remote(src, wo_out.at[slot, where], od_send.at[k], od_recv.at[k], to_core)

    def zw_copy(up, t):
        spot = wo_all.at[t, f, blk(flag, o_half)]
        where = jnp.minimum(z + 1, last) if up else jnp.maximum(z - 1, 0)
        src = spot if t is not z else wo_ref.at[blk(flag, o_half)]
        return remote(src, spot, zw_send.at[up, t], zw_recv.at[t], {"tp": where})

    def zw_tick(r):
        for up, t, here in ((0, z + r, z + r <= last), (1, z - r, z >= r)):
            at = jnp.clip(t, 0, last)

            @pl.when(here)
            def _():
                zw_copy(up, at).wait_recv()

            @pl.when(here & (z < last if up else z > 0))
            def _():
                zw_copy(up, at).start()

    def wx_copy(k, r, slot):
        spot = wo_all.at[lax.rem(z + r, n_line), slot, blk(flag, o_half)]
        return remote(spot, spot, wx_send.at[k], wx_recv.at[k], to_x)

    def ot_copy(up, j, owner):
        src = o_ref.at[blk(j, tq)]
        where = jnp.minimum(z + 1, last) if up else jnp.maximum(z - 1, 0)
        return remote(src, o_all.at[owner, blk(j, tq)], ot_send.at[up, j], ot_recv.at[up, j], {"tp": where})

    steps_x = nearest(z, last)
    for up in SIDES:
        @pl.when(z < last if up else z > 0)
        def _():
            zw_copy(up, z).start()

    gains = [(k, where, where["fsdp"]) for k, where in enumerate((to_core, to_x, to_diag))]
    for k, where, _ in gains:
        g_copy(k, where, f).start()
    for j in range(PIECES):
        x_copy(j).start()
    own_copy(f).start()
    for j in range(O_PIECES):
        ox_copy(j, f).start()
    all_rows = pl.ds(0, o_rows)
    od_copy(0, wo_ref, f, all_rows).start()
    local_w = pltpu.make_async_copy(w_ref, wbuf.at[f], out_sem.at[0])
    local_w.start()
    local_o = pltpu.make_async_copy(wo_ref, wo_out.at[f], out_sem.at[1])
    local_o.start()
    gbuf[f] = gain_ref[...]
    for k, where, slot in gains:
        g_copy(k, where, slot).wait_recv()
    for k in range(gbuf.shape[0]):
        gfull_ref[:, blk(k, feat)] = gbuf[k]

    for tile in range(TILES):
        h_load(tile).wait()
        strip = min(32, tq)

        @pl.loop(0, tq // strip)
        def _(i):
            vals = hbuf[tile % 2, blk(i, strip), :].astype(F32)
            inv = lax.rsqrt(lane_mean(vals * vals) + NORM_EPS)
            nbuf[pl.ds(pl.multiple_of(tile * tq + i * strip, strip), strip), :] = (vals * inv * gfull_ref[...]).astype(BF)

        if tile + 2 < TILES:
            h_load(tile + 2).start()
    put_n = pltpu.make_async_copy(nbuf, n_out, out_sem.at[2])
    put_n.start()

    def project(slot, start, rows, first=False):
        cols = pl.ds(pl.multiple_of(slot * feat + start, 128), rows)

        @pl.loop(0, TILES)
        def _(tile):
            here = blk(tile, tq)
            part = dot(nbuf[here, cols], wbuf[slot, pl.ds(start, rows), :], NN)
            acc[here, :] = part if first else acc[here, :] + part

    def x_tick(j):
        x_in(j).wait_recv()
        y_copy(j, flag).start()
        d_copy(j, flag, f_x).start()

    def y_tick(j):
        y_copy(j, far).wait_recv()
        d_copy(j, 1 - flag, f_x).start()

    local_w.wait()
    project(f, 0, feat, first=True)
    x_tick(0)
    own_copy(f_core).wait_recv()
    project(f_core, 0, feat)
    x_tick(1)
    y_tick(0)
    zw_tick(1)
    wx_copy(0, steps_x[0], f).start()
    x_tick(2)
    y_tick(1)
    x_tick(3)
    for j in range(PIECES):
        d_copy(j, flag, f_diag).wait_recv()
    first_half = pl.multiple_of(flag * half, half)
    project(f_x, first_half, half)
    y_tick(2)
    project(f_diag, first_half, half)
    y_tick(3)
    for j in range(PIECES):
        d_copy(j, 1 - flag, f_diag).wait_recv()
    second_half = pl.multiple_of(far * half, half)
    project(f_x, second_half, half)
    project(f_diag, second_half, half)
    zw_tick(2)
    wx_copy(1, steps_x[1], f).start()
    put_w = pltpu.make_async_copy(wbuf, w_out, out_sem.at[3])
    put_w.start()

    @pl.loop(0, TILES)
    def _(tile):
        here = blk(tile, tq)
        cos, sin = cos_ref[here, :], sin_ref[here, :]
        for h in range(kv_heads):
            k_at = q_width // head_dim + h
            kl_ref[here, blk(h, head_dim)] = rope(acc[here, blk(k_at, head_dim)], cos, sin, half_dim).astype(BF)
            vl_ref[here, blk(h, head_dim)] = acc[here, blk(k_at + kv_heads, head_dim)].astype(BF)

    kv_pairs = ((kl_ref, kp_ref), (vl_ref, vp_ref))

    def kv_copy(k):
        return remote(kv_pairs[k][0], kv_pairs[k][1], kv_send.at[k], kv_recv.at[k], {"cp": 1})

    @pl.loop(0, TILES)
    def _(tile):
        here = blk(tile, tq)
        cos, sin = cos_ref[here, :], sin_ref[here, :]
        for h in range(group * kv_heads):
            cols = blk(h, head_dim)
            qr_ref[here, cols] = rope(acc[here, cols], cos, sin, half_dim).astype(BF)

    @pl.when(flag == 0)
    def _():
        zero(kp_ref)
        zero(vp_ref)
        for k in range(len(kv_pairs)):
            kv_copy(k).start()

    def load_q(item):
        g, tile = lax.rem(item, kv_heads), item // kv_heads
        rows = blk(tile, tq)
        for h in range(group):
            qs[:, blk(h, tq)] = qr_ref[rows, blk(g * group + h, head_dim)].T

    def key_piece(item, k_ref, side, start, masked):
        g = lax.rem(item, kv_heads)
        scores = dot(k_ref[start, blk(g, head_dim)], qs[...], NN)
        if masked:
            scores = causal(scores, tq)
        m_old = m_all[item]
        m_new = jnp.maximum(m_old, jnp.max(scores, axis=0, keepdims=True))
        probs = jnp.exp2((scores - m_new) * scale)
        fade = jnp.exp2((m_old - m_new) * scale)
        m_all[item] = m_new
        l_all[item] = l_all[item] * fade + row_sum(probs)
        acc_all[item] = acc_all[item] * fade + dot(vt[g, side, :, start], probs.astype(BF), NN)

    for g in range(kv_heads):
        vt[g, 0] = vl_ref[:, blk(g, head_dim)].T

    @pl.loop(0, kv_heads * TILES)
    def _(item):
        tile = item // kv_heads
        load_q(item)
        m_all[item] = jnp.full_like(m_all[item], NEG_BIG)
        l_all[item] = jnp.zeros_like(l_all[item])
        acc_all[item] = jnp.zeros_like(acc_all[item])
        key_piece(item, kl_ref, 0, blk(tile, tq), True)

        @pl.loop(0, tile // 2)
        def _(i):
            key_piece(item, kl_ref, 0, blk(i, 2 * tq), False)

        @pl.when(parity(tile) == 1)
        def _():
            key_piece(item, kl_ref, 0, blk(tile - 1, tq), False)

    for j in range(O_PIECES):
        ox_copy(j, f_x).wait_recv()
        oy_copy(j, flag).start()
        od_copy(1 + j, wo_out.at[f_x, o_span(flag, j)], f_x, o_span(flag, j)).start()

    @pl.when(flag == 1)
    def _():
        for k in range(len(kv_pairs)):
            kv_copy(k).wait_recv()
        for g in range(kv_heads):
            vt[g, 1] = vp_ref[:, blk(g, head_dim)].T

    @pl.loop(0, kv_heads * TILES)
    def _(item):
        g, tile = lax.rem(item, kv_heads), item // kv_heads
        rows = blk(tile, tq)

        @pl.when(flag == 1)
        def _():
            load_q(item)

        @pl.loop(0, flag * TILES // 2)
        def _(i):
            key_piece(item, kp_ref, 1, blk(i, 2 * tq), False)

        total = l_all[item]
        lse_ref[g * TILES + tile] = m_all[item] * scale + jnp.log2(total)
        out_t = acc_all[item] / total
        for h in range(group):
            o_ref[rows, blk(g * group + h, head_dim)] = out_t[:, h * tq:h * tq + tq].T.astype(BF)

        for j in range(O_EARLY):
            @pl.when((item == (j + 1) * kv_heads) & (z > 0))
            def _():
                ot_copy(0, j, z).start()

            @pl.when((item == (j + 1) * kv_heads) & (z < last))
            def _():
                ot_copy(1, j, z).start()

        for j in range(O_PIECES):
            @pl.when(item == (j + 1) * kv_heads * TILES // O_PIECES - 1)
            def _():
                oy_copy(j, far).wait_recv()
                od_copy(1 + O_PIECES + j, wo_out.at[f_x, o_span(1 - flag, j)], f_x, o_span(1 - flag, j)).start()

    od_copy(0, wo_ref, f_core, all_rows).wait_recv()
    for j in range(O_PIECES):
        od_copy(1 + j, wo_out.at[f_x, o_span(flag, j)], f_diag, o_span(flag, j)).wait_recv()
        od_copy(1 + O_PIECES + j, wo_out.at[f_x, o_span(1 - flag, j)], f_diag, o_span(1 - flag, j)).wait_recv()

    for r in range(3, n_line):
        zw_tick(r)

    @pl.loop(0, n_line)
    def _(t):
        for up in SIDES:
            @pl.when((t <= z) & (z < last) if up else (t >= z) & (z > 0))
            def _():
                zw_copy(up, t).wait_send()

    for k, r in enumerate(steps_x):
        wx_copy(k, r, f_x).wait_recv()
        wx_copy(k, r, f).wait_send()
    for j in range(O_EARLY):
        for up in SIDES:
            @pl.when(z < last if up else z > 0)
            def _():
                ot_copy(up, j, z).wait_send()
                ot_copy(1 - up, j, z + 1 if up else z - 1).wait_recv()

    for k, where, _ in gains:
        g_copy(k, where, f).wait_send()
    own_copy(f).wait_send()
    od_copy(0, wo_ref, f, all_rows).wait_send()
    for j in range(PIECES):
        x_copy(j).wait_send()
        y_copy(j, flag).wait_send()
        d_copy(j, flag, f_x).wait_send()
        d_copy(j, 1 - flag, f_x).wait_send()
    for j in range(O_PIECES):
        ox_copy(j, f).wait_send()
        oy_copy(j, flag).wait_send()
        od_copy(1 + j, wo_out.at[f_x, o_span(flag, j)], f_x, o_span(flag, j)).wait_send()
        od_copy(1 + O_PIECES + j, wo_out.at[f_x, o_span(1 - flag, j)], f_x, o_span(1 - flag, j)).wait_send()

    @pl.when(flag == 0)
    def _():
        for k in range(len(kv_pairs)):
            kv_copy(k).wait_send()

    for local in (local_o, put_n, put_w):
        local.wait()


def front(hidden, gain, w_qkv, w_out, cosines, sines, group, kv_width, n_line, cid):
    q_len, model_dim = hidden.shape
    feat, width = w_qkv.shape
    head_dim = cosines.shape[1]
    q_width = width - 2 * kv_width
    kv_heads = kv_width // head_dim
    o_rows, o_cols = w_out.shape
    n_fsdp = model_dim // feat
    tq = q_len // TILES
    wide = group * tq
    items = kv_heads * TILES
    sds = jax.ShapeDtypeStruct
    kv = sds((q_len, kv_width), BF)
    q_like = sds((q_len, q_width), BF)
    line = pltpu.VMEM((items, 1, wide), F32)
    own, pair, trio = DMA(()), DMA((2,)), DMA((n_fsdp - 1,))
    early = DMA((2, O_EARLY))
    w_link, w_side, o_link, o_core = DMA((PIECES,)), DMA((2, PIECES)), DMA((O_PIECES,)), DMA((1 + 2 * O_PIECES,))
    return pl.pallas_call(
        functools.partial(front_kernel, group, n_line),
        in_specs=[ANY] + [VMEM] * 5,
        out_specs=[VMEM] * 8 + [ANY] * 4,
        out_shape=[q_like, q_like, sds((items, 1, wide), F32), kv, kv, kv, kv, sds((1, model_dim), F32), sds((q_len, model_dim), BF), sds((n_fsdp, feat, width), BF), sds((n_line, n_fsdp, o_rows, o_cols), BF), sds((n_line, q_len, q_width), BF)],
        scratch_shapes=[
            pltpu.VMEM((n_fsdp, feat, width), BF),
            pltpu.VMEM((q_len, model_dim), BF),
            pltpu.VMEM((q_len, width), F32),
            pltpu.VMEM((2, tq, model_dim), BF),
            pltpu.VMEM((n_fsdp, 1, feat), F32),
            pltpu.VMEM((head_dim, wide), BF),
            pltpu.VMEM((kv_heads, 2, head_dim, q_len), BF),
            line,
            line,
            pltpu.VMEM((items, head_dim, wide), F32),
        ] + [pair, trio, trio, own, own, w_link, w_link, w_link, w_link, w_side, w_side, pair, pair, o_link, o_link, o_link, o_link, o_core, o_core, DMA((2, n_line)), DMA((n_line,)), pair, pair, early, early, DMA((4,))],
        compiler_params=params(cid),
        name="front",
    )(hidden, gain, w_qkv, w_out, cosines, sines)


def back_kernel(n_line, group, o_ref, q_ref, lse_ref, cos_ref, sin_ref, kl_ref, vl_ref, kp_ref, vp_ref, _wo_in, _o_in, ct_ref, d_ref, o_all, wo_all, w_ref, ctb_ref, do_ref, dkl_ref, dvl_ref, dkp_ref, dvp_ref, qs_ref, dos_ref, delta_ref, kt_ref, dqt_ref, load_sem, keep_sem, ct_sem, od_send, ou_send, o_recv, y_send, y_recv, x_send, x_recv, c_send, c_recv, cx_send, cx_recv, kv_send, kv_recv):
    last = n_line - 1
    z, flag, f = lax.axis_index("tp"), lax.axis_index("cp"), lax.axis_index("fsdp")
    far = 1 - flag
    f_core, f_x, f_diag = fsdp_peers(f)
    q_len, width = o_ref.shape
    head_dim = cos_ref.shape[1]
    half_dim = head_dim // 2
    kv_width = kl_ref.shape[1]
    kv_heads = kv_width // head_dim
    tq = q_len // TILES
    wide = group * tq
    score_scale = head_dim ** -0.5
    n_parts, o_rows, part = w_ref.shape
    o_half = o_rows // 2
    load = pltpu.make_async_copy(wo_all.at[z], w_ref, load_sem)
    load.start()
    keep = pltpu.make_async_copy(o_ref, o_all.at[z], keep_sem)
    keep.start()

    def ct_load(tile):
        slot = parity(tile)
        return pltpu.make_async_copy(ct_ref.at[blk(tile, tq)], ctb_ref.at[slot], ct_sem.at[slot])

    ct_load(0).start()
    ct_load(1).start()

    to_core, to_x, to_y = {"fsdp": f_core}, {"fsdp": f_x}, {"cp": far}
    meet([to_core, to_x, to_y] + others("tp", z, n_line))

    def tile_rows(j):
        return blk(j, tq)

    def o_down(t, j, src):
        return remote(src, o_all.at[t, tile_rows(j)], od_send.at[t, j], o_recv.at[t, j], {"tp": jnp.maximum(z - 1, 0)})

    def o_up(t, j, src):
        return remote(src, o_all.at[t, tile_rows(j)], ou_send.at[t, j], o_recv.at[t, j], {"tp": jnp.minimum(z + 1, last)})

    def wo_half(r, slot, side):
        return wo_all.at[lax.rem(z + r, n_line), slot, blk(side, o_half)]

    def y_copy(r, side):
        return remote(wo_half(r, f, side), wo_half(r, f, side), y_send.at[r - 1], y_recv.at[r - 1], to_y)

    def x_copy(r, side, slot):
        return remote(wo_half(r, slot, side), wo_half(r, slot, side), x_send.at[side, r - 1], x_recv.at[side, r - 1], to_x)

    def c_copy(r, side, slot):
        return remote(wo_half(r, slot, side), wo_half(r, slot, side), c_send.at[side, r - 1], c_recv.at[side, r - 1], to_core)

    def cx_copy(r, side, slot):
        return remote(wo_half(r, slot, side), wo_half(r, slot, side), cx_send.at[side, r - 1], cx_recv.at[side, r - 1], to_core)

    for j in range(O_EARLY, TILES):
        @pl.when(z > 0)
        def _():
            o_down(z, j, o_ref.at[tile_rows(j)]).start()

        @pl.when(z < last)
        def _():
            o_up(z, j, o_ref.at[tile_rows(j)]).start()

    for j in range(O_EARLY):
        @pl.when((z > 0) & (z < last))
        def _():
            o_down(z + 1, j, o_all.at[z + 1, tile_rows(j)]).start()
            o_up(z - 1, j, o_all.at[z - 1, tile_rows(j)]).start()

    steps_x = nearest(z, last)
    third = n_line * last // 2 - sum(steps_x)
    x_copy(third, flag, f).start()
    for r in steps_x:
        cx_copy(r, flag, f_x).start()
    for r in range(1, n_line):
        y_copy(r, flag).start()
        c_copy(r, flag, f).start()

    def o_tick(k):
        r, j = k // TILES + 1, lax.rem(k, TILES)

        @pl.when(z + r <= last)
        def _():
            t = jnp.minimum(z + r, last)
            o_down(t, j, o_all.at[t, tile_rows(j)]).wait_recv()

            @pl.when(z > 0)
            def _():
                o_down(t, j, o_all.at[t, tile_rows(j)]).start()

        @pl.when(z - r >= 0)
        def _():
            t = jnp.maximum(z - r, 0)
            o_up(t, j, o_all.at[t, tile_rows(j)]).wait_recv()

            @pl.when(z < last)
            def _():
                o_up(t, j, o_all.at[t, tile_rows(j)]).start()

    def y_tick(r):
        y_copy(r, far).wait_recv()
        x_copy(r, far, f).start()
        c_copy(r, far, f).start()

    def x_tick(q):
        r, side = (q, far) if q else (third, flag)
        x_copy(r, side, f_x).wait_recv()
        cx_copy(r, side, f_x).start()

    zero(dkl_ref)
    zero(dvl_ref)

    @pl.when(flag == 1)
    def _():
        zero(dkp_ref)
        zero(dvp_ref)

    load.wait()

    def do_tile(tile):
        ct_load(tile).wait()
        slot = parity(tile)
        total = sum(dot(ctb_ref[slot, :, blk(k, part)], w_ref[k], NT) for k in range(n_parts))
        do_ref[tile_rows(tile), :] = total.astype(BF)

        @pl.when(tile + 2 < TILES)
        def _():
            ct_load(tile + 2).start()

    def bwd_item(item):
        g, tile = item // TILES, lax.rem(item, TILES)
        kv_cols = blk(g, head_dim)
        rows = blk(tile, tq)

        @pl.when(tile == 0)
        def _():
            kt_ref[0] = kl_ref[:, kv_cols].T
            kt_ref[1] = kp_ref[:, kv_cols].T

        for h in range(group):
            cols = blk(g * group + h, head_dim)
            stack = blk(h, tq)
            qs_ref[stack, :] = q_ref[rows, cols]
            d_h = do_ref[rows, cols]
            dos_ref[stack, :] = d_h
            prod = d_h.astype(F32) * o_ref[rows, cols].astype(F32)
            delta_ref[:, stack] = row_sum(prod.T)
        zero(dqt_ref)

        def piece(k_ref, v_ref, dk_ref, dv_ref, side, span, masked):
            scores = dot(k_ref[span, kv_cols], qs_ref[...], NT)
            if masked:
                scores = causal(scores, tq)
            probs = jnp.exp2(scores * (score_scale * LOG2E) - lse_ref[item])
            d_probs = dot(v_ref[span, kv_cols], dos_ref[...], NT)
            d_scores = (probs * (d_probs - delta_ref[...])).astype(BF)
            dv_ref[g, span, :] += dot(probs.astype(BF), dos_ref[...], NN)
            dk_ref[g, span, :] += dot(d_scores, qs_ref[...], NN)
            dqt_ref[...] += dot(kt_ref[side, :, span], d_scores, NN)

        piece(kl_ref, vl_ref, dkl_ref, dvl_ref, 0, blk(tile, tq), True)

        @pl.loop(0, tile // 2)
        def _(i):
            piece(kl_ref, vl_ref, dkl_ref, dvl_ref, 0, blk(i, 2 * tq), False)

        @pl.when(parity(tile) == 1)
        def _():
            piece(kl_ref, vl_ref, dkl_ref, dvl_ref, 0, blk(tile - 1, tq), False)

        @pl.loop(0, flag * TILES // 2)
        def _(i):
            piece(kp_ref, vp_ref, dkp_ref, dvp_ref, 1, blk(i, 2 * tq), False)

        for h in range(group):
            dq_h = dqt_ref[:, blk(h, tq)].T * score_scale
            d_ref[rows, blk(g * group + h, head_dim)] = rope(dq_h, cos_ref[rows, :], -sin_ref[rows, :], half_dim).astype(BF)

        @pl.when((tile == TILES - 1) & (flag == 1))
        def _():
            for copy in back(g):
                copy.start()

    def back(g):
        return [remote(ref.at[g], ref.at[g], kv_send.at[k, g], kv_recv.at[k, g], {"cp": 0}) for k, ref in enumerate((dkp_ref, dvp_ref))]

    def kv_done(g):
        @pl.when(flag == 0)
        def _():
            for copy in back(g):
                copy.wait_recv()
            dkl_ref[g] += dkp_ref[g]
            dvl_ref[g] += dvp_ref[g]

        dk = rope(dkl_ref[g] * score_scale, cos_ref[...], -sin_ref[...], half_dim)
        k_at = width // head_dim + g
        d_ref[:, blk(k_at, head_dim)] = dk.astype(BF)
        d_ref[:, blk(k_at + kv_heads, head_dim)] = dvl_ref[g].astype(BF)

        @pl.when(flag == 1)
        def _():
            for copy in back(g):
                copy.wait_send()

    items = TILES * (kv_heads + 1)
    o_ticks = TILES * last
    x_at = {5: 0, 8: 1, 11: 2}

    @pl.loop(0, items)
    def _(item):
        @pl.when(item < TILES)
        def _():
            do_tile(item)

        @pl.when(item >= TILES)
        def _():
            bwd_item(item - TILES)

        @pl.when((parity(item) == 1) & (item > 1))
        def _():
            o_tick(item // 2 - 1 + O_EARLY)

        for r in range(1, n_line):
            @pl.when(item == 3 * r + 1)
            def _():
                y_tick(r)

        for at, q in x_at.items():
            @pl.when(item == at)
            def _():
                x_tick(q)

    done = items // 2 - 1 + O_EARLY
    tail = [("x", q) for q in range(len(x_at), n_line)] + [("kv", g) for g in range(kv_heads)]
    for k in range(done, o_ticks):
        o_tick(jnp.int32(k))
        if (k - done) % 2 == 1 and tail:
            kind, arg = tail.pop(0)
            x_tick(arg) if kind == "x" else kv_done(arg)
            later = [t for t in tail if t[0] == "kv"]
            if later:
                tail.remove(later[0])
                kv_done(later[0][1])
    for kind, arg in tail:
        x_tick(arg) if kind == "x" else kv_done(arg)

    for r in range(1, n_line):
        for side in (flag, far):
            c_copy(r, side, f_core).wait_recv()
            cx_copy(r, side, f_diag).wait_recv()
            c_copy(r, side, f).wait_send()
            cx_copy(r, side, f_x).wait_send()
        x_copy(r, far, f).wait_send()
        y_copy(r, flag).wait_send()
    x_copy(third, flag, f).wait_send()

    @pl.loop(0, n_line)
    def _(t):
        @pl.when((t >= z) & (z > 0))
        def _():
            @pl.loop(jnp.where(t == z, O_EARLY, 0), TILES)
            def _(j):
                o_down(t, j, o_all.at[t, tile_rows(j)]).wait_send()

        @pl.when((t <= z) & (z < last))
        def _():
            @pl.loop(jnp.where(t == z, O_EARLY, 0), TILES)
            def _(j):
                o_up(t, j, o_all.at[t, tile_rows(j)]).wait_send()

    keep.wait()


def attn_back(attn_out, q_rot, lse, cosines, sines, k_loc, v_loc, k_prev, v_prev, wo_all, o_all, cotangent, n_line, group, cid):
    q_len, width = attn_out.shape
    head_dim = cosines.shape[1]
    kv_width = k_loc.shape[1]
    kv_heads = kv_width // head_dim
    _, n_fsdp, o_rows, o_cols = wo_all.shape
    tq = q_len // TILES
    wide = group * tq
    acc = pltpu.VMEM((kv_heads, q_len, head_dim), F32)
    stack = pltpu.VMEM((wide, head_dim), BF)
    own, pair, tiles, hop, side, kv = DMA(()), DMA((2,)), DMA((n_line, TILES)), DMA((n_line - 1,)), DMA((2, n_line - 1)), DMA((2, kv_heads))
    return pl.pallas_call(
        functools.partial(back_kernel, n_line, group),
        in_specs=[VMEM] * 9 + [ANY] * 3,
        out_specs=[VMEM, ANY, ANY],
        out_shape=[jax.ShapeDtypeStruct((q_len, width + 2 * kv_width), BF), jax.ShapeDtypeStruct((n_line, q_len, width), BF), jax.ShapeDtypeStruct(wo_all.shape, BF)],
        input_output_aliases={9: 2, 10: 1},
        scratch_shapes=[
            pltpu.VMEM((n_fsdp, o_rows, o_cols), BF),
            pltpu.VMEM((2, tq, cotangent.shape[1]), BF),
            pltpu.VMEM((q_len, width), BF),
            acc, acc, acc, acc,
            stack,
            stack,
            pltpu.VMEM((1, wide), F32),
            pltpu.VMEM((2, head_dim, q_len), BF),
            pltpu.VMEM((head_dim, wide), F32),
        ] + [own, own, pair, tiles, tiles, tiles, hop, hop, side, side, side, side, side, side, kv, kv],
        compiler_params=params(cid),
        name="attn_back",
    )(attn_out, q_rot, lse, cosines, sines, k_loc, v_loc, k_prev, v_prev, wo_all, o_all, cotangent)


class Line:
    def __init__(self, n_line, buf_ref, pbuf_ref, send_sem, recv_sem, fill, finish):
        self.last = n_line - 1
        self.z = lax.axis_index("tp")
        self.buf, self.pbuf, self.send_sem, self.recv_sem = buf_ref, pbuf_ref, send_sem, recv_sem
        self.chunks, self.rows = buf_ref.shape[1], buf_ref.shape[2]
        self.block = pbuf_ref.shape[1]
        self.per_block = self.block // self.rows
        self.fill, self.finish = fill, finish
        self.steps = self.chunks + self.last

    def dist(self, side):
        return self.z if side else self.last - self.z

    def toward(self, side, back=False):
        up = bool(side) != back
        return {"tp": jnp.clip(self.z + 1 if up else self.z - 1, 0, self.last)}

    def copy(self, side, chunk):
        spot = self.buf.at[side, chunk]
        return remote(spot, spot, self.send_sem.at[side, chunk], self.recv_sem.at[side, chunk], self.toward(side))

    def live(self, side, step):
        chunk = step - self.dist(side)
        return chunk, (chunk >= 0) & (chunk < self.chunks)

    def prepare(self, step):
        for side in SIDES:
            chunk, ok = self.live(side, step)

            @pl.when(ok & (lax.rem(chunk, self.per_block) == 0))
            def _():
                self.fill(self.pbuf.at[side], blk((side * self.chunks + chunk) // self.per_block, self.block))

    def tick(self, step):
        for side in SIDES:
            chunk, ok = self.live(side, step)
            dist = self.dist(side)
            part = blk(lax.rem(jnp.maximum(chunk, 0), self.per_block), self.rows)

            @pl.when(ok & (dist == 0))
            def _():
                self.buf[side, chunk] = self.pbuf[side, part, :]

            @pl.when(ok & (dist > 0))
            def _():
                self.copy(side, chunk).wait_recv()
                self.buf[side, chunk] += self.pbuf[side, part, :]

            @pl.when(ok & (dist < self.last))
            def _():
                self.copy(side, chunk).start()

            @pl.when(ok & (dist == self.last))
            def _():
                self.finish(chunk, self.buf[side, chunk])

        self.prepare(step + 1)

    def drain(self):
        for side in SIDES:
            @pl.when(self.dist(side) < self.last)
            def _():
                @pl.loop(0, self.chunks)
                def _(chunk):
                    self.copy(side, chunk).wait_send()


def close_kernel(n_line, n_fsdp, d_ref, o_ref, gain_ref, hid_ref, ct_ref, n_ref, w_all, o_all, wo_all, out_ref, blk_ref, gg_ref, ts, yr, dl, xs, ks, xr, buf, gp, ga, gs, gb, gt, gc, ebuf, fb_in, fb_ct, fb_out, send_sem, recv_sem, w_sem, f_sem, ct_sem, fo_sem, lhs_sem, a_send, a_recv, ld_sem, st_sem, x_send, x_recv, e_sem, es_sem, y_send, y_recv, out_send, out_recv, o_sem, wl_sem, h_sem, r_sem, ga_send, ga_recv, gb_send, gb_recv, gc_send, gc_recv):
    last = n_line - 1
    z, flag, f = lax.axis_index("tp"), lax.axis_index("cp"), lax.axis_index("fsdp")
    far = 1 - flag
    f_core, f_x, f_diag = fsdp_peers(f)
    to_core, to_x, to_y = {"fsdp": f_core}, {"fsdp": f_x}, {"cp": far}
    _, feat, width = w_all.shape
    chunks, rows = buf.shape[1], buf.shape[2]
    half = chunks * rows
    g_rows = feat // GRAD_CHUNKS
    owner = (z == 0) | (z == last)
    own_base = jnp.where(z == last, chunks, 0)
    copy = pltpu.make_async_copy

    def own_span(chunk):
        return blk(own_base + chunk, rows)

    def f_loads(chunk):
        slot = parity(chunk)
        return copy(hid_ref.at[own_span(chunk)], fb_in.at[slot], f_sem.at[slot]), copy(ct_ref.at[own_span(chunk)], fb_ct.at[slot], ct_sem.at[slot])

    def f_store(chunk):
        slot = parity(chunk)
        return copy(fb_out.at[slot], out_ref.at[own_span(chunk)], fo_sem.at[slot])

    @pl.when(owner)
    def _():
        for chunk in SIDES:
            for load in f_loads(chunk):
                load.start()

    zero(gp)
    meet([to_core, to_x, to_y] + others("tp", z, n_line) + [{"fsdp": f_diag}])

    def finish(chunk, total):
        slot = parity(chunk)
        for load in f_loads(chunk):
            load.wait()

        @pl.when(chunk > 1)
        def _():
            f_store(chunk - 2).wait()

        x_in = fb_in[slot].astype(F32)
        inv = lax.rsqrt(lane_mean(x_in * x_in) + NORM_EPS)
        x_hat = x_in * inv
        gp[...] += row_sum(total * x_hat)
        scaled = total * gain_ref[...]
        fb_out[slot] = (fb_ct[slot].astype(F32) + inv * (scaled - x_hat * lane_mean(scaled * x_hat))).astype(BF)
        f_store(chunk).start()

        @pl.when(chunk + 2 < chunks)
        def _():
            for load in f_loads(chunk + 2):
                load.start()

    kinds = range(2)

    def g_at(ref, j):
        return ref.at[blk(j, g_rows)]

    def x_copy(j):
        return remote(g_at(xs, j), g_at(xr, j), x_send.at[j], x_recv.at[j], to_x)

    def y_copy(j):
        return remote(g_at(ts, j), g_at(yr, j), y_send.at[j], y_recv.at[j], to_y)

    def e_store(j):
        return copy(ebuf.at[0], g_at(ts, j), es_sem)

    def meet_x(j):
        x_copy(j).wait_recv()
        loads = [copy(g_at(src, j), ebuf.at[k], e_sem.at[k]) for k, src in enumerate((ks, xr))]
        for load in loads:
            load.start()
        for load in loads:
            load.wait()
        ebuf[0] += ebuf[1]
        e_store(j).start()

    def send_y(j):
        e_store(j).wait()
        y_copy(j).start()

    steps = chunks + last - 1

    def dist(side):
        return z if side else last - z

    def hop(side, chunk):
        span = blk(side * chunks + chunk, rows)
        up = z - 1 if side else z + 1
        return remote(out_ref.at[span], out_ref.at[span], out_send.at[side, chunk], out_recv.at[side, chunk], {"tp": jnp.clip(up, 0, last)})

    ends = [(end, z == (last if end else 0)) for end in SIDES]

    def owner_send(first, stop):
        for end, here in ends:
            @pl.when(here)
            def _():
                @pl.loop(first, stop)
                def _(c):
                    hop(end, c).start()

    def pass_on(step):
        for side in SIDES:
            chunk = step - (last - 1 - dist(side))

            @pl.when((dist(side) < last) & (chunk >= 0) & (chunk < chunks))
            def _():
                hop(side, chunk).wait_recv()

                @pl.when(dist(side) > 0)
                def _():
                    hop(side, chunk).start()

    def sum_phase(wbuf, pbuf, abuf, bbuf, lbuf, lhs):
        w_load = copy(w_all, wbuf, w_sem)
        w_load.start()

        def fill(dst, span):
            for k in range(n_fsdp):
                dst[:, blk(k, feat)] = dot(d_ref[span, :], wbuf[k], NT)

        line = Line(n_line, buf, pbuf, send_sem, recv_sem, fill, finish)
        slots = (f_diag, f_core, f_x, f)

        def lhs_loads(j):
            return [copy(src.at[:, blk(slot * GRAD_CHUNKS + j, g_rows)], lhs.at[m, k], lhs_sem.at[m, k]) for m, src in enumerate((n_ref, ct_ref)) for k, slot in enumerate(slots)]

        def a_copy(kind, j):
            return remote(abuf.at[kind], dl.at[kind, blk(j, g_rows)], a_send.at[kind], a_recv.at[kind, j], to_core)

        def b_stores(j):
            return [copy(bbuf.at[k], g_at(dst, j), st_sem.at[k]) for k, dst in enumerate((xs, ks))]

        def send_x(j):
            for kind in kinds:
                a_copy(kind, j).wait_send()
            for store in b_stores(j):
                store.wait()
            x_copy(j).start()

        def make(j):
            for load in lhs_loads(j):
                load.wait()
            for k in range(len(slots)):
                dst = (abuf, bbuf)[k // 2].at[k % 2]
                dst[:, :width] = dot(lhs[0, k], d_ref[...], TN)
                dst[:, width:] = dot(lhs[1, k], o_ref[...], TN)
            for kind in kinds:
                a_copy(kind, j).start()

            @pl.when(j + 1 < GRAD_CHUNKS)
            def _():
                for load in lhs_loads(j + 1):
                    load.start()

        def meet_core(j):
            loads = [copy(dl.at[kind, blk(j, g_rows)], lbuf.at[kind], ld_sem.at[kind]) for kind in kinds]
            for kind in kinds:
                a_copy(kind, j).wait_recv()
                loads[kind].start()
            for kind in kinds:
                loads[kind].wait()
                bbuf[kind] += lbuf[kind]
            for store in b_stores(j):
                store.start()

        for load in lhs_loads(0):
            load.start()
        w_load.wait()
        line.prepare(0)

        @pl.loop(0, line.steps)
        def _(fine):
            line.tick(fine)
            step = fine // PER_STEP
            whole = lax.rem(fine, PER_STEP) == 0
            j, odd = step // 2, parity(step)

            @pl.when(whole & (odd == 0) & (j > 0) & (j <= GRAD_CHUNKS))
            def _():
                send_x(j - 1)

            @pl.when(whole & (odd == 0) & (j < GRAD_CHUNKS))
            def _():
                make(j)

            @pl.when(whole & (odd == 1) & (j < GRAD_CHUNKS))
            def _():
                meet_core(j)

            for late in SIDES:
                k = (step - FIRST_X - late) * 2 // 5

                @pl.when(whole & (k >= 0) & (k < EARLY) & (step - late == FIRST_X + (5 * k + 1) // 2))
                def _():
                    send_y(k) if late else meet_x(k)

            @pl.when(fine >= chunks)
            def _():
                ready = fine - last - 1
                owner_send(jnp.where(fine == chunks, 0, ready - 1), ready)

            @pl.when(fine > chunks)
            def _():
                for k in range(PER_STEP):
                    pass_on((fine - chunks - 1) * PER_STEP + k)

        @pl.when(owner)
        def _():
            for chunk in range(chunks - 2, chunks):
                f_store(chunk).wait()

        owner_send(chunks - 2, chunks)
        line.drain()

    pl.run_scoped(
        sum_phase,
        pltpu.VMEM(w_all.shape, BF),
        pltpu.VMEM((2, min(128, half), buf.shape[3]), F32),
        pltpu.VMEM((2, g_rows, ts.shape[1]), F32),
        pltpu.VMEM((2, g_rows, ts.shape[1]), F32),
        pltpu.VMEM((2, g_rows, ts.shape[1]), F32),
        pltpu.VMEM((2, n_fsdp, d_ref.shape[0], g_rows), BF),
    )
    def ga_copy(end, k):
        return remote(gp, ga.at[end], ga_send.at[k], ga_recv.at[end], {"tp": k if end else 1 + k})

    def gb_copy():
        return remote(gs, gb, gb_send, gb_recv, to_y)

    def gc_copy(k, slot):
        to = lax.rem(f + k, n_fsdp)
        return remote(gt.at[to], gc.at[slot], gc_send.at[k - 1], gc_recv.at[k - 1], {"fsdp": to})

    def spread_phase(obuf, wbuf, hbuf, rbuf):
        o_load = copy(o_all, obuf, o_sem)
        o_load.start()
        q_len, n_cols = hbuf.shape[1], hbuf.shape[2]
        per_part = wo_all.shape[3] // n_cols
        items = per_part * n_fsdp

        def item_loads(item):
            slot = parity(item)
            return copy(wo_all.at[:, item // per_part, :, blk(lax.rem(item, per_part), n_cols)], wbuf.at[slot], wl_sem.at[slot]), copy(hid_ref.at[:, blk(item, n_cols)], hbuf.at[slot], h_sem.at[slot])

        def item_store(item):
            slot = parity(item)
            return copy(rbuf.at[slot], blk_ref.at[:, blk(item, n_cols)], r_sem.at[slot])

        for item in SIDES:
            for load in item_loads(item):
                load.start()

        for end, here in ends:
            @pl.when(here)
            def _():
                ga[end] = gp[...]
                for k in range(last):
                    ga_copy(end, k).start()


        def project(item):
            slot = parity(item)
            for load in item_loads(item):
                load.wait()

            @pl.when(item > 1)
            def _():
                item_store(item - 2).wait()

            @pl.loop(0, TILES)
            def _(tile):
                span = blk(tile, q_len // TILES)
                total = sum(dot(obuf[t, span, :], wbuf[slot, t], NN) for t in range(n_line))
                rbuf[slot, span, :] = (hbuf[slot, span, :].astype(F32) + total).astype(BF)

            item_store(item).start()

            @pl.when(item + 2 < items)
            def _():
                for load in item_loads(item + 2):
                    load.start()

        for end, here in ends:
            @pl.when(jnp.logical_not(here))
            def _():
                ga_copy(end, 0).wait_recv()
        gs[...] = ga[0] + ga[1]
        o_load.wait()
        gb_copy().start()

        early = (last - 1) * PER_STEP

        @pl.loop(0, steps - early)
        def _(step):
            pass_on(step + early)

            @pl.when((parity(step) == 0) & (step // 2 < items))
            def _():
                project(step // 2)

            for k, at in LATE:
                @pl.when(step == at)
                def _():
                    meet_x(k)

            for k, at in ((EARLY - 1, -1),) + LATE:
                @pl.when(step == at + 1)
                def _():
                    send_y(k)

        for item in range(items - 2, items):
            item_store(item).wait()

    pl.run_scoped(
        spread_phase,
        pltpu.VMEM(o_all.shape, BF),
        pltpu.VMEM((2, n_line, wo_all.shape[2], min(512, feat)), BF),
        pltpu.VMEM((2, d_ref.shape[0], min(512, feat)), BF),
        pltpu.VMEM((2, d_ref.shape[0], min(512, feat)), BF),
    )

    gb_copy().wait()
    for k in range(n_fsdp):
        gt[k] = gs[:, blk(k, feat)] + gb[:, blk(k, feat)]
    gc[f] = gt[f]
    for side in SIDES:
        @pl.when(dist(side) > 0)
        def _():
            @pl.loop(0, chunks)
            def _(chunk):
                hop(side, chunk).wait_send()

    @pl.loop(0, GRAD_CHUNKS)
    def _(j):
        x_copy(j).wait_send()

    for k in range(1, n_fsdp):
        gc_copy(k, f).start()
    for k in range(1, n_fsdp):
        gc_copy(k, lax.rem(f + n_fsdp - k, n_fsdp)).wait_recv()
    gg_ref[...] = sum(gc[k] for k in range(n_fsdp))
    for k in range(1, n_fsdp):
        gc_copy(k, f).wait_send()
    for end, here in ends:
        @pl.when(here)
        def _():
            for k in range(last):
                ga_copy(end, k).wait_send()

    @pl.loop(0, GRAD_CHUNKS)
    def _(j):
        y_copy(j).wait()


def close(d_lin, attn_out, gain, hidden, cotangent, normed, w_full, o_all, wo_all, cid):
    q_len, model_dim = hidden.shape
    n_line, n_fsdp = wo_all.shape[:2]
    _, feat, width = w_full.shape
    g_width = width + attn_out.shape[1]
    half = q_len // 2
    rows = half // CHUNKS
    sds = jax.ShapeDtypeStruct
    row = pltpu.VMEM((1, model_dim), F32)
    slices = pltpu.VMEM((n_fsdp, 1, feat), F32)
    strip = pltpu.VMEM((2, rows, model_dim), BF)
    own, pair, line, grad, grads = DMA(()), DMA((2,)), DMA((2, CHUNKS)), DMA((GRAD_CHUNKS,)), DMA((2, GRAD_CHUNKS))
    z_trio, f_trio = DMA((n_line - 1,)), DMA((n_fsdp - 1,))
    act, g_part = sds((q_len, model_dim), BF), sds((feat, g_width), F32)
    return pl.pallas_call(
        functools.partial(close_kernel, n_line, n_fsdp),
        in_specs=[VMEM] * 3 + [ANY] * 6,
        out_specs=[ANY, ANY, VMEM] + [ANY] * 6,
        out_shape=[act, act, sds((1, feat), F32), g_part, g_part, sds((2, feat, g_width), F32), g_part, g_part, g_part],
        scratch_shapes=[
            pltpu.VMEM((2, CHUNKS, rows, model_dim), F32),
            row,
            pltpu.VMEM((2, 1, model_dim), F32),
            row,
            row,
            slices,
            slices,
            pltpu.VMEM((2, feat // GRAD_CHUNKS, g_width), F32),
            strip,
            strip,
            strip,
        ] + [line, line, own, pair, pair, pair, DMA((2, n_fsdp)), pair, grads, pair, pair, grad, grad, pair, own, grad, grad, line, line, own, pair, pair, pair, z_trio, pair, own, own, f_trio, f_trio],
        compiler_params=params(cid),
        name="close",
    )(d_lin, attn_out, gain, hidden, cotangent, normed, w_full, o_all, wo_all)


def tail_kernel(head_dim, blk_ref, hid_ref, mine_ref, theirs_ref, blk_out, hid_out, q_out, k_out, v_out, o_out):
    blk_out[...] = blk_ref[...]
    hid_out[...] = hid_ref[...]
    at = 0
    for ref in (q_out, k_out, v_out):
        for h in range(ref.shape[1]):
            cols = blk(at, head_dim)
            ref[:, h, :] = mine_ref[:, cols] + theirs_ref[:, cols]
            at += 1
    rest = slice(at * head_dim, None)
    o_out[...] = (mine_ref[:, rest] + theirs_ref[:, rest]).T


def tail(block_out, grad_hidden, mine, theirs, q_heads, kv_heads, head_dim):
    q_len, model_dim = block_out.shape
    feat = mine.shape[0]
    sds = jax.ShapeDtypeStruct
    act = pl.BlockSpec((q_len // GRAD_CHUNKS, model_dim), lambda i: (i, 0))
    part = pl.BlockSpec((feat // GRAD_CHUNKS, mine.shape[1]), lambda i: (i, 0))

    def heads(n):
        return pl.BlockSpec((feat // GRAD_CHUNKS, n, head_dim), lambda i: (i, 0, 0))

    def like(n):
        return sds((feat, n, head_dim), F32)

    o_rows = q_heads * head_dim
    return pl.pallas_call(
        functools.partial(tail_kernel, head_dim),
        grid=(GRAD_CHUNKS,),
        in_specs=[act, act, part, part],
        out_specs=[act, act, heads(q_heads), heads(kv_heads), heads(kv_heads), pl.BlockSpec((o_rows, feat // GRAD_CHUNKS), lambda i: (0, i))],
        out_shape=[sds(block_out.shape, BF), sds(block_out.shape, BF), like(q_heads), like(kv_heads), like(kv_heads), sds((o_rows, feat), F32)],
        compiler_params=pltpu.CompilerParams(vmem_limit_bytes=VMEM_BYTES),
        name="tail",
    )(block_out, grad_hidden, mine, theirs)


def solution(mesh):
    act_spec = P("fsdp", "cp", None)
    proj_spec = P("fsdp", "tp", None)
    wout_spec = P("tp", None, "fsdp")
    n_line = mesh.shape["tp"]

    def device_step(hidden, cotangent, positions, gain, w_query, w_key, w_value, w_out):
        hidden, cotangent = hidden[0], cotangent[0]
        assert hidden.shape[0] * mesh.shape["cp"] <= WINDOW_LEN
        feat, q_heads, head_dim = w_query.shape
        kv_heads = w_key.shape[1]
        group = q_heads // kv_heads
        q_width, kv_width = q_heads * head_dim, kv_heads * head_dim
        w_qkv = jnp.concatenate([w_query.reshape(feat, q_width), w_key.reshape(feat, kv_width), w_value.reshape(feat, kv_width)], axis=1)
        cosines, sines = rope_tables(positions, head_dim)
        attn_out, q_rot, lse, k_loc, v_loc, k_prev, v_prev, gain_full, normed, w_full, wo_all, o_all = front(hidden, gain.astype(F32)[None], w_qkv, w_out.reshape(q_width, feat), cosines, sines, group, kv_width, n_line, 0)
        d_lin, o_all, wo_all = attn_back(attn_out, q_rot, lse, cosines, sines, k_loc, v_loc, k_prev, v_prev, wo_all, o_all, cotangent, n_line, group, 1)
        grad_hidden, block_out, grad_gain, mine, theirs = close(d_lin, attn_out, gain_full, hidden, cotangent, normed, w_full, o_all, wo_all, 2)[:5]
        block_out, grad_hidden, g_query, g_key, g_value, g_out = tail(block_out, grad_hidden, mine, theirs, q_heads, kv_heads, head_dim)
        return block_out[None], grad_hidden[None], grad_gain[0], g_query, g_key, g_value, g_out.reshape(w_out.shape)

    specs = (act_spec, act_spec, P("fsdp"), proj_spec, proj_spec, proj_spec, wout_spec)
    return jax.shard_map(device_step, mesh=mesh, in_specs=specs[:2] + (P("cp"),) + specs[2:], out_specs=specs, check_vma=False)
```

```python
import functools
import math

import jax
import jax.numpy as jnp
from jax import lax
from jax.experimental import pallas as pl
from jax.experimental.pallas import tpu as pltpu
from jax.sharding import PartitionSpec as P

WINDOW_LEN = 4096
ROPE_BASE = 10000.0
NORM_EPS = 1e-5
NEG_BIG = -1e30
LOG2E = math.log2(math.e)
TILES = 4
CHUNKS = 16
PER_STEP = 1
LEAD = 2
PIECES = 4
O_PIECES = 2
O_EARLY = 2
GRAD_CHUNKS = 8
FIRST_X = 5
EARLY = 6
LATE = ((6, 2), (7, 7))
VMEM_BYTES = 67043328
SIDES = range(2)

MESH = pl.DeviceIdType.MESH
ANY = pl.BlockSpec(memory_space=pl.ANY)
VMEM = pl.BlockSpec(memory_space=pltpu.VMEM)
DMA = pltpu.SemaphoreType.DMA
BF, F32 = jnp.bfloat16, jnp.float32

NT = (((1,), (1,)), ((), ()))
NN = (((1,), (0,)), ((), ()))
TN = (((0,), (0,)), ((), ()))


def dot(a, b, dims):
    return lax.dot_general(a, b, dims, preferred_element_type=F32)


def parity(k):
    return lax.rem(k, 2)


def blk(k, n):
    return pl.ds(k * n if isinstance(k, int) else pl.multiple_of(k * n, n), n)


def lane_mean(vals):
    return jnp.mean(vals, axis=1, keepdims=True)


def row_sum(vals):
    return jnp.sum(vals, axis=0, keepdims=True)


def zero(ref):
    ref[...] = jnp.zeros_like(ref)


def remote(src, dst, send, recv, where):
    return pltpu.make_async_remote_copy(src_ref=src, dst_ref=dst, send_sem=send, recv_sem=recv, device_id=where, device_id_type=MESH)


def meet(peers):
    barrier = pltpu.get_barrier_semaphore()
    for where in peers:
        pl.semaphore_signal(barrier, inc=1, device_id=where, device_id_type=MESH)
    pl.semaphore_wait(barrier, len(peers))


def fsdp_peers(f):
    core = parity(f)
    other = f + 1 - 2 * core
    far = lax.rem(f + 2, 4)
    return other, far, lax.rem(other + 2, 4)


def others(axis, index, count):
    return [{axis: lax.rem(index + k, count)} for k in range(1, count)]


def nearest(z, last):
    near = jnp.where(z > 0, last, 1)
    second = jnp.where(z == 0, 2, jnp.where(z == last, last - 1, 1))
    return near, second


def rope(vals, cos, sin, half_dim):
    return vals * cos + pltpu.roll(vals, half_dim, 1) * sin


def causal(scores, tq):
    key_idx = lax.broadcasted_iota(jnp.int32, scores.shape, 0)
    q_idx = lax.rem(lax.broadcasted_iota(jnp.int32, scores.shape, 1), tq)
    return jnp.where(key_idx <= q_idx, scores, NEG_BIG)


def params(cid):
    return pltpu.CompilerParams(collective_id=cid, has_side_effects=True, vmem_limit_bytes=VMEM_BYTES)


def rope_tables(positions, head_dim):
    inv_freq = ROPE_BASE ** (-jnp.arange(0, head_dim, 2).astype(F32) / head_dim)
    angles = positions.astype(F32)[:, None] * inv_freq[None, :]
    cosines, sines = jnp.cos(angles), jnp.sin(angles)
    return jnp.concatenate([cosines, cosines], axis=1), jnp.concatenate([-sines, sines], axis=1)


def front_kernel(group, n_line, hid_ref, gain_ref, w_ref, wo_ref, cos_ref, sin_ref, o_ref, qr_ref, lse_ref, kl_ref, vl_ref, kp_ref, vp_ref, gfull_ref, n_out, w_out, wo_all, o_all, wbuf, nbuf, acc, hbuf, gbuf, qs, vt, m_all, l_all, acc_all, h_sem, g_send, g_recv, own_send, own_recv, x_send, x_recv, y_send, y_recv, d_send, d_recv, kv_send, kv_recv, ox_send, ox_recv, oy_send, oy_recv, od_send, od_recv, zw_send, zw_recv, wx_send, wx_recv, ot_send, ot_recv, out_sem):
    q_len, feat = hid_ref.shape[0], w_ref.shape[0]
    head_dim = cos_ref.shape[1]
    half_dim = head_dim // 2
    kv_width = kl_ref.shape[1]
    kv_heads = kv_width // head_dim
    q_width = qr_ref.shape[1]
    tq = q_len // TILES
    wide = group * tq
    scale = head_dim ** -0.5 * LOG2E
    half = feat // 2
    piece = half // PIECES
    o_rows = wo_ref.shape[0]
    o_half = o_rows // 2
    o_piece = o_half // O_PIECES
    flag, f, z = lax.axis_index("cp"), lax.axis_index("fsdp"), lax.axis_index("tp")
    wo_out = wo_all.at[z]
    last = n_line - 1
    far = 1 - flag
    f_core, f_x, f_diag = fsdp_peers(f)
    to_core, to_x, to_diag, to_y = {"fsdp": f_core}, {"fsdp": f_x}, {"fsdp": f_diag}, {"cp": far}

    def h_load(tile):
        slot = parity(tile)
        return pltpu.make_async_copy(hid_ref.at[blk(tile, tq)], hbuf.at[slot], h_sem.at[slot])

    h_load(0).start()
    h_load(1).start()
    meet([to_core, to_x, to_diag, to_y] + others("tp", z, n_line))

    def span(side, j):
        return blk(side * PIECES + j, piece)

    def x_copy(j):
        return remote(w_ref.at[span(flag, j)], wbuf.at[f, span(flag, j)], x_send.at[j], x_recv.at[j], to_x)

    def x_in(j):
        return remote(w_ref.at[span(flag, j)], wbuf.at[f_x, span(flag, j)], x_send.at[j], x_recv.at[j], to_x)

    def y_copy(j, side):
        return remote(wbuf.at[f_x, span(side, j)], wbuf.at[f_x, span(side, j)], y_send.at[j], y_recv.at[j], to_y)

    def d_copy(j, side, slot):
        return remote(wbuf.at[slot, span(side, j)], wbuf.at[slot, span(side, j)], d_send.at[side, j], d_recv.at[side, j], to_core)

    def g_copy(k, where, slot):
        return remote(gain_ref, gbuf.at[slot], g_send.at[k], g_recv.at[k], where)

    def own_copy(slot):
        return remote(w_ref, wbuf.at[slot], own_send, own_recv, to_core)

    def o_span(side, j):
        return blk(side * O_PIECES + j, o_piece)

    def ox_copy(j, slot):
        return remote(wo_ref.at[o_span(flag, j)], wo_out.at[slot, o_span(flag, j)], ox_send.at[j], ox_recv.at[j], to_x)

    def oy_copy(j, side):
        return remote(wo_out.at[f_x, o_span(side, j)], wo_out.at[f_x, o_span(side, j)], oy_send.at[j], oy_recv.at[j], to_y)

    def od_copy(k, src, slot, where):
        return remote(src, wo_out.at[slot, where], od_send.at[k], od_recv.at[k], to_core)

    def zw_copy(up, t):
        spot = wo_all.at[t, f, blk(flag, o_half)]
        where = jnp.minimum(z + 1, last) if up else jnp.maximum(z - 1, 0)
        src = spot if t is not z else wo_ref.at[blk(flag, o_half)]
        return remote(src, spot, zw_send.at[up, t], zw_recv.at[t], {"tp": where})

    def zw_tick(r):
        for up, t, here in ((0, z + r, z + r <= last), (1, z - r, z >= r)):
            at = jnp.clip(t, 0, last)

            @pl.when(here)
            def _():
                zw_copy(up, at).wait_recv()

            @pl.when(here & (z < last if up else z > 0))
            def _():
                zw_copy(up, at).start()

    def wx_copy(k, r, slot):
        spot = wo_all.at[lax.rem(z + r, n_line), slot, blk(flag, o_half)]
        return remote(spot, spot, wx_send.at[k], wx_recv.at[k], to_x)

    def ot_copy(up, j, owner):
        src = o_ref.at[blk(j, tq)]
        where = jnp.minimum(z + 1, last) if up else jnp.maximum(z - 1, 0)
        return remote(src, o_all.at[owner, blk(j, tq)], ot_send.at[up, j], ot_recv.at[up, j], {"tp": where})

    gains = [(k, where, where["fsdp"]) for k, where in enumerate((to_core, to_x, to_diag))]
    for k, where, _ in gains:
        g_copy(k, where, f).start()
    sends = [x_copy(j) for j in range(PIECES)] + [ox_copy(j, f) for j in range(O_PIECES)]
    for j in range(LEAD):
        sends[j].start()
    own_copy(f).start()
    all_rows = pl.ds(0, o_rows)
    steps_x = nearest(z, last)
    for up in SIDES:
        @pl.when(z < last if up else z > 0)
        def _():
            zw_copy(up, z).start()

    local_w = pltpu.make_async_copy(w_ref, wbuf.at[f], out_sem.at[0])
    local_w.start()
    local_o = pltpu.make_async_copy(wo_ref, wo_out.at[f], out_sem.at[1])
    local_o.start()
    gbuf[f] = gain_ref[...]
    for k, where, slot in gains:
        g_copy(k, where, slot).wait_recv()
    for k in range(gbuf.shape[0]):
        gfull_ref[:, blk(k, feat)] = gbuf[k]

    for tile in range(TILES):
        h_load(tile).wait()
        strip = min(32, tq)

        @pl.loop(0, tq // strip)
        def _(i):
            vals = hbuf[tile % 2, blk(i, strip), :].astype(F32)
            inv = lax.rsqrt(lane_mean(vals * vals) + NORM_EPS)
            nbuf[pl.ds(pl.multiple_of(tile * tq + i * strip, strip), strip), :] = (vals * inv * gfull_ref[...]).astype(BF)

        if tile + 2 < TILES:
            h_load(tile + 2).start()
    put_n = pltpu.make_async_copy(nbuf, n_out, out_sem.at[2])
    put_n.start()

    def project(slot, start, rows, first=False):
        cols = pl.ds(pl.multiple_of(slot * feat + start, 128), rows)

        @pl.loop(0, TILES)
        def _(tile):
            here = blk(tile, tq)
            part = dot(nbuf[here, cols], wbuf[slot, pl.ds(start, rows), :], NN)
            acc[here, :] = part if first else acc[here, :] + part

    def x_tick(j):
        x_in(j).wait_recv()
        y_copy(j, flag).start()
        d_copy(j, flag, f_x).start()
        sends[j + LEAD].start()

    def y_tick(j):
        y_copy(j, far).wait_recv()
        d_copy(j, 1 - flag, f_x).start()

    local_w.wait()
    project(f, 0, feat, first=True)
    x_tick(0)
    own_copy(f_core).wait_recv()
    od_copy(0, wo_ref, f, all_rows).start()
    project(f_core, 0, feat)
    x_tick(1)
    y_tick(0)
    zw_tick(1)
    x_tick(2)
    y_tick(1)
    x_tick(3)
    for j in range(PIECES):
        d_copy(j, flag, f_diag).wait_recv()
    first_half = pl.multiple_of(flag * half, half)
    project(f_x, first_half, half)
    y_tick(2)
    project(f_diag, first_half, half)
    y_tick(3)
    for j in range(PIECES):
        d_copy(j, 1 - flag, f_diag).wait_recv()
    second_half = pl.multiple_of(far * half, half)
    project(f_x, second_half, half)
    project(f_diag, second_half, half)
    zw_tick(2)
    wx_copy(0, steps_x[0], f).start()
    put_w = pltpu.make_async_copy(wbuf, w_out, out_sem.at[3])
    put_w.start()

    @pl.loop(0, TILES)
    def _(tile):
        here = blk(tile, tq)
        cos, sin = cos_ref[here, :], sin_ref[here, :]
        for h in range(kv_heads):
            k_at = q_width // head_dim + h
            kl_ref[here, blk(h, head_dim)] = rope(acc[here, blk(k_at, head_dim)], cos, sin, half_dim).astype(BF)
            vl_ref[here, blk(h, head_dim)] = acc[here, blk(k_at + kv_heads, head_dim)].astype(BF)

    kv_pairs = ((kl_ref, kp_ref), (vl_ref, vp_ref))

    def kv_copy(k):
        return remote(kv_pairs[k][0], kv_pairs[k][1], kv_send.at[k], kv_recv.at[k], {"cp": 1})

    @pl.loop(0, TILES)
    def _(tile):
        here = blk(tile, tq)
        cos, sin = cos_ref[here, :], sin_ref[here, :]
        for h in range(group * kv_heads):
            cols = blk(h, head_dim)
            qr_ref[here, cols] = rope(acc[here, cols], cos, sin, half_dim).astype(BF)

    @pl.when(flag == 0)
    def _():
        zero(kp_ref)
        zero(vp_ref)
        for k in range(len(kv_pairs)):
            kv_copy(k).start()

    def load_q(item):
        g, tile = lax.rem(item, kv_heads), item // kv_heads
        rows = blk(tile, tq)
        for h in range(group):
            qs[:, blk(h, tq)] = qr_ref[rows, blk(g * group + h, head_dim)].T

    def key_piece(item, k_ref, side, start, masked):
        g = lax.rem(item, kv_heads)
        scores = dot(k_ref[start, blk(g, head_dim)], qs[...], NN)
        if masked:
            scores = causal(scores, tq)
        m_old = m_all[item]
        m_new = jnp.maximum(m_old, jnp.max(scores, axis=0, keepdims=True))
        probs = jnp.exp2((scores - m_new) * scale)
        fade = jnp.exp2((m_old - m_new) * scale)
        m_all[item] = m_new
        l_all[item] = l_all[item] * fade + row_sum(probs)
        acc_all[item] = acc_all[item] * fade + dot(vt[g, side, :, start], probs.astype(BF), NN)

    for g in range(kv_heads):
        vt[g, 0] = vl_ref[:, blk(g, head_dim)].T

    @pl.loop(0, kv_heads * TILES)
    def _(item):
        tile = item // kv_heads
        load_q(item)
        m_all[item] = jnp.full_like(m_all[item], NEG_BIG)
        l_all[item] = jnp.zeros_like(l_all[item])
        acc_all[item] = jnp.zeros_like(acc_all[item])
        key_piece(item, kl_ref, 0, blk(tile, tq), True)

        @pl.loop(0, tile // 2)
        def _(i):
            key_piece(item, kl_ref, 0, blk(i, 2 * tq), False)

        @pl.when(parity(tile) == 1)
        def _():
            key_piece(item, kl_ref, 0, blk(tile - 1, tq), False)

    for j in range(O_PIECES):
        ox_copy(j, f_x).wait_recv()
        oy_copy(j, flag).start()
        od_copy(1 + j, wo_out.at[f_x, o_span(flag, j)], f_x, o_span(flag, j)).start()

    wx_copy(1, steps_x[1], f).start()

    @pl.when(flag == 1)
    def _():
        for k in range(len(kv_pairs)):
            kv_copy(k).wait_recv()
        for g in range(kv_heads):
            vt[g, 1] = vp_ref[:, blk(g, head_dim)].T

    @pl.loop(0, kv_heads * TILES)
    def _(item):
        g, tile = lax.rem(item, kv_heads), item // kv_heads
        rows = blk(tile, tq)

        @pl.when(flag == 1)
        def _():
            load_q(item)

        @pl.loop(0, flag * TILES // 2)
        def _(i):
            key_piece(item, kp_ref, 1, blk(i, 2 * tq), False)

        total = l_all[item]
        lse_ref[g * TILES + tile] = m_all[item] * scale + jnp.log2(total)
        out_t = acc_all[item] / total
        for h in range(group):
            o_ref[rows, blk(g * group + h, head_dim)] = out_t[:, h * tq:h * tq + tq].T.astype(BF)

        for j in range(O_EARLY):
            @pl.when((item == (j + 1) * kv_heads) & (z > 0))
            def _():
                ot_copy(0, j, z).start()

            @pl.when((item == (j + 1) * kv_heads) & (z < last))
            def _():
                ot_copy(1, j, z).start()

        for j in range(O_PIECES):
            @pl.when(item == (j + 1) * kv_heads * TILES // O_PIECES - 1)
            def _():
                oy_copy(j, far).wait_recv()
                od_copy(1 + O_PIECES + j, wo_out.at[f_x, o_span(1 - flag, j)], f_x, o_span(1 - flag, j)).start()

    od_copy(0, wo_ref, f_core, all_rows).wait_recv()
    for j in range(O_PIECES):
        od_copy(1 + j, wo_out.at[f_x, o_span(flag, j)], f_diag, o_span(flag, j)).wait_recv()
        od_copy(1 + O_PIECES + j, wo_out.at[f_x, o_span(1 - flag, j)], f_diag, o_span(1 - flag, j)).wait_recv()

    for r in range(3, n_line):
        zw_tick(r)

    @pl.loop(0, n_line)
    def _(t):
        for up in SIDES:
            @pl.when((t <= z) & (z < last) if up else (t >= z) & (z > 0))
            def _():
                zw_copy(up, t).wait_send()

    for k, r in enumerate(steps_x):
        wx_copy(k, r, f_x).wait_recv()
        wx_copy(k, r, f).wait_send()
    for j in range(O_EARLY):
        for up in SIDES:
            @pl.when(z < last if up else z > 0)
            def _():
                ot_copy(up, j, z).wait_send()
                ot_copy(1 - up, j, z + 1 if up else z - 1).wait_recv()

    for k, where, _ in gains:
        g_copy(k, where, f).wait_send()
    own_copy(f).wait_send()
    od_copy(0, wo_ref, f, all_rows).wait_send()
    for j in range(PIECES):
        x_copy(j).wait_send()
        y_copy(j, flag).wait_send()
        d_copy(j, flag, f_x).wait_send()
        d_copy(j, 1 - flag, f_x).wait_send()
    for j in range(O_PIECES):
        ox_copy(j, f).wait_send()
        oy_copy(j, flag).wait_send()
        od_copy(1 + j, wo_out.at[f_x, o_span(flag, j)], f_x, o_span(flag, j)).wait_send()
        od_copy(1 + O_PIECES + j, wo_out.at[f_x, o_span(1 - flag, j)], f_x, o_span(1 - flag, j)).wait_send()

    @pl.when(flag == 0)
    def _():
        for k in range(len(kv_pairs)):
            kv_copy(k).wait_send()

    for local in (local_o, put_n, put_w):
        local.wait()


def front(hidden, gain, w_qkv, w_out, cosines, sines, group, kv_width, n_line, cid):
    q_len, model_dim = hidden.shape
    feat, width = w_qkv.shape
    head_dim = cosines.shape[1]
    q_width = width - 2 * kv_width
    kv_heads = kv_width // head_dim
    o_rows, o_cols = w_out.shape
    n_fsdp = model_dim // feat
    tq = q_len // TILES
    wide = group * tq
    items = kv_heads * TILES
    sds = jax.ShapeDtypeStruct
    kv = sds((q_len, kv_width), BF)
    q_like = sds((q_len, q_width), BF)
    line = pltpu.VMEM((items, 1, wide), F32)
    own, pair, trio = DMA(()), DMA((2,)), DMA((n_fsdp - 1,))
    early = DMA((2, O_EARLY))
    w_link, w_side, o_link, o_core = DMA((PIECES,)), DMA((2, PIECES)), DMA((O_PIECES,)), DMA((1 + 2 * O_PIECES,))
    return pl.pallas_call(
        functools.partial(front_kernel, group, n_line),
        in_specs=[ANY] + [VMEM] * 5,
        out_specs=[VMEM] * 8 + [ANY] * 4,
        out_shape=[q_like, q_like, sds((items, 1, wide), F32), kv, kv, kv, kv, sds((1, model_dim), F32), sds((q_len, model_dim), BF), sds((n_fsdp, feat, width), BF), sds((n_line, n_fsdp, o_rows, o_cols), BF), sds((n_line, q_len, q_width), BF)],
        scratch_shapes=[
            pltpu.VMEM((n_fsdp, feat, width), BF),
            pltpu.VMEM((q_len, model_dim), BF),
            pltpu.VMEM((q_len, width), F32),
            pltpu.VMEM((2, tq, model_dim), BF),
            pltpu.VMEM((n_fsdp, 1, feat), F32),
            pltpu.VMEM((head_dim, wide), BF),
            pltpu.VMEM((kv_heads, 2, head_dim, q_len), BF),
            line,
            line,
            pltpu.VMEM((items, head_dim, wide), F32),
        ] + [pair, trio, trio, own, own, w_link, w_link, w_link, w_link, w_side, w_side, pair, pair, o_link, o_link, o_link, o_link, o_core, o_core, DMA((2, n_line)), DMA((n_line,)), pair, pair, early, early, DMA((4,))],
        compiler_params=params(cid),
        name="front",
    )(hidden, gain, w_qkv, w_out, cosines, sines)


def back_kernel(n_line, group, o_ref, q_ref, lse_ref, cos_ref, sin_ref, kl_ref, vl_ref, kp_ref, vp_ref, _wo_in, _o_in, ct_ref, d_ref, o_all, wo_all, w_ref, ctb_ref, do_ref, dkl_ref, dvl_ref, dkp_ref, dvp_ref, qs_ref, dos_ref, delta_ref, kt_ref, dqt_ref, load_sem, keep_sem, ct_sem, od_send, ou_send, o_recv, y_send, y_recv, x_send, x_recv, c_send, c_recv, cx_send, cx_recv, kv_send, kv_recv):
    last = n_line - 1
    z, flag, f = lax.axis_index("tp"), lax.axis_index("cp"), lax.axis_index("fsdp")
    far = 1 - flag
    f_core, f_x, f_diag = fsdp_peers(f)
    q_len, width = o_ref.shape
    head_dim = cos_ref.shape[1]
    half_dim = head_dim // 2
    kv_width = kl_ref.shape[1]
    kv_heads = kv_width // head_dim
    tq = q_len // TILES
    wide = group * tq
    score_scale = head_dim ** -0.5
    n_parts, o_rows, part = w_ref.shape
    o_half = o_rows // 2
    load = pltpu.make_async_copy(wo_all.at[z], w_ref, load_sem)
    load.start()
    keep = pltpu.make_async_copy(o_ref, o_all.at[z], keep_sem)
    keep.start()

    def ct_load(tile):
        slot = parity(tile)
        return pltpu.make_async_copy(ct_ref.at[blk(tile, tq)], ctb_ref.at[slot], ct_sem.at[slot])

    ct_load(0).start()
    ct_load(1).start()

    to_core, to_x, to_y = {"fsdp": f_core}, {"fsdp": f_x}, {"cp": far}
    meet([to_core, to_x, to_y] + others("tp", z, n_line))

    def tile_rows(j):
        return blk(j, tq)

    def o_down(t, j, src):
        return remote(src, o_all.at[t, tile_rows(j)], od_send.at[t, j], o_recv.at[t, j], {"tp": jnp.maximum(z - 1, 0)})

    def o_up(t, j, src):
        return remote(src, o_all.at[t, tile_rows(j)], ou_send.at[t, j], o_recv.at[t, j], {"tp": jnp.minimum(z + 1, last)})

    def wo_half(r, slot, side):
        return wo_all.at[lax.rem(z + r, n_line), slot, blk(side, o_half)]

    def y_copy(r, side):
        return remote(wo_half(r, f, side), wo_half(r, f, side), y_send.at[r - 1], y_recv.at[r - 1], to_y)

    def x_copy(r, side, slot):
        return remote(wo_half(r, slot, side), wo_half(r, slot, side), x_send.at[side, r - 1], x_recv.at[side, r - 1], to_x)

    def c_copy(r, side, slot):
        return remote(wo_half(r, slot, side), wo_half(r, slot, side), c_send.at[side, r - 1], c_recv.at[side, r - 1], to_core)

    def cx_copy(r, side, slot):
        return remote(wo_half(r, slot, side), wo_half(r, slot, side), cx_send.at[side, r - 1], cx_recv.at[side, r - 1], to_core)

    for j in range(O_EARLY, TILES):
        @pl.when(z > 0)
        def _():
            o_down(z, j, o_ref.at[tile_rows(j)]).start()

        @pl.when(z < last)
        def _():
            o_up(z, j, o_ref.at[tile_rows(j)]).start()

    def o_early(j):
        @pl.when((z > 0) & (z < last))
        def _():
            o_down(z + 1, j, o_all.at[z + 1, tile_rows(j)]).start()
            o_up(z - 1, j, o_all.at[z - 1, tile_rows(j)]).start()

    o_early(0)
    steps_x = nearest(z, last)
    third = n_line * last // 2 - sum(steps_x)
    x_copy(third, flag, f).start()
    for r in range(1, n_line - 1):
        y_copy(r, flag).start()

    def o_tick(k):
        r, j = k // TILES + 1, lax.rem(k, TILES)

        @pl.when(k == O_EARLY)
        def _():
            for early in range(1, O_EARLY):
                o_early(early)

        @pl.when(z + r <= last)
        def _():
            t = jnp.minimum(z + r, last)
            o_down(t, j, o_all.at[t, tile_rows(j)]).wait_recv()

            @pl.when(z > 0)
            def _():
                o_down(t, j, o_all.at[t, tile_rows(j)]).start()

        @pl.when(z - r >= 0)
        def _():
            t = jnp.maximum(z - r, 0)
            o_up(t, j, o_all.at[t, tile_rows(j)]).wait_recv()

            @pl.when(z < last)
            def _():
                o_up(t, j, o_all.at[t, tile_rows(j)]).start()

    def y_tick(r):
        y_copy(r, far).wait_recv()
        x_copy(r, far, f).start()
        for side in (flag, far):
            c_copy(r, side, f).start()
        if r == 1:
            y_copy(n_line - 1, flag).start()
        if r < n_line - 1:
            cx_copy(steps_x[r - 1], flag, f_x).start()

    def x_tick(q):
        r, side = (q, far) if q else (third, flag)
        x_copy(r, side, f_x).wait_recv()
        cx_copy(r, side, f_x).start()

    zero(dkl_ref)
    zero(dvl_ref)

    @pl.when(flag == 1)
    def _():
        zero(dkp_ref)
        zero(dvp_ref)

    load.wait()

    def do_tile(tile):
        ct_load(tile).wait()
        slot = parity(tile)
        total = sum(dot(ctb_ref[slot, :, blk(k, part)], w_ref[k], NT) for k in range(n_parts))
        do_ref[tile_rows(tile), :] = total.astype(BF)

        @pl.when(tile + 2 < TILES)
        def _():
            ct_load(tile + 2).start()

    def bwd_item(item):
        g, tile = item // TILES, lax.rem(item, TILES)
        kv_cols = blk(g, head_dim)
        rows = blk(tile, tq)

        @pl.when(tile == 0)
        def _():
            kt_ref[0] = kl_ref[:, kv_cols].T
            kt_ref[1] = kp_ref[:, kv_cols].T

        for h in range(group):
            cols = blk(g * group + h, head_dim)
            stack = blk(h, tq)
            qs_ref[stack, :] = q_ref[rows, cols]
            d_h = do_ref[rows, cols]
            dos_ref[stack, :] = d_h
            prod = d_h.astype(F32) * o_ref[rows, cols].astype(F32)
            delta_ref[:, stack] = row_sum(prod.T)
        zero(dqt_ref)

        def piece(k_ref, v_ref, dk_ref, dv_ref, side, span, masked):
            scores = dot(k_ref[span, kv_cols], qs_ref[...], NT)
            if masked:
                scores = causal(scores, tq)
            probs = jnp.exp2(scores * (score_scale * LOG2E) - lse_ref[item])
            d_probs = dot(v_ref[span, kv_cols], dos_ref[...], NT)
            d_scores = (probs * (d_probs - delta_ref[...])).astype(BF)
            dv_ref[g, span, :] += dot(probs.astype(BF), dos_ref[...], NN)
            dk_ref[g, span, :] += dot(d_scores, qs_ref[...], NN)
            dqt_ref[...] += dot(kt_ref[side, :, span], d_scores, NN)

        piece(kl_ref, vl_ref, dkl_ref, dvl_ref, 0, blk(tile, tq), True)

        @pl.loop(0, tile // 2)
        def _(i):
            piece(kl_ref, vl_ref, dkl_ref, dvl_ref, 0, blk(i, 2 * tq), False)

        @pl.when(parity(tile) == 1)
        def _():
            piece(kl_ref, vl_ref, dkl_ref, dvl_ref, 0, blk(tile - 1, tq), False)

        @pl.loop(0, flag * TILES // 2)
        def _(i):
            piece(kp_ref, vp_ref, dkp_ref, dvp_ref, 1, blk(i, 2 * tq), False)

        for h in range(group):
            dq_h = dqt_ref[:, blk(h, tq)].T * score_scale
            d_ref[rows, blk(g * group + h, head_dim)] = rope(dq_h, cos_ref[rows, :], -sin_ref[rows, :], half_dim).astype(BF)

        @pl.when((tile == TILES - 1) & (flag == 1))
        def _():
            for copy in back(g):
                copy.start()

    def back(g):
        return [remote(ref.at[g], ref.at[g], kv_send.at[k, g], kv_recv.at[k, g], {"cp": 0}) for k, ref in enumerate((dkp_ref, dvp_ref))]

    def kv_done(g):
        @pl.when(flag == 0)
        def _():
            for copy in back(g):
                copy.wait_recv()
            dkl_ref[g] += dkp_ref[g]
            dvl_ref[g] += dvp_ref[g]

        dk = rope(dkl_ref[g] * score_scale, cos_ref[...], -sin_ref[...], half_dim)
        k_at = width // head_dim + g
        d_ref[:, blk(k_at, head_dim)] = dk.astype(BF)
        d_ref[:, blk(k_at + kv_heads, head_dim)] = dvl_ref[g].astype(BF)

        @pl.when(flag == 1)
        def _():
            for copy in back(g):
                copy.wait_send()

    items = TILES * (kv_heads + 1)
    o_ticks = TILES * last
    x_at = {5: 0, 8: 1, 11: 2}

    @pl.loop(0, items)
    def _(item):
        @pl.when(item < TILES)
        def _():
            do_tile(item)

        @pl.when(item >= TILES)
        def _():
            bwd_item(item - TILES)

        @pl.when((parity(item) == 1) & (item > 1))
        def _():
            o_tick(item // 2 - 1 + O_EARLY)

        for r in range(1, n_line):
            @pl.when(item == 3 * r + 1)
            def _():
                y_tick(r)

        for at, q in x_at.items():
            @pl.when(item == at)
            def _():
                x_tick(q)

    done = items // 2 - 1 + O_EARLY
    tail = [("x", q) for q in range(len(x_at), n_line)] + [("kv", g) for g in range(kv_heads)]
    for k in range(done, o_ticks):
        o_tick(jnp.int32(k))
        if (k - done) % 2 == 1 and tail:
            kind, arg = tail.pop(0)
            x_tick(arg) if kind == "x" else kv_done(arg)
            later = [t for t in tail if t[0] == "kv"]
            if later:
                tail.remove(later[0])
                kv_done(later[0][1])
    for kind, arg in tail:
        x_tick(arg) if kind == "x" else kv_done(arg)

    for r in range(1, n_line):
        for side in (flag, far):
            c_copy(r, side, f_core).wait_recv()
            cx_copy(r, side, f_diag).wait_recv()
            c_copy(r, side, f).wait_send()
            cx_copy(r, side, f_x).wait_send()
        x_copy(r, far, f).wait_send()
        y_copy(r, flag).wait_send()
    x_copy(third, flag, f).wait_send()

    @pl.loop(0, n_line)
    def _(t):
        @pl.when((t >= z) & (z > 0))
        def _():
            @pl.loop(jnp.where(t == z, O_EARLY, 0), TILES)
            def _(j):
                o_down(t, j, o_all.at[t, tile_rows(j)]).wait_send()

        @pl.when((t <= z) & (z < last))
        def _():
            @pl.loop(jnp.where(t == z, O_EARLY, 0), TILES)
            def _(j):
                o_up(t, j, o_all.at[t, tile_rows(j)]).wait_send()

    keep.wait()


def attn_back(attn_out, q_rot, lse, cosines, sines, k_loc, v_loc, k_prev, v_prev, wo_all, o_all, cotangent, n_line, group, cid):
    q_len, width = attn_out.shape
    head_dim = cosines.shape[1]
    kv_width = k_loc.shape[1]
    kv_heads = kv_width // head_dim
    _, n_fsdp, o_rows, o_cols = wo_all.shape
    tq = q_len // TILES
    wide = group * tq
    acc = pltpu.VMEM((kv_heads, q_len, head_dim), F32)
    stack = pltpu.VMEM((wide, head_dim), BF)
    own, pair, tiles, hop, side, kv = DMA(()), DMA((2,)), DMA((n_line, TILES)), DMA((n_line - 1,)), DMA((2, n_line - 1)), DMA((2, kv_heads))
    return pl.pallas_call(
        functools.partial(back_kernel, n_line, group),
        in_specs=[VMEM] * 9 + [ANY] * 3,
        out_specs=[VMEM, ANY, ANY],
        out_shape=[jax.ShapeDtypeStruct((q_len, width + 2 * kv_width), BF), jax.ShapeDtypeStruct((n_line, q_len, width), BF), jax.ShapeDtypeStruct(wo_all.shape, BF)],
        input_output_aliases={9: 2, 10: 1},
        scratch_shapes=[
            pltpu.VMEM((n_fsdp, o_rows, o_cols), BF),
            pltpu.VMEM((2, tq, cotangent.shape[1]), BF),
            pltpu.VMEM((q_len, width), BF),
            acc, acc, acc, acc,
            stack,
            stack,
            pltpu.VMEM((1, wide), F32),
            pltpu.VMEM((2, head_dim, q_len), BF),
            pltpu.VMEM((head_dim, wide), F32),
        ] + [own, own, pair, tiles, tiles, tiles, hop, hop, side, side, side, side, side, side, kv, kv],
        compiler_params=params(cid),
        name="attn_back",
    )(attn_out, q_rot, lse, cosines, sines, k_loc, v_loc, k_prev, v_prev, wo_all, o_all, cotangent)


class Line:
    def __init__(self, n_line, buf_ref, pbuf_ref, send_sem, recv_sem, fill, finish):
        self.last = n_line - 1
        self.z = lax.axis_index("tp")
        self.buf, self.pbuf, self.send_sem, self.recv_sem = buf_ref, pbuf_ref, send_sem, recv_sem
        self.chunks, self.rows = buf_ref.shape[1], buf_ref.shape[2]
        self.block = pbuf_ref.shape[1]
        self.per_block = self.block // self.rows
        self.fill, self.finish = fill, finish
        self.steps = self.chunks + self.last

    def dist(self, side):
        return self.z if side else self.last - self.z

    def toward(self, side, back=False):
        up = bool(side) != back
        return {"tp": jnp.clip(self.z + 1 if up else self.z - 1, 0, self.last)}

    def copy(self, side, chunk):
        spot = self.buf.at[side, chunk]
        return remote(spot, spot, self.send_sem.at[side, chunk], self.recv_sem.at[side, chunk], self.toward(side))

    def live(self, side, step):
        chunk = step - self.dist(side)
        return chunk, (chunk >= 0) & (chunk < self.chunks)

    def prepare(self, step):
        for side in SIDES:
            chunk, ok = self.live(side, step)

            @pl.when(ok & (lax.rem(chunk, self.per_block) == 0))
            def _():
                self.fill(self.pbuf.at[side], blk((side * self.chunks + chunk) // self.per_block, self.block))

    def tick(self, step):
        for side in SIDES:
            chunk, ok = self.live(side, step)
            dist = self.dist(side)
            part = blk(lax.rem(jnp.maximum(chunk, 0), self.per_block), self.rows)

            @pl.when(ok & (dist == 0))
            def _():
                self.buf[side, chunk] = self.pbuf[side, part, :]

            @pl.when(ok & (dist > 0))
            def _():
                self.copy(side, chunk).wait_recv()
                self.buf[side, chunk] += self.pbuf[side, part, :]

            @pl.when(ok & (dist < self.last))
            def _():
                self.copy(side, chunk).start()

            @pl.when(ok & (dist == self.last))
            def _():
                self.finish(chunk, self.buf[side, chunk])

        self.prepare(step + 1)

    def drain(self):
        for side in SIDES:
            @pl.when(self.dist(side) < self.last)
            def _():
                @pl.loop(0, self.chunks)
                def _(chunk):
                    self.copy(side, chunk).wait_send()


def close_kernel(n_line, n_fsdp, d_ref, o_ref, gain_ref, hid_ref, ct_ref, n_ref, w_all, o_all, wo_all, out_ref, blk_ref, gg_ref, ts, yr, dl, xs, ks, xr, buf, gp, ga, gs, gb, gt, gc, ebuf, fb_in, fb_ct, fb_out, send_sem, recv_sem, w_sem, f_sem, ct_sem, fo_sem, lhs_sem, a_send, a_recv, ld_sem, st_sem, x_send, x_recv, e_sem, es_sem, y_send, y_recv, out_send, out_recv, o_sem, wl_sem, h_sem, r_sem, ga_send, ga_recv, gb_send, gb_recv, gc_send, gc_recv):
    last = n_line - 1
    z, flag, f = lax.axis_index("tp"), lax.axis_index("cp"), lax.axis_index("fsdp")
    far = 1 - flag
    f_core, f_x, f_diag = fsdp_peers(f)
    to_core, to_x, to_y = {"fsdp": f_core}, {"fsdp": f_x}, {"cp": far}
    _, feat, width = w_all.shape
    chunks, rows = buf.shape[1], buf.shape[2]
    half = chunks * rows
    g_rows = feat // GRAD_CHUNKS
    owner = (z == 0) | (z == last)
    own_base = jnp.where(z == last, chunks, 0)
    copy = pltpu.make_async_copy

    def own_span(chunk):
        return blk(own_base + chunk, rows)

    def f_loads(chunk):
        slot = parity(chunk)
        return copy(hid_ref.at[own_span(chunk)], fb_in.at[slot], f_sem.at[slot]), copy(ct_ref.at[own_span(chunk)], fb_ct.at[slot], ct_sem.at[slot])

    def f_store(chunk):
        slot = parity(chunk)
        return copy(fb_out.at[slot], out_ref.at[own_span(chunk)], fo_sem.at[slot])

    @pl.when(owner)
    def _():
        for chunk in SIDES:
            for load in f_loads(chunk):
                load.start()

    zero(gp)
    meet([to_core, to_x, to_y] + others("tp", z, n_line) + [{"fsdp": f_diag}])

    def finish(chunk, total):
        slot = parity(chunk)
        for load in f_loads(chunk):
            load.wait()

        @pl.when(chunk > 1)
        def _():
            f_store(chunk - 2).wait()

        x_in = fb_in[slot].astype(F32)
        inv = lax.rsqrt(lane_mean(x_in * x_in) + NORM_EPS)
        x_hat = x_in * inv
        gp[...] += row_sum(total * x_hat)
        scaled = total * gain_ref[...]
        fb_out[slot] = (fb_ct[slot].astype(F32) + inv * (scaled - x_hat * lane_mean(scaled * x_hat))).astype(BF)
        f_store(chunk).start()

        @pl.when(chunk + 2 < chunks)
        def _():
            for load in f_loads(chunk + 2):
                load.start()

    kinds = range(2)

    def g_at(ref, j):
        return ref.at[blk(j, g_rows)]

    def x_copy(j):
        return remote(g_at(xs, j), g_at(xr, j), x_send.at[j], x_recv.at[j], to_x)

    def y_copy(j):
        return remote(g_at(ts, j), g_at(yr, j), y_send.at[j], y_recv.at[j], to_y)

    def e_store(j):
        return copy(ebuf.at[0], g_at(ts, j), es_sem)

    def meet_x(j):
        x_copy(j).wait_recv()
        loads = [copy(g_at(src, j), ebuf.at[k], e_sem.at[k]) for k, src in enumerate((ks, xr))]
        for load in loads:
            load.start()
        for load in loads:
            load.wait()
        ebuf[0] += ebuf[1]
        e_store(j).start()

    def send_y(j):
        e_store(j).wait()
        y_copy(j).start()

    steps = chunks + last - 1

    def dist(side):
        return z if side else last - z

    def hop(side, chunk):
        span = blk(side * chunks + chunk, rows)
        up = z - 1 if side else z + 1
        return remote(out_ref.at[span], out_ref.at[span], out_send.at[side, chunk], out_recv.at[side, chunk], {"tp": jnp.clip(up, 0, last)})

    ends = [(end, z == (last if end else 0)) for end in SIDES]

    def owner_send(first, stop):
        for end, here in ends:
            @pl.when(here)
            def _():
                @pl.loop(first, stop)
                def _(c):
                    hop(end, c).start()

    def pass_on(step):
        for side in SIDES:
            chunk = step - (last - 1 - dist(side))

            @pl.when((dist(side) < last) & (chunk >= 0) & (chunk < chunks))
            def _():
                hop(side, chunk).wait_recv()

                @pl.when(dist(side) > 0)
                def _():
                    hop(side, chunk).start()

    def sum_phase(wbuf, pbuf, abuf, bbuf, lbuf, lhs):
        w_load = copy(w_all, wbuf, w_sem)
        w_load.start()

        def fill(dst, span):
            for k in range(n_fsdp):
                dst[:, blk(k, feat)] = dot(d_ref[span, :], wbuf[k], NT)

        line = Line(n_line, buf, pbuf, send_sem, recv_sem, fill, finish)
        slots = (f_diag, f_core, f_x, f)

        def lhs_loads(j):
            return [copy(src.at[:, blk(slot * GRAD_CHUNKS + j, g_rows)], lhs.at[m, k], lhs_sem.at[m, k]) for m, src in enumerate((n_ref, ct_ref)) for k, slot in enumerate(slots)]

        def a_copy(kind, j):
            return remote(abuf.at[kind], dl.at[kind, blk(j, g_rows)], a_send.at[kind], a_recv.at[kind, j], to_core)

        def b_stores(j):
            return [copy(bbuf.at[k], g_at(dst, j), st_sem.at[k]) for k, dst in enumerate((xs, ks))]

        def send_x(j):
            for kind in kinds:
                a_copy(kind, j).wait_send()
            for store in b_stores(j):
                store.wait()
            x_copy(j).start()

        def make(j):
            for load in lhs_loads(j):
                load.wait()
            for k in range(len(slots)):
                dst = (abuf, bbuf)[k // 2].at[k % 2]
                dst[:, :width] = dot(lhs[0, k], d_ref[...], TN)
                dst[:, width:] = dot(lhs[1, k], o_ref[...], TN)
            for kind in kinds:
                a_copy(kind, j).start()

            @pl.when(j + 1 < GRAD_CHUNKS)
            def _():
                for load in lhs_loads(j + 1):
                    load.start()

        def meet_core(j):
            loads = [copy(dl.at[kind, blk(j, g_rows)], lbuf.at[kind], ld_sem.at[kind]) for kind in kinds]
            for kind in kinds:
                a_copy(kind, j).wait_recv()
                loads[kind].start()
            for kind in kinds:
                loads[kind].wait()
                bbuf[kind] += lbuf[kind]
            for store in b_stores(j):
                store.start()

        for load in lhs_loads(0):
            load.start()
        w_load.wait()
        line.prepare(0)

        @pl.loop(0, line.steps)
        def _(fine):
            line.tick(fine)
            step = fine // PER_STEP
            whole = lax.rem(fine, PER_STEP) == 0
            j, odd = step // 2, parity(step)

            @pl.when(whole & (odd == 0) & (j > 0) & (j <= GRAD_CHUNKS))
            def _():
                send_x(j - 1)

            @pl.when(whole & (odd == 0) & (j < GRAD_CHUNKS))
            def _():
                make(j)

            @pl.when(whole & (odd == 1) & (j < GRAD_CHUNKS))
            def _():
                meet_core(j)

            for late in SIDES:
                k = (step - FIRST_X - late) * 2 // 5

                @pl.when(whole & (k >= 0) & (k < EARLY) & (step - late == FIRST_X + (5 * k + 1) // 2))
                def _():
                    send_y(k) if late else meet_x(k)

            @pl.when(fine >= chunks)
            def _():
                owner_send((fine - chunks) * LEAD, (fine - chunks + 1) * LEAD)

            @pl.when(fine > chunks)
            def _():
                for k in range(PER_STEP):
                    pass_on((fine - chunks - 1) * PER_STEP + k)

        @pl.when(owner)
        def _():
            for chunk in range(chunks - 2, chunks):
                f_store(chunk).wait()

        line.drain()

    pl.run_scoped(
        sum_phase,
        pltpu.VMEM(w_all.shape, BF),
        pltpu.VMEM((2, min(128, half), buf.shape[3]), F32),
        pltpu.VMEM((2, g_rows, ts.shape[1]), F32),
        pltpu.VMEM((2, g_rows, ts.shape[1]), F32),
        pltpu.VMEM((2, g_rows, ts.shape[1]), F32),
        pltpu.VMEM((2, n_fsdp, d_ref.shape[0], g_rows), BF),
    )
    def ga_copy(end, k):
        return remote(gp, ga.at[end], ga_send.at[k], ga_recv.at[end], {"tp": k if end else 1 + k})

    def gb_copy():
        return remote(gs, gb, gb_send, gb_recv, to_y)

    def gc_copy(k, slot):
        to = lax.rem(f + k, n_fsdp)
        return remote(gt.at[to], gc.at[slot], gc_send.at[k - 1], gc_recv.at[k - 1], {"fsdp": to})

    def spread_phase(obuf, wbuf, hbuf, rbuf):
        o_load = copy(o_all, obuf, o_sem)
        o_load.start()
        q_len, n_cols = hbuf.shape[1], hbuf.shape[2]
        per_part = wo_all.shape[3] // n_cols
        items = per_part * n_fsdp

        def item_loads(item):
            slot = parity(item)
            return copy(wo_all.at[:, item // per_part, :, blk(lax.rem(item, per_part), n_cols)], wbuf.at[slot], wl_sem.at[slot]), copy(hid_ref.at[:, blk(item, n_cols)], hbuf.at[slot], h_sem.at[slot])

        def item_store(item):
            slot = parity(item)
            return copy(rbuf.at[slot], blk_ref.at[:, blk(item, n_cols)], r_sem.at[slot])

        for item in SIDES:
            for load in item_loads(item):
                load.start()

        for end, here in ends:
            @pl.when(here)
            def _():
                ga[end] = gp[...]
                for k in range(last):
                    ga_copy(end, k).start()


        def project(item):
            slot = parity(item)
            for load in item_loads(item):
                load.wait()

            @pl.when(item > 1)
            def _():
                item_store(item - 2).wait()

            @pl.loop(0, TILES)
            def _(tile):
                span = blk(tile, q_len // TILES)
                total = sum(dot(obuf[t, span, :], wbuf[slot, t], NN) for t in range(n_line))
                rbuf[slot, span, :] = (hbuf[slot, span, :].astype(F32) + total).astype(BF)

            item_store(item).start()

            @pl.when(item + 2 < items)
            def _():
                for load in item_loads(item + 2):
                    load.start()

        for end, here in ends:
            @pl.when(jnp.logical_not(here))
            def _():
                ga_copy(end, 0).wait_recv()
        gs[...] = ga[0] + ga[1]
        o_load.wait()
        gb_copy().start()

        early = (last - 1) * PER_STEP

        @pl.loop(0, steps - early)
        def _(step):
            sent = step + last * LEAD
            owner_send(sent, jnp.minimum(sent + 1, chunks))
            pass_on(step + early)

            @pl.when((parity(step) == 0) & (step // 2 < items))
            def _():
                project(step // 2)

            for k, at in LATE:
                @pl.when(step == at)
                def _():
                    meet_x(k)

            for k, at in ((EARLY - 1, -1),) + LATE:
                @pl.when(step == at + 1)
                def _():
                    send_y(k)

        for item in range(items - 2, items):
            item_store(item).wait()

    pl.run_scoped(
        spread_phase,
        pltpu.VMEM(o_all.shape, BF),
        pltpu.VMEM((2, n_line, wo_all.shape[2], min(512, feat)), BF),
        pltpu.VMEM((2, d_ref.shape[0], min(512, feat)), BF),
        pltpu.VMEM((2, d_ref.shape[0], min(512, feat)), BF),
    )

    gb_copy().wait()
    for k in range(n_fsdp):
        gt[k] = gs[:, blk(k, feat)] + gb[:, blk(k, feat)]
    gc[f] = gt[f]
    for side in SIDES:
        @pl.when(dist(side) > 0)
        def _():
            @pl.loop(0, chunks)
            def _(chunk):
                hop(side, chunk).wait_send()

    @pl.loop(0, GRAD_CHUNKS)
    def _(j):
        x_copy(j).wait_send()

    for k in range(1, n_fsdp):
        gc_copy(k, f).start()
    for k in range(1, n_fsdp):
        gc_copy(k, lax.rem(f + n_fsdp - k, n_fsdp)).wait_recv()
    gg_ref[...] = sum(gc[k] for k in range(n_fsdp))
    for k in range(1, n_fsdp):
        gc_copy(k, f).wait_send()
    for end, here in ends:
        @pl.when(here)
        def _():
            for k in range(last):
                ga_copy(end, k).wait_send()

    @pl.loop(0, GRAD_CHUNKS)
    def _(j):
        y_copy(j).wait()


def close(d_lin, attn_out, gain, hidden, cotangent, normed, w_full, o_all, wo_all, cid):
    q_len, model_dim = hidden.shape
    n_line, n_fsdp = wo_all.shape[:2]
    _, feat, width = w_full.shape
    g_width = width + attn_out.shape[1]
    half = q_len // 2
    rows = half // CHUNKS
    sds = jax.ShapeDtypeStruct
    row = pltpu.VMEM((1, model_dim), F32)
    slices = pltpu.VMEM((n_fsdp, 1, feat), F32)
    strip = pltpu.VMEM((2, rows, model_dim), BF)
    own, pair, line, grad, grads = DMA(()), DMA((2,)), DMA((2, CHUNKS)), DMA((GRAD_CHUNKS,)), DMA((2, GRAD_CHUNKS))
    z_trio, f_trio = DMA((n_line - 1,)), DMA((n_fsdp - 1,))
    act, g_part = sds((q_len, model_dim), BF), sds((feat, g_width), F32)
    return pl.pallas_call(
        functools.partial(close_kernel, n_line, n_fsdp),
        in_specs=[VMEM] * 3 + [ANY] * 6,
        out_specs=[ANY, ANY, VMEM] + [ANY] * 6,
        out_shape=[act, act, sds((1, feat), F32), g_part, g_part, sds((2, feat, g_width), F32), g_part, g_part, g_part],
        scratch_shapes=[
            pltpu.VMEM((2, CHUNKS, rows, model_dim), F32),
            row,
            pltpu.VMEM((2, 1, model_dim), F32),
            row,
            row,
            slices,
            slices,
            pltpu.VMEM((2, feat // GRAD_CHUNKS, g_width), F32),
            strip,
            strip,
            strip,
        ] + [line, line, own, pair, pair, pair, DMA((2, n_fsdp)), pair, grads, pair, pair, grad, grad, pair, own, grad, grad, line, line, own, pair, pair, pair, z_trio, pair, own, own, f_trio, f_trio],
        compiler_params=params(cid),
        name="close",
    )(d_lin, attn_out, gain, hidden, cotangent, normed, w_full, o_all, wo_all)


def tail_kernel(head_dim, blk_ref, hid_ref, mine_ref, theirs_ref, blk_out, hid_out, q_out, k_out, v_out, o_out):
    blk_out[...] = blk_ref[...]
    hid_out[...] = hid_ref[...]
    at = 0
    for ref in (q_out, k_out, v_out):
        for h in range(ref.shape[1]):
            cols = blk(at, head_dim)
            ref[:, h, :] = mine_ref[:, cols] + theirs_ref[:, cols]
            at += 1
    rest = slice(at * head_dim, None)
    o_out[...] = (mine_ref[:, rest] + theirs_ref[:, rest]).T


def tail(block_out, grad_hidden, mine, theirs, q_heads, kv_heads, head_dim):
    q_len, model_dim = block_out.shape
    feat = mine.shape[0]
    sds = jax.ShapeDtypeStruct
    act = pl.BlockSpec((q_len // GRAD_CHUNKS, model_dim), lambda i: (i, 0))
    part = pl.BlockSpec((feat // GRAD_CHUNKS, mine.shape[1]), lambda i: (i, 0))

    def heads(n):
        return pl.BlockSpec((feat // GRAD_CHUNKS, n, head_dim), lambda i: (i, 0, 0))

    def like(n):
        return sds((feat, n, head_dim), F32)

    o_rows = q_heads * head_dim
    return pl.pallas_call(
        functools.partial(tail_kernel, head_dim),
        grid=(GRAD_CHUNKS,),
        in_specs=[act, act, part, part],
        out_specs=[act, act, heads(q_heads), heads(kv_heads), heads(kv_heads), pl.BlockSpec((o_rows, feat // GRAD_CHUNKS), lambda i: (0, i))],
        out_shape=[sds(block_out.shape, BF), sds(block_out.shape, BF), like(q_heads), like(kv_heads), like(kv_heads), sds((o_rows, feat), F32)],
        compiler_params=pltpu.CompilerParams(vmem_limit_bytes=VMEM_BYTES),
        name="tail",
    )(block_out, grad_hidden, mine, theirs)


def solution(mesh):
    act_spec = P("fsdp", "cp", None)
    proj_spec = P("fsdp", "tp", None)
    wout_spec = P("tp", None, "fsdp")
    n_line = mesh.shape["tp"]

    def device_step(hidden, cotangent, positions, gain, w_query, w_key, w_value, w_out):
        hidden, cotangent = hidden[0], cotangent[0]
        assert hidden.shape[0] * mesh.shape["cp"] <= WINDOW_LEN
        feat, q_heads, head_dim = w_query.shape
        kv_heads = w_key.shape[1]
        group = q_heads // kv_heads
        q_width, kv_width = q_heads * head_dim, kv_heads * head_dim
        w_qkv = jnp.concatenate([w_query.reshape(feat, q_width), w_key.reshape(feat, kv_width), w_value.reshape(feat, kv_width)], axis=1)
        cosines, sines = rope_tables(positions, head_dim)
        attn_out, q_rot, lse, k_loc, v_loc, k_prev, v_prev, gain_full, normed, w_full, wo_all, o_all = front(hidden, gain.astype(F32)[None], w_qkv, w_out.reshape(q_width, feat), cosines, sines, group, kv_width, n_line, 0)
        d_lin, o_all, wo_all = attn_back(attn_out, q_rot, lse, cosines, sines, k_loc, v_loc, k_prev, v_prev, wo_all, o_all, cotangent, n_line, group, 1)
        grad_hidden, block_out, grad_gain, mine, theirs = close(d_lin, attn_out, gain_full, hidden, cotangent, normed, w_full, o_all, wo_all, 2)[:5]
        block_out, grad_hidden, g_query, g_key, g_value, g_out = tail(block_out, grad_hidden, mine, theirs, q_heads, kv_heads, head_dim)
        return block_out[None], grad_hidden[None], grad_gain[0], g_query, g_key, g_value, g_out.reshape(w_out.shape)

    specs = (act_spec, act_spec, P("fsdp"), proj_spec, proj_spec, proj_spec, wout_spec)
    return jax.shard_map(device_step, mesh=mesh, in_specs=specs[:2] + (P("cp"),) + specs[2:], out_specs=specs, check_vma=False)
```

```python
import functools
import math

import jax
import jax.numpy as jnp
from jax import lax
from jax.experimental import pallas as pl
from jax.experimental.pallas import tpu as pltpu
from jax.sharding import PartitionSpec as P

WINDOW_LEN = 4096
ROPE_BASE = 10000.0
NORM_EPS = 1e-5
NEG_BIG = -1e30
LOG2E = math.log2(math.e)
TILES = 4
CHUNKS = 16
PER_STEP = 1
LEAD = 2
PIECES = 8
O_PIECES = 2
GRAD_CHUNKS = 8
FIRST_X = 5
EARLY = 6
LATE = ((6, 2), (7, 7))
VMEM_BYTES = 67043328
SIDES = range(2)

MESH = pl.DeviceIdType.MESH
ANY = pl.BlockSpec(memory_space=pl.ANY)
VMEM = pl.BlockSpec(memory_space=pltpu.VMEM)
DMA = pltpu.SemaphoreType.DMA
BF, F32 = jnp.bfloat16, jnp.float32

NT = (((1,), (1,)), ((), ()))
NN = (((1,), (0,)), ((), ()))
TN = (((0,), (0,)), ((), ()))


def dot(a, b, dims):
    return lax.dot_general(a, b, dims, preferred_element_type=F32)


def parity(k):
    return lax.rem(k, 2)


def blk(k, n):
    return pl.ds(k * n if isinstance(k, int) else pl.multiple_of(k * n, n), n)


def lane_mean(vals):
    return jnp.mean(vals, axis=1, keepdims=True)


def row_sum(vals):
    return jnp.sum(vals, axis=0, keepdims=True)


def zero(ref):
    ref[...] = jnp.zeros_like(ref)


def remote(src, dst, send, recv, where):
    return pltpu.make_async_remote_copy(src_ref=src, dst_ref=dst, send_sem=send, recv_sem=recv, device_id=where, device_id_type=MESH)


def meet(peers):
    barrier = pltpu.get_barrier_semaphore()
    for where in peers:
        pl.semaphore_signal(barrier, inc=1, device_id=where, device_id_type=MESH)
    pl.semaphore_wait(barrier, len(peers))


def fsdp_peers(f):
    core = parity(f)
    other = f + 1 - 2 * core
    far = lax.rem(f + 2, 4)
    return other, far, lax.rem(other + 2, 4)


def others(axis, index, count):
    return [{axis: lax.rem(index + k, count)} for k in range(1, count)]


def nearest(z, last):
    near = jnp.where(z > 0, last, 1)
    second = jnp.where(z == 0, 2, jnp.where(z == last, last - 1, 1))
    return near, second


def rope(vals, cos, sin, half_dim):
    return vals * cos + pltpu.roll(vals, half_dim, 1) * sin


def causal(scores, tq):
    key_idx = lax.broadcasted_iota(jnp.int32, scores.shape, 0)
    q_idx = lax.rem(lax.broadcasted_iota(jnp.int32, scores.shape, 1), tq)
    return jnp.where(key_idx <= q_idx, scores, NEG_BIG)


def params(cid):
    return pltpu.CompilerParams(collective_id=cid, has_side_effects=True, vmem_limit_bytes=VMEM_BYTES)


def rope_tables(positions, head_dim):
    inv_freq = ROPE_BASE ** (-jnp.arange(0, head_dim, 2).astype(F32) / head_dim)
    angles = positions.astype(F32)[:, None] * inv_freq[None, :]
    cosines, sines = jnp.cos(angles), jnp.sin(angles)
    return jnp.concatenate([cosines, cosines], axis=1), jnp.concatenate([-sines, sines], axis=1)


def core_kernel(group, n_line, hid_ref, gain_ref, w_ref, wo_ref, cos_ref, sin_ref, ct_ref, d_ref, o_ref, gfull_ref, n_out, w_out, wo_all, o_all, wbuf, nbuf, acc, hbuf, gbuf, qs, vt, m_all, l_all, acc_all, q_ref, lse_ref, kl_ref, vl_ref, kp_ref, vp_ref, do_ref, dkl_ref, dvl_ref, dkp_ref, dvp_ref, qs_ref, dos_ref, delta_ref, kt_ref, dqt_ref, h_sem, g_send, g_recv, own_send, own_recv, x_send, x_recv, y_send, y_recv, d_send, d_recv, kv_send, kv_recv, ox_send, ox_recv, oy_send, oy_recv, od_send, od_recv, zw_send, zw_recv, out_sem, ct_sem, on_send, ou_send, o_recv, wy_send, wy_recv, wx_send, wx_recv, wc_send, wc_recv, cx_send, cx_recv, dk_send, dk_recv):
    q_len, feat = hid_ref.shape[0], w_ref.shape[0]
    head_dim = cos_ref.shape[1]
    half_dim = head_dim // 2
    kv_width = kl_ref.shape[1]
    kv_heads = kv_width // head_dim
    q_width = q_ref.shape[1]
    tq = q_len // TILES
    wide = group * tq
    score_scale = head_dim ** -0.5
    scale = head_dim ** -0.5 * LOG2E
    half = feat // 2
    piece = half // PIECES
    o_rows = wo_ref.shape[0]
    o_half = o_rows // 2
    o_piece = o_half // O_PIECES
    flag, f, z = lax.axis_index("cp"), lax.axis_index("fsdp"), lax.axis_index("tp")
    wo_out = wo_all.at[z]
    last = n_line - 1
    far = 1 - flag
    f_core, f_x, f_diag = fsdp_peers(f)
    to_core, to_x, to_diag, to_y = {"fsdp": f_core}, {"fsdp": f_x}, {"fsdp": f_diag}, {"cp": far}

    def h_load(tile):
        slot = parity(tile)
        return pltpu.make_async_copy(hid_ref.at[blk(tile, tq)], hbuf.at[slot], h_sem.at[slot])

    h_load(0).start()
    h_load(1).start()
    meet([to_core, to_x, to_diag, to_y] + others("tp", z, n_line))

    def span(side, j):
        return blk(side * PIECES + j, piece)

    def x_copy(j):
        return remote(w_ref.at[span(flag, j)], wbuf.at[f, span(flag, j)], x_send.at[j], x_recv.at[j], to_x)

    def x_in(j):
        return remote(w_ref.at[span(flag, j)], wbuf.at[f_x, span(flag, j)], x_send.at[j], x_recv.at[j], to_x)

    def y_copy(j, side):
        return remote(wbuf.at[f_x, span(side, j)], wbuf.at[f_x, span(side, j)], y_send.at[j], y_recv.at[j], to_y)

    def d_copy(j, side, slot):
        return remote(wbuf.at[slot, span(side, j)], wbuf.at[slot, span(side, j)], d_send.at[side, j], d_recv.at[side, j], to_core)

    def g_copy(k, where, slot):
        return remote(gain_ref, gbuf.at[slot], g_send.at[k], g_recv.at[k], where)

    def own_copy(slot):
        return remote(w_ref, wbuf.at[slot], own_send, own_recv, to_core)

    def o_span(side, j):
        return blk(side * O_PIECES + j, o_piece)

    def ox_copy(j, slot):
        return remote(wo_ref.at[o_span(flag, j)], wo_out.at[slot, o_span(flag, j)], ox_send.at[j], ox_recv.at[j], to_x)

    def oy_copy(j, side):
        return remote(wo_out.at[f_x, o_span(side, j)], wo_out.at[f_x, o_span(side, j)], oy_send.at[j], oy_recv.at[j], to_y)

    def od_copy(k, src, slot, where):
        return remote(src, wo_out.at[slot, where], od_send.at[k], od_recv.at[k], to_core)

    def zw_copy(up, t):
        spot = wo_all.at[t, f, blk(flag, o_half)]
        where = jnp.minimum(z + 1, last) if up else jnp.maximum(z - 1, 0)
        src = spot if t is not z else wo_ref.at[blk(flag, o_half)]
        return remote(src, spot, zw_send.at[up, t], zw_recv.at[t], {"tp": where})

    def zw_tick(r):
        for up, t, here in ((0, z + r, z + r <= last), (1, z - r, z >= r)):
            at = jnp.clip(t, 0, last)

            @pl.when(here)
            def _():
                zw_copy(up, at).wait_recv()

            @pl.when(here & (z < last if up else z > 0))
            def _():
                zw_copy(up, at).start()

    def tile_rows(j):
        return blk(j, tq)

    def o_down(t, j, src):
        return remote(src, o_all.at[t, tile_rows(j)], on_send.at[t, j], o_recv.at[t, j], {"tp": jnp.maximum(z - 1, 0)})

    def o_up(t, j, src):
        return remote(src, o_all.at[t, tile_rows(j)], ou_send.at[t, j], o_recv.at[t, j], {"tp": jnp.minimum(z + 1, last)})

    def wo_half(r, slot, side):
        return wo_all.at[lax.rem(z + r, n_line), slot, blk(side, o_half)]

    def wy_copy(r, side):
        return remote(wo_half(r, f, side), wo_half(r, f, side), wy_send.at[r - 1], wy_recv.at[r - 1], to_y)

    def wx_copy(r, side, slot):
        return remote(wo_half(r, slot, side), wo_half(r, slot, side), wx_send.at[side, r - 1], wx_recv.at[side, r - 1], to_x)

    def wc_copy(r, side, slot):
        return remote(wo_half(r, slot, side), wo_half(r, slot, side), wc_send.at[side, r - 1], wc_recv.at[side, r - 1], to_core)

    def cx_copy(r, side, slot):
        return remote(wo_half(r, slot, side), wo_half(r, slot, side), cx_send.at[side, r - 1], cx_recv.at[side, r - 1], to_core)

    def o_tick(k):
        r, j = k // TILES + 1, lax.rem(k, TILES)

        @pl.when(z + r <= last)
        def _():
            t = jnp.minimum(z + r, last)
            o_down(t, j, o_all.at[t, tile_rows(j)]).wait_recv()

            @pl.when(z > 0)
            def _():
                o_down(t, j, o_all.at[t, tile_rows(j)]).start()

        @pl.when(z - r >= 0)
        def _():
            t = jnp.maximum(z - r, 0)
            o_up(t, j, o_all.at[t, tile_rows(j)]).wait_recv()

            @pl.when(z < last)
            def _():
                o_up(t, j, o_all.at[t, tile_rows(j)]).start()

    def wy_tick(r):
        wy_copy(r, far).wait_recv()
        wx_copy(r, far, f).start()
        for side in (flag, far):
            wc_copy(r, side, f).start()
        if r == 1:
            wy_copy(last, flag).start()

    near, second = nearest(z, last)
    own_order = (near, second, n_line * last // 2 - near - second)

    def wx_tick(q):
        r, side = (own_order[q], flag) if q < last else (q - last + 1, far)
        wx_copy(r, side, f_x).wait_recv()
        cx_copy(r, side, f_x).start()

    def o_send(j):
        @pl.when(z > 0)
        def _():
            o_down(z, j, o_ref.at[tile_rows(j)]).start()

        @pl.when(z < last)
        def _():
            o_up(z, j, o_ref.at[tile_rows(j)]).start()

    gains = [(k, where, where["fsdp"]) for k, where in enumerate((to_core, to_x, to_diag))]
    for k, where, _ in gains:
        g_copy(k, where, f).start()
    sends = [x_copy(j) for j in range(PIECES)] + [ox_copy(j, f) for j in range(O_PIECES)]
    for j in range(LEAD):
        sends[j].start()
    own_copy(f).start()
    all_rows = pl.ds(0, o_rows)
    for up in SIDES:
        @pl.when(z < last if up else z > 0)
        def _():
            zw_copy(up, z).start()

    local_w = pltpu.make_async_copy(w_ref, wbuf.at[f], out_sem.at[0])
    local_w.start()
    local_o = pltpu.make_async_copy(wo_ref, wo_out.at[f], out_sem.at[1])
    local_o.start()
    gbuf[f] = gain_ref[...]
    for k, where, slot in gains:
        g_copy(k, where, slot).wait_recv()
    for k in range(gbuf.shape[0]):
        gfull_ref[:, blk(k, feat)] = gbuf[k]

    for tile in range(TILES):
        h_load(tile).wait()
        strip = min(32, tq)

        @pl.loop(0, tq // strip)
        def _(i):
            vals = hbuf[tile % 2, blk(i, strip), :].astype(F32)
            inv = lax.rsqrt(lane_mean(vals * vals) + NORM_EPS)
            nbuf[pl.ds(pl.multiple_of(tile * tq + i * strip, strip), strip), :] = (vals * inv * gfull_ref[...]).astype(BF)

        if tile + 2 < TILES:
            h_load(tile + 2).start()
    put_n = pltpu.make_async_copy(nbuf.at[pl.ds(0, q_len)], n_out, out_sem.at[2])
    put_n.start()

    def project(slot, start, rows, first=False):
        cols = pl.ds(pl.multiple_of(slot * feat + start, 128), rows)

        @pl.loop(0, TILES)
        def _(tile):
            here = blk(tile, tq)
            part = dot(nbuf[here, cols], wbuf[slot, pl.ds(start, rows), :], NN)
            acc[here, :] = part if first else acc[here, :] + part

    def x_tick(j):
        x_in(j).wait_recv()
        y_copy(j, flag).start()
        d_copy(j, flag, f_x).start()
        sends[j + LEAD].start()

    def y_tick(j):
        y_copy(j, far).wait_recv()
        d_copy(j, 1 - flag, f_x).start()

    local_w.wait()
    project(f, 0, feat, first=True)
    x_tick(0)
    x_tick(1)
    own_copy(f_core).wait_recv()
    od_copy(0, wo_ref, f, all_rows).start()
    project(f_core, 0, feat)
    for j in range(2, PIECES):
        x_tick(j)
        y_tick(j - 2)
        if j == PIECES // 2:
            zw_tick(1)
    for j in range(PIECES):
        d_copy(j, flag, f_diag).wait_recv()
    first_half = pl.multiple_of(flag * half, half)
    project(f_x, first_half, half)
    y_tick(PIECES - 2)
    project(f_diag, first_half, half)
    y_tick(PIECES - 1)
    for j in range(PIECES):
        d_copy(j, far, f_diag).wait_recv()
    second_half = pl.multiple_of(far * half, half)
    project(f_x, second_half, half)
    project(f_diag, second_half, half)
    zw_tick(2)
    wx_copy(near, flag, f).start()
    put_w = pltpu.make_async_copy(wbuf, w_out, out_sem.at[3])
    put_w.start()

    @pl.loop(0, TILES)
    def _(tile):
        here = blk(tile, tq)
        cos, sin = cos_ref[here, :], sin_ref[here, :]
        for h in range(kv_heads):
            k_at = q_width // head_dim + h
            kl_ref[here, blk(h, head_dim)] = rope(acc[here, blk(k_at, head_dim)], cos, sin, half_dim).astype(BF)
            vl_ref[here, blk(h, head_dim)] = acc[here, blk(k_at + kv_heads, head_dim)].astype(BF)

    kv_pairs = ((kl_ref, kp_ref), (vl_ref, vp_ref))

    def kv_copies(g):
        return [remote(src.at[:, blk(g, head_dim)], dst.at[:, blk(g, head_dim)], kv_send.at[k, g], kv_recv.at[k, g], {"cp": 1}) for k, (src, dst) in enumerate(kv_pairs)]

    @pl.when(flag == 0)
    def _():
        zero(kp_ref)
        zero(vp_ref)
        for g in range(kv_heads):
            for copy in kv_copies(g):
                copy.start()

    @pl.loop(0, TILES)
    def _(tile):
        here = blk(tile, tq)
        cos, sin = cos_ref[here, :], sin_ref[here, :]
        for h in range(group * kv_heads):
            cols = blk(h, head_dim)
            q_ref[here, cols] = rope(acc[here, cols], cos, sin, half_dim).astype(BF)

    def load_q(item):
        g, tile = item // TILES, lax.rem(item, TILES)
        rows = blk(tile, tq)
        for h in range(group):
            qs[:, blk(h, tq)] = q_ref[rows, blk(g * group + h, head_dim)].T

    def key_piece(item, k_ref, side, start, masked):
        g = item // TILES
        scores = dot(k_ref[start, blk(g, head_dim)], qs[...], NN)
        if masked:
            scores = causal(scores, tq)
        m_old = m_all[item]
        m_new = jnp.maximum(m_old, jnp.max(scores, axis=0, keepdims=True))
        probs = jnp.exp2((scores - m_new) * scale)
        fade = jnp.exp2((m_old - m_new) * scale)
        m_all[item] = m_new
        l_all[item] = l_all[item] * fade + row_sum(probs)
        acc_all[item] = acc_all[item] * fade + dot(vt[g, side, :, start], probs.astype(BF), NN)

    for g in range(kv_heads):
        vt[g, 0] = vl_ref[:, blk(g, head_dim)].T

    @pl.loop(0, kv_heads * TILES)
    def _(item):
        tile = lax.rem(item, TILES)
        load_q(item)
        m_all[item] = jnp.full_like(m_all[item], NEG_BIG)
        l_all[item] = jnp.zeros_like(l_all[item])
        acc_all[item] = jnp.zeros_like(acc_all[item])
        key_piece(item, kl_ref, 0, blk(tile, tq), True)

        @pl.loop(0, tile // 2)
        def _(i):
            key_piece(item, kl_ref, 0, blk(i, 2 * tq), False)

        @pl.when(parity(tile) == 1)
        def _():
            key_piece(item, kl_ref, 0, blk(tile - 1, tq), False)

    for j in range(O_PIECES):
        ox_copy(j, f_x).wait_recv()
        oy_copy(j, flag).start()
        od_copy(1 + j, wo_out.at[f_x, o_span(flag, j)], f_x, o_span(flag, j)).start()

    wx_copy(second, flag, f).start()
    zw_tick(last)

    @pl.loop(0, kv_heads * TILES)
    def _(item):
        g, tile = item // TILES, lax.rem(item, TILES)
        rows = blk(tile, tq)

        @pl.when((flag == 1) & (tile == 0))
        def _():
            for copy in kv_copies(g):
                copy.wait_recv()
            vt[g, 1] = vp_ref[:, blk(g, head_dim)].T

        @pl.when(flag == 1)
        def _():
            load_q(item)

        @pl.loop(0, flag * TILES // 2)
        def _(i):
            key_piece(item, kp_ref, 1, blk(i, 2 * tq), False)

        total = l_all[item]
        lse_ref[item] = m_all[item] * scale + jnp.log2(total)
        out_t = acc_all[item] / total
        for h in range(group):
            o_ref[rows, blk(g * group + h, head_dim)] = out_t[:, h * tq:h * tq + tq].T.astype(BF)

        ready = item - TILES * (kv_heads - 1) - 1

        @pl.when(ready >= 0)
        def _():
            o_send(ready)

        for j in range(O_PIECES):
            @pl.when(item == (j + 1) * kv_heads * TILES // O_PIECES - 1)
            def _():
                oy_copy(j, far).wait_recv()
                od_copy(1 + O_PIECES + j, wo_out.at[f_x, o_span(1 - flag, j)], f_x, o_span(1 - flag, j)).start()

    o_send(TILES - 1)
    wx_copy(own_order[last - 1], flag, f).start()
    for r in range(1, last):
        wy_copy(r, flag).start()
    od_copy(0, wo_ref, f_core, all_rows).wait_recv()
    for j in range(O_PIECES):
        od_copy(1 + j, wo_out.at[f_x, o_span(flag, j)], f_diag, o_span(flag, j)).wait_recv()
        od_copy(1 + O_PIECES + j, wo_out.at[f_x, o_span(1 - flag, j)], f_diag, o_span(1 - flag, j)).wait_recv()

    put_n.wait()
    local_o.wait()
    n_parts, _, part = wo_out.shape
    loads = [pltpu.make_async_copy(wo_out.at[k], nbuf.at[pl.ds(0, o_rows), blk(k, part)], out_sem.at[4 + k]) for k in range(n_parts)]
    for load in loads:
        load.start()
    keep = pltpu.make_async_copy(o_ref, o_all.at[z], out_sem.at[2])
    keep.start()

    def ct_load(tile):
        slot = parity(tile)
        return pltpu.make_async_copy(ct_ref.at[blk(tile, tq)], hbuf.at[slot], ct_sem.at[slot])

    ct_load(0).start()
    ct_load(1).start()
    zero(dkl_ref)
    zero(dvl_ref)

    @pl.when(flag == 1)
    def _():
        zero(dkp_ref)
        zero(dvp_ref)

    wx_tick(0)
    o_tick(jnp.int32(0))
    for load in loads:
        load.wait()

    def do_tile(tile):
        ct_load(tile).wait()
        do_ref[tile_rows(tile), :] = dot(hbuf[parity(tile)], nbuf[pl.ds(0, o_rows), :], NT).astype(BF)

        @pl.when(tile + 2 < TILES)
        def _():
            ct_load(tile + 2).start()

    def bwd_item(item):
        g, tile = item // TILES, lax.rem(item, TILES)
        kv_cols = blk(g, head_dim)
        rows = blk(tile, tq)

        @pl.when(tile == 0)
        def _():
            kt_ref[0] = kl_ref[:, kv_cols].T
            kt_ref[1] = kp_ref[:, kv_cols].T

        for h in range(group):
            cols = blk(g * group + h, head_dim)
            stack = blk(h, tq)
            qs_ref[stack, :] = q_ref[rows, cols]
            d_h = do_ref[rows, cols]
            dos_ref[stack, :] = d_h
            prod = d_h.astype(F32) * o_ref[rows, cols].astype(F32)
            delta_ref[:, stack] = row_sum(prod.T)
        zero(dqt_ref)

        def piece(k_ref, v_ref, dk_ref, dv_ref, side, span, masked):
            scores = dot(k_ref[span, kv_cols], qs_ref[...], NT)
            if masked:
                scores = causal(scores, tq)
            probs = jnp.exp2(scores * (score_scale * LOG2E) - lse_ref[item])
            d_probs = dot(v_ref[span, kv_cols], dos_ref[...], NT)
            d_scores = (probs * (d_probs - delta_ref[...])).astype(BF)
            dv_ref[g, span, :] += dot(probs.astype(BF), dos_ref[...], NN)
            dk_ref[g, span, :] += dot(d_scores, qs_ref[...], NN)
            dqt_ref[...] += dot(kt_ref[side, :, span], d_scores, NN)

        piece(kl_ref, vl_ref, dkl_ref, dvl_ref, 0, blk(tile, tq), True)

        @pl.loop(0, tile // 2)
        def _(i):
            piece(kl_ref, vl_ref, dkl_ref, dvl_ref, 0, blk(i, 2 * tq), False)

        @pl.when(parity(tile) == 1)
        def _():
            piece(kl_ref, vl_ref, dkl_ref, dvl_ref, 0, blk(tile - 1, tq), False)

        @pl.loop(0, flag * TILES // 2)
        def _(i):
            piece(kp_ref, vp_ref, dkp_ref, dvp_ref, 1, blk(i, 2 * tq), False)

        for h in range(group):
            dq_h = dqt_ref[:, blk(h, tq)].T * score_scale
            d_ref[rows, blk(g * group + h, head_dim)] = rope(dq_h, cos_ref[rows, :], -sin_ref[rows, :], half_dim).astype(BF)

        @pl.when((tile == TILES - 1) & (flag == 1))
        def _():
            for copy in back(g):
                copy.start()

    def back(g):
        return [remote(ref.at[g], ref.at[g], dk_send.at[k, g], dk_recv.at[k, g], {"cp": 0}) for k, ref in enumerate((dkp_ref, dvp_ref))]

    def kv_done(g):
        @pl.when(flag == 0)
        def _():
            for copy in back(g):
                copy.wait_recv()
            dkl_ref[g] += dkp_ref[g]
            dvl_ref[g] += dvp_ref[g]

        dk = rope(dkl_ref[g] * score_scale, cos_ref[...], -sin_ref[...], half_dim)
        k_at = q_width // head_dim + g
        d_ref[:, blk(k_at, head_dim)] = dk.astype(BF)
        d_ref[:, blk(k_at + kv_heads, head_dim)] = dvl_ref[g].astype(BF)

        @pl.when(flag == 1)
        def _():
            for copy in back(g):
                copy.wait_send()

    items = TILES * (kv_heads + 1)
    plan = {1: [(o_tick, 1), (wx_tick, 1)], 4: [(o_tick, 2)], 5: [(wy_tick, 1)], 6: [(o_tick, 3), (wx_tick, 2)], 8: [(o_tick, 4), (wy_tick, 2)], 9: [(o_tick, 5), (wx_tick, 3)], 11: [(o_tick, 6)]}

    def run(tick, arg):
        tick(jnp.int32(arg) if tick is o_tick else arg)

    @pl.loop(0, items)
    def _(item):
        @pl.when(item < TILES)
        def _():
            do_tile(item)

        @pl.when(item >= TILES)
        def _():
            bwd_item(item - TILES)

        for at, jobs in plan.items():
            @pl.when(item == at)
            def _():
                for tick, arg in jobs:
                    run(tick, arg)

    for tick, arg in [(wy_tick, 3), (o_tick, 7), (wx_tick, 4), (o_tick, 8), (kv_done, 0), (o_tick, 9), (wx_tick, 5), (o_tick, 10), (kv_done, 1), (o_tick, 11)]:
        run(tick, arg)

    for r in range(1, n_line):
        for side in (flag, far):
            wc_copy(r, side, f_core).wait_recv()
            cx_copy(r, side, f_diag).wait_recv()
            wc_copy(r, side, f).wait_send()
            cx_copy(r, side, f_x).wait_send()
            wx_copy(r, side, f).wait_send()
        wy_copy(r, flag).wait_send()

    @pl.loop(0, n_line)
    def _(t):
        for j in range(TILES):
            @pl.when((t >= z) & (z > 0))
            def _():
                o_down(t, j, o_all.at[t, tile_rows(j)]).wait_send()

            @pl.when((t <= z) & (z < last))
            def _():
                o_up(t, j, o_all.at[t, tile_rows(j)]).wait_send()

    @pl.loop(0, n_line)
    def _(t):
        for up in SIDES:
            @pl.when((t <= z) & (z < last) if up else (t >= z) & (z > 0))
            def _():
                zw_copy(up, t).wait_send()

    for k, where, _ in gains:
        g_copy(k, where, f).wait_send()
    own_copy(f).wait_send()
    od_copy(0, wo_ref, f, all_rows).wait_send()
    for j in range(PIECES):
        x_copy(j).wait_send()
        y_copy(j, flag).wait_send()
        d_copy(j, flag, f_x).wait_send()
        d_copy(j, 1 - flag, f_x).wait_send()
    for j in range(O_PIECES):
        ox_copy(j, f).wait_send()
        oy_copy(j, flag).wait_send()
        od_copy(1 + j, wo_out.at[f_x, o_span(flag, j)], f_x, o_span(flag, j)).wait_send()
        od_copy(1 + O_PIECES + j, wo_out.at[f_x, o_span(1 - flag, j)], f_x, o_span(1 - flag, j)).wait_send()

    @pl.when(flag == 0)
    def _():
        for g in range(kv_heads):
            for copy in kv_copies(g):
                copy.wait_send()

    for local in (keep, put_w):
        local.wait()


def core(hidden, gain, w_qkv, w_out, cosines, sines, cotangent, group, kv_width, n_line, cid):
    q_len, model_dim = hidden.shape
    feat, width = w_qkv.shape
    head_dim = cosines.shape[1]
    q_width = width - 2 * kv_width
    kv_heads = kv_width // head_dim
    o_rows, o_cols = w_out.shape
    n_fsdp = model_dim // feat
    tq = q_len // TILES
    wide = group * tq
    items = kv_heads * TILES
    sds = jax.ShapeDtypeStruct
    line = pltpu.VMEM((items, 1, wide), F32)
    kv = pltpu.VMEM((q_len, kv_width), BF)
    heads = pltpu.VMEM((q_len, q_width), BF)
    sums = pltpu.VMEM((kv_heads, q_len, head_dim), F32)
    stack = pltpu.VMEM((wide, head_dim), BF)
    own, pair, trio = DMA(()), DMA((2,)), DMA((n_fsdp - 1,))
    w_link, w_side, o_link, o_core = DMA((PIECES,)), DMA((2, PIECES)), DMA((O_PIECES,)), DMA((1 + 2 * O_PIECES,))
    tiles, hop, side, dkv = DMA((n_line, TILES)), DMA((n_line - 1,)), DMA((2, n_line - 1)), DMA((2, kv_heads))
    return pl.pallas_call(
        functools.partial(core_kernel, group, n_line),
        in_specs=[ANY] + [VMEM] * 5 + [ANY],
        out_specs=[VMEM] * 3 + [ANY] * 4,
        out_shape=[sds((q_len, width), BF), sds((q_len, q_width), BF), sds((1, model_dim), F32), sds((q_len, model_dim), BF), sds((n_fsdp, feat, width), BF), sds((n_line, n_fsdp, o_rows, o_cols), BF), sds((n_line, q_len, q_width), BF)],
        scratch_shapes=[
            pltpu.VMEM((n_fsdp, feat, width), BF),
            pltpu.VMEM((max(q_len, o_rows), model_dim), BF),
            pltpu.VMEM((q_len, width), F32),
            pltpu.VMEM((2, tq, model_dim), BF),
            pltpu.VMEM((n_fsdp, 1, feat), F32),
            pltpu.VMEM((head_dim, wide), BF),
            pltpu.VMEM((kv_heads, 2, head_dim, q_len), BF),
            line,
            line,
            pltpu.VMEM((items, head_dim, wide), F32),
            heads,
            line,
            kv, kv, kv, kv,
            heads,
            sums, sums, sums, sums,
            stack,
            stack,
            pltpu.VMEM((1, wide), F32),
            pltpu.VMEM((2, head_dim, q_len), BF),
            pltpu.VMEM((head_dim, wide), F32),
        ] + [pair, trio, trio, own, own, w_link, w_link, w_link, w_link, w_side, w_side, dkv, dkv, o_link, o_link, o_link, o_link, o_core, o_core, DMA((2, n_line)), DMA((n_line,)), DMA((4 + n_fsdp,)), pair, tiles, tiles, tiles, hop, hop, side, side, side, side, side, side, dkv, dkv],
        compiler_params=params(cid),
        name="core",
    )(hidden, gain, w_qkv, w_out, cosines, sines, cotangent)


class Line:
    def __init__(self, n_line, buf_ref, pbuf_ref, send_sem, recv_sem, fill, finish):
        self.last = n_line - 1
        self.z = lax.axis_index("tp")
        self.buf, self.pbuf, self.send_sem, self.recv_sem = buf_ref, pbuf_ref, send_sem, recv_sem
        self.chunks, self.rows = buf_ref.shape[1], buf_ref.shape[2]
        self.block = pbuf_ref.shape[1]
        self.per_block = self.block // self.rows
        self.fill, self.finish = fill, finish
        self.steps = self.chunks + self.last

    def dist(self, side):
        return self.z if side else self.last - self.z

    def toward(self, side, back=False):
        up = bool(side) != back
        return {"tp": jnp.clip(self.z + 1 if up else self.z - 1, 0, self.last)}

    def copy(self, side, chunk):
        spot = self.buf.at[side, chunk]
        return remote(spot, spot, self.send_sem.at[side, chunk], self.recv_sem.at[side, chunk], self.toward(side))

    def live(self, side, step):
        chunk = step - self.dist(side)
        return chunk, (chunk >= 0) & (chunk < self.chunks)

    def prepare(self, step):
        for side in SIDES:
            chunk, ok = self.live(side, step)

            @pl.when(ok & (lax.rem(chunk, self.per_block) == 0))
            def _():
                self.fill(self.pbuf.at[side], blk((side * self.chunks + chunk) // self.per_block, self.block))

    def tick(self, step):
        for side in SIDES:
            chunk, ok = self.live(side, step)
            dist = self.dist(side)
            part = blk(lax.rem(jnp.maximum(chunk, 0), self.per_block), self.rows)

            @pl.when(ok & (dist == 0))
            def _():
                self.buf[side, chunk] = self.pbuf[side, part, :]

            @pl.when(ok & (dist > 0))
            def _():
                self.copy(side, chunk).wait_recv()
                self.buf[side, chunk] += self.pbuf[side, part, :]

            @pl.when(ok & (dist < self.last))
            def _():
                self.copy(side, chunk).start()

            @pl.when(ok & (dist == self.last))
            def _():
                self.finish(chunk, self.buf[side, chunk])

        self.prepare(step + 1)

    def drain(self):
        for side in SIDES:
            @pl.when(self.dist(side) < self.last)
            def _():
                @pl.loop(0, self.chunks)
                def _(chunk):
                    self.copy(side, chunk).wait_send()


def close_kernel(n_line, n_fsdp, d_ref, o_ref, gain_ref, hid_ref, ct_ref, n_ref, w_all, o_all, wo_all, out_ref, blk_ref, gg_ref, ts, yr, dl, xs, ks, xr, buf, gp, ga, gs, gb, gt, gc, ebuf, fb_in, fb_ct, fb_out, send_sem, recv_sem, w_sem, f_sem, ct_sem, fo_sem, lhs_sem, a_send, a_recv, ld_sem, st_sem, x_send, x_recv, e_sem, es_sem, y_send, y_recv, out_send, out_recv, o_sem, wl_sem, h_sem, r_sem, ga_send, ga_recv, gb_send, gb_recv, gc_send, gc_recv):
    last = n_line - 1
    z, flag, f = lax.axis_index("tp"), lax.axis_index("cp"), lax.axis_index("fsdp")
    far = 1 - flag
    f_core, f_x, f_diag = fsdp_peers(f)
    to_core, to_x, to_y = {"fsdp": f_core}, {"fsdp": f_x}, {"cp": far}
    _, feat, width = w_all.shape
    chunks, rows = buf.shape[1], buf.shape[2]
    half = chunks * rows
    g_rows = feat // GRAD_CHUNKS
    owner = (z == 0) | (z == last)
    own_base = jnp.where(z == last, chunks, 0)
    copy = pltpu.make_async_copy

    def own_span(chunk):
        return blk(own_base + chunk, rows)

    def f_loads(chunk):
        slot = parity(chunk)
        return copy(hid_ref.at[own_span(chunk)], fb_in.at[slot], f_sem.at[slot]), copy(ct_ref.at[own_span(chunk)], fb_ct.at[slot], ct_sem.at[slot])

    def f_store(chunk):
        slot = parity(chunk)
        return copy(fb_out.at[slot], out_ref.at[own_span(chunk)], fo_sem.at[slot])

    @pl.when(owner)
    def _():
        for chunk in SIDES:
            for load in f_loads(chunk):
                load.start()

    zero(gp)
    meet([to_core, to_x, to_y] + others("tp", z, n_line) + [{"fsdp": f_diag}])

    def finish(chunk, total):
        slot = parity(chunk)
        for load in f_loads(chunk):
            load.wait()

        @pl.when(chunk > 1)
        def _():
            f_store(chunk - 2).wait()

        x_in = fb_in[slot].astype(F32)
        inv = lax.rsqrt(lane_mean(x_in * x_in) + NORM_EPS)
        x_hat = x_in * inv
        gp[...] += row_sum(total * x_hat)
        scaled = total * gain_ref[...]
        fb_out[slot] = (fb_ct[slot].astype(F32) + inv * (scaled - x_hat * lane_mean(scaled * x_hat))).astype(BF)
        f_store(chunk).start()

        @pl.when(chunk + 2 < chunks)
        def _():
            for load in f_loads(chunk + 2):
                load.start()

    kinds = range(2)

    def g_at(ref, j):
        return ref.at[blk(j, g_rows)]

    def x_copy(j):
        return remote(g_at(xs, j), g_at(xr, j), x_send.at[j], x_recv.at[j], to_x)

    def y_copy(j):
        return remote(g_at(ts, j), g_at(yr, j), y_send.at[j], y_recv.at[j], to_y)

    def e_store(j):
        return copy(ebuf.at[0], g_at(ts, j), es_sem)

    def meet_x(j):
        x_copy(j).wait_recv()
        loads = [copy(g_at(src, j), ebuf.at[k], e_sem.at[k]) for k, src in enumerate((ks, xr))]
        for load in loads:
            load.start()
        for load in loads:
            load.wait()
        ebuf[0] += ebuf[1]
        e_store(j).start()

    def send_y(j):
        e_store(j).wait()
        y_copy(j).start()

    steps = chunks + last - 1

    def dist(side):
        return z if side else last - z

    def hop(side, chunk):
        span = blk(side * chunks + chunk, rows)
        up = z - 1 if side else z + 1
        return remote(out_ref.at[span], out_ref.at[span], out_send.at[side, chunk], out_recv.at[side, chunk], {"tp": jnp.clip(up, 0, last)})

    ends = [(end, z == (last if end else 0)) for end in SIDES]

    def owner_send(first, stop):
        for end, here in ends:
            @pl.when(here)
            def _():
                @pl.loop(first, stop)
                def _(c):
                    hop(end, c).start()

    def pass_on(step):
        for side in SIDES:
            chunk = step - (last - 1 - dist(side))

            @pl.when((dist(side) < last) & (chunk >= 0) & (chunk < chunks))
            def _():
                hop(side, chunk).wait_recv()

                @pl.when(dist(side) > 0)
                def _():
                    hop(side, chunk).start()

    def sum_phase(wbuf, pbuf, abuf, bbuf, lbuf, lhs):
        w_load = copy(w_all, wbuf, w_sem)
        w_load.start()

        def fill(dst, span):
            for k in range(n_fsdp):
                dst[:, blk(k, feat)] = dot(d_ref[span, :], wbuf[k], NT)

        line = Line(n_line, buf, pbuf, send_sem, recv_sem, fill, finish)
        slots = (f_diag, f_core, f_x, f)

        def lhs_loads(j):
            return [copy(src.at[:, blk(slot * GRAD_CHUNKS + j, g_rows)], lhs.at[m, k], lhs_sem.at[m, k]) for m, src in enumerate((n_ref, ct_ref)) for k, slot in enumerate(slots)]

        def a_copy(kind, j):
            return remote(abuf.at[kind], dl.at[kind, blk(j, g_rows)], a_send.at[kind], a_recv.at[kind, j], to_core)

        def b_stores(j):
            return [copy(bbuf.at[k], g_at(dst, j), st_sem.at[k]) for k, dst in enumerate((xs, ks))]

        def send_x(j):
            for kind in kinds:
                a_copy(kind, j).wait_send()
            for store in b_stores(j):
                store.wait()
            x_copy(j).start()

        def make(j):
            for load in lhs_loads(j):
                load.wait()
            for k in range(len(slots)):
                dst = (abuf, bbuf)[k // 2].at[k % 2]
                dst[:, :width] = dot(lhs[0, k], d_ref[...], TN)
                dst[:, width:] = dot(lhs[1, k], o_ref[...], TN)
            for kind in kinds:
                a_copy(kind, j).start()

            @pl.when(j + 1 < GRAD_CHUNKS)
            def _():
                for load in lhs_loads(j + 1):
                    load.start()

        def meet_core(j):
            loads = [copy(dl.at[kind, blk(j, g_rows)], lbuf.at[kind], ld_sem.at[kind]) for kind in kinds]
            for kind in kinds:
                a_copy(kind, j).wait_recv()
                loads[kind].start()
            for kind in kinds:
                loads[kind].wait()
                bbuf[kind] += lbuf[kind]
            for store in b_stores(j):
                store.start()

        for load in lhs_loads(0):
            load.start()
        w_load.wait()
        line.prepare(0)

        @pl.loop(0, line.steps)
        def _(fine):
            line.tick(fine)
            step = fine // PER_STEP
            whole = lax.rem(fine, PER_STEP) == 0
            j, odd = step // 2, parity(step)

            @pl.when(whole & (odd == 0) & (j > 0) & (j <= GRAD_CHUNKS))
            def _():
                send_x(j - 1)

            @pl.when(whole & (odd == 0) & (j < GRAD_CHUNKS))
            def _():
                make(j)

            @pl.when(whole & (odd == 1) & (j < GRAD_CHUNKS))
            def _():
                meet_core(j)

            for late in SIDES:
                k = (step - FIRST_X - late) * 2 // 5

                @pl.when(whole & (k >= 0) & (k < EARLY) & (step - late == FIRST_X + (5 * k + 1) // 2))
                def _():
                    send_y(k) if late else meet_x(k)

            @pl.when(fine >= chunks)
            def _():
                owner_send((fine - chunks) * LEAD, (fine - chunks + 1) * LEAD)

            @pl.when(fine > chunks)
            def _():
                for k in range(PER_STEP):
                    pass_on((fine - chunks - 1) * PER_STEP + k)

        @pl.when(owner)
        def _():
            for chunk in range(chunks - 2, chunks):
                f_store(chunk).wait()

        line.drain()

    pl.run_scoped(
        sum_phase,
        pltpu.VMEM(w_all.shape, BF),
        pltpu.VMEM((2, min(128, half), buf.shape[3]), F32),
        pltpu.VMEM((2, g_rows, ts.shape[1]), F32),
        pltpu.VMEM((2, g_rows, ts.shape[1]), F32),
        pltpu.VMEM((2, g_rows, ts.shape[1]), F32),
        pltpu.VMEM((2, n_fsdp, d_ref.shape[0], g_rows), BF),
    )
    def ga_copy(end, k):
        return remote(gp, ga.at[end], ga_send.at[k], ga_recv.at[end], {"tp": k if end else 1 + k})

    def gb_copy():
        return remote(gs, gb, gb_send, gb_recv, to_y)

    def gc_copy(k, slot):
        to = lax.rem(f + k, n_fsdp)
        return remote(gt.at[to], gc.at[slot], gc_send.at[k - 1], gc_recv.at[k - 1], {"fsdp": to})

    def spread_phase(obuf, wbuf, hbuf, rbuf):
        o_load = copy(o_all, obuf, o_sem)
        o_load.start()
        q_len, n_cols = hbuf.shape[1], hbuf.shape[2]
        per_part = wo_all.shape[3] // n_cols
        items = per_part * n_fsdp

        def item_loads(item):
            slot = parity(item)
            return copy(wo_all.at[:, item // per_part, :, blk(lax.rem(item, per_part), n_cols)], wbuf.at[slot], wl_sem.at[slot]), copy(hid_ref.at[:, blk(item, n_cols)], hbuf.at[slot], h_sem.at[slot])

        def item_store(item):
            slot = parity(item)
            return copy(rbuf.at[slot], blk_ref.at[:, blk(item, n_cols)], r_sem.at[slot])

        for item in SIDES:
            for load in item_loads(item):
                load.start()

        for end, here in ends:
            @pl.when(here)
            def _():
                ga[end] = gp[...]
                for k in range(last):
                    ga_copy(end, k).start()


        def project(item):
            slot = parity(item)
            for load in item_loads(item):
                load.wait()

            @pl.when(item > 1)
            def _():
                item_store(item - 2).wait()

            @pl.loop(0, TILES)
            def _(tile):
                span = blk(tile, q_len // TILES)
                total = sum(dot(obuf[t, span, :], wbuf[slot, t], NN) for t in range(n_line))
                rbuf[slot, span, :] = (hbuf[slot, span, :].astype(F32) + total).astype(BF)

            item_store(item).start()

            @pl.when(item + 2 < items)
            def _():
                for load in item_loads(item + 2):
                    load.start()

        for end, here in ends:
            @pl.when(jnp.logical_not(here))
            def _():
                ga_copy(end, 0).wait_recv()
        gs[...] = ga[0] + ga[1]
        o_load.wait()
        gb_copy().start()

        early = (last - 1) * PER_STEP

        @pl.loop(0, steps - early)
        def _(step):
            sent = step + last * LEAD
            owner_send(sent, jnp.minimum(sent + 1, chunks))
            pass_on(step + early)

            @pl.when((parity(step) == 0) & (step // 2 < items))
            def _():
                project(step // 2)

            for k, at in LATE:
                @pl.when(step == at)
                def _():
                    meet_x(k)

            for k, at in ((EARLY - 1, -1),) + LATE:
                @pl.when(step == at + 1)
                def _():
                    send_y(k)

        for item in range(items - 2, items):
            item_store(item).wait()

    pl.run_scoped(
        spread_phase,
        pltpu.VMEM(o_all.shape, BF),
        pltpu.VMEM((2, n_line, wo_all.shape[2], min(512, feat)), BF),
        pltpu.VMEM((2, d_ref.shape[0], min(512, feat)), BF),
        pltpu.VMEM((2, d_ref.shape[0], min(512, feat)), BF),
    )

    gb_copy().wait()
    for k in range(n_fsdp):
        gt[k] = gs[:, blk(k, feat)] + gb[:, blk(k, feat)]
    gc[f] = gt[f]
    for side in SIDES:
        @pl.when(dist(side) > 0)
        def _():
            @pl.loop(0, chunks)
            def _(chunk):
                hop(side, chunk).wait_send()

    @pl.loop(0, GRAD_CHUNKS)
    def _(j):
        x_copy(j).wait_send()

    for k in range(1, n_fsdp):
        gc_copy(k, f).start()
    for k in range(1, n_fsdp):
        gc_copy(k, lax.rem(f + n_fsdp - k, n_fsdp)).wait_recv()
    gg_ref[...] = sum(gc[k] for k in range(n_fsdp))
    for k in range(1, n_fsdp):
        gc_copy(k, f).wait_send()
    for end, here in ends:
        @pl.when(here)
        def _():
            for k in range(last):
                ga_copy(end, k).wait_send()

    @pl.loop(0, GRAD_CHUNKS)
    def _(j):
        y_copy(j).wait()


def close(d_lin, attn_out, gain, hidden, cotangent, normed, w_full, o_all, wo_all, cid):
    q_len, model_dim = hidden.shape
    n_line, n_fsdp = wo_all.shape[:2]
    _, feat, width = w_full.shape
    g_width = width + attn_out.shape[1]
    half = q_len // 2
    rows = half // CHUNKS
    sds = jax.ShapeDtypeStruct
    row = pltpu.VMEM((1, model_dim), F32)
    slices = pltpu.VMEM((n_fsdp, 1, feat), F32)
    strip = pltpu.VMEM((2, rows, model_dim), BF)
    own, pair, line, grad, grads = DMA(()), DMA((2,)), DMA((2, CHUNKS)), DMA((GRAD_CHUNKS,)), DMA((2, GRAD_CHUNKS))
    z_trio, f_trio = DMA((n_line - 1,)), DMA((n_fsdp - 1,))
    act, g_part = sds((q_len, model_dim), BF), sds((feat, g_width), F32)
    return pl.pallas_call(
        functools.partial(close_kernel, n_line, n_fsdp),
        in_specs=[VMEM] * 3 + [ANY] * 6,
        out_specs=[ANY, ANY, VMEM] + [ANY] * 6,
        out_shape=[act, act, sds((1, feat), F32), g_part, g_part, sds((2, feat, g_width), F32), g_part, g_part, g_part],
        scratch_shapes=[
            pltpu.VMEM((2, CHUNKS, rows, model_dim), F32),
            row,
            pltpu.VMEM((2, 1, model_dim), F32),
            row,
            row,
            slices,
            slices,
            pltpu.VMEM((2, feat // GRAD_CHUNKS, g_width), F32),
            strip,
            strip,
            strip,
        ] + [line, line, own, pair, pair, pair, DMA((2, n_fsdp)), pair, grads, pair, pair, grad, grad, pair, own, grad, grad, line, line, own, pair, pair, pair, z_trio, pair, own, own, f_trio, f_trio],
        compiler_params=params(cid),
        name="close",
    )(d_lin, attn_out, gain, hidden, cotangent, normed, w_full, o_all, wo_all)


def tail_kernel(head_dim, blk_ref, hid_ref, mine_ref, theirs_ref, blk_out, hid_out, q_out, k_out, v_out, o_out):
    blk_out[...] = blk_ref[...]
    hid_out[...] = hid_ref[...]
    at = 0
    for ref in (q_out, k_out, v_out):
        for h in range(ref.shape[1]):
            cols = blk(at, head_dim)
            ref[:, h, :] = mine_ref[:, cols] + theirs_ref[:, cols]
            at += 1
    rest = slice(at * head_dim, None)
    o_out[...] = (mine_ref[:, rest] + theirs_ref[:, rest]).T


def tail(block_out, grad_hidden, mine, theirs, q_heads, kv_heads, head_dim):
    q_len, model_dim = block_out.shape
    feat = mine.shape[0]
    sds = jax.ShapeDtypeStruct
    act = pl.BlockSpec((q_len // GRAD_CHUNKS, model_dim), lambda i: (i, 0))
    part = pl.BlockSpec((feat // GRAD_CHUNKS, mine.shape[1]), lambda i: (i, 0))

    def heads(n):
        return pl.BlockSpec((feat // GRAD_CHUNKS, n, head_dim), lambda i: (i, 0, 0))

    def like(n):
        return sds((feat, n, head_dim), F32)

    o_rows = q_heads * head_dim
    return pl.pallas_call(
        functools.partial(tail_kernel, head_dim),
        grid=(GRAD_CHUNKS,),
        in_specs=[act, act, part, part],
        out_specs=[act, act, heads(q_heads), heads(kv_heads), heads(kv_heads), pl.BlockSpec((o_rows, feat // GRAD_CHUNKS), lambda i: (0, i))],
        out_shape=[sds(block_out.shape, BF), sds(block_out.shape, BF), like(q_heads), like(kv_heads), like(kv_heads), sds((o_rows, feat), F32)],
        compiler_params=pltpu.CompilerParams(vmem_limit_bytes=VMEM_BYTES),
        name="tail",
    )(block_out, grad_hidden, mine, theirs)


def solution(mesh):
    act_spec = P("fsdp", "cp", None)
    proj_spec = P("fsdp", "tp", None)
    wout_spec = P("tp", None, "fsdp")
    n_line = mesh.shape["tp"]

    def device_step(hidden, cotangent, positions, gain, w_query, w_key, w_value, w_out):
        hidden, cotangent = hidden[0], cotangent[0]
        assert hidden.shape[0] * mesh.shape["cp"] <= WINDOW_LEN
        feat, q_heads, head_dim = w_query.shape
        kv_heads = w_key.shape[1]
        group = q_heads // kv_heads
        q_width, kv_width = q_heads * head_dim, kv_heads * head_dim
        w_qkv = jnp.concatenate([w_query.reshape(feat, q_width), w_key.reshape(feat, kv_width), w_value.reshape(feat, kv_width)], axis=1)
        cosines, sines = rope_tables(positions, head_dim)
        d_lin, attn_out, gain_full, normed, w_full, wo_all, o_all = core(hidden, gain.astype(F32)[None], w_qkv, w_out.reshape(q_width, feat), cosines, sines, cotangent, group, kv_width, n_line, 0)
        grad_hidden, block_out, grad_gain, mine, theirs = close(d_lin, attn_out, gain_full, hidden, cotangent, normed, w_full, o_all, wo_all, 1)[:5]
        block_out, grad_hidden, g_query, g_key, g_value, g_out = tail(block_out, grad_hidden, mine, theirs, q_heads, kv_heads, head_dim)
        return block_out[None], grad_hidden[None], grad_gain[0], g_query, g_key, g_value, g_out.reshape(w_out.shape)

    specs = (act_spec, act_spec, P("fsdp"), proj_spec, proj_spec, proj_spec, wout_spec)
    return jax.shard_map(device_step, mesh=mesh, in_specs=specs[:2] + (P("cp"),) + specs[2:], out_specs=specs, check_vma=False)
```

```python
import functools
import math

import jax
import jax.numpy as jnp
from jax import lax
from jax.experimental import pallas as pl
from jax.experimental.pallas import tpu as pltpu
from jax.sharding import PartitionSpec as P

WINDOW_LEN = 4096
ROPE_BASE = 10000.0
NORM_EPS = 1e-5
NEG_BIG = -1e30
LOG2E = math.log2(math.e)
TILES = 4
CHUNKS = 16
PER_STEP = 1
LEAD = 2
PIECES = 8
O_PIECES = 2
GRAD_CHUNKS = 8
FIRST_X = 5
EARLY = 6
LATE = ((6, 2), (7, 7))
VMEM_BYTES = 67043328
SIDES = range(2)

MESH = pl.DeviceIdType.MESH
ANY = pl.BlockSpec(memory_space=pl.ANY)
VMEM = pl.BlockSpec(memory_space=pltpu.VMEM)
DMA = pltpu.SemaphoreType.DMA
BF, F32 = jnp.bfloat16, jnp.float32

NT = (((1,), (1,)), ((), ()))
NN = (((1,), (0,)), ((), ()))
TN = (((0,), (0,)), ((), ()))


def dot(a, b, dims):
    return lax.dot_general(a, b, dims, preferred_element_type=F32)


def parity(k):
    return lax.rem(k, 2)


def blk(k, n):
    return pl.ds(k * n if isinstance(k, int) else pl.multiple_of(k * n, n), n)


def lane_mean(vals):
    return jnp.mean(vals, axis=1, keepdims=True)


def row_sum(vals):
    return jnp.sum(vals, axis=0, keepdims=True)


def zero(ref):
    ref[...] = jnp.zeros_like(ref)


def remote(src, dst, send, recv, where):
    return pltpu.make_async_remote_copy(src_ref=src, dst_ref=dst, send_sem=send, recv_sem=recv, device_id=where, device_id_type=MESH)


def meet(peers):
    barrier = pltpu.get_barrier_semaphore()
    for where in peers:
        pl.semaphore_signal(barrier, inc=1, device_id=where, device_id_type=MESH)
    pl.semaphore_wait(barrier, len(peers))


def fsdp_peers(f):
    core = parity(f)
    other = f + 1 - 2 * core
    far = lax.rem(f + 2, 4)
    return other, far, lax.rem(other + 2, 4)


def others(axis, index, count):
    return [{axis: lax.rem(index + k, count)} for k in range(1, count)]


def nearest(z, last):
    near = jnp.where(z > 0, last, 1)
    second = jnp.where(z == 0, 2, jnp.where(z == last, last - 1, 1))
    return near, second


def rope(vals, cos, sin, half_dim):
    return vals * cos + pltpu.roll(vals, half_dim, 1) * sin


def causal(scores, tq):
    key_idx = lax.broadcasted_iota(jnp.int32, scores.shape, 0)
    q_idx = lax.rem(lax.broadcasted_iota(jnp.int32, scores.shape, 1), tq)
    return jnp.where(key_idx <= q_idx, scores, NEG_BIG)


def params(cid):
    return pltpu.CompilerParams(collective_id=cid, has_side_effects=True, vmem_limit_bytes=VMEM_BYTES)


def rope_tables(positions, head_dim):
    inv_freq = ROPE_BASE ** (-jnp.arange(0, head_dim, 2).astype(F32) / head_dim)
    angles = positions.astype(F32)[:, None] * inv_freq[None, :]
    cosines, sines = jnp.cos(angles), jnp.sin(angles)
    return jnp.concatenate([cosines, cosines], axis=1), jnp.concatenate([-sines, sines], axis=1)


def core_kernel(group, n_line, hid_ref, gain_ref, w_ref, wo_ref, cos_ref, sin_ref, ct_ref, d_ref, o_ref, gfull_ref, n_out, w_out, wo_all, o_all, wbuf, nbuf, acc, hbuf, gbuf, qs, vt, m_all, l_all, acc_all, q_ref, lse_ref, kl_ref, vl_ref, kp_ref, vp_ref, do_ref, dkl_ref, dvl_ref, dkp_ref, dvp_ref, qs_ref, dos_ref, delta_ref, kt_ref, dqt_ref, h_sem, g_send, g_recv, own_send, own_recv, x_send, x_recv, y_send, y_recv, d_send, d_recv, kv_send, kv_recv, ox_send, ox_recv, oy_send, oy_recv, od_send, od_recv, zw_send, zw_recv, out_sem, ct_sem, o_sems, o_recv, wy_send, wy_recv, wx_send, wx_recv, wc_send, wc_recv, cx_send, cx_recv, dk_send, dk_recv):
    q_len, feat = hid_ref.shape[0], w_ref.shape[0]
    head_dim = cos_ref.shape[1]
    half_dim = head_dim // 2
    kv_width = kl_ref.shape[1]
    kv_heads = kv_width // head_dim
    q_width = q_ref.shape[1]
    tq = q_len // TILES
    wide = group * tq
    score_scale = head_dim ** -0.5
    scale = head_dim ** -0.5 * LOG2E
    half = feat // 2
    piece = half // PIECES
    o_rows = wo_ref.shape[0]
    o_half = o_rows // 2
    o_piece = o_half // O_PIECES
    flag, f, z = lax.axis_index("cp"), lax.axis_index("fsdp"), lax.axis_index("tp")
    wo_out = wo_all.at[z]
    last = n_line - 1
    far = 1 - flag
    f_core, f_x, f_diag = fsdp_peers(f)
    to_core, to_x, to_diag, to_y = {"fsdp": f_core}, {"fsdp": f_x}, {"fsdp": f_diag}, {"cp": far}

    def h_load(tile):
        slot = parity(tile)
        return pltpu.make_async_copy(hid_ref.at[blk(tile, tq)], hbuf.at[slot], h_sem.at[slot])

    h_load(0).start()
    h_load(1).start()
    meet([to_core, to_x, to_diag, to_y] + others("tp", z, n_line))

    def span(side, j):
        return blk(side * PIECES + j, piece)

    def x_copy(j):
        return remote(w_ref.at[span(flag, j)], wbuf.at[f, span(flag, j)], x_send.at[j], x_recv.at[j], to_x)

    def x_in(j):
        return remote(w_ref.at[span(flag, j)], wbuf.at[f_x, span(flag, j)], x_send.at[j], x_recv.at[j], to_x)

    def y_copy(j, side):
        return remote(wbuf.at[f_x, span(side, j)], wbuf.at[f_x, span(side, j)], y_send.at[j], y_recv.at[j], to_y)

    def d_copy(j, side, slot):
        return remote(wbuf.at[slot, span(side, j)], wbuf.at[slot, span(side, j)], d_send.at[side, j], d_recv.at[side, j], to_core)

    def g_copy(k, where, slot):
        return remote(gain_ref, gbuf.at[slot], g_send.at[k], g_recv.at[k], where)

    def own_copy(slot):
        return remote(w_ref, wbuf.at[slot], own_send, own_recv, to_core)

    def o_span(side, j):
        return blk(side * O_PIECES + j, o_piece)

    def ox_copy(j, slot):
        return remote(wo_ref.at[o_span(flag, j)], wo_out.at[slot, o_span(flag, j)], ox_send.at[j], ox_recv.at[j], to_x)

    def oy_copy(j, side):
        return remote(wo_out.at[f_x, o_span(side, j)], wo_out.at[f_x, o_span(side, j)], oy_send.at[j], oy_recv.at[j], to_y)

    def od_copy(k, src, slot, where):
        return remote(src, wo_out.at[slot, where], od_send.at[k], od_recv.at[k], to_core)

    def zw_copy(up, t):
        spot = wo_all.at[t, f, blk(flag, o_half)]
        where = jnp.minimum(z + 1, last) if up else jnp.maximum(z - 1, 0)
        src = spot if t is not z else wo_ref.at[blk(flag, o_half)]
        return remote(src, spot, zw_send.at[up, t], zw_recv.at[t], {"tp": where})

    def zw_tick(r):
        for up, t, here in ((0, z + r, z + r <= last), (1, z - r, z >= r)):
            at = jnp.clip(t, 0, last)

            @pl.when(here)
            def _():
                zw_copy(up, at).wait_recv()

            @pl.when(here & (z < last if up else z > 0))
            def _():
                zw_copy(up, at).start()

    def tile_rows(j):
        return blk(j, tq)

    o_parts = kv_heads * TILES

    def o_piece_at(ref, j):
        return ref.at[tile_rows(lax.rem(j, TILES)), blk(j // TILES, group * head_dim)]

    def o_copy(up, t, j, own=False):
        spot = o_piece_at(o_all.at[t], j)
        src = o_piece_at(o_ref, j) if own else spot
        where = jnp.minimum(z + 1, last) if up else jnp.maximum(z - 1, 0)
        return remote(src, spot, o_sems.at[up, t, j], o_recv.at[t, j], {"tp": where})

    def wo_half(r, slot, side):
        return wo_all.at[lax.rem(z + r, n_line), slot, blk(side, o_half)]

    def wy_copy(r, side):
        return remote(wo_half(r, f, side), wo_half(r, f, side), wy_send.at[r - 1], wy_recv.at[r - 1], to_y)

    def wx_copy(r, side, slot):
        return remote(wo_half(r, slot, side), wo_half(r, slot, side), wx_send.at[side, r - 1], wx_recv.at[side, r - 1], to_x)

    def wc_copy(r, side, slot):
        return remote(wo_half(r, slot, side), wo_half(r, slot, side), wc_send.at[side, r - 1], wc_recv.at[side, r - 1], to_core)

    def cx_copy(r, side, slot):
        return remote(wo_half(r, slot, side), wo_half(r, slot, side), cx_send.at[side, r - 1], cx_recv.at[side, r - 1], to_core)

    def o_tick(k):
        r, j = k // o_parts + 1, lax.rem(k, o_parts)
        for up, t, here in ((0, z + r, z + r <= last), (1, z - r, z >= r)):
            at = jnp.clip(t, 0, last)

            @pl.when(here)
            def _():
                o_copy(up, at, j).wait_recv()

            @pl.when(here & (z < last if up else z > 0))
            def _():
                o_copy(up, at, j).start()

    def wy_tick(r):
        wy_copy(r, far).wait_recv()
        wx_copy(r, far, f).start()
        for side in (flag, far):
            wc_copy(r, side, f).start()
        if r == 1:
            wy_copy(last, flag).start()

    near, second = nearest(z, last)
    own_order = (near, second, n_line * last // 2 - near - second)

    def wx_tick(q):
        r, side = (own_order[q], flag) if q < last else (q - last + 1, far)
        wx_copy(r, side, f_x).wait_recv()
        cx_copy(r, side, f_x).start()

    def o_send(j):
        for up in SIDES:
            @pl.when(z < last if up else z > 0)
            def _():
                o_copy(up, z, j, True).start()

    gains = [(k, where, where["fsdp"]) for k, where in enumerate((to_core, to_x, to_diag))]
    for k, where, _ in gains:
        g_copy(k, where, f).start()
    sends = [x_copy(j) for j in range(PIECES)] + [ox_copy(j, f) for j in range(O_PIECES)]
    for j in range(LEAD):
        sends[j].start()
    own_copy(f).start()
    all_rows = pl.ds(0, o_rows)
    for up in SIDES:
        @pl.when(z < last if up else z > 0)
        def _():
            zw_copy(up, z).start()

    local_w = pltpu.make_async_copy(w_ref, wbuf.at[f], out_sem.at[0])
    local_w.start()
    local_o = pltpu.make_async_copy(wo_ref, wo_out.at[f], out_sem.at[1])
    local_o.start()
    gbuf[f] = gain_ref[...]
    for k, where, slot in gains:
        g_copy(k, where, slot).wait_recv()
    for k in range(gbuf.shape[0]):
        gfull_ref[:, blk(k, feat)] = gbuf[k]

    for tile in range(TILES):
        h_load(tile).wait()
        strip = min(32, tq)

        @pl.loop(0, tq // strip)
        def _(i):
            vals = hbuf[tile % 2, blk(i, strip), :].astype(F32)
            inv = lax.rsqrt(lane_mean(vals * vals) + NORM_EPS)
            nbuf[pl.ds(pl.multiple_of(tile * tq + i * strip, strip), strip), :] = (vals * inv * gfull_ref[...]).astype(BF)

        if tile + 2 < TILES:
            h_load(tile + 2).start()
    put_n = pltpu.make_async_copy(nbuf.at[pl.ds(0, q_len)], n_out, out_sem.at[2])
    put_n.start()

    def project(slot, start, rows, first=False):
        cols = pl.ds(pl.multiple_of(slot * feat + start, 128), rows)

        @pl.loop(0, TILES)
        def _(tile):
            here = blk(tile, tq)
            part = dot(nbuf[here, cols], wbuf[slot, pl.ds(start, rows), :], NN)
            acc[here, :] = part if first else acc[here, :] + part

    def x_tick(j):
        x_in(j).wait_recv()
        y_copy(j, flag).start()
        d_copy(j, flag, f_x).start()
        sends[j + LEAD].start()

    def y_tick(j):
        y_copy(j, far).wait_recv()
        d_copy(j, 1 - flag, f_x).start()

    local_w.wait()
    project(f, 0, feat, first=True)
    x_tick(0)
    x_tick(1)
    own_copy(f_core).wait_recv()
    od_copy(0, wo_ref, f, all_rows).start()
    project(f_core, 0, feat)
    for j in range(2, PIECES):
        x_tick(j)
        y_tick(j - 2)
        if j == PIECES // 2:
            zw_tick(1)
    for j in range(PIECES):
        d_copy(j, flag, f_diag).wait_recv()
    first_half = pl.multiple_of(flag * half, half)
    project(f_x, first_half, half)
    y_tick(PIECES - 2)
    project(f_diag, first_half, half)
    y_tick(PIECES - 1)
    for j in range(PIECES):
        d_copy(j, far, f_diag).wait_recv()
    second_half = pl.multiple_of(far * half, half)
    project(f_x, second_half, half)
    project(f_diag, second_half, half)
    zw_tick(2)
    wx_copy(near, flag, f).start()
    put_w = pltpu.make_async_copy(wbuf, w_out, out_sem.at[3])
    put_w.start()

    @pl.loop(0, TILES)
    def _(tile):
        here = blk(tile, tq)
        cos, sin = cos_ref[here, :], sin_ref[here, :]
        for h in range(kv_heads):
            k_at = q_width // head_dim + h
            kl_ref[here, blk(h, head_dim)] = rope(acc[here, blk(k_at, head_dim)], cos, sin, half_dim).astype(BF)
            vl_ref[here, blk(h, head_dim)] = acc[here, blk(k_at + kv_heads, head_dim)].astype(BF)

    kv_pairs = ((kl_ref, kp_ref), (vl_ref, vp_ref))

    def kv_copies(g):
        return [remote(src.at[:, blk(g, head_dim)], dst.at[:, blk(g, head_dim)], kv_send.at[k, g], kv_recv.at[k, g], {"cp": 1}) for k, (src, dst) in enumerate(kv_pairs)]

    @pl.when(flag == 0)
    def _():
        zero(kp_ref)
        zero(vp_ref)
        for g in range(kv_heads):
            for copy in kv_copies(g):
                copy.start()

    @pl.loop(0, TILES)
    def _(tile):
        here = blk(tile, tq)
        cos, sin = cos_ref[here, :], sin_ref[here, :]
        for h in range(group * kv_heads):
            cols = blk(h, head_dim)
            q_ref[here, cols] = rope(acc[here, cols], cos, sin, half_dim).astype(BF)

    def load_q(item):
        g, tile = item // TILES, lax.rem(item, TILES)
        rows = blk(tile, tq)
        for h in range(group):
            qs[:, blk(h, tq)] = q_ref[rows, blk(g * group + h, head_dim)].T

    def key_piece(item, k_ref, side, start, masked):
        g = item // TILES
        scores = dot(k_ref[start, blk(g, head_dim)], qs[...], NN)
        if masked:
            scores = causal(scores, tq)
        m_old = m_all[item]
        m_new = jnp.maximum(m_old, jnp.max(scores, axis=0, keepdims=True))
        probs = jnp.exp2((scores - m_new) * scale)
        fade = jnp.exp2((m_old - m_new) * scale)
        m_all[item] = m_new
        l_all[item] = l_all[item] * fade + row_sum(probs)
        acc_all[item] = acc_all[item] * fade + dot(vt[g, side, :, start], probs.astype(BF), NN)

    for g in range(kv_heads):
        vt[g, 0] = vl_ref[:, blk(g, head_dim)].T

    @pl.loop(0, kv_heads * TILES)
    def _(item):
        tile = lax.rem(item, TILES)
        load_q(item)
        m_all[item] = jnp.full_like(m_all[item], NEG_BIG)
        l_all[item] = jnp.zeros_like(l_all[item])
        acc_all[item] = jnp.zeros_like(acc_all[item])
        key_piece(item, kl_ref, 0, blk(tile, tq), True)

        @pl.loop(0, tile // 2)
        def _(i):
            key_piece(item, kl_ref, 0, blk(i, 2 * tq), False)

        @pl.when(parity(tile) == 1)
        def _():
            key_piece(item, kl_ref, 0, blk(tile - 1, tq), False)

    for j in range(O_PIECES):
        ox_copy(j, f_x).wait_recv()
        oy_copy(j, flag).start()
        od_copy(1 + j, wo_out.at[f_x, o_span(flag, j)], f_x, o_span(flag, j)).start()

    wx_copy(second, flag, f).start()
    zw_tick(last)

    @pl.loop(0, kv_heads * TILES)
    def _(item):
        g, tile = item // TILES, lax.rem(item, TILES)
        rows = blk(tile, tq)

        @pl.when((flag == 1) & (tile == 0))
        def _():
            for copy in kv_copies(g):
                copy.wait_recv()
            vt[g, 1] = vp_ref[:, blk(g, head_dim)].T

        @pl.when(flag == 1)
        def _():
            load_q(item)

        @pl.loop(0, flag * TILES // 2)
        def _(i):
            key_piece(item, kp_ref, 1, blk(i, 2 * tq), False)

        total = l_all[item]
        lse_ref[item] = m_all[item] * scale + jnp.log2(total)
        out_t = acc_all[item] / total
        for h in range(group):
            o_ref[rows, blk(g * group + h, head_dim)] = out_t[:, h * tq:h * tq + tq].T.astype(BF)

        @pl.when(item > 0)
        def _():
            o_send(item - 1)

        for j in range(O_PIECES):
            @pl.when(item == (j + 1) * kv_heads * TILES // O_PIECES - 1)
            def _():
                oy_copy(j, far).wait_recv()
                od_copy(1 + O_PIECES + j, wo_out.at[f_x, o_span(1 - flag, j)], f_x, o_span(1 - flag, j)).start()

    o_send(o_parts - 1)
    wx_copy(own_order[last - 1], flag, f).start()
    for r in range(1, last):
        wy_copy(r, flag).start()
    od_copy(0, wo_ref, f_core, all_rows).wait_recv()
    for j in range(O_PIECES):
        od_copy(1 + j, wo_out.at[f_x, o_span(flag, j)], f_diag, o_span(flag, j)).wait_recv()
        od_copy(1 + O_PIECES + j, wo_out.at[f_x, o_span(1 - flag, j)], f_diag, o_span(1 - flag, j)).wait_recv()

    put_n.wait()
    local_o.wait()
    n_parts, _, part = wo_out.shape
    loads = [pltpu.make_async_copy(wo_out.at[k], nbuf.at[pl.ds(0, o_rows), blk(k, part)], out_sem.at[4 + k]) for k in range(n_parts)]
    for load in loads:
        load.start()
    keep = pltpu.make_async_copy(o_ref, o_all.at[z], out_sem.at[2])
    keep.start()

    def ct_load(tile):
        slot = parity(tile)
        return pltpu.make_async_copy(ct_ref.at[blk(tile, tq)], hbuf.at[slot], ct_sem.at[slot])

    ct_load(0).start()
    ct_load(1).start()
    zero(dkl_ref)
    zero(dvl_ref)

    @pl.when(flag == 1)
    def _():
        zero(dkp_ref)
        zero(dvp_ref)

    wx_tick(0)
    for k in SIDES:
        o_tick(jnp.int32(k))
    for load in loads:
        load.wait()

    def do_tile(tile):
        ct_load(tile).wait()
        do_ref[tile_rows(tile), :] = dot(hbuf[parity(tile)], nbuf[pl.ds(0, o_rows), :], NT).astype(BF)

        @pl.when(tile + 2 < TILES)
        def _():
            ct_load(tile + 2).start()

    def bwd_item(item):
        g, tile = item // TILES, lax.rem(item, TILES)
        kv_cols = blk(g, head_dim)
        rows = blk(tile, tq)

        @pl.when(tile == 0)
        def _():
            kt_ref[0] = kl_ref[:, kv_cols].T
            kt_ref[1] = kp_ref[:, kv_cols].T

        for h in range(group):
            cols = blk(g * group + h, head_dim)
            stack = blk(h, tq)
            qs_ref[stack, :] = q_ref[rows, cols]
            d_h = do_ref[rows, cols]
            dos_ref[stack, :] = d_h
            prod = d_h.astype(F32) * o_ref[rows, cols].astype(F32)
            delta_ref[:, stack] = row_sum(prod.T)
        zero(dqt_ref)

        def piece(k_ref, v_ref, dk_ref, dv_ref, side, span, masked):
            scores = dot(k_ref[span, kv_cols], qs_ref[...], NT)
            if masked:
                scores = causal(scores, tq)
            probs = jnp.exp2(scores * (score_scale * LOG2E) - lse_ref[item])
            d_probs = dot(v_ref[span, kv_cols], dos_ref[...], NT)
            d_scores = (probs * (d_probs - delta_ref[...])).astype(BF)
            dv_ref[g, span, :] += dot(probs.astype(BF), dos_ref[...], NN)
            dk_ref[g, span, :] += dot(d_scores, qs_ref[...], NN)
            dqt_ref[...] += dot(kt_ref[side, :, span], d_scores, NN)

        piece(kl_ref, vl_ref, dkl_ref, dvl_ref, 0, blk(tile, tq), True)

        @pl.loop(0, tile // 2)
        def _(i):
            piece(kl_ref, vl_ref, dkl_ref, dvl_ref, 0, blk(i, 2 * tq), False)

        @pl.when(parity(tile) == 1)
        def _():
            piece(kl_ref, vl_ref, dkl_ref, dvl_ref, 0, blk(tile - 1, tq), False)

        @pl.loop(0, flag * TILES // 2)
        def _(i):
            piece(kp_ref, vp_ref, dkp_ref, dvp_ref, 1, blk(i, 2 * tq), False)

        for h in range(group):
            dq_h = dqt_ref[:, blk(h, tq)].T * score_scale
            d_ref[rows, blk(g * group + h, head_dim)] = rope(dq_h, cos_ref[rows, :], -sin_ref[rows, :], half_dim).astype(BF)

        @pl.when((tile == TILES - 1) & (flag == 1))
        def _():
            for copy in back(g):
                copy.start()

    def back(g):
        return [remote(ref.at[g], ref.at[g], dk_send.at[k, g], dk_recv.at[k, g], {"cp": 0}) for k, ref in enumerate((dkp_ref, dvp_ref))]

    def kv_done(g):
        @pl.when(flag == 0)
        def _():
            for copy in back(g):
                copy.wait_recv()
            dkl_ref[g] += dkp_ref[g]
            dvl_ref[g] += dvp_ref[g]

        dk = rope(dkl_ref[g] * score_scale, cos_ref[...], -sin_ref[...], half_dim)
        k_at = q_width // head_dim + g
        d_ref[:, blk(k_at, head_dim)] = dk.astype(BF)
        d_ref[:, blk(k_at + kv_heads, head_dim)] = dvl_ref[g].astype(BF)

        @pl.when(flag == 1)
        def _():
            for copy in back(g):
                copy.wait_send()

    items = TILES * (kv_heads + 1)
    plan = {1: [(wx_tick, 1)], 5: [(wy_tick, 1)], 6: [(wx_tick, 2)], 8: [(wy_tick, 2)], 9: [(wx_tick, 3)]}

    @pl.loop(0, items)
    def _(item):
        @pl.when(item < TILES)
        def _():
            do_tile(item)

        @pl.when(item >= TILES)
        def _():
            bwd_item(item - TILES)

        @pl.when(item != 1)
        def _():
            o_tick(jnp.where(item > 1, item + 1, 2))

        for at, jobs in plan.items():
            @pl.when(item == at)
            def _():
                for tick, arg in jobs:
                    tick(arg)

    rest = {1: (wy_tick, 3), 2: (wx_tick, 4), 5: (kv_done, 0), 6: (wx_tick, 5), 9: (kv_done, 1)}
    for k in range(items + 1, o_parts * last):
        o_tick(jnp.int32(k))
        if k - items in rest:
            tick, arg = rest[k - items]
            tick(arg)

    for r in range(1, n_line):
        for side in (flag, far):
            wc_copy(r, side, f_core).wait_recv()
            cx_copy(r, side, f_diag).wait_recv()
            wc_copy(r, side, f).wait_send()
            cx_copy(r, side, f_x).wait_send()
            wx_copy(r, side, f).wait_send()
        wy_copy(r, flag).wait_send()

    @pl.loop(0, n_line)
    def _(t):
        for up in SIDES:
            @pl.when((t <= z) & (z < last) if up else (t >= z) & (z > 0))
            def _():
                for j in range(o_parts):
                    o_copy(up, t, j).wait_send()

    @pl.loop(0, n_line)
    def _(t):
        for up in SIDES:
            @pl.when((t <= z) & (z < last) if up else (t >= z) & (z > 0))
            def _():
                zw_copy(up, t).wait_send()

    for k, where, _ in gains:
        g_copy(k, where, f).wait_send()
    own_copy(f).wait_send()
    od_copy(0, wo_ref, f, all_rows).wait_send()
    for j in range(PIECES):
        x_copy(j).wait_send()
        y_copy(j, flag).wait_send()
        d_copy(j, flag, f_x).wait_send()
        d_copy(j, 1 - flag, f_x).wait_send()
    for j in range(O_PIECES):
        ox_copy(j, f).wait_send()
        oy_copy(j, flag).wait_send()
        od_copy(1 + j, wo_out.at[f_x, o_span(flag, j)], f_x, o_span(flag, j)).wait_send()
        od_copy(1 + O_PIECES + j, wo_out.at[f_x, o_span(1 - flag, j)], f_x, o_span(1 - flag, j)).wait_send()

    @pl.when(flag == 0)
    def _():
        for g in range(kv_heads):
            for copy in kv_copies(g):
                copy.wait_send()

    for local in (keep, put_w):
        local.wait()


def core(hidden, gain, w_qkv, w_out, cosines, sines, cotangent, group, kv_width, n_line, cid):
    q_len, model_dim = hidden.shape
    feat, width = w_qkv.shape
    head_dim = cosines.shape[1]
    q_width = width - 2 * kv_width
    kv_heads = kv_width // head_dim
    o_rows, o_cols = w_out.shape
    n_fsdp = model_dim // feat
    tq = q_len // TILES
    wide = group * tq
    items = kv_heads * TILES
    sds = jax.ShapeDtypeStruct
    line = pltpu.VMEM((items, 1, wide), F32)
    kv = pltpu.VMEM((q_len, kv_width), BF)
    heads = pltpu.VMEM((q_len, q_width), BF)
    sums = pltpu.VMEM((kv_heads, q_len, head_dim), F32)
    stack = pltpu.VMEM((wide, head_dim), BF)
    own, pair, trio = DMA(()), DMA((2,)), DMA((n_fsdp - 1,))
    w_link, w_side, o_link, o_core = DMA((PIECES,)), DMA((2, PIECES)), DMA((O_PIECES,)), DMA((1 + 2 * O_PIECES,))
    hop, side, dkv = DMA((n_line - 1,)), DMA((2, n_line - 1)), DMA((2, kv_heads))
    return pl.pallas_call(
        functools.partial(core_kernel, group, n_line),
        in_specs=[ANY] + [VMEM] * 5 + [ANY],
        out_specs=[VMEM] * 3 + [ANY] * 4,
        out_shape=[sds((q_len, width), BF), sds((q_len, q_width), BF), sds((1, model_dim), F32), sds((q_len, model_dim), BF), sds((n_fsdp, feat, width), BF), sds((n_line, n_fsdp, o_rows, o_cols), BF), sds((n_line, q_len, q_width), BF)],
        scratch_shapes=[
            pltpu.VMEM((n_fsdp, feat, width), BF),
            pltpu.VMEM((max(q_len, o_rows), model_dim), BF),
            pltpu.VMEM((q_len, width), F32),
            pltpu.VMEM((2, tq, model_dim), BF),
            pltpu.VMEM((n_fsdp, 1, feat), F32),
            pltpu.VMEM((head_dim, wide), BF),
            pltpu.VMEM((kv_heads, 2, head_dim, q_len), BF),
            line,
            line,
            pltpu.VMEM((items, head_dim, wide), F32),
            heads,
            line,
            kv, kv, kv, kv,
            heads,
            sums, sums, sums, sums,
            stack,
            stack,
            pltpu.VMEM((1, wide), F32),
            pltpu.VMEM((2, head_dim, q_len), BF),
            pltpu.VMEM((head_dim, wide), F32),
        ] + [pair, trio, trio, own, own, w_link, w_link, w_link, w_link, w_side, w_side, dkv, dkv, o_link, o_link, o_link, o_link, o_core, o_core, DMA((2, n_line)), DMA((n_line,)), DMA((4 + n_fsdp,)), pair, DMA((2, n_line, items)), DMA((n_line, items)), hop, hop, side, side, side, side, side, side, dkv, dkv],
        compiler_params=params(cid),
        name="core",
    )(hidden, gain, w_qkv, w_out, cosines, sines, cotangent)


class Line:
    def __init__(self, n_line, buf_ref, pbuf_ref, send_sem, recv_sem, fill, finish):
        self.last = n_line - 1
        self.z = lax.axis_index("tp")
        self.buf, self.pbuf, self.send_sem, self.recv_sem = buf_ref, pbuf_ref, send_sem, recv_sem
        self.chunks, self.rows = buf_ref.shape[1], buf_ref.shape[2]
        self.block = pbuf_ref.shape[1]
        self.per_block = self.block // self.rows
        self.fill, self.finish = fill, finish
        self.steps = self.chunks + self.last

    def dist(self, side):
        return self.z if side else self.last - self.z

    def toward(self, side, back=False):
        up = bool(side) != back
        return {"tp": jnp.clip(self.z + 1 if up else self.z - 1, 0, self.last)}

    def copy(self, side, chunk):
        spot = self.buf.at[side, chunk]
        return remote(spot, spot, self.send_sem.at[side, chunk], self.recv_sem.at[side, chunk], self.toward(side))

    def live(self, side, step):
        chunk = step - self.dist(side)
        return chunk, (chunk >= 0) & (chunk < self.chunks)

    def prepare(self, step):
        for side in SIDES:
            chunk, ok = self.live(side, step)

            @pl.when(ok & (lax.rem(chunk, self.per_block) == 0))
            def _():
                self.fill(self.pbuf.at[side], blk((side * self.chunks + chunk) // self.per_block, self.block))

    def tick(self, step):
        for side in SIDES:
            chunk, ok = self.live(side, step)
            dist = self.dist(side)
            part = blk(lax.rem(jnp.maximum(chunk, 0), self.per_block), self.rows)

            @pl.when(ok & (dist == 0))
            def _():
                self.buf[side, chunk] = self.pbuf[side, part, :]

            @pl.when(ok & (dist > 0))
            def _():
                self.copy(side, chunk).wait_recv()
                self.buf[side, chunk] += self.pbuf[side, part, :]

            @pl.when(ok & (dist < self.last))
            def _():
                self.copy(side, chunk).start()

            @pl.when(ok & (dist == self.last))
            def _():
                self.finish(chunk, self.buf[side, chunk])

        self.prepare(step + 1)

    def drain(self):
        for side in SIDES:
            @pl.when(self.dist(side) < self.last)
            def _():
                @pl.loop(0, self.chunks)
                def _(chunk):
                    self.copy(side, chunk).wait_send()


def close_kernel(n_line, n_fsdp, d_ref, o_ref, gain_ref, hid_ref, ct_ref, n_ref, w_all, o_all, wo_all, out_ref, blk_ref, gg_ref, ts, yr, dl, xs, ks, xr, buf, gp, ga, gs, gb, gt, gc, ebuf, fb_in, fb_ct, fb_out, send_sem, recv_sem, w_sem, f_sem, ct_sem, fo_sem, lhs_sem, a_send, a_recv, ld_sem, st_sem, x_send, x_recv, e_sem, es_sem, y_send, y_recv, out_send, out_recv, o_sem, wl_sem, h_sem, r_sem, ga_send, ga_recv, gb_send, gb_recv, gc_send, gc_recv):
    last = n_line - 1
    z, flag, f = lax.axis_index("tp"), lax.axis_index("cp"), lax.axis_index("fsdp")
    far = 1 - flag
    f_core, f_x, f_diag = fsdp_peers(f)
    to_core, to_x, to_y = {"fsdp": f_core}, {"fsdp": f_x}, {"cp": far}
    _, feat, width = w_all.shape
    chunks, rows = buf.shape[1], buf.shape[2]
    half = chunks * rows
    g_rows = feat // GRAD_CHUNKS
    owner = (z == 0) | (z == last)
    own_base = jnp.where(z == last, chunks, 0)
    copy = pltpu.make_async_copy

    def own_span(chunk):
        return blk(own_base + chunk, rows)

    def f_loads(chunk):
        slot = parity(chunk)
        return copy(hid_ref.at[own_span(chunk)], fb_in.at[slot], f_sem.at[slot]), copy(ct_ref.at[own_span(chunk)], fb_ct.at[slot], ct_sem.at[slot])

    def f_store(chunk):
        slot = parity(chunk)
        return copy(fb_out.at[slot], out_ref.at[own_span(chunk)], fo_sem.at[slot])

    @pl.when(owner)
    def _():
        for chunk in SIDES:
            for load in f_loads(chunk):
                load.start()

    zero(gp)
    meet([to_core, to_x, to_y] + others("tp", z, n_line) + [{"fsdp": f_diag}])

    def finish(chunk, total):
        slot = parity(chunk)
        for load in f_loads(chunk):
            load.wait()

        @pl.when(chunk > 1)
        def _():
            f_store(chunk - 2).wait()

        x_in = fb_in[slot].astype(F32)
        inv = lax.rsqrt(lane_mean(x_in * x_in) + NORM_EPS)
        x_hat = x_in * inv
        gp[...] += row_sum(total * x_hat)
        scaled = total * gain_ref[...]
        fb_out[slot] = (fb_ct[slot].astype(F32) + inv * (scaled - x_hat * lane_mean(scaled * x_hat))).astype(BF)
        f_store(chunk).start()

        @pl.when(chunk + 2 < chunks)
        def _():
            for load in f_loads(chunk + 2):
                load.start()

    kinds = range(2)

    def g_at(ref, j):
        return ref.at[blk(j, g_rows)]

    def x_copy(j):
        return remote(g_at(xs, j), g_at(xr, j), x_send.at[j], x_recv.at[j], to_x)

    def y_copy(j):
        return remote(g_at(ts, j), g_at(yr, j), y_send.at[j], y_recv.at[j], to_y)

    def e_store(j):
        return copy(ebuf.at[0], g_at(ts, j), es_sem)

    def meet_x(j):
        x_copy(j).wait_recv()
        loads = [copy(g_at(src, j), ebuf.at[k], e_sem.at[k]) for k, src in enumerate((ks, xr))]
        for load in loads:
            load.start()
        for load in loads:
            load.wait()
        ebuf[0] += ebuf[1]
        e_store(j).start()

    def send_y(j):
        e_store(j).wait()
        y_copy(j).start()

    steps = chunks + last - 1

    def dist(side):
        return z if side else last - z

    def hop(side, chunk):
        span = blk(side * chunks + chunk, rows)
        up = z - 1 if side else z + 1
        return remote(out_ref.at[span], out_ref.at[span], out_send.at[side, chunk], out_recv.at[side, chunk], {"tp": jnp.clip(up, 0, last)})

    ends = [(end, z == (last if end else 0)) for end in SIDES]

    def owner_send(first, stop):
        for end, here in ends:
            @pl.when(here)
            def _():
                @pl.loop(first, stop)
                def _(c):
                    hop(end, c).start()

    def pass_on(step):
        for side in SIDES:
            chunk = step - (last - 1 - dist(side))

            @pl.when((dist(side) < last) & (chunk >= 0) & (chunk < chunks))
            def _():
                hop(side, chunk).wait_recv()

                @pl.when(dist(side) > 0)
                def _():
                    hop(side, chunk).start()

    def sum_phase(wbuf, pbuf, abuf, bbuf, lbuf, lhs):
        w_load = copy(w_all, wbuf, w_sem)
        w_load.start()

        def fill(dst, span):
            for k in range(n_fsdp):
                dst[:, blk(k, feat)] = dot(d_ref[span, :], wbuf[k], NT)

        line = Line(n_line, buf, pbuf, send_sem, recv_sem, fill, finish)
        slots = (f_diag, f_core, f_x, f)

        def lhs_loads(j):
            return [copy(src.at[:, blk(slot * GRAD_CHUNKS + j, g_rows)], lhs.at[m, k], lhs_sem.at[m, k]) for m, src in enumerate((n_ref, ct_ref)) for k, slot in enumerate(slots)]

        def a_copy(kind, j):
            return remote(abuf.at[kind], dl.at[kind, blk(j, g_rows)], a_send.at[kind], a_recv.at[kind, j], to_core)

        def b_stores(j):
            return [copy(bbuf.at[k], g_at(dst, j), st_sem.at[k]) for k, dst in enumerate((xs, ks))]

        def send_x(j):
            for kind in kinds:
                a_copy(kind, j).wait_send()
            for store in b_stores(j):
                store.wait()
            x_copy(j).start()

        def make(j):
            for load in lhs_loads(j):
                load.wait()
            for k in range(len(slots)):
                dst = (abuf, bbuf)[k // 2].at[k % 2]
                dst[:, :width] = dot(lhs[0, k], d_ref[...], TN)
                dst[:, width:] = dot(lhs[1, k], o_ref[...], TN)
            for kind in kinds:
                a_copy(kind, j).start()

            @pl.when(j + 1 < GRAD_CHUNKS)
            def _():
                for load in lhs_loads(j + 1):
                    load.start()

        def meet_core(j):
            loads = [copy(dl.at[kind, blk(j, g_rows)], lbuf.at[kind], ld_sem.at[kind]) for kind in kinds]
            for kind in kinds:
                a_copy(kind, j).wait_recv()
                loads[kind].start()
            for kind in kinds:
                loads[kind].wait()
                bbuf[kind] += lbuf[kind]
            for store in b_stores(j):
                store.start()

        for load in lhs_loads(0):
            load.start()
        w_load.wait()
        line.prepare(0)

        @pl.loop(0, line.steps)
        def _(fine):
            line.tick(fine)
            step = fine // PER_STEP
            whole = lax.rem(fine, PER_STEP) == 0
            j, odd = step // 2, parity(step)

            @pl.when(whole & (odd == 0) & (j < GRAD_CHUNKS))
            def _():
                make(j)

            @pl.when(whole & (odd == 1) & (j < GRAD_CHUNKS))
            def _():
                meet_core(j)
                send_x(j)

            k = ((step - FIRST_X) * 2 + 1) // 5

            @pl.when(whole & (k >= 0) & (k < EARLY) & (step == FIRST_X + 5 * k // 2))
            def _():
                meet_x(k)
                send_y(k)

            @pl.when(fine >= chunks)
            def _():
                owner_send((fine - chunks) * LEAD, (fine - chunks + 1) * LEAD)

            @pl.when(fine > chunks)
            def _():
                for k in range(PER_STEP):
                    pass_on((fine - chunks - 1) * PER_STEP + k)

        @pl.when(owner)
        def _():
            for chunk in range(chunks - 2, chunks):
                f_store(chunk).wait()

        line.drain()

    pl.run_scoped(
        sum_phase,
        pltpu.VMEM(w_all.shape, BF),
        pltpu.VMEM((2, min(128, half), buf.shape[3]), F32),
        pltpu.VMEM((2, g_rows, ts.shape[1]), F32),
        pltpu.VMEM((2, g_rows, ts.shape[1]), F32),
        pltpu.VMEM((2, g_rows, ts.shape[1]), F32),
        pltpu.VMEM((2, n_fsdp, d_ref.shape[0], g_rows), BF),
    )
    def ga_copy(end, k):
        return remote(gp, ga.at[end], ga_send.at[k], ga_recv.at[end], {"tp": k if end else 1 + k})

    def gb_copy():
        return remote(gs, gb, gb_send, gb_recv, to_y)

    def gc_copy(k, slot):
        to = lax.rem(f + k, n_fsdp)
        return remote(gt.at[to], gc.at[slot], gc_send.at[k - 1], gc_recv.at[k - 1], {"fsdp": to})

    def spread_phase(obuf, wbuf, hbuf, rbuf):
        o_load = copy(o_all, obuf, o_sem)
        o_load.start()
        q_len, n_cols = hbuf.shape[1], hbuf.shape[2]
        per_part = wo_all.shape[3] // n_cols
        items = per_part * n_fsdp

        def item_loads(item):
            slot = parity(item)
            return copy(wo_all.at[:, item // per_part, :, blk(lax.rem(item, per_part), n_cols)], wbuf.at[slot], wl_sem.at[slot]), copy(hid_ref.at[:, blk(item, n_cols)], hbuf.at[slot], h_sem.at[slot])

        def item_store(item):
            slot = parity(item)
            return copy(rbuf.at[slot], blk_ref.at[:, blk(item, n_cols)], r_sem.at[slot])

        for item in SIDES:
            for load in item_loads(item):
                load.start()

        for end, here in ends:
            @pl.when(here)
            def _():
                ga[end] = gp[...]
                for k in range(last):
                    ga_copy(end, k).start()


        def project(item):
            slot = parity(item)
            for load in item_loads(item):
                load.wait()

            @pl.when(item > 1)
            def _():
                item_store(item - 2).wait()

            @pl.loop(0, TILES)
            def _(tile):
                span = blk(tile, q_len // TILES)
                total = sum(dot(obuf[t, span, :], wbuf[slot, t], NN) for t in range(n_line))
                rbuf[slot, span, :] = (hbuf[slot, span, :].astype(F32) + total).astype(BF)

            item_store(item).start()

            @pl.when(item + 2 < items)
            def _():
                for load in item_loads(item + 2):
                    load.start()

        for end, here in ends:
            @pl.when(jnp.logical_not(here))
            def _():
                ga_copy(end, 0).wait_recv()
        gs[...] = ga[0] + ga[1]
        o_load.wait()
        gb_copy().start()

        early = (last - 1) * PER_STEP

        @pl.loop(0, steps - early)
        def _(step):
            sent = step + last * LEAD
            owner_send(sent, jnp.minimum(sent + 1, chunks))
            pass_on(step + early)

            @pl.when((parity(step) == 0) & (step // 2 < items))
            def _():
                project(step // 2)

            for k, at in LATE:
                @pl.when(step == at)
                def _():
                    meet_x(k)
                    send_y(k)

        for item in range(items - 2, items):
            item_store(item).wait()

    pl.run_scoped(
        spread_phase,
        pltpu.VMEM(o_all.shape, BF),
        pltpu.VMEM((2, n_line, wo_all.shape[2], min(512, feat)), BF),
        pltpu.VMEM((2, d_ref.shape[0], min(512, feat)), BF),
        pltpu.VMEM((2, d_ref.shape[0], min(512, feat)), BF),
    )

    gb_copy().wait()
    for k in range(n_fsdp):
        gt[k] = gs[:, blk(k, feat)] + gb[:, blk(k, feat)]
    gc[f] = gt[f]
    for side in SIDES:
        @pl.when(dist(side) > 0)
        def _():
            @pl.loop(0, chunks)
            def _(chunk):
                hop(side, chunk).wait_send()

    @pl.loop(0, GRAD_CHUNKS)
    def _(j):
        x_copy(j).wait_send()

    for k in range(1, n_fsdp):
        gc_copy(k, f).start()
    for k in range(1, n_fsdp):
        gc_copy(k, lax.rem(f + n_fsdp - k, n_fsdp)).wait_recv()
    gg_ref[...] = sum(gc[k] for k in range(n_fsdp))
    for k in range(1, n_fsdp):
        gc_copy(k, f).wait_send()
    for end, here in ends:
        @pl.when(here)
        def _():
            for k in range(last):
                ga_copy(end, k).wait_send()

    @pl.loop(0, GRAD_CHUNKS)
    def _(j):
        y_copy(j).wait()


def close(d_lin, attn_out, gain, hidden, cotangent, normed, w_full, o_all, wo_all, cid):
    q_len, model_dim = hidden.shape
    n_line, n_fsdp = wo_all.shape[:2]
    _, feat, width = w_full.shape
    g_width = width + attn_out.shape[1]
    half = q_len // 2
    rows = half // CHUNKS
    sds = jax.ShapeDtypeStruct
    row = pltpu.VMEM((1, model_dim), F32)
    slices = pltpu.VMEM((n_fsdp, 1, feat), F32)
    strip = pltpu.VMEM((2, rows, model_dim), BF)
    own, pair, line, grad, grads = DMA(()), DMA((2,)), DMA((2, CHUNKS)), DMA((GRAD_CHUNKS,)), DMA((2, GRAD_CHUNKS))
    z_trio, f_trio = DMA((n_line - 1,)), DMA((n_fsdp - 1,))
    act, g_part = sds((q_len, model_dim), BF), sds((feat, g_width), F32)
    return pl.pallas_call(
        functools.partial(close_kernel, n_line, n_fsdp),
        in_specs=[VMEM] * 3 + [ANY] * 6,
        out_specs=[ANY, ANY, VMEM] + [ANY] * 6,
        out_shape=[act, act, sds((1, feat), F32), g_part, g_part, sds((2, feat, g_width), F32), g_part, g_part, g_part],
        scratch_shapes=[
            pltpu.VMEM((2, CHUNKS, rows, model_dim), F32),
            row,
            pltpu.VMEM((2, 1, model_dim), F32),
            row,
            row,
            slices,
            slices,
            pltpu.VMEM((2, feat // GRAD_CHUNKS, g_width), F32),
            strip,
            strip,
            strip,
        ] + [line, line, own, pair, pair, pair, DMA((2, n_fsdp)), pair, grads, pair, pair, grad, grad, pair, own, grad, grad, line, line, own, pair, pair, pair, z_trio, pair, own, own, f_trio, f_trio],
        compiler_params=params(cid),
        name="close",
    )(d_lin, attn_out, gain, hidden, cotangent, normed, w_full, o_all, wo_all)


def tail_kernel(head_dim, blk_ref, hid_ref, mine_ref, theirs_ref, blk_out, hid_out, q_out, k_out, v_out, o_out):
    blk_out[...] = blk_ref[...]
    hid_out[...] = hid_ref[...]
    at = 0
    for ref in (q_out, k_out, v_out):
        for h in range(ref.shape[1]):
            cols = blk(at, head_dim)
            ref[:, h, :] = mine_ref[:, cols] + theirs_ref[:, cols]
            at += 1
    rest = slice(at * head_dim, None)
    o_out[...] = (mine_ref[:, rest] + theirs_ref[:, rest]).T


def tail(block_out, grad_hidden, mine, theirs, q_heads, kv_heads, head_dim):
    q_len, model_dim = block_out.shape
    feat = mine.shape[0]
    sds = jax.ShapeDtypeStruct
    act = pl.BlockSpec((q_len // GRAD_CHUNKS, model_dim), lambda i: (i, 0))
    part = pl.BlockSpec((feat // GRAD_CHUNKS, mine.shape[1]), lambda i: (i, 0))

    def heads(n):
        return pl.BlockSpec((feat // GRAD_CHUNKS, n, head_dim), lambda i: (i, 0, 0))

    def like(n):
        return sds((feat, n, head_dim), F32)

    o_rows = q_heads * head_dim
    return pl.pallas_call(
        functools.partial(tail_kernel, head_dim),
        grid=(GRAD_CHUNKS,),
        in_specs=[act, act, part, part],
        out_specs=[act, act, heads(q_heads), heads(kv_heads), heads(kv_heads), pl.BlockSpec((o_rows, feat // GRAD_CHUNKS), lambda i: (0, i))],
        out_shape=[sds(block_out.shape, BF), sds(block_out.shape, BF), like(q_heads), like(kv_heads), like(kv_heads), sds((o_rows, feat), F32)],
        compiler_params=pltpu.CompilerParams(vmem_limit_bytes=VMEM_BYTES),
        name="tail",
    )(block_out, grad_hidden, mine, theirs)


def solution(mesh):
    act_spec = P("fsdp", "cp", None)
    proj_spec = P("fsdp", "tp", None)
    wout_spec = P("tp", None, "fsdp")
    n_line = mesh.shape["tp"]

    def device_step(hidden, cotangent, positions, gain, w_query, w_key, w_value, w_out):
        hidden, cotangent = hidden[0], cotangent[0]
        assert hidden.shape[0] * mesh.shape["cp"] <= WINDOW_LEN
        feat, q_heads, head_dim = w_query.shape
        kv_heads = w_key.shape[1]
        group = q_heads // kv_heads
        q_width, kv_width = q_heads * head_dim, kv_heads * head_dim
        w_qkv = jnp.concatenate([w_query.reshape(feat, q_width), w_key.reshape(feat, kv_width), w_value.reshape(feat, kv_width)], axis=1)
        cosines, sines = rope_tables(positions, head_dim)
        d_lin, attn_out, gain_full, normed, w_full, wo_all, o_all = core(hidden, gain.astype(F32)[None], w_qkv, w_out.reshape(q_width, feat), cosines, sines, cotangent, group, kv_width, n_line, 0)
        grad_hidden, block_out, grad_gain, mine, theirs = close(d_lin, attn_out, gain_full, hidden, cotangent, normed, w_full, o_all, wo_all, 1)[:5]
        block_out, grad_hidden, g_query, g_key, g_value, g_out = tail(block_out, grad_hidden, mine, theirs, q_heads, kv_heads, head_dim)
        return block_out[None], grad_hidden[None], grad_gain[0], g_query, g_key, g_value, g_out.reshape(w_out.shape)

    specs = (act_spec, act_spec, P("fsdp"), proj_spec, proj_spec, proj_spec, wout_spec)
    return jax.shard_map(device_step, mesh=mesh, in_specs=specs[:2] + (P("cp"),) + specs[2:], out_specs=specs, check_vma=False)
```

```python
import functools
import math

import jax
import jax.numpy as jnp
from jax import lax
from jax.experimental import pallas as pl
from jax.experimental.pallas import tpu as pltpu
from jax.sharding import PartitionSpec as P

WINDOW_LEN = 4096
ROPE_BASE = 10000.0
NORM_EPS = 1e-5
NEG_BIG = -1e30
LOG2E = math.log2(math.e)
TILES = 4
CHUNKS = 16
PER_STEP = 1
LEAD = 2
QUARTERS = 3
PIECES = 8
O_PIECES = 2
GRAD_CHUNKS = 8
FIRST_X = 5
EARLY = 6
LATE = ((6, 2), (7, 7))
VMEM_BYTES = 67043328
SIDES = range(2)

MESH = pl.DeviceIdType.MESH
ANY = pl.BlockSpec(memory_space=pl.ANY)
VMEM = pl.BlockSpec(memory_space=pltpu.VMEM)
DMA = pltpu.SemaphoreType.DMA
BF, F32 = jnp.bfloat16, jnp.float32

NT = (((1,), (1,)), ((), ()))
NN = (((1,), (0,)), ((), ()))
TN = (((0,), (0,)), ((), ()))


def dot(a, b, dims):
    return lax.dot_general(a, b, dims, preferred_element_type=F32)


def parity(k):
    return lax.rem(k, 2)


def blk(k, n):
    return pl.ds(k * n if isinstance(k, int) else pl.multiple_of(k * n, n), n)


def lane_mean(vals):
    return jnp.mean(vals, axis=1, keepdims=True)


def row_sum(vals):
    return jnp.sum(vals, axis=0, keepdims=True)


def zero(ref):
    ref[...] = jnp.zeros_like(ref)


def remote(src, dst, send, recv, where):
    return pltpu.make_async_remote_copy(src_ref=src, dst_ref=dst, send_sem=send, recv_sem=recv, device_id=where, device_id_type=MESH)


def meet(peers):
    barrier = pltpu.get_barrier_semaphore()
    for where in peers:
        pl.semaphore_signal(barrier, inc=1, device_id=where, device_id_type=MESH)
    pl.semaphore_wait(barrier, len(peers))


def fsdp_peers(f):
    core = parity(f)
    other = f + 1 - 2 * core
    far = lax.rem(f + 2, 4)
    return other, far, lax.rem(other + 2, 4)


def others(axis, index, count):
    return [{axis: lax.rem(index + k, count)} for k in range(1, count)]


def nearest(z, last):
    near = jnp.where(z > 0, last, 1)
    second = jnp.where(z == 0, 2, jnp.where(z == last, last - 1, 1))
    return near, second


def rope(vals, cos, sin, half_dim):
    return vals * cos + pltpu.roll(vals, half_dim, 1) * sin


def causal(scores, tq):
    key_idx = lax.broadcasted_iota(jnp.int32, scores.shape, 0)
    q_idx = lax.rem(lax.broadcasted_iota(jnp.int32, scores.shape, 1), tq)
    return jnp.where(key_idx <= q_idx, scores, NEG_BIG)


def params(cid):
    return pltpu.CompilerParams(collective_id=cid, has_side_effects=True, vmem_limit_bytes=VMEM_BYTES)


def rope_tables(positions, head_dim):
    inv_freq = ROPE_BASE ** (-jnp.arange(0, head_dim, 2).astype(F32) / head_dim)
    angles = positions.astype(F32)[:, None] * inv_freq[None, :]
    cosines, sines = jnp.cos(angles), jnp.sin(angles)
    return jnp.concatenate([cosines, cosines], axis=1), jnp.concatenate([-sines, sines], axis=1)


def core_kernel(group, n_line, hid_ref, gain_ref, w_ref, wo_ref, cos_ref, sin_ref, ct_ref, d_ref, o_ref, gfull_ref, n_out, w_out, wo_all, o_all, wbuf, nbuf, acc, hbuf, gbuf, qs, vt, m_all, l_all, acc_all, q_ref, lse_ref, kl_ref, vl_ref, kp_ref, vp_ref, do_ref, dkl_ref, dvl_ref, dkp_ref, dvp_ref, qs_ref, dos_ref, delta_ref, kt_ref, dqt_ref, h_sem, g_send, g_recv, own_send, own_recv, x_send, x_recv, y_send, y_recv, d_send, d_recv, kv_send, kv_recv, ox_send, ox_recv, oy_send, oy_recv, od_send, od_recv, zw_send, zw_recv, out_sem, ct_sem, o_sems, o_recv, wy_send, wy_recv, wx_send, wx_recv, wc_send, wc_recv, cx_send, cx_recv, dk_send, dk_recv):
    q_len, feat = hid_ref.shape[0], w_ref.shape[0]
    head_dim = cos_ref.shape[1]
    half_dim = head_dim // 2
    kv_width = kl_ref.shape[1]
    kv_heads = kv_width // head_dim
    q_width = q_ref.shape[1]
    tq = q_len // TILES
    wide = group * tq
    score_scale = head_dim ** -0.5
    scale = head_dim ** -0.5 * LOG2E
    half = feat // 2
    piece = half // PIECES
    o_rows = wo_ref.shape[0]
    o_half = o_rows // 2
    o_piece = o_half // O_PIECES
    flag, f, z = lax.axis_index("cp"), lax.axis_index("fsdp"), lax.axis_index("tp")
    wo_out = wo_all.at[z]
    last = n_line - 1
    far = 1 - flag
    f_core, f_x, f_diag = fsdp_peers(f)
    to_core, to_x, to_diag, to_y = {"fsdp": f_core}, {"fsdp": f_x}, {"fsdp": f_diag}, {"cp": far}

    def h_load(tile):
        slot = parity(tile)
        return pltpu.make_async_copy(hid_ref.at[blk(tile, tq)], hbuf.at[slot], h_sem.at[slot])

    h_load(0).start()
    h_load(1).start()
    meet([to_core, to_x, to_diag, to_y] + others("tp", z, n_line))

    def span(side, j):
        return blk(side * PIECES + j, piece)

    def x_copy(j):
        return remote(w_ref.at[span(flag, j)], wbuf.at[f, span(flag, j)], x_send.at[j], x_recv.at[j], to_x)

    def x_in(j):
        return remote(w_ref.at[span(flag, j)], wbuf.at[f_x, span(flag, j)], x_send.at[j], x_recv.at[j], to_x)

    def y_copy(j, side):
        return remote(wbuf.at[f_x, span(side, j)], wbuf.at[f_x, span(side, j)], y_send.at[j], y_recv.at[j], to_y)

    def d_copy(j, side, slot):
        return remote(wbuf.at[slot, span(side, j)], wbuf.at[slot, span(side, j)], d_send.at[side, j], d_recv.at[side, j], to_core)

    def g_copy(k, where, slot):
        return remote(gain_ref, gbuf.at[slot], g_send.at[k], g_recv.at[k], where)

    def own_copy(slot):
        return remote(w_ref, wbuf.at[slot], own_send, own_recv, to_core)

    def o_span(side, j):
        return blk(side * O_PIECES + j, o_piece)

    def ox_copy(j, slot):
        return remote(wo_ref.at[o_span(flag, j)], wo_out.at[slot, o_span(flag, j)], ox_send.at[j], ox_recv.at[j], to_x)

    def oy_copy(j, side):
        return remote(wo_out.at[f_x, o_span(side, j)], wo_out.at[f_x, o_span(side, j)], oy_send.at[j], oy_recv.at[j], to_y)

    def od_copy(k, src, slot, where):
        return remote(src, wo_out.at[slot, where], od_send.at[k], od_recv.at[k], to_core)

    def zw_copy(up, t):
        spot = wo_all.at[t, f, blk(flag, o_half)]
        where = jnp.minimum(z + 1, last) if up else jnp.maximum(z - 1, 0)
        src = spot if t is not z else wo_ref.at[blk(flag, o_half)]
        return remote(src, spot, zw_send.at[up, t], zw_recv.at[t], {"tp": where})

    def zw_tick(r):
        for up, t, here in ((0, z + r, z + r <= last), (1, z - r, z >= r)):
            at = jnp.clip(t, 0, last)

            @pl.when(here)
            def _():
                zw_copy(up, at).wait_recv()

            @pl.when(here & (z < last if up else z > 0))
            def _():
                zw_copy(up, at).start()

    def tile_rows(j):
        return blk(j, tq)

    o_parts = kv_heads * TILES

    def o_piece_at(ref, j):
        return ref.at[tile_rows(lax.rem(j, TILES)), blk(j // TILES, group * head_dim)]

    def o_copy(up, t, j, own=False):
        spot = o_piece_at(o_all.at[t], j)
        src = o_piece_at(o_ref, j) if own else spot
        where = jnp.minimum(z + 1, last) if up else jnp.maximum(z - 1, 0)
        return remote(src, spot, o_sems.at[up, t, j], o_recv.at[t, j], {"tp": where})

    def wo_half(r, slot, side):
        return wo_all.at[lax.rem(z + r, n_line), slot, blk(side, o_half)]

    def wy_copy(r, side):
        return remote(wo_half(r, f, side), wo_half(r, f, side), wy_send.at[r - 1], wy_recv.at[r - 1], to_y)

    def wx_copy(r, side, slot):
        return remote(wo_half(r, slot, side), wo_half(r, slot, side), wx_send.at[side, r - 1], wx_recv.at[side, r - 1], to_x)

    def wc_copy(r, side, slot):
        return remote(wo_half(r, slot, side), wo_half(r, slot, side), wc_send.at[side, r - 1], wc_recv.at[side, r - 1], to_core)

    def cx_copy(r, side, slot):
        return remote(wo_half(r, slot, side), wo_half(r, slot, side), cx_send.at[side, r - 1], cx_recv.at[side, r - 1], to_core)

    def o_tick(k):
        r, j = k // o_parts + 1, lax.rem(k, o_parts)
        for up, t, here in ((0, z + r, z + r <= last), (1, z - r, z >= r)):
            at = jnp.clip(t, 0, last)

            @pl.when(here)
            def _():
                o_copy(up, at, j).wait_recv()

            @pl.when(here & (z < last if up else z > 0))
            def _():
                o_copy(up, at, j).start()

    def wy_tick(r):
        wy_copy(r, far).wait_recv()
        wx_copy(r, far, f).start()
        for side in (flag, far):
            wc_copy(r, side, f).start()
        if r == 1:
            wy_copy(last, flag).start()

    near, second = nearest(z, last)
    own_order = (near, second, n_line * last // 2 - near - second)

    def wx_tick(q):
        r, side = (own_order[q], flag) if q < last else (q - last + 1, far)
        wx_copy(r, side, f_x).wait_recv()
        cx_copy(r, side, f_x).start()

    def o_send(j):
        for up in SIDES:
            @pl.when(z < last if up else z > 0)
            def _():
                o_copy(up, z, j, True).start()

    gains = [(k, where, where["fsdp"]) for k, where in enumerate((to_core, to_x, to_diag))]
    for k, where, _ in gains:
        g_copy(k, where, f).start()
    sends = [x_copy(j) for j in range(PIECES)] + [ox_copy(j, f) for j in range(O_PIECES)]
    for j in range(LEAD):
        sends[j].start()
    own_copy(f).start()
    all_rows = pl.ds(0, o_rows)
    for up in SIDES:
        @pl.when(z < last if up else z > 0)
        def _():
            zw_copy(up, z).start()

    local_w = pltpu.make_async_copy(w_ref, wbuf.at[f], out_sem.at[0])
    local_w.start()
    local_o = pltpu.make_async_copy(wo_ref, wo_out.at[f], out_sem.at[1])
    local_o.start()
    gbuf[f] = gain_ref[...]
    for k, where, slot in gains:
        g_copy(k, where, slot).wait_recv()
    for k in range(gbuf.shape[0]):
        gfull_ref[:, blk(k, feat)] = gbuf[k].astype(F32)

    for tile in range(TILES):
        h_load(tile).wait()
        strip = min(32, tq)

        @pl.loop(0, tq // strip)
        def _(i):
            vals = hbuf[tile % 2, blk(i, strip), :].astype(F32)
            inv = lax.rsqrt(lane_mean(vals * vals) + NORM_EPS)
            nbuf[pl.ds(pl.multiple_of(tile * tq + i * strip, strip), strip), :] = (vals * inv * gfull_ref[...]).astype(BF)

        if tile + 2 < TILES:
            h_load(tile + 2).start()
    put_n = pltpu.make_async_copy(nbuf.at[pl.ds(0, q_len)], n_out, out_sem.at[2])
    put_n.start()

    def project(slot, start, rows, first=False):
        cols = pl.ds(pl.multiple_of(slot * feat + start, 128), rows)

        @pl.loop(0, TILES)
        def _(tile):
            here = blk(tile, tq)
            part = dot(nbuf[here, cols], wbuf[slot, pl.ds(start, rows), :], NN)
            acc[here, :] = part if first else acc[here, :] + part

    def x_tick(j):
        x_in(j).wait_recv()
        y_copy(j, flag).start()
        d_copy(j, flag, f_x).start()
        sends[j + LEAD].start()

    def y_tick(j):
        y_copy(j, far).wait_recv()
        d_copy(j, 1 - flag, f_x).start()

    local_w.wait()
    project(f, 0, feat, first=True)
    x_tick(0)
    x_tick(1)
    own_copy(f_core).wait_recv()
    od_copy(0, wo_ref, f, all_rows).start()
    project(f_core, 0, feat)
    for j in range(2, PIECES):
        x_tick(j)
        y_tick(j - 2)
        if j == PIECES // 2:
            zw_tick(1)
    for j in range(PIECES):
        d_copy(j, flag, f_diag).wait_recv()
    first_half = pl.multiple_of(flag * half, half)
    project(f_x, first_half, half)
    y_tick(PIECES - 2)
    project(f_diag, first_half, half)
    y_tick(PIECES - 1)
    for j in range(PIECES):
        d_copy(j, far, f_diag).wait_recv()
    second_half = pl.multiple_of(far * half, half)
    project(f_x, second_half, half)
    project(f_diag, second_half, half)
    zw_tick(2)
    wx_copy(near, flag, f).start()
    put_w = pltpu.make_async_copy(wbuf, w_out, out_sem.at[3])
    put_w.start()

    @pl.loop(0, TILES)
    def _(tile):
        here = blk(tile, tq)
        cos, sin = cos_ref[here, :], sin_ref[here, :]
        for h in range(kv_heads):
            k_at = q_width // head_dim + h
            kl_ref[here, blk(h, head_dim)] = rope(acc[here, blk(k_at, head_dim)], cos, sin, half_dim).astype(BF)
            vl_ref[here, blk(h, head_dim)] = acc[here, blk(k_at + kv_heads, head_dim)].astype(BF)

    kv_pairs = ((kl_ref, kp_ref), (vl_ref, vp_ref))

    def kv_copies(g):
        return [remote(src.at[:, blk(g, head_dim)], dst.at[:, blk(g, head_dim)], kv_send.at[k, g], kv_recv.at[k, g], {"cp": 1}) for k, (src, dst) in enumerate(kv_pairs)]

    @pl.when(flag == 0)
    def _():
        zero(kp_ref)
        zero(vp_ref)
        for g in range(kv_heads):
            for copy in kv_copies(g):
                copy.start()

    @pl.loop(0, TILES)
    def _(tile):
        here = blk(tile, tq)
        cos, sin = cos_ref[here, :], sin_ref[here, :]
        for h in range(group * kv_heads):
            cols = blk(h, head_dim)
            q_ref[here, cols] = rope(acc[here, cols], cos, sin, half_dim).astype(BF)

    def load_q(item):
        g, tile = item // TILES, lax.rem(item, TILES)
        rows = blk(tile, tq)
        for h in range(group):
            qs[:, blk(h, tq)] = q_ref[rows, blk(g * group + h, head_dim)].T

    def key_piece(item, k_ref, side, start, masked):
        g = item // TILES
        scores = dot(k_ref[start, blk(g, head_dim)], qs[...], NN)
        if masked:
            scores = causal(scores, tq)
        m_old = m_all[item]
        m_new = jnp.maximum(m_old, jnp.max(scores, axis=0, keepdims=True))
        probs = jnp.exp2((scores - m_new) * scale)
        fade = jnp.exp2((m_old - m_new) * scale)
        m_all[item] = m_new
        l_all[item] = l_all[item] * fade + row_sum(probs)
        acc_all[item] = acc_all[item] * fade + dot(vt[g, side, :, start], probs.astype(BF), NN)

    for g in range(kv_heads):
        vt[g, 0] = vl_ref[:, blk(g, head_dim)].T

    @pl.loop(0, kv_heads * TILES)
    def _(item):
        tile = lax.rem(item, TILES)
        load_q(item)
        m_all[item] = jnp.full_like(m_all[item], NEG_BIG)
        l_all[item] = jnp.zeros_like(l_all[item])
        acc_all[item] = jnp.zeros_like(acc_all[item])
        key_piece(item, kl_ref, 0, blk(tile, tq), True)

        @pl.loop(0, tile // 2)
        def _(i):
            key_piece(item, kl_ref, 0, blk(i, 2 * tq), False)

        @pl.when(parity(tile) == 1)
        def _():
            key_piece(item, kl_ref, 0, blk(tile - 1, tq), False)

    for j in range(O_PIECES):
        ox_copy(j, f_x).wait_recv()
        oy_copy(j, flag).start()
        od_copy(1 + j, wo_out.at[f_x, o_span(flag, j)], f_x, o_span(flag, j)).start()

    wx_copy(second, flag, f).start()
    zw_tick(last)

    @pl.loop(0, kv_heads * TILES)
    def _(item):
        g, tile = item // TILES, lax.rem(item, TILES)
        rows = blk(tile, tq)

        @pl.when((flag == 1) & (tile == 0))
        def _():
            for copy in kv_copies(g):
                copy.wait_recv()
            vt[g, 1] = vp_ref[:, blk(g, head_dim)].T

        @pl.when(flag == 1)
        def _():
            load_q(item)

        @pl.loop(0, flag * TILES // 2)
        def _(i):
            key_piece(item, kp_ref, 1, blk(i, 2 * tq), False)

        total = l_all[item]
        lse_ref[item] = m_all[item] * scale + jnp.log2(total)
        out_t = acc_all[item] / total
        for h in range(group):
            o_ref[rows, blk(g * group + h, head_dim)] = out_t[:, h * tq:h * tq + tq].T.astype(BF)

        @pl.when(item > 0)
        def _():
            o_send(item - 1)

        for j in range(O_PIECES):
            @pl.when(item == (j + 1) * kv_heads * TILES // O_PIECES - 1)
            def _():
                oy_copy(j, far).wait_recv()
                od_copy(1 + O_PIECES + j, wo_out.at[f_x, o_span(1 - flag, j)], f_x, o_span(1 - flag, j)).start()

    o_send(o_parts - 1)
    wx_copy(own_order[last - 1], flag, f).start()
    for r in range(1, last):
        wy_copy(r, flag).start()
    od_copy(0, wo_ref, f_core, all_rows).wait_recv()
    for j in range(O_PIECES):
        od_copy(1 + j, wo_out.at[f_x, o_span(flag, j)], f_diag, o_span(flag, j)).wait_recv()
        od_copy(1 + O_PIECES + j, wo_out.at[f_x, o_span(1 - flag, j)], f_diag, o_span(1 - flag, j)).wait_recv()

    put_n.wait()
    local_o.wait()
    n_parts, _, part = wo_out.shape
    loads = [pltpu.make_async_copy(wo_out.at[k], nbuf.at[pl.ds(0, o_rows), blk(k, part)], out_sem.at[4 + k]) for k in range(n_parts)]
    for load in loads:
        load.start()
    keep = pltpu.make_async_copy(o_ref, o_all.at[z], out_sem.at[2])
    keep.start()

    def ct_load(tile):
        slot = parity(tile)
        return pltpu.make_async_copy(ct_ref.at[blk(tile, tq)], hbuf.at[slot], ct_sem.at[slot])

    ct_load(0).start()
    ct_load(1).start()
    zero(dkl_ref)
    zero(dvl_ref)

    @pl.when(flag == 1)
    def _():
        zero(dkp_ref)
        zero(dvp_ref)

    wx_tick(0)
    for k in SIDES:
        o_tick(jnp.int32(k))
    for load in loads:
        load.wait()

    def do_tile(tile):
        ct_load(tile).wait()
        do_ref[tile_rows(tile), :] = dot(hbuf[parity(tile)], nbuf[pl.ds(0, o_rows), :], NT).astype(BF)

        @pl.when(tile + 2 < TILES)
        def _():
            ct_load(tile + 2).start()

    def bwd_item(item):
        g, tile = item // TILES, lax.rem(item, TILES)
        kv_cols = blk(g, head_dim)
        rows = blk(tile, tq)

        @pl.when(tile == 0)
        def _():
            kt_ref[0] = kl_ref[:, kv_cols].T
            kt_ref[1] = kp_ref[:, kv_cols].T

        for h in range(group):
            cols = blk(g * group + h, head_dim)
            stack = blk(h, tq)
            qs_ref[stack, :] = q_ref[rows, cols]
            d_h = do_ref[rows, cols]
            dos_ref[stack, :] = d_h
            prod = d_h.astype(F32) * o_ref[rows, cols].astype(F32)
            delta_ref[:, stack] = row_sum(prod.T)
        zero(dqt_ref)

        def piece(k_ref, v_ref, dk_ref, dv_ref, side, span, masked):
            scores = dot(k_ref[span, kv_cols], qs_ref[...], NT)
            if masked:
                scores = causal(scores, tq)
            probs = jnp.exp2(scores * (score_scale * LOG2E) - lse_ref[item])
            d_probs = dot(v_ref[span, kv_cols], dos_ref[...], NT)
            d_scores = (probs * (d_probs - delta_ref[...])).astype(BF)
            dv_ref[g, span, :] += dot(probs.astype(BF), dos_ref[...], NN)
            dk_ref[g, span, :] += dot(d_scores, qs_ref[...], NN)
            dqt_ref[...] += dot(kt_ref[side, :, span], d_scores, NN)

        piece(kl_ref, vl_ref, dkl_ref, dvl_ref, 0, blk(tile, tq), True)

        @pl.loop(0, tile // 2)
        def _(i):
            piece(kl_ref, vl_ref, dkl_ref, dvl_ref, 0, blk(i, 2 * tq), False)

        @pl.when(parity(tile) == 1)
        def _():
            piece(kl_ref, vl_ref, dkl_ref, dvl_ref, 0, blk(tile - 1, tq), False)

        @pl.loop(0, flag * TILES // 2)
        def _(i):
            piece(kp_ref, vp_ref, dkp_ref, dvp_ref, 1, blk(i, 2 * tq), False)

        for h in range(group):
            dq_h = dqt_ref[:, blk(h, tq)].T * score_scale
            d_ref[rows, blk(g * group + h, head_dim)] = rope(dq_h, cos_ref[rows, :], -sin_ref[rows, :], half_dim).astype(BF)

        @pl.when((tile == TILES - 1) & (flag == 1))
        def _():
            for copy in back(g):
                copy.start()

    def back(g):
        return [remote(ref.at[g], ref.at[g], dk_send.at[k, g], dk_recv.at[k, g], {"cp": 0}) for k, ref in enumerate((dkp_ref, dvp_ref))]

    def kv_done(g):
        @pl.when(flag == 0)
        def _():
            for copy in back(g):
                copy.wait_recv()
            dkl_ref[g] += dkp_ref[g]
            dvl_ref[g] += dvp_ref[g]

        dk = rope(dkl_ref[g] * score_scale, cos_ref[...], -sin_ref[...], half_dim)
        k_at = q_width // head_dim + g
        d_ref[:, blk(k_at, head_dim)] = dk.astype(BF)
        d_ref[:, blk(k_at + kv_heads, head_dim)] = dvl_ref[g].astype(BF)

        @pl.when(flag == 1)
        def _():
            for copy in back(g):
                copy.wait_send()

    items = TILES * (kv_heads + 1)
    plan = {1: [(wx_tick, 1)], 5: [(wy_tick, 1)], 6: [(wx_tick, 2)], 8: [(wy_tick, 2)], 9: [(wx_tick, 3)]}

    @pl.loop(0, items)
    def _(item):
        @pl.when(item < TILES)
        def _():
            do_tile(item)

        @pl.when(item >= TILES)
        def _():
            bwd_item(item - TILES)

        @pl.when(item != 1)
        def _():
            o_tick(jnp.where(item > 1, item + 1, 2))

        for at, jobs in plan.items():
            @pl.when(item == at)
            def _():
                for tick, arg in jobs:
                    tick(arg)

    rest = {1: (wy_tick, 3), 2: (wx_tick, 4), 5: (kv_done, 0), 6: (wx_tick, 5), 9: (kv_done, 1)}
    for k in range(items + 1, o_parts * last):
        o_tick(jnp.int32(k))
        if k - items in rest:
            tick, arg = rest[k - items]
            tick(arg)

    for r in range(1, n_line):
        for side in (flag, far):
            wc_copy(r, side, f_core).wait_recv()
            cx_copy(r, side, f_diag).wait_recv()
            wc_copy(r, side, f).wait_send()
            cx_copy(r, side, f_x).wait_send()
            wx_copy(r, side, f).wait_send()
        wy_copy(r, flag).wait_send()

    @pl.loop(0, n_line)
    def _(t):
        for up in SIDES:
            @pl.when((t <= z) & (z < last) if up else (t >= z) & (z > 0))
            def _():
                for j in range(o_parts):
                    o_copy(up, t, j).wait_send()

    @pl.loop(0, n_line)
    def _(t):
        for up in SIDES:
            @pl.when((t <= z) & (z < last) if up else (t >= z) & (z > 0))
            def _():
                zw_copy(up, t).wait_send()

    for k, where, _ in gains:
        g_copy(k, where, f).wait_send()
    own_copy(f).wait_send()
    od_copy(0, wo_ref, f, all_rows).wait_send()
    for j in range(PIECES):
        x_copy(j).wait_send()
        y_copy(j, flag).wait_send()
        d_copy(j, flag, f_x).wait_send()
        d_copy(j, 1 - flag, f_x).wait_send()
    for j in range(O_PIECES):
        ox_copy(j, f).wait_send()
        oy_copy(j, flag).wait_send()
        od_copy(1 + j, wo_out.at[f_x, o_span(flag, j)], f_x, o_span(flag, j)).wait_send()
        od_copy(1 + O_PIECES + j, wo_out.at[f_x, o_span(1 - flag, j)], f_x, o_span(1 - flag, j)).wait_send()

    @pl.when(flag == 0)
    def _():
        for g in range(kv_heads):
            for copy in kv_copies(g):
                copy.wait_send()

    for local in (keep, put_w):
        local.wait()


def core(hidden, gain, w_qkv, w_out, cosines, sines, cotangent, group, kv_width, n_line, cid):
    q_len, model_dim = hidden.shape
    feat, width = w_qkv.shape
    head_dim = cosines.shape[1]
    q_width = width - 2 * kv_width
    kv_heads = kv_width // head_dim
    o_rows, o_cols = w_out.shape
    n_fsdp = model_dim // feat
    tq = q_len // TILES
    wide = group * tq
    items = kv_heads * TILES
    sds = jax.ShapeDtypeStruct
    line = pltpu.VMEM((items, 1, wide), F32)
    kv = pltpu.VMEM((q_len, kv_width), BF)
    heads = pltpu.VMEM((q_len, q_width), BF)
    sums = pltpu.VMEM((kv_heads, q_len, head_dim), F32)
    stack = pltpu.VMEM((wide, head_dim), BF)
    own, pair, trio = DMA(()), DMA((2,)), DMA((n_fsdp - 1,))
    w_link, w_side, o_link, o_core = DMA((PIECES,)), DMA((2, PIECES)), DMA((O_PIECES,)), DMA((1 + 2 * O_PIECES,))
    hop, side, dkv = DMA((n_line - 1,)), DMA((2, n_line - 1)), DMA((2, kv_heads))
    return pl.pallas_call(
        functools.partial(core_kernel, group, n_line),
        in_specs=[ANY] + [VMEM] * 5 + [ANY],
        out_specs=[VMEM] * 3 + [ANY] * 4,
        out_shape=[sds((q_len, width), BF), sds((q_len, q_width), BF), sds((1, model_dim), F32), sds((q_len, model_dim), BF), sds((n_fsdp, feat, width), BF), sds((n_line, n_fsdp, o_rows, o_cols), BF), sds((n_line, q_len, q_width), BF)],
        scratch_shapes=[
            pltpu.VMEM((n_fsdp, feat, width), BF),
            pltpu.VMEM((max(q_len, o_rows), model_dim), BF),
            pltpu.VMEM((q_len, width), F32),
            pltpu.VMEM((2, tq, model_dim), BF),
            pltpu.VMEM((n_fsdp, 1, feat), BF),
            pltpu.VMEM((head_dim, wide), BF),
            pltpu.VMEM((kv_heads, 2, head_dim, q_len), BF),
            line,
            line,
            pltpu.VMEM((items, head_dim, wide), F32),
            heads,
            line,
            kv, kv, kv, kv,
            heads,
            sums, sums, sums, sums,
            stack,
            stack,
            pltpu.VMEM((1, wide), F32),
            pltpu.VMEM((2, head_dim, q_len), BF),
            pltpu.VMEM((head_dim, wide), F32),
        ] + [pair, trio, trio, own, own, w_link, w_link, w_link, w_link, w_side, w_side, dkv, dkv, o_link, o_link, o_link, o_link, o_core, o_core, DMA((2, n_line)), DMA((n_line,)), DMA((4 + n_fsdp,)), pair, DMA((2, n_line, items)), DMA((n_line, items)), hop, hop, side, side, side, side, side, side, dkv, dkv],
        compiler_params=params(cid),
        name="core",
    )(hidden, gain, w_qkv, w_out, cosines, sines, cotangent)


class Line:
    def __init__(self, n_line, buf_ref, pbuf_ref, send_sem, recv_sem, fill, finish):
        self.last = n_line - 1
        self.z = lax.axis_index("tp")
        self.buf, self.pbuf, self.send_sem, self.recv_sem = buf_ref, pbuf_ref, send_sem, recv_sem
        self.chunks, self.rows = buf_ref.shape[1], buf_ref.shape[2]
        self.block = pbuf_ref.shape[1]
        self.per_block = self.block // self.rows
        self.fill, self.finish = fill, finish
        self.steps = self.chunks + self.last

    def dist(self, side):
        return self.z if side else self.last - self.z

    def toward(self, side, back=False):
        up = bool(side) != back
        return {"tp": jnp.clip(self.z + 1 if up else self.z - 1, 0, self.last)}

    def copy(self, side, chunk):
        spot = self.buf.at[side, chunk]
        return remote(spot, spot, self.send_sem.at[side, chunk], self.recv_sem.at[side, chunk], self.toward(side))

    def live(self, side, step):
        chunk = step - self.dist(side)
        return chunk, (chunk >= 0) & (chunk < self.chunks)

    def prepare(self, step):
        for side in SIDES:
            chunk, ok = self.live(side, step)

            @pl.when(ok & (lax.rem(chunk, self.per_block) == 0))
            def _():
                self.fill(self.pbuf.at[side], blk((side * self.chunks + chunk) // self.per_block, self.block))

    def tick(self, step):
        for side in SIDES:
            chunk, ok = self.live(side, step)
            dist = self.dist(side)
            part = blk(lax.rem(jnp.maximum(chunk, 0), self.per_block), self.rows)

            @pl.when(ok & (dist == 0))
            def _():
                self.buf[side, chunk] = self.pbuf[side, part, :]

            @pl.when(ok & (dist > 0))
            def _():
                self.copy(side, chunk).wait_recv()
                self.buf[side, chunk] += self.pbuf[side, part, :]

            @pl.when(ok & (dist < self.last))
            def _():
                self.copy(side, chunk).start()

            @pl.when(ok & (dist == self.last))
            def _():
                self.finish(chunk, self.buf[side, chunk])

        self.prepare(step + 1)

    def drain(self):
        for side in SIDES:
            @pl.when(self.dist(side) < self.last)
            def _():
                @pl.loop(0, self.chunks)
                def _(chunk):
                    self.copy(side, chunk).wait_send()


def close_kernel(n_line, n_fsdp, d_ref, o_ref, gain_ref, hid_ref, ct_ref, n_ref, w_all, o_all, wo_all, out_ref, blk_ref, gg_ref, ts, yr, dl, xs, ks, xr, buf, gp, ga, gs, gb, gt, gc, ebuf, fb_in, fb_ct, fb_out, send_sem, recv_sem, w_sem, f_sem, ct_sem, fo_sem, lhs_sem, a_send, a_recv, ld_sem, st_sem, x_send, x_recv, e_sem, es_sem, y_send, y_recv, out_send, out_recv, o_sem, wl_sem, h_sem, r_sem, ga_send, ga_recv, gb_send, gb_recv, gc_send, gc_recv):
    last = n_line - 1
    z, flag, f = lax.axis_index("tp"), lax.axis_index("cp"), lax.axis_index("fsdp")
    far = 1 - flag
    f_core, f_x, f_diag = fsdp_peers(f)
    to_core, to_x, to_y = {"fsdp": f_core}, {"fsdp": f_x}, {"cp": far}
    _, feat, width = w_all.shape
    chunks, rows = buf.shape[1], buf.shape[2]
    half = chunks * rows
    g_rows = feat // GRAD_CHUNKS
    owner = (z == 0) | (z == last)
    own_base = jnp.where(z == last, chunks, 0)
    copy = pltpu.make_async_copy

    def own_span(chunk):
        return blk(own_base + chunk, rows)

    def f_loads(chunk):
        slot = parity(chunk)
        return copy(hid_ref.at[own_span(chunk)], fb_in.at[slot], f_sem.at[slot]), copy(ct_ref.at[own_span(chunk)], fb_ct.at[slot], ct_sem.at[slot])

    def f_store(chunk):
        slot = parity(chunk)
        return copy(fb_out.at[slot], out_ref.at[own_span(chunk)], fo_sem.at[slot])

    @pl.when(owner)
    def _():
        for chunk in SIDES:
            for load in f_loads(chunk):
                load.start()

    zero(gp)
    meet([to_core, to_x, to_y] + others("tp", z, n_line) + [{"fsdp": f_diag}])

    def finish(chunk, total):
        slot = parity(chunk)
        for load in f_loads(chunk):
            load.wait()

        @pl.when(chunk > 1)
        def _():
            f_store(chunk - 2).wait()

        x_in = fb_in[slot].astype(F32)
        inv = lax.rsqrt(lane_mean(x_in * x_in) + NORM_EPS)
        x_hat = x_in * inv
        gp[...] += row_sum(total * x_hat)
        scaled = total * gain_ref[...]
        fb_out[slot] = (fb_ct[slot].astype(F32) + inv * (scaled - x_hat * lane_mean(scaled * x_hat))).astype(BF)
        f_store(chunk).start()

        @pl.when(chunk + 2 < chunks)
        def _():
            for load in f_loads(chunk + 2):
                load.start()

    kinds = range(2)

    def g_at(ref, j):
        return ref.at[blk(j, g_rows)]

    def x_copy(j):
        return remote(g_at(xs, j), g_at(xr, j), x_send.at[j], x_recv.at[j], to_x)

    def y_copy(j):
        return remote(g_at(ts, j), g_at(yr, j), y_send.at[j], y_recv.at[j], to_y)

    def e_store(j):
        return copy(ebuf.at[0], g_at(ts, j), es_sem)

    def meet_x(j):
        x_copy(j).wait_recv()
        loads = [copy(g_at(src, j), ebuf.at[k], e_sem.at[k]) for k, src in enumerate((ks, xr))]
        for load in loads:
            load.start()
        for load in loads:
            load.wait()
        ebuf[0] += ebuf[1]
        e_store(j).start()

    def send_y(j):
        e_store(j).wait()
        y_copy(j).start()

    steps = chunks + last - 1

    def dist(side):
        return z if side else last - z

    def hop(side, chunk):
        span = blk(side * chunks + chunk, rows)
        up = z - 1 if side else z + 1
        return remote(out_ref.at[span], out_ref.at[span], out_send.at[side, chunk], out_recv.at[side, chunk], {"tp": jnp.clip(up, 0, last)})

    ends = [(end, z == (last if end else 0)) for end in SIDES]

    def owner_send(first, stop):
        for end, here in ends:
            @pl.when(here)
            def _():
                @pl.loop(first, stop)
                def _(c):
                    hop(end, c).start()

    def pass_on(step):
        for side in SIDES:
            chunk = step - (last - 1 - dist(side))

            @pl.when((dist(side) < last) & (chunk >= 0) & (chunk < chunks))
            def _():
                hop(side, chunk).wait_recv()

                @pl.when(dist(side) > 0)
                def _():
                    hop(side, chunk).start()

    def sum_phase(wbuf, pbuf, abuf, bbuf, lbuf, lhs):
        w_load = copy(w_all, wbuf, w_sem)
        w_load.start()

        def fill(dst, span):
            for k in range(n_fsdp):
                dst[:, blk(k, feat)] = dot(d_ref[span, :], wbuf[k], NT)

        line = Line(n_line, buf, pbuf, send_sem, recv_sem, fill, finish)
        slots = (f_diag, f_core, f_x, f)

        def lhs_loads(j):
            return [copy(src.at[:, blk(slot * GRAD_CHUNKS + j, g_rows)], lhs.at[m, k], lhs_sem.at[m, k]) for m, src in enumerate((n_ref, ct_ref)) for k, slot in enumerate(slots)]

        def a_copy(kind, j):
            return remote(abuf.at[kind], dl.at[kind, blk(j, g_rows)], a_send.at[kind], a_recv.at[kind, j], to_core)

        def b_stores(j):
            return [copy(bbuf.at[k], g_at(dst, j), st_sem.at[k]) for k, dst in enumerate((xs, ks))]

        def send_x(j):
            for kind in kinds:
                a_copy(kind, j).wait_send()
            for store in b_stores(j):
                store.wait()
            x_copy(j).start()

        def make(j):
            for load in lhs_loads(j):
                load.wait()
            for k in range(len(slots)):
                dst = (abuf, bbuf)[k // 2].at[k % 2]
                dst[:, :width] = dot(lhs[0, k], d_ref[...], TN)
                dst[:, width:] = dot(lhs[1, k], o_ref[...], TN)
            for kind in kinds:
                a_copy(kind, j).start()

            @pl.when(j + 1 < GRAD_CHUNKS)
            def _():
                for load in lhs_loads(j + 1):
                    load.start()

        def meet_core(j):
            loads = [copy(dl.at[kind, blk(j, g_rows)], lbuf.at[kind], ld_sem.at[kind]) for kind in kinds]
            for kind in kinds:
                a_copy(kind, j).wait_recv()
                loads[kind].start()
            for kind in kinds:
                loads[kind].wait()
                bbuf[kind] += lbuf[kind]
            for store in b_stores(j):
                store.start()

        for load in lhs_loads(0):
            load.start()
        w_load.wait()
        line.prepare(0)

        @pl.loop(0, line.steps)
        def _(fine):
            line.tick(fine)
            step = fine // PER_STEP
            whole = lax.rem(fine, PER_STEP) == 0
            j, odd = step // 2, parity(step)

            @pl.when(whole & (odd == 0) & (j < GRAD_CHUNKS))
            def _():
                make(j)

            @pl.when(whole & (odd == 1) & (j < GRAD_CHUNKS))
            def _():
                meet_core(j)
                send_x(j)

            k = ((step - FIRST_X) * 2 + 1) // 5

            @pl.when(whole & (k >= 0) & (k < EARLY) & (step == FIRST_X + 5 * k // 2))
            def _():
                meet_x(k)
                send_y(k)

            @pl.when(fine >= chunks)
            def _():
                owner_send((fine - chunks) * LEAD, (fine - chunks + 1) * LEAD)

            @pl.when(fine > chunks)
            def _():
                for k in range(PER_STEP):
                    pass_on((fine - chunks - 1) * PER_STEP + k)

        @pl.when(owner)
        def _():
            for chunk in range(chunks - 2, chunks):
                f_store(chunk).wait()

        line.drain()

    pl.run_scoped(
        sum_phase,
        pltpu.VMEM(w_all.shape, BF),
        pltpu.VMEM((2, min(128, half), buf.shape[3]), F32),
        pltpu.VMEM((2, g_rows, ts.shape[1]), F32),
        pltpu.VMEM((2, g_rows, ts.shape[1]), F32),
        pltpu.VMEM((2, g_rows, ts.shape[1]), F32),
        pltpu.VMEM((2, n_fsdp, d_ref.shape[0], g_rows), BF),
    )
    def ga_copy(end, k):
        return remote(gp, ga.at[end], ga_send.at[k], ga_recv.at[end], {"tp": k if end else 1 + k})

    def gb_copy():
        return remote(gs, gb, gb_send, gb_recv, to_y)

    def gc_copy(k, slot):
        to = lax.rem(f + k, n_fsdp)
        return remote(gt.at[to], gc.at[slot], gc_send.at[k - 1], gc_recv.at[k - 1], {"fsdp": to})

    def spread_phase(obuf, wbuf, hbuf, rbuf):
        o_load = copy(o_all, obuf, o_sem)
        o_load.start()
        q_len, n_cols = hbuf.shape[1], hbuf.shape[2]
        per_part = wo_all.shape[3] // n_cols
        items = per_part * n_fsdp

        def item_loads(item):
            slot = parity(item)
            return copy(wo_all.at[:, item // per_part, :, blk(lax.rem(item, per_part), n_cols)], wbuf.at[slot], wl_sem.at[slot]), copy(hid_ref.at[:, blk(item, n_cols)], hbuf.at[slot], h_sem.at[slot])

        def item_store(item):
            slot = parity(item)
            return copy(rbuf.at[slot], blk_ref.at[:, blk(item, n_cols)], r_sem.at[slot])

        for item in SIDES:
            for load in item_loads(item):
                load.start()

        for end, here in ends:
            @pl.when(here)
            def _():
                ga[end] = gp[...]
                for k in range(last):
                    ga_copy(end, k).start()


        def project(quarter):
            item, tile = quarter // TILES, lax.rem(quarter, TILES)
            slot = parity(item)

            @pl.when(tile == 0)
            def _():
                for load in item_loads(item):
                    load.wait()

            @pl.when((tile == 0) & (item > 1))
            def _():
                item_store(item - 2).wait()

            span = blk(tile, q_len // TILES)
            total = sum(dot(obuf[t, span, :], wbuf[slot, t], NN) for t in range(n_line))
            rbuf[slot, span, :] = (hbuf[slot, span, :].astype(F32) + total).astype(BF)

            @pl.when(tile == TILES - 1)
            def _():
                item_store(item).start()

                @pl.when(item + 2 < items)
                def _():
                    for load in item_loads(item + 2):
                        load.start()

        for end, here in ends:
            @pl.when(jnp.logical_not(here))
            def _():
                ga_copy(end, 0).wait_recv()
        gs[...] = ga[0] + ga[1]
        gb_copy().start()

        early = (last - 1) * PER_STEP

        @pl.loop(0, steps - early)
        def _(step):
            sent = step + last * LEAD
            owner_send(sent, jnp.minimum(sent + 1, chunks))
            pass_on(step + early)

            @pl.when(step == 1)
            def _():
                o_load.wait()

            @pl.when(step > 0)
            def _():
                first = (step - 1) * QUARTERS

                @pl.loop(first, jnp.minimum(first + QUARTERS, items * TILES))
                def _(quarter):
                    project(quarter)

            for k, at in LATE:
                @pl.when(step == at)
                def _():
                    meet_x(k)
                    send_y(k)

        for item in range(items - 2, items):
            item_store(item).wait()

    pl.run_scoped(
        spread_phase,
        pltpu.VMEM(o_all.shape, BF),
        pltpu.VMEM((2, n_line, wo_all.shape[2], min(512, feat)), BF),
        pltpu.VMEM((2, d_ref.shape[0], min(512, feat)), BF),
        pltpu.VMEM((2, d_ref.shape[0], min(512, feat)), BF),
    )

    gb_copy().wait()
    for k in range(n_fsdp):
        gt[k] = gs[:, blk(k, feat)] + gb[:, blk(k, feat)]
    gc[f] = gt[f]
    for side in SIDES:
        @pl.when(dist(side) > 0)
        def _():
            @pl.loop(0, chunks)
            def _(chunk):
                hop(side, chunk).wait_send()

    @pl.loop(0, GRAD_CHUNKS)
    def _(j):
        x_copy(j).wait_send()

    for k in range(1, n_fsdp):
        gc_copy(k, f).start()
    for k in range(1, n_fsdp):
        gc_copy(k, lax.rem(f + n_fsdp - k, n_fsdp)).wait_recv()
    gg_ref[...] = sum(gc[k] for k in range(n_fsdp))
    for k in range(1, n_fsdp):
        gc_copy(k, f).wait_send()
    for end, here in ends:
        @pl.when(here)
        def _():
            for k in range(last):
                ga_copy(end, k).wait_send()

    @pl.loop(0, GRAD_CHUNKS)
    def _(j):
        y_copy(j).wait()


def close(d_lin, attn_out, gain, hidden, cotangent, normed, w_full, o_all, wo_all, cid):
    q_len, model_dim = hidden.shape
    n_line, n_fsdp = wo_all.shape[:2]
    _, feat, width = w_full.shape
    g_width = width + attn_out.shape[1]
    half = q_len // 2
    rows = half // CHUNKS
    sds = jax.ShapeDtypeStruct
    row = pltpu.VMEM((1, model_dim), F32)
    slices = pltpu.VMEM((n_fsdp, 1, feat), F32)
    strip = pltpu.VMEM((2, rows, model_dim), BF)
    own, pair, line, grad, grads = DMA(()), DMA((2,)), DMA((2, CHUNKS)), DMA((GRAD_CHUNKS,)), DMA((2, GRAD_CHUNKS))
    z_trio, f_trio = DMA((n_line - 1,)), DMA((n_fsdp - 1,))
    act, g_part = sds((q_len, model_dim), BF), sds((feat, g_width), F32)
    return pl.pallas_call(
        functools.partial(close_kernel, n_line, n_fsdp),
        in_specs=[VMEM] * 3 + [ANY] * 6,
        out_specs=[ANY, ANY, VMEM] + [ANY] * 6,
        out_shape=[act, act, sds((1, feat), F32), g_part, g_part, sds((2, feat, g_width), F32), g_part, g_part, g_part],
        scratch_shapes=[
            pltpu.VMEM((2, CHUNKS, rows, model_dim), F32),
            row,
            pltpu.VMEM((2, 1, model_dim), F32),
            row,
            row,
            slices,
            slices,
            pltpu.VMEM((2, feat // GRAD_CHUNKS, g_width), F32),
            strip,
            strip,
            strip,
        ] + [line, line, own, pair, pair, pair, DMA((2, n_fsdp)), pair, grads, pair, pair, grad, grad, pair, own, grad, grad, line, line, own, pair, pair, pair, z_trio, pair, own, own, f_trio, f_trio],
        compiler_params=params(cid),
        name="close",
    )(d_lin, attn_out, gain, hidden, cotangent, normed, w_full, o_all, wo_all)


def tail_kernel(head_dim, blk_ref, hid_ref, mine_ref, theirs_ref, blk_out, hid_out, q_out, k_out, v_out, o_out):
    blk_out[...] = blk_ref[...]
    hid_out[...] = hid_ref[...]
    at = 0
    for ref in (q_out, k_out, v_out):
        for h in range(ref.shape[1]):
            cols = blk(at, head_dim)
            ref[:, h, :] = mine_ref[:, cols] + theirs_ref[:, cols]
            at += 1
    rest = slice(at * head_dim, None)
    o_out[...] = (mine_ref[:, rest] + theirs_ref[:, rest]).T


def tail(block_out, grad_hidden, mine, theirs, q_heads, kv_heads, head_dim):
    q_len, model_dim = block_out.shape
    feat = mine.shape[0]
    sds = jax.ShapeDtypeStruct
    act = pl.BlockSpec((q_len // GRAD_CHUNKS, model_dim), lambda i: (i, 0))
    part = pl.BlockSpec((feat // GRAD_CHUNKS, mine.shape[1]), lambda i: (i, 0))

    def heads(n):
        return pl.BlockSpec((feat // GRAD_CHUNKS, n, head_dim), lambda i: (i, 0, 0))

    def like(n):
        return sds((feat, n, head_dim), F32)

    o_rows = q_heads * head_dim
    return pl.pallas_call(
        functools.partial(tail_kernel, head_dim),
        grid=(GRAD_CHUNKS,),
        in_specs=[act, act, part, part],
        out_specs=[act, act, heads(q_heads), heads(kv_heads), heads(kv_heads), pl.BlockSpec((o_rows, feat // GRAD_CHUNKS), lambda i: (0, i))],
        out_shape=[sds(block_out.shape, BF), sds(block_out.shape, BF), like(q_heads), like(kv_heads), like(kv_heads), sds((o_rows, feat), F32)],
        compiler_params=pltpu.CompilerParams(vmem_limit_bytes=VMEM_BYTES),
        name="tail",
    )(block_out, grad_hidden, mine, theirs)


def solution(mesh):
    act_spec = P("fsdp", "cp", None)
    proj_spec = P("fsdp", "tp", None)
    wout_spec = P("tp", None, "fsdp")
    n_line = mesh.shape["tp"]

    def device_step(hidden, cotangent, positions, gain, w_query, w_key, w_value, w_out):
        hidden, cotangent = hidden[0], cotangent[0]
        assert hidden.shape[0] * mesh.shape["cp"] <= WINDOW_LEN
        feat, q_heads, head_dim = w_query.shape
        kv_heads = w_key.shape[1]
        group = q_heads // kv_heads
        q_width, kv_width = q_heads * head_dim, kv_heads * head_dim
        w_qkv = jnp.concatenate([w_query.reshape(feat, q_width), w_key.reshape(feat, kv_width), w_value.reshape(feat, kv_width)], axis=1)
        cosines, sines = rope_tables(positions, head_dim)
        d_lin, attn_out, gain_full, normed, w_full, wo_all, o_all = core(hidden, gain[None], w_qkv, w_out.reshape(q_width, feat), cosines, sines, cotangent, group, kv_width, n_line, 0)
        grad_hidden, block_out, grad_gain, mine, theirs = close(d_lin, attn_out, gain_full, hidden, cotangent, normed, w_full, o_all, wo_all, 1)[:5]
        block_out, grad_hidden, g_query, g_key, g_value, g_out = tail(block_out, grad_hidden, mine, theirs, q_heads, kv_heads, head_dim)
        return block_out[None], grad_hidden[None], grad_gain[0], g_query, g_key, g_value, g_out.reshape(w_out.shape)

    specs = (act_spec, act_spec, P("fsdp"), proj_spec, proj_spec, proj_spec, wout_spec)
    return jax.shard_map(device_step, mesh=mesh, in_specs=specs[:2] + (P("cp"),) + specs[2:], out_specs=specs, check_vma=False)
```

```python
import functools
import math

import jax
import jax.numpy as jnp
from jax import lax
from jax.experimental import pallas as pl
from jax.experimental.pallas import tpu as pltpu
from jax.sharding import PartitionSpec as P

WINDOW_LEN = 4096
ROPE_BASE = 10000.0
NORM_EPS = 1e-5
NEG_BIG = -1e30
LOG2E = math.log2(math.e)
TILES = 4
CHUNKS = 16
LEAD = 2
QUARTERS = 3
PIECES = 8
O_PIECES = 2
GRAD_CHUNKS = 8
FIRST_X = 6
EARLY = 6
LATE = ((6, 4), (7, 9))
VMEM_BYTES = 67043328
SIDES = range(2)

MESH = pl.DeviceIdType.MESH
ANY = pl.BlockSpec(memory_space=pl.ANY)
VMEM = pl.BlockSpec(memory_space=pltpu.VMEM)
DMA = pltpu.SemaphoreType.DMA
BF, F32 = jnp.bfloat16, jnp.float32

NT = (((1,), (1,)), ((), ()))
NN = (((1,), (0,)), ((), ()))
TN = (((0,), (0,)), ((), ()))


def dot(a, b, dims):
    return lax.dot_general(a, b, dims, preferred_element_type=F32)


def parity(k):
    return lax.rem(k, 2)


def blk(k, n):
    return pl.ds(k * n if isinstance(k, int) else pl.multiple_of(k * n, n), n)


def lane_mean(vals):
    return jnp.mean(vals, axis=1, keepdims=True)


def row_sum(vals):
    return jnp.sum(vals, axis=0, keepdims=True)


def zero(ref):
    ref[...] = jnp.zeros_like(ref)


def remote(src, dst, send, recv, where):
    return pltpu.make_async_remote_copy(src_ref=src, dst_ref=dst, send_sem=send, recv_sem=recv, device_id=where, device_id_type=MESH)


def meet(peers):
    barrier = pltpu.get_barrier_semaphore()
    for where in peers:
        pl.semaphore_signal(barrier, inc=1, device_id=where, device_id_type=MESH)
    pl.semaphore_wait(barrier, len(peers))


def fsdp_peers(f):
    core = parity(f)
    other = f + 1 - 2 * core
    far = lax.rem(f + 2, 4)
    return other, far, lax.rem(other + 2, 4)


def others(axis, index, count):
    return [{axis: lax.rem(index + k, count)} for k in range(1, count)]


def nearest(z, last):
    near = jnp.where(z > 0, last, 1)
    second = jnp.where(z == 0, 2, jnp.where(z == last, last - 1, 1))
    return near, second


def rope(vals, cos, sin, half_dim):
    return vals * cos + pltpu.roll(vals, half_dim, 1) * sin


def causal(scores, tq):
    key_idx = lax.broadcasted_iota(jnp.int32, scores.shape, 0)
    q_idx = lax.rem(lax.broadcasted_iota(jnp.int32, scores.shape, 1), tq)
    return jnp.where(key_idx <= q_idx, scores, NEG_BIG)


def params(cid):
    return pltpu.CompilerParams(collective_id=cid, has_side_effects=True, vmem_limit_bytes=VMEM_BYTES)


def rope_tables(positions, head_dim):
    inv_freq = ROPE_BASE ** (-jnp.arange(0, head_dim, 2).astype(F32) / head_dim)
    angles = positions.astype(F32)[:, None] * inv_freq[None, :]
    cosines, sines = jnp.cos(angles), jnp.sin(angles)
    return jnp.concatenate([cosines, cosines], axis=1), jnp.concatenate([-sines, sines], axis=1)


def core_kernel(group, n_line, hid_ref, gain_ref, w_ref, wo_ref, cos_ref, sin_ref, ct_ref, d_ref, o_ref, gfull_ref, n_out, w_out, wo_all, o_all, wbuf, nbuf, acc, hbuf, gbuf, qs, vt, m_all, l_all, acc_all, q_ref, lse_ref, kl_ref, vl_ref, kp_ref, vp_ref, do_ref, dkl_ref, dvl_ref, dkp_ref, dvp_ref, qs_ref, dos_ref, delta_ref, kt_ref, dqt_ref, h_sem, g_send, g_recv, own_send, own_recv, x_send, x_recv, y_send, y_recv, d_send, d_recv, kv_send, kv_recv, ox_send, ox_recv, oy_send, oy_recv, od_send, od_recv, zw_send, zw_recv, out_sem, ct_sem, o_sems, o_recv, wy_send, wy_recv, wx_send, wx_recv, wc_send, wc_recv, cx_send, cx_recv, dk_send, dk_recv):
    q_len, feat = hid_ref.shape[0], w_ref.shape[0]
    head_dim = cos_ref.shape[1]
    half_dim = head_dim // 2
    kv_width = kl_ref.shape[1]
    kv_heads = kv_width // head_dim
    q_width = q_ref.shape[1]
    tq = q_len // TILES
    wide = group * tq
    score_scale = head_dim ** -0.5
    scale = head_dim ** -0.5 * LOG2E
    half = feat // 2
    piece = half // PIECES
    o_rows = wo_ref.shape[0]
    o_half = o_rows // 2
    o_piece = o_half // O_PIECES
    flag, f, z = lax.axis_index("cp"), lax.axis_index("fsdp"), lax.axis_index("tp")
    wo_out = wo_all.at[z]
    last = n_line - 1
    far = 1 - flag
    f_core, f_x, f_diag = fsdp_peers(f)
    to_core, to_x, to_diag, to_y = {"fsdp": f_core}, {"fsdp": f_x}, {"fsdp": f_diag}, {"cp": far}

    def h_load(tile):
        slot = parity(tile)
        return pltpu.make_async_copy(hid_ref.at[blk(tile, tq)], hbuf.at[slot], h_sem.at[slot])

    h_load(0).start()
    h_load(1).start()
    meet([to_core, to_x, to_diag, to_y] + others("tp", z, n_line))

    def span(side, j):
        return blk(side * PIECES + j, piece)

    def x_copy(j):
        return remote(w_ref.at[span(flag, j)], wbuf.at[f, span(flag, j)], x_send.at[j], x_recv.at[j], to_x)

    def x_in(j):
        return remote(w_ref.at[span(flag, j)], wbuf.at[f_x, span(flag, j)], x_send.at[j], x_recv.at[j], to_x)

    def y_copy(j, side):
        return remote(wbuf.at[f_x, span(side, j)], wbuf.at[f_x, span(side, j)], y_send.at[j], y_recv.at[j], to_y)

    def d_copy(j, side, slot):
        return remote(wbuf.at[slot, span(side, j)], wbuf.at[slot, span(side, j)], d_send.at[side, j], d_recv.at[side, j], to_core)

    def g_copy(k, where, slot):
        return remote(gain_ref, gbuf.at[slot], g_send.at[k], g_recv.at[k], where)

    def own_copy(slot):
        return remote(w_ref, wbuf.at[slot], own_send, own_recv, to_core)

    def o_span(side, j):
        return blk(side * O_PIECES + j, o_piece)

    def ox_copy(j, slot):
        return remote(wo_ref.at[o_span(flag, j)], wo_out.at[slot, o_span(flag, j)], ox_send.at[j], ox_recv.at[j], to_x)

    def oy_copy(j, side):
        return remote(wo_out.at[f_x, o_span(side, j)], wo_out.at[f_x, o_span(side, j)], oy_send.at[j], oy_recv.at[j], to_y)

    def od_copy(k, src, slot, where):
        return remote(src, wo_out.at[slot, where], od_send.at[k], od_recv.at[k], to_core)

    def zw_copy(up, t):
        spot = wo_all.at[t, f, blk(flag, o_half)]
        where = jnp.minimum(z + 1, last) if up else jnp.maximum(z - 1, 0)
        src = spot if t is not z else wo_ref.at[blk(flag, o_half)]
        return remote(src, spot, zw_send.at[up, t], zw_recv.at[t], {"tp": where})

    def zw_tick(r):
        for up, t, here in ((0, z + r, z + r <= last), (1, z - r, z >= r)):
            at = jnp.clip(t, 0, last)

            @pl.when(here)
            def _():
                zw_copy(up, at).wait_recv()

            @pl.when(here & (z < last if up else z > 0))
            def _():
                zw_copy(up, at).start()

    def tile_rows(j):
        return blk(j, tq)

    o_parts = kv_heads * TILES

    def o_piece_at(ref, j):
        return ref.at[tile_rows(lax.rem(j, TILES)), blk(j // TILES, group * head_dim)]

    def o_copy(up, t, j, own=False):
        spot = o_piece_at(o_all.at[t], j)
        src = o_piece_at(o_ref, j) if own else spot
        where = jnp.minimum(z + 1, last) if up else jnp.maximum(z - 1, 0)
        return remote(src, spot, o_sems.at[up, t, j], o_recv.at[t, j], {"tp": where})

    def wo_half(r, slot, side):
        return wo_all.at[lax.rem(z + r, n_line), slot, blk(side, o_half)]

    def wy_copy(r, side):
        return remote(wo_half(r, f, side), wo_half(r, f, side), wy_send.at[r - 1], wy_recv.at[r - 1], to_y)

    def wx_copy(r, side, slot):
        return remote(wo_half(r, slot, side), wo_half(r, slot, side), wx_send.at[side, r - 1], wx_recv.at[side, r - 1], to_x)

    def wc_copy(r, side, slot):
        return remote(wo_half(r, slot, side), wo_half(r, slot, side), wc_send.at[side, r - 1], wc_recv.at[side, r - 1], to_core)

    def cx_copy(r, side, slot):
        return remote(wo_half(r, slot, side), wo_half(r, slot, side), cx_send.at[side, r - 1], cx_recv.at[side, r - 1], to_core)

    def o_tick(k):
        r, j = k // o_parts + 1, lax.rem(k, o_parts)
        for up, t, here in ((0, z + r, z + r <= last), (1, z - r, z >= r)):
            at = jnp.clip(t, 0, last)

            @pl.when(here)
            def _():
                o_copy(up, at, j).wait_recv()

            @pl.when(here & (z < last if up else z > 0))
            def _():
                o_copy(up, at, j).start()

    def wy_tick(r):
        wy_copy(r, far).wait_recv()
        wx_copy(r, far, f).start()
        for side in (flag, far):
            wc_copy(r, side, f).start()
        if r == 1:
            wy_copy(last, flag).start()

    near, second = nearest(z, last)
    own_order = (near, second, n_line * last // 2 - near - second)

    def wx_tick(q):
        r, side = (own_order[q], flag) if q < last else (q - last + 1, far)
        wx_copy(r, side, f_x).wait_recv()
        cx_copy(r, side, f_x).start()

    def o_send(j):
        for up in SIDES:
            @pl.when(z < last if up else z > 0)
            def _():
                o_copy(up, z, j, True).start()

    gains = [(k, where, where["fsdp"]) for k, where in enumerate((to_core, to_x, to_diag))]
    for k, where, _ in gains:
        g_copy(k, where, f).start()
    sends = [x_copy(j) for j in range(PIECES)] + [ox_copy(j, f) for j in range(O_PIECES)]
    for j in range(LEAD):
        sends[j].start()
    own_copy(f).start()
    all_rows = pl.ds(0, o_rows)
    for up in SIDES:
        @pl.when(z < last if up else z > 0)
        def _():
            zw_copy(up, z).start()

    local_w = pltpu.make_async_copy(w_ref, wbuf.at[f], out_sem.at[0])
    local_w.start()
    local_o = pltpu.make_async_copy(wo_ref, wo_out.at[f], out_sem.at[1])
    local_o.start()
    gbuf[f] = gain_ref[...]
    for k, where, slot in gains:
        g_copy(k, where, slot).wait_recv()
    for k in range(gbuf.shape[0]):
        gfull_ref[:, blk(k, feat)] = gbuf[k].astype(F32)

    for tile in range(TILES):
        h_load(tile).wait()
        strip = min(32, tq)

        @pl.loop(0, tq // strip)
        def _(i):
            vals = hbuf[tile % 2, blk(i, strip), :].astype(F32)
            inv = lax.rsqrt(lane_mean(vals * vals) + NORM_EPS)
            nbuf[pl.ds(pl.multiple_of(tile * tq + i * strip, strip), strip), :] = (vals * inv * gfull_ref[...]).astype(BF)

        if tile + 2 < TILES:
            h_load(tile + 2).start()
    put_n = pltpu.make_async_copy(nbuf.at[pl.ds(0, q_len)], n_out, out_sem.at[2])
    put_n.start()

    def project(slot, start, rows, first=False):
        cols = pl.ds(pl.multiple_of(slot * feat + start, 128), rows)

        @pl.loop(0, TILES)
        def _(tile):
            here = blk(tile, tq)
            part = dot(nbuf[here, cols], wbuf[slot, pl.ds(start, rows), :], NN)
            acc[here, :] = part if first else acc[here, :] + part

    def x_tick(j):
        x_in(j).wait_recv()
        y_copy(j, flag).start()
        d_copy(j, flag, f_x).start()
        sends[j + LEAD].start()

    def y_tick(j):
        y_copy(j, far).wait_recv()
        d_copy(j, 1 - flag, f_x).start()

    local_w.wait()
    project(f, 0, feat, first=True)
    x_tick(0)
    x_tick(1)
    own_copy(f_core).wait_recv()
    od_copy(0, wo_ref, f, all_rows).start()
    project(f_core, 0, feat)
    for j in range(2, PIECES):
        x_tick(j)
        y_tick(j - 2)
        if j == PIECES // 2:
            zw_tick(1)
    for j in range(PIECES):
        d_copy(j, flag, f_diag).wait_recv()
    first_half = pl.multiple_of(flag * half, half)
    project(f_x, first_half, half)
    y_tick(PIECES - 2)
    project(f_diag, first_half, half)
    y_tick(PIECES - 1)
    for j in range(PIECES):
        d_copy(j, far, f_diag).wait_recv()
    second_half = pl.multiple_of(far * half, half)
    project(f_x, second_half, half)
    project(f_diag, second_half, half)
    zw_tick(2)
    wx_copy(near, flag, f).start()
    put_w = pltpu.make_async_copy(wbuf, w_out, out_sem.at[3])
    put_w.start()

    @pl.loop(0, TILES)
    def _(tile):
        here = blk(tile, tq)
        cos, sin = cos_ref[here, :], sin_ref[here, :]
        for h in range(kv_heads):
            k_at = q_width // head_dim + h
            kl_ref[here, blk(h, head_dim)] = rope(acc[here, blk(k_at, head_dim)], cos, sin, half_dim).astype(BF)
            vl_ref[here, blk(h, head_dim)] = acc[here, blk(k_at + kv_heads, head_dim)].astype(BF)

    kv_pairs = ((kl_ref, kp_ref), (vl_ref, vp_ref))

    def kv_copies(g):
        return [remote(src.at[:, blk(g, head_dim)], dst.at[:, blk(g, head_dim)], kv_send.at[k, g], kv_recv.at[k, g], {"cp": 1}) for k, (src, dst) in enumerate(kv_pairs)]

    @pl.when(flag == 0)
    def _():
        zero(kp_ref)
        zero(vp_ref)
        for g in range(kv_heads):
            for copy in kv_copies(g):
                copy.start()

    @pl.loop(0, TILES)
    def _(tile):
        here = blk(tile, tq)
        cos, sin = cos_ref[here, :], sin_ref[here, :]
        for h in range(group * kv_heads):
            cols = blk(h, head_dim)
            q_ref[here, cols] = rope(acc[here, cols], cos, sin, half_dim).astype(BF)

    def load_q(item):
        g, tile = item // TILES, lax.rem(item, TILES)
        rows = blk(tile, tq)
        for h in range(group):
            qs[:, blk(h, tq)] = q_ref[rows, blk(g * group + h, head_dim)].T

    def key_piece(item, k_ref, side, start, masked):
        g = item // TILES
        scores = dot(k_ref[start, blk(g, head_dim)], qs[...], NN)
        if masked:
            scores = causal(scores, tq)
        m_old = m_all[item]
        m_new = jnp.maximum(m_old, jnp.max(scores, axis=0, keepdims=True))
        probs = jnp.exp2((scores - m_new) * scale)
        fade = jnp.exp2((m_old - m_new) * scale)
        m_all[item] = m_new
        l_all[item] = l_all[item] * fade + row_sum(probs)
        acc_all[item] = acc_all[item] * fade + dot(vt[g, side, :, start], probs.astype(BF), NN)

    for g in range(kv_heads):
        vt[g, 0] = vl_ref[:, blk(g, head_dim)].T

    @pl.loop(0, kv_heads * TILES)
    def _(item):
        tile = lax.rem(item, TILES)
        load_q(item)
        m_all[item] = jnp.full_like(m_all[item], NEG_BIG)
        l_all[item] = jnp.zeros_like(l_all[item])
        acc_all[item] = jnp.zeros_like(acc_all[item])
        key_piece(item, kl_ref, 0, blk(tile, tq), True)

        @pl.loop(0, tile // 2)
        def _(i):
            key_piece(item, kl_ref, 0, blk(i, 2 * tq), False)

        @pl.when(parity(tile) == 1)
        def _():
            key_piece(item, kl_ref, 0, blk(tile - 1, tq), False)

    for j in range(O_PIECES):
        ox_copy(j, f_x).wait_recv()
        oy_copy(j, flag).start()
        od_copy(1 + j, wo_out.at[f_x, o_span(flag, j)], f_x, o_span(flag, j)).start()

    wx_copy(second, flag, f).start()
    zw_tick(last)

    @pl.loop(0, kv_heads * TILES)
    def _(item):
        g, tile = item // TILES, lax.rem(item, TILES)
        rows = blk(tile, tq)

        @pl.when((flag == 1) & (tile == 0))
        def _():
            for copy in kv_copies(g):
                copy.wait_recv()
            vt[g, 1] = vp_ref[:, blk(g, head_dim)].T

        @pl.when(flag == 1)
        def _():
            load_q(item)

        @pl.loop(0, flag * TILES // 2)
        def _(i):
            key_piece(item, kp_ref, 1, blk(i, 2 * tq), False)

        total = l_all[item]
        lse_ref[item] = m_all[item] * scale + jnp.log2(total)
        out_t = acc_all[item] / total
        for h in range(group):
            o_ref[rows, blk(g * group + h, head_dim)] = out_t[:, h * tq:h * tq + tq].T.astype(BF)

        @pl.when(item > 0)
        def _():
            o_send(item - 1)

        for j in range(O_PIECES):
            @pl.when(item == (j + 1) * kv_heads * TILES // O_PIECES - 1)
            def _():
                oy_copy(j, far).wait_recv()
                od_copy(1 + O_PIECES + j, wo_out.at[f_x, o_span(1 - flag, j)], f_x, o_span(1 - flag, j)).start()

    o_send(o_parts - 1)
    wx_copy(own_order[last - 1], flag, f).start()
    for r in range(1, last):
        wy_copy(r, flag).start()
    od_copy(0, wo_ref, f_core, all_rows).wait_recv()
    for j in range(O_PIECES):
        od_copy(1 + j, wo_out.at[f_x, o_span(flag, j)], f_diag, o_span(flag, j)).wait_recv()
        od_copy(1 + O_PIECES + j, wo_out.at[f_x, o_span(1 - flag, j)], f_diag, o_span(1 - flag, j)).wait_recv()

    put_n.wait()
    local_o.wait()
    n_parts, _, part = wo_out.shape
    loads = [pltpu.make_async_copy(wo_out.at[k], nbuf.at[pl.ds(0, o_rows), blk(k, part)], out_sem.at[4 + k]) for k in range(n_parts)]
    for load in loads:
        load.start()
    keep = pltpu.make_async_copy(o_ref, o_all.at[z], out_sem.at[2])
    keep.start()

    def ct_load(tile):
        slot = parity(tile)
        return pltpu.make_async_copy(ct_ref.at[blk(tile, tq)], hbuf.at[slot], ct_sem.at[slot])

    ct_load(0).start()
    ct_load(1).start()
    zero(dkl_ref)
    zero(dvl_ref)

    @pl.when(flag == 1)
    def _():
        zero(dkp_ref)
        zero(dvp_ref)

    wx_tick(0)
    for k in SIDES:
        o_tick(jnp.int32(k))
    for load in loads:
        load.wait()

    def do_tile(tile):
        ct_load(tile).wait()
        do_ref[tile_rows(tile), :] = dot(hbuf[parity(tile)], nbuf[pl.ds(0, o_rows), :], NT).astype(BF)

        @pl.when(tile + 2 < TILES)
        def _():
            ct_load(tile + 2).start()

    def bwd_item(item):
        g, tile = item // TILES, lax.rem(item, TILES)
        kv_cols = blk(g, head_dim)
        rows = blk(tile, tq)

        @pl.when(tile == 0)
        def _():
            kt_ref[0] = kl_ref[:, kv_cols].T
            kt_ref[1] = kp_ref[:, kv_cols].T

        for h in range(group):
            cols = blk(g * group + h, head_dim)
            stack = blk(h, tq)
            qs_ref[stack, :] = q_ref[rows, cols]
            d_h = do_ref[rows, cols]
            dos_ref[stack, :] = d_h
            prod = d_h.astype(F32) * o_ref[rows, cols].astype(F32)
            delta_ref[:, stack] = row_sum(prod.T)
        zero(dqt_ref)

        def piece(k_ref, v_ref, dk_ref, dv_ref, side, span, masked):
            scores = dot(k_ref[span, kv_cols], qs_ref[...], NT)
            if masked:
                scores = causal(scores, tq)
            probs = jnp.exp2(scores * (score_scale * LOG2E) - lse_ref[item])
            d_probs = dot(v_ref[span, kv_cols], dos_ref[...], NT)
            d_scores = (probs * (d_probs - delta_ref[...])).astype(BF)
            dv_ref[g, span, :] += dot(probs.astype(BF), dos_ref[...], NN)
            dk_ref[g, span, :] += dot(d_scores, qs_ref[...], NN)
            dqt_ref[...] += dot(kt_ref[side, :, span], d_scores, NN)

        piece(kl_ref, vl_ref, dkl_ref, dvl_ref, 0, blk(tile, tq), True)

        @pl.loop(0, tile // 2)
        def _(i):
            piece(kl_ref, vl_ref, dkl_ref, dvl_ref, 0, blk(i, 2 * tq), False)

        @pl.when(parity(tile) == 1)
        def _():
            piece(kl_ref, vl_ref, dkl_ref, dvl_ref, 0, blk(tile - 1, tq), False)

        @pl.loop(0, flag * TILES // 2)
        def _(i):
            piece(kp_ref, vp_ref, dkp_ref, dvp_ref, 1, blk(i, 2 * tq), False)

        for h in range(group):
            dq_h = dqt_ref[:, blk(h, tq)].T * score_scale
            d_ref[rows, blk(g * group + h, head_dim)] = rope(dq_h, cos_ref[rows, :], -sin_ref[rows, :], half_dim).astype(BF)

        @pl.when((tile == TILES - 1) & (flag == 1))
        def _():
            for copy in back(g):
                copy.start()

    def back(g):
        return [remote(ref.at[g], ref.at[g], dk_send.at[k, g], dk_recv.at[k, g], {"cp": 0}) for k, ref in enumerate((dkp_ref, dvp_ref))]

    def kv_done(g):
        @pl.when(flag == 0)
        def _():
            for copy in back(g):
                copy.wait_recv()
            dkl_ref[g] += dkp_ref[g]
            dvl_ref[g] += dvp_ref[g]

        dk = rope(dkl_ref[g] * score_scale, cos_ref[...], -sin_ref[...], half_dim)
        k_at = q_width // head_dim + g
        d_ref[:, blk(k_at, head_dim)] = dk.astype(BF)
        d_ref[:, blk(k_at + kv_heads, head_dim)] = dvl_ref[g].astype(BF)

        @pl.when(flag == 1)
        def _():
            for copy in back(g):
                copy.wait_send()

    items = TILES * (kv_heads + 1)
    plan = {1: [(wx_tick, 1)], 5: [(wy_tick, 1)], 6: [(wx_tick, 2)], 8: [(wy_tick, 2)], 9: [(wx_tick, 3)]}

    @pl.loop(0, items)
    def _(item):
        @pl.when(item < TILES)
        def _():
            do_tile(item)

        @pl.when(item >= TILES)
        def _():
            bwd_item(item - TILES)

        @pl.when(item != 1)
        def _():
            o_tick(jnp.where(item > 1, item + 1, 2))

        for at, jobs in plan.items():
            @pl.when(item == at)
            def _():
                for tick, arg in jobs:
                    tick(arg)

    rest = {1: (wy_tick, 3), 2: (wx_tick, 4), 5: (kv_done, 0), 6: (wx_tick, 5), 9: (kv_done, 1)}
    for k in range(items + 1, o_parts * last):
        o_tick(jnp.int32(k))
        if k - items in rest:
            tick, arg = rest[k - items]
            tick(arg)

    for r in range(1, n_line):
        for side in (flag, far):
            wc_copy(r, side, f_core).wait_recv()
            cx_copy(r, side, f_diag).wait_recv()
            wc_copy(r, side, f).wait_send()
            cx_copy(r, side, f_x).wait_send()
            wx_copy(r, side, f).wait_send()
        wy_copy(r, flag).wait_send()

    @pl.loop(0, n_line)
    def _(t):
        for up in SIDES:
            @pl.when((t <= z) & (z < last) if up else (t >= z) & (z > 0))
            def _():
                for j in range(o_parts):
                    o_copy(up, t, j).wait_send()

    @pl.loop(0, n_line)
    def _(t):
        for up in SIDES:
            @pl.when((t <= z) & (z < last) if up else (t >= z) & (z > 0))
            def _():
                zw_copy(up, t).wait_send()

    for k, where, _ in gains:
        g_copy(k, where, f).wait_send()
    own_copy(f).wait_send()
    od_copy(0, wo_ref, f, all_rows).wait_send()
    for j in range(PIECES):
        x_copy(j).wait_send()
        y_copy(j, flag).wait_send()
        d_copy(j, flag, f_x).wait_send()
        d_copy(j, 1 - flag, f_x).wait_send()
    for j in range(O_PIECES):
        ox_copy(j, f).wait_send()
        oy_copy(j, flag).wait_send()
        od_copy(1 + j, wo_out.at[f_x, o_span(flag, j)], f_x, o_span(flag, j)).wait_send()
        od_copy(1 + O_PIECES + j, wo_out.at[f_x, o_span(1 - flag, j)], f_x, o_span(1 - flag, j)).wait_send()

    @pl.when(flag == 0)
    def _():
        for g in range(kv_heads):
            for copy in kv_copies(g):
                copy.wait_send()

    for local in (keep, put_w):
        local.wait()


def core(hidden, gain, w_qkv, w_out, cosines, sines, cotangent, group, kv_width, n_line, cid):
    q_len, model_dim = hidden.shape
    feat, width = w_qkv.shape
    head_dim = cosines.shape[1]
    q_width = width - 2 * kv_width
    kv_heads = kv_width // head_dim
    o_rows, o_cols = w_out.shape
    n_fsdp = model_dim // feat
    tq = q_len // TILES
    wide = group * tq
    items = kv_heads * TILES
    sds = jax.ShapeDtypeStruct
    line = pltpu.VMEM((items, 1, wide), F32)
    kv = pltpu.VMEM((q_len, kv_width), BF)
    heads = pltpu.VMEM((q_len, q_width), BF)
    sums = pltpu.VMEM((kv_heads, q_len, head_dim), F32)
    stack = pltpu.VMEM((wide, head_dim), BF)
    own, pair, trio = DMA(()), DMA((2,)), DMA((n_fsdp - 1,))
    w_link, w_side, o_link, o_core = DMA((PIECES,)), DMA((2, PIECES)), DMA((O_PIECES,)), DMA((1 + 2 * O_PIECES,))
    hop, side, dkv = DMA((n_line - 1,)), DMA((2, n_line - 1)), DMA((2, kv_heads))
    return pl.pallas_call(
        functools.partial(core_kernel, group, n_line),
        in_specs=[ANY] + [VMEM] * 5 + [ANY],
        out_specs=[VMEM] * 3 + [ANY] * 4,
        out_shape=[sds((q_len, width), BF), sds((q_len, q_width), BF), sds((1, model_dim), F32), sds((q_len, model_dim), BF), sds((n_fsdp, feat, width), BF), sds((n_line, n_fsdp, o_rows, o_cols), BF), sds((n_line, q_len, q_width), BF)],
        scratch_shapes=[
            pltpu.VMEM((n_fsdp, feat, width), BF),
            pltpu.VMEM((max(q_len, o_rows), model_dim), BF),
            pltpu.VMEM((q_len, width), F32),
            pltpu.VMEM((2, tq, model_dim), BF),
            pltpu.VMEM((n_fsdp, 1, feat), BF),
            pltpu.VMEM((head_dim, wide), BF),
            pltpu.VMEM((kv_heads, 2, head_dim, q_len), BF),
            line,
            line,
            pltpu.VMEM((items, head_dim, wide), F32),
            heads,
            line,
            kv, kv, kv, kv,
            heads,
            sums, sums, sums, sums,
            stack,
            stack,
            pltpu.VMEM((1, wide), F32),
            pltpu.VMEM((2, head_dim, q_len), BF),
            pltpu.VMEM((head_dim, wide), F32),
        ] + [pair, trio, trio, own, own, w_link, w_link, w_link, w_link, w_side, w_side, dkv, dkv, o_link, o_link, o_link, o_link, o_core, o_core, DMA((2, n_line)), DMA((n_line,)), DMA((4 + n_fsdp,)), pair, DMA((2, n_line, items)), DMA((n_line, items)), hop, hop, side, side, side, side, side, side, dkv, dkv],
        compiler_params=params(cid),
        name="core",
    )(hidden, gain, w_qkv, w_out, cosines, sines, cotangent)


class Line:
    def __init__(self, n_line, buf_ref, pbuf_ref, send_sem, recv_sem, fill, finish):
        self.last = n_line - 1
        self.z = lax.axis_index("tp")
        self.buf, self.pbuf, self.send_sem, self.recv_sem = buf_ref, pbuf_ref, send_sem, recv_sem
        self.chunks, self.rows = buf_ref.shape[1], buf_ref.shape[2]
        self.block = pbuf_ref.shape[1]
        self.per_block = self.block // self.rows
        self.fill, self.finish = fill, finish
        self.steps = self.chunks + self.last

    def dist(self, side):
        return self.z if side else self.last - self.z

    def toward(self, side, back=False):
        up = bool(side) != back
        return {"tp": jnp.clip(self.z + 1 if up else self.z - 1, 0, self.last)}

    def copy(self, side, chunk):
        spot = self.buf.at[side, chunk]
        return remote(spot, spot, self.send_sem.at[side, chunk], self.recv_sem.at[side, chunk], self.toward(side))

    def live(self, side, step):
        chunk = step - self.dist(side)
        return chunk, (chunk >= 0) & (chunk < self.chunks)

    def prepare(self, step):
        for side in SIDES:
            chunk, ok = self.live(side, step)

            @pl.when(ok & (lax.rem(chunk, self.per_block) == 0))
            def _():
                self.fill(self.pbuf.at[side], blk((side * self.chunks + chunk) // self.per_block, self.block))

    def tick(self, step):
        for side in SIDES:
            chunk, ok = self.live(side, step)
            dist = self.dist(side)
            part = blk(lax.rem(jnp.maximum(chunk, 0), self.per_block), self.rows)

            @pl.when(ok & (dist == 0))
            def _():
                self.buf[side, chunk] = self.pbuf[side, part, :]

            @pl.when(ok & (dist > 0))
            def _():
                self.copy(side, chunk).wait_recv()
                self.buf[side, chunk] += self.pbuf[side, part, :]

            @pl.when(ok & (dist < self.last))
            def _():
                self.copy(side, chunk).start()

            @pl.when(ok & (dist == self.last))
            def _():
                self.finish(chunk, self.buf[side, chunk])

        self.prepare(step + 1)

    def drain(self):
        for side in SIDES:
            @pl.when(self.dist(side) < self.last)
            def _():
                @pl.loop(0, self.chunks)
                def _(chunk):
                    self.copy(side, chunk).wait_send()


def close_kernel(n_line, n_fsdp, d_ref, o_ref, gain_ref, hid_ref, ct_ref, n_ref, w_all, o_all, wo_all, out_ref, blk_ref, gg_ref, ts, yr, dl, xs, ks, xr, buf, gp, ga, gs, gb, gt, gc, ebuf, fb_in, fb_ct, fb_out, send_sem, recv_sem, w_sem, f_sem, ct_sem, fo_sem, lhs_sem, a_send, a_recv, ld_sem, st_sem, x_send, x_recv, e_sem, es_sem, y_send, y_recv, out_send, out_recv, o_sem, wl_sem, h_sem, r_sem, ga_send, ga_recv, gb_send, gb_recv, gc_send, gc_recv):
    last = n_line - 1
    z, flag, f = lax.axis_index("tp"), lax.axis_index("cp"), lax.axis_index("fsdp")
    far = 1 - flag
    f_core, f_x, f_diag = fsdp_peers(f)
    to_core, to_x, to_y = {"fsdp": f_core}, {"fsdp": f_x}, {"cp": far}
    _, feat, width = w_all.shape
    chunks, rows = buf.shape[1], buf.shape[2]
    half = chunks * rows
    g_rows = feat // GRAD_CHUNKS
    owner = (z == 0) | (z == last)
    own_base = jnp.where(z == last, chunks, 0)
    copy = pltpu.make_async_copy

    def own_span(chunk):
        return blk(own_base + chunk, rows)

    def f_loads(chunk):
        slot = parity(chunk)
        return copy(hid_ref.at[own_span(chunk)], fb_in.at[slot], f_sem.at[slot]), copy(ct_ref.at[own_span(chunk)], fb_ct.at[slot], ct_sem.at[slot])

    def f_store(chunk):
        slot = parity(chunk)
        return copy(fb_out.at[slot], out_ref.at[own_span(chunk)], fo_sem.at[slot])

    @pl.when(owner)
    def _():
        for chunk in SIDES:
            for load in f_loads(chunk):
                load.start()

    zero(gp)

    def finish(chunk, total):
        slot = parity(chunk)
        for load in f_loads(chunk):
            load.wait()

        @pl.when(chunk > 1)
        def _():
            f_store(chunk - 2).wait()

        x_in = fb_in[slot].astype(F32)
        inv = lax.rsqrt(lane_mean(x_in * x_in) + NORM_EPS)
        x_hat = x_in * inv
        gp[...] += row_sum(total * x_hat)
        scaled = total * gain_ref[...]
        fb_out[slot] = (fb_ct[slot].astype(F32) + inv * (scaled - x_hat * lane_mean(scaled * x_hat))).astype(BF)
        f_store(chunk).start()

        @pl.when(chunk + 2 < chunks)
        def _():
            for load in f_loads(chunk + 2):
                load.start()

    kinds = range(2)

    def g_at(ref, j):
        return ref.at[blk(j, g_rows)]

    def x_copy(j):
        return remote(g_at(xs, j), g_at(xr, j), x_send.at[j], x_recv.at[j], to_x)

    def y_copy(j):
        return remote(g_at(ts, j), g_at(yr, j), y_send.at[j], y_recv.at[j], to_y)

    def e_store(j):
        return copy(ebuf.at[0], g_at(ts, j), es_sem)

    def meet_x(j):
        x_copy(j).wait_recv()
        loads = [copy(g_at(src, j), ebuf.at[k], e_sem.at[k]) for k, src in enumerate((ks, xr))]
        for load in loads:
            load.start()
        for load in loads:
            load.wait()
        ebuf[0] += ebuf[1]
        e_store(j).start()

    def send_y(j):
        e_store(j).wait()
        y_copy(j).start()

    steps = chunks + last - 1

    def dist(side):
        return z if side else last - z

    def hop(side, chunk):
        span = blk(side * chunks + chunk, rows)
        up = z - 1 if side else z + 1
        return remote(out_ref.at[span], out_ref.at[span], out_send.at[side, chunk], out_recv.at[side, chunk], {"tp": jnp.clip(up, 0, last)})

    ends = [(end, z == (last if end else 0)) for end in SIDES]

    def owner_send(first, stop):
        for end, here in ends:
            @pl.when(here)
            def _():
                @pl.loop(first, stop)
                def _(c):
                    hop(end, c).start()

    def pass_on(step):
        for side in SIDES:
            chunk = step - (last - 1 - dist(side))

            @pl.when((dist(side) < last) & (chunk >= 0) & (chunk < chunks))
            def _():
                hop(side, chunk).wait_recv()

                @pl.when(dist(side) > 0)
                def _():
                    hop(side, chunk).start()

    def sum_phase(wbuf, pbuf, abuf, bbuf, lbuf, lhs):
        w_load = copy(w_all, wbuf, w_sem)
        w_load.start()

        def fill(dst, span):
            for k in range(n_fsdp):
                dst[:, blk(k, feat)] = dot(d_ref[span, :], wbuf[k], NT)

        line = Line(n_line, buf, pbuf, send_sem, recv_sem, fill, finish)
        slots = (f_diag, f_core, f_x, f)

        def lhs_loads(j):
            return [copy(src.at[:, blk(slot * GRAD_CHUNKS + j, g_rows)], lhs.at[m, k], lhs_sem.at[m, k]) for m, src in enumerate((n_ref, ct_ref)) for k, slot in enumerate(slots)]

        def a_copy(kind, j):
            return remote(abuf.at[kind], dl.at[kind, blk(j, g_rows)], a_send.at[kind], a_recv.at[kind, j], to_core)

        def b_stores(j):
            return [copy(bbuf.at[k], g_at(dst, j), st_sem.at[k]) for k, dst in enumerate((xs, ks))]

        def send_x(j):
            for kind in kinds:
                a_copy(kind, j).wait_send()
            for store in b_stores(j):
                store.wait()
            x_copy(j).start()

        def make(j):
            for load in lhs_loads(j):
                load.wait()
            for k in range(len(slots)):
                dst = (abuf, bbuf)[k // 2].at[k % 2]
                dst[:, :width] = dot(lhs[0, k], d_ref[...], TN)
                dst[:, width:] = dot(lhs[1, k], o_ref[...], TN)
            for kind in kinds:
                a_copy(kind, j).start()

            @pl.when(j + 1 < GRAD_CHUNKS)
            def _():
                for load in lhs_loads(j + 1):
                    load.start()

        def meet_core(j):
            loads = [copy(dl.at[kind, blk(j, g_rows)], lbuf.at[kind], ld_sem.at[kind]) for kind in kinds]
            for kind in kinds:
                a_copy(kind, j).wait_recv()
                loads[kind].start()
            for kind in kinds:
                loads[kind].wait()
                bbuf[kind] += lbuf[kind]
            for store in b_stores(j):
                store.start()

        for load in lhs_loads(0):
            load.start()
        w_load.wait()
        line.prepare(0)
        meet([to_core, to_x, to_y] + others("tp", z, n_line) + [{"fsdp": f_diag}])

        @pl.loop(0, line.steps)
        def _(fine):
            line.tick(fine)
            j, odd = fine // 2, parity(fine)

            @pl.when((odd == 0) & (j < GRAD_CHUNKS))
            def _():
                make(j)

            @pl.when((odd == 1) & (j < GRAD_CHUNKS))
            def _():
                meet_core(j)
                send_x(j)

            k = ((fine - FIRST_X) * 2 + 1) // 5

            @pl.when((k >= 0) & (k < EARLY) & (fine == FIRST_X + 5 * k // 2))
            def _():
                meet_x(k)
                send_y(k)

            @pl.when(fine >= chunks)
            def _():
                owner_send((fine - chunks) * LEAD, (fine - chunks + 1) * LEAD)

            @pl.when(fine > chunks)
            def _():
                for k in range(LEAD):
                    pass_on((fine - chunks - 1) * LEAD + k)

        @pl.when(owner)
        def _():
            for chunk in range(chunks - 2, chunks):
                f_store(chunk).wait()

        line.drain()

    pl.run_scoped(
        sum_phase,
        pltpu.VMEM(w_all.shape, BF),
        pltpu.VMEM((2, min(128, half), buf.shape[3]), F32),
        pltpu.VMEM((2, g_rows, ts.shape[1]), F32),
        pltpu.VMEM((2, g_rows, ts.shape[1]), F32),
        pltpu.VMEM((2, g_rows, ts.shape[1]), F32),
        pltpu.VMEM((2, n_fsdp, d_ref.shape[0], g_rows), BF),
    )
    def ga_copy(end, k):
        return remote(gp, ga.at[end], ga_send.at[k], ga_recv.at[end], {"tp": k if end else 1 + k})

    def gb_copy():
        return remote(gs, gb, gb_send, gb_recv, to_y)

    def gc_copy(k, slot):
        to = lax.rem(f + k, n_fsdp)
        return remote(gt.at[to], gc.at[slot], gc_send.at[k - 1], gc_recv.at[k - 1], {"fsdp": to})

    def spread_phase(obuf, wbuf, hbuf, rbuf):
        o_load = copy(o_all, obuf, o_sem)
        o_load.start()
        q_len, n_cols = hbuf.shape[1], hbuf.shape[2]
        per_part = wo_all.shape[3] // n_cols
        items = per_part * n_fsdp

        def item_loads(item):
            slot = parity(item)
            return copy(wo_all.at[:, item // per_part, :, blk(lax.rem(item, per_part), n_cols)], wbuf.at[slot], wl_sem.at[slot]), copy(hid_ref.at[:, blk(item, n_cols)], hbuf.at[slot], h_sem.at[slot])

        def item_store(item):
            slot = parity(item)
            return copy(rbuf.at[slot], blk_ref.at[:, blk(item, n_cols)], r_sem.at[slot])

        for item in SIDES:
            for load in item_loads(item):
                load.start()

        for end, here in ends:
            @pl.when(here)
            def _():
                ga[end] = gp[...]
                for k in range(last):
                    ga_copy(end, k).start()


        def project(quarter):
            item, tile = quarter // TILES, lax.rem(quarter, TILES)
            slot = parity(item)

            @pl.when(tile == 0)
            def _():
                for load in item_loads(item):
                    load.wait()

            @pl.when((tile == 0) & (item > 1))
            def _():
                item_store(item - 2).wait()

            span = blk(tile, q_len // TILES)
            total = sum(dot(obuf[t, span, :], wbuf[slot, t], NN) for t in range(n_line))
            rbuf[slot, span, :] = (hbuf[slot, span, :].astype(F32) + total).astype(BF)

            @pl.when(tile == TILES - 1)
            def _():
                item_store(item).start()

                @pl.when(item + 2 < items)
                def _():
                    for load in item_loads(item + 2):
                        load.start()

        for end, here in ends:
            @pl.when(jnp.logical_not(here))
            def _():
                ga_copy(end, 0).wait_recv()
        gs[...] = ga[0] + ga[1]
        gb_copy().start()

        early = (last - 1) * LEAD

        @pl.loop(0, steps - early)
        def _(step):
            sent = step + last * LEAD
            owner_send(sent, jnp.minimum(sent + 1, chunks))
            pass_on(step + early)

            @pl.when(step == 1)
            def _():
                o_load.wait()

            @pl.when(step > 0)
            def _():
                first = (step - 1) * QUARTERS

                @pl.loop(first, jnp.minimum(first + QUARTERS, items * TILES))
                def _(quarter):
                    project(quarter)

            for k, at in LATE:
                @pl.when(step == at)
                def _():
                    meet_x(k)
                    send_y(k)

        for item in range(items - 2, items):
            item_store(item).wait()

    pl.run_scoped(
        spread_phase,
        pltpu.VMEM(o_all.shape, BF),
        pltpu.VMEM((2, n_line, wo_all.shape[2], min(512, feat)), BF),
        pltpu.VMEM((2, d_ref.shape[0], min(512, feat)), BF),
        pltpu.VMEM((2, d_ref.shape[0], min(512, feat)), BF),
    )

    gb_copy().wait()
    for k in range(n_fsdp):
        gt[k] = gs[:, blk(k, feat)] + gb[:, blk(k, feat)]
    gc[f] = gt[f]
    for side in SIDES:
        @pl.when(dist(side) > 0)
        def _():
            @pl.loop(0, chunks)
            def _(chunk):
                hop(side, chunk).wait_send()

    @pl.loop(0, GRAD_CHUNKS)
    def _(j):
        x_copy(j).wait_send()

    for k in range(1, n_fsdp):
        gc_copy(k, f).start()
    for k in range(1, n_fsdp):
        gc_copy(k, lax.rem(f + n_fsdp - k, n_fsdp)).wait_recv()
    gg_ref[...] = sum(gc[k] for k in range(n_fsdp))
    for k in range(1, n_fsdp):
        gc_copy(k, f).wait_send()
    for end, here in ends:
        @pl.when(here)
        def _():
            for k in range(last):
                ga_copy(end, k).wait_send()

    @pl.loop(0, GRAD_CHUNKS)
    def _(j):
        y_copy(j).wait()


def close(d_lin, attn_out, gain, hidden, cotangent, normed, w_full, o_all, wo_all, cid):
    q_len, model_dim = hidden.shape
    n_line, n_fsdp = wo_all.shape[:2]
    _, feat, width = w_full.shape
    g_width = width + attn_out.shape[1]
    half = q_len // 2
    rows = half // CHUNKS
    sds = jax.ShapeDtypeStruct
    row = pltpu.VMEM((1, model_dim), F32)
    slices = pltpu.VMEM((n_fsdp, 1, feat), F32)
    strip = pltpu.VMEM((2, rows, model_dim), BF)
    own, pair, line, grad, grads = DMA(()), DMA((2,)), DMA((2, CHUNKS)), DMA((GRAD_CHUNKS,)), DMA((2, GRAD_CHUNKS))
    z_trio, f_trio = DMA((n_line - 1,)), DMA((n_fsdp - 1,))
    act, g_part = sds((q_len, model_dim), BF), sds((feat, g_width), F32)
    return pl.pallas_call(
        functools.partial(close_kernel, n_line, n_fsdp),
        in_specs=[VMEM] * 3 + [ANY] * 6,
        out_specs=[ANY, ANY, VMEM] + [ANY] * 6,
        out_shape=[act, act, sds((1, feat), F32), g_part, g_part, sds((2, feat, g_width), F32), g_part, g_part, g_part],
        scratch_shapes=[
            pltpu.VMEM((2, CHUNKS, rows, model_dim), F32),
            row,
            pltpu.VMEM((2, 1, model_dim), F32),
            row,
            row,
            slices,
            slices,
            pltpu.VMEM((2, feat // GRAD_CHUNKS, g_width), F32),
            strip,
            strip,
            strip,
        ] + [line, line, own, pair, pair, pair, DMA((2, n_fsdp)), pair, grads, pair, pair, grad, grad, pair, own, grad, grad, line, line, own, pair, pair, pair, z_trio, pair, own, own, f_trio, f_trio],
        compiler_params=params(cid),
        name="close",
    )(d_lin, attn_out, gain, hidden, cotangent, normed, w_full, o_all, wo_all)


def tail_kernel(head_dim, blk_ref, hid_ref, mine_ref, theirs_ref, blk_out, hid_out, q_out, k_out, v_out, o_out):
    blk_out[...] = blk_ref[...]
    hid_out[...] = hid_ref[...]
    at = 0
    for ref in (q_out, k_out, v_out):
        for h in range(ref.shape[1]):
            cols = blk(at, head_dim)
            ref[:, h, :] = mine_ref[:, cols] + theirs_ref[:, cols]
            at += 1
    rest = slice(at * head_dim, None)
    o_out[...] = (mine_ref[:, rest] + theirs_ref[:, rest]).T


def tail(block_out, grad_hidden, mine, theirs, q_heads, kv_heads, head_dim):
    q_len, model_dim = block_out.shape
    feat = mine.shape[0]
    sds = jax.ShapeDtypeStruct
    act = pl.BlockSpec((q_len // GRAD_CHUNKS, model_dim), lambda i: (i, 0))
    part = pl.BlockSpec((feat // GRAD_CHUNKS, mine.shape[1]), lambda i: (i, 0))

    def heads(n):
        return pl.BlockSpec((feat // GRAD_CHUNKS, n, head_dim), lambda i: (i, 0, 0))

    def like(n):
        return sds((feat, n, head_dim), F32)

    o_rows = q_heads * head_dim
    return pl.pallas_call(
        functools.partial(tail_kernel, head_dim),
        grid=(GRAD_CHUNKS,),
        in_specs=[act, act, part, part],
        out_specs=[act, act, heads(q_heads), heads(kv_heads), heads(kv_heads), pl.BlockSpec((o_rows, feat // GRAD_CHUNKS), lambda i: (0, i))],
        out_shape=[sds(block_out.shape, BF), sds(block_out.shape, BF), like(q_heads), like(kv_heads), like(kv_heads), sds((o_rows, feat), F32)],
        compiler_params=pltpu.CompilerParams(vmem_limit_bytes=VMEM_BYTES),
        name="tail",
    )(block_out, grad_hidden, mine, theirs)


def solution(mesh):
    act_spec = P("fsdp", "cp", None)
    proj_spec = P("fsdp", "tp", None)
    wout_spec = P("tp", None, "fsdp")
    n_line = mesh.shape["tp"]

    def device_step(hidden, cotangent, positions, gain, w_query, w_key, w_value, w_out):
        hidden, cotangent = hidden[0], cotangent[0]
        assert hidden.shape[0] * mesh.shape["cp"] <= WINDOW_LEN
        feat, q_heads, head_dim = w_query.shape
        kv_heads = w_key.shape[1]
        group = q_heads // kv_heads
        q_width, kv_width = q_heads * head_dim, kv_heads * head_dim
        w_qkv = jnp.concatenate([w_query.reshape(feat, q_width), w_key.reshape(feat, kv_width), w_value.reshape(feat, kv_width)], axis=1)
        cosines, sines = rope_tables(positions, head_dim)
        d_lin, attn_out, gain_full, normed, w_full, wo_all, o_all = core(hidden, gain[None], w_qkv, w_out.reshape(q_width, feat), cosines, sines, cotangent, group, kv_width, n_line, 0)
        grad_hidden, block_out, grad_gain, mine, theirs = close(d_lin, attn_out, gain_full, hidden, cotangent, normed, w_full, o_all, wo_all, 1)[:5]
        block_out, grad_hidden, g_query, g_key, g_value, g_out = tail(block_out, grad_hidden, mine, theirs, q_heads, kv_heads, head_dim)
        return block_out[None], grad_hidden[None], grad_gain[0], g_query, g_key, g_value, g_out.reshape(w_out.shape)

    specs = (act_spec, act_spec, P("fsdp"), proj_spec, proj_spec, proj_spec, wout_spec)
    return jax.shard_map(device_step, mesh=mesh, in_specs=specs[:2] + (P("cp"),) + specs[2:], out_specs=specs, check_vma=False)
```

```python
import functools
import math

import jax
import jax.numpy as jnp
from jax import lax
from jax.experimental import pallas as pl
from jax.experimental.pallas import tpu as pltpu
from jax.sharding import PartitionSpec as P

WINDOW_LEN = 4096
ROPE_BASE = 10000.0
NORM_EPS = 1e-5
NEG_BIG = -1e30
LOG2E = math.log2(math.e)
TILES = 4
CHUNKS = 16
LEAD = 2
X_LEAD = 4
QUARTERS = 3
PIECES = 8
O_PIECES = 2
GRAD_CHUNKS = 8
FIRST_X = 6
EARLY = 6
LATE = ((6, 3), (7, 8))
VMEM_BYTES = 67043328
SIDES = range(2)

MESH = pl.DeviceIdType.MESH
ANY = pl.BlockSpec(memory_space=pl.ANY)
VMEM = pl.BlockSpec(memory_space=pltpu.VMEM)
DMA = pltpu.SemaphoreType.DMA
BF, F32 = jnp.bfloat16, jnp.float32

NT = (((1,), (1,)), ((), ()))
NN = (((1,), (0,)), ((), ()))
TN = (((0,), (0,)), ((), ()))


def dot(a, b, dims):
    return lax.dot_general(a, b, dims, preferred_element_type=F32)


def parity(k):
    return lax.rem(k, 2)


def blk(k, n):
    return pl.ds(k * n if isinstance(k, int) else pl.multiple_of(k * n, n), n)


def lane_mean(vals):
    return jnp.mean(vals, axis=1, keepdims=True)


def row_sum(vals):
    return jnp.sum(vals, axis=0, keepdims=True)


def zero(ref):
    ref[...] = jnp.zeros_like(ref)


def remote(src, dst, send, recv, where):
    return pltpu.make_async_remote_copy(src_ref=src, dst_ref=dst, send_sem=send, recv_sem=recv, device_id=where, device_id_type=MESH)


def meet(peers):
    barrier = pltpu.get_barrier_semaphore()
    for where in peers:
        pl.semaphore_signal(barrier, inc=1, device_id=where, device_id_type=MESH)
    pl.semaphore_wait(barrier, len(peers))


def fsdp_peers(f):
    core = parity(f)
    other = f + 1 - 2 * core
    far = lax.rem(f + 2, 4)
    return other, far, lax.rem(other + 2, 4)


def others(axis, index, count):
    return [{axis: lax.rem(index + k, count)} for k in range(1, count)]


def nearest(z, last):
    near = jnp.where(z > 0, last, 1)
    second = jnp.where(z == 0, 2, jnp.where(z == last, last - 1, 1))
    return near, second


def rope(vals, cos, sin, half_dim):
    return vals * cos + pltpu.roll(vals, half_dim, 1) * sin


def causal(scores, tq):
    key_idx = lax.broadcasted_iota(jnp.int32, scores.shape, 0)
    q_idx = lax.rem(lax.broadcasted_iota(jnp.int32, scores.shape, 1), tq)
    return jnp.where(key_idx <= q_idx, scores, NEG_BIG)


def params(cid):
    return pltpu.CompilerParams(collective_id=cid, has_side_effects=True, vmem_limit_bytes=VMEM_BYTES)


def rope_tables(positions, head_dim):
    inv_freq = ROPE_BASE ** (-jnp.arange(0, head_dim, 2).astype(F32) / head_dim)
    angles = positions.astype(F32)[:, None] * inv_freq[None, :]
    cosines, sines = jnp.cos(angles), jnp.sin(angles)
    return jnp.concatenate([cosines, cosines], axis=1), jnp.concatenate([-sines, sines], axis=1)


def core_kernel(group, n_line, hid_ref, gain_ref, w_ref, wo_ref, cos_ref, sin_ref, ct_ref, d_ref, o_ref, gfull_ref, n_out, w_out, wo_all, o_all, wbuf, nbuf, acc, hbuf, gbuf, qs, vt, m_all, l_all, acc_all, q_ref, lse_ref, kl_ref, vl_ref, kp_ref, vp_ref, do_ref, dkl_ref, dvl_ref, dkp_ref, dvp_ref, qs_ref, dos_ref, delta_ref, kt_ref, dqt_ref, h_sem, g_send, g_recv, own_send, own_recv, x_send, x_recv, y_send, y_recv, d_send, d_recv, kv_send, kv_recv, ox_send, ox_recv, oy_send, oy_recv, od_send, od_recv, zw_send, zw_recv, out_sem, ct_sem, o_sems, o_recv, wy_send, wy_recv, wx_send, wx_recv, wc_send, wc_recv, cx_send, cx_recv, dk_send, dk_recv):
    q_len, feat = hid_ref.shape[0], w_ref.shape[0]
    head_dim = cos_ref.shape[1]
    half_dim = head_dim // 2
    kv_width = kl_ref.shape[1]
    kv_heads = kv_width // head_dim
    q_width = q_ref.shape[1]
    tq = q_len // TILES
    wide = group * tq
    score_scale = head_dim ** -0.5
    scale = head_dim ** -0.5 * LOG2E
    half = feat // 2
    piece = half // PIECES
    o_rows = wo_ref.shape[0]
    o_half = o_rows // 2
    o_piece = o_half // O_PIECES
    flag, f, z = lax.axis_index("cp"), lax.axis_index("fsdp"), lax.axis_index("tp")
    wo_out = wo_all.at[z]
    last = n_line - 1
    far = 1 - flag
    f_core, f_x, f_diag = fsdp_peers(f)
    to_core, to_x, to_diag, to_y = {"fsdp": f_core}, {"fsdp": f_x}, {"fsdp": f_diag}, {"cp": far}

    def h_load(tile):
        slot = parity(tile)
        return pltpu.make_async_copy(hid_ref.at[blk(tile, tq)], hbuf.at[slot], h_sem.at[slot])

    h_load(0).start()
    h_load(1).start()
    meet([to_core, to_x, to_diag, to_y] + others("tp", z, n_line))

    def span(side, j):
        return blk(side * PIECES + j, piece)

    def x_copy(j):
        return remote(w_ref.at[span(flag, j)], wbuf.at[f, span(flag, j)], x_send.at[j], x_recv.at[j], to_x)

    def x_in(j):
        return remote(w_ref.at[span(flag, j)], wbuf.at[f_x, span(flag, j)], x_send.at[j], x_recv.at[j], to_x)

    def y_copy(j, side):
        return remote(wbuf.at[f_x, span(side, j)], wbuf.at[f_x, span(side, j)], y_send.at[j], y_recv.at[j], to_y)

    def d_copy(j, side, slot):
        return remote(wbuf.at[slot, span(side, j)], wbuf.at[slot, span(side, j)], d_send.at[side, j], d_recv.at[side, j], to_core)

    def g_copy(k, where, slot):
        return remote(gain_ref, gbuf.at[slot], g_send.at[k], g_recv.at[k], where)

    def own_copy(slot):
        return remote(w_ref, wbuf.at[slot], own_send, own_recv, to_core)

    def o_span(side, j):
        return blk(side * O_PIECES + j, o_piece)

    def ox_copy(j, slot):
        return remote(wo_ref.at[o_span(flag, j)], wo_out.at[slot, o_span(flag, j)], ox_send.at[j], ox_recv.at[j], to_x)

    def oy_copy(j, side):
        return remote(wo_out.at[f_x, o_span(side, j)], wo_out.at[f_x, o_span(side, j)], oy_send.at[j], oy_recv.at[j], to_y)

    def od_copy(k, src, slot, where):
        return remote(src, wo_out.at[slot, where], od_send.at[k], od_recv.at[k], to_core)

    def zw_copy(up, t):
        spot = wo_all.at[t, f, blk(flag, o_half)]
        where = jnp.minimum(z + 1, last) if up else jnp.maximum(z - 1, 0)
        src = spot if t is not z else wo_ref.at[blk(flag, o_half)]
        return remote(src, spot, zw_send.at[up, t], zw_recv.at[t], {"tp": where})

    def zw_tick(r):
        for up, t, here in ((0, z + r, z + r <= last), (1, z - r, z >= r)):
            at = jnp.clip(t, 0, last)

            @pl.when(here)
            def _():
                zw_copy(up, at).wait_recv()

            @pl.when(here & (z < last if up else z > 0))
            def _():
                zw_copy(up, at).start()

    def tile_rows(j):
        return blk(j, tq)

    o_parts = kv_heads * TILES

    def o_piece_at(ref, j):
        return ref.at[tile_rows(lax.rem(j, TILES)), blk(j // TILES, group * head_dim)]

    def o_copy(up, t, j, own=False):
        spot = o_piece_at(o_all.at[t], j)
        src = o_piece_at(o_ref, j) if own else spot
        where = jnp.minimum(z + 1, last) if up else jnp.maximum(z - 1, 0)
        return remote(src, spot, o_sems.at[up, t, j], o_recv.at[t, j], {"tp": where})

    def wo_half(r, slot, side):
        return wo_all.at[lax.rem(z + r, n_line), slot, blk(side, o_half)]

    def wy_copy(r, side):
        return remote(wo_half(r, f, side), wo_half(r, f, side), wy_send.at[r - 1], wy_recv.at[r - 1], to_y)

    def wx_copy(r, side, slot):
        return remote(wo_half(r, slot, side), wo_half(r, slot, side), wx_send.at[side, r - 1], wx_recv.at[side, r - 1], to_x)

    def wc_copy(r, side, slot):
        return remote(wo_half(r, slot, side), wo_half(r, slot, side), wc_send.at[side, r - 1], wc_recv.at[side, r - 1], to_core)

    def cx_copy(r, side, slot):
        return remote(wo_half(r, slot, side), wo_half(r, slot, side), cx_send.at[side, r - 1], cx_recv.at[side, r - 1], to_core)

    def o_tick(k):
        r, j = k // o_parts + 1, lax.rem(k, o_parts)
        for up, t, here in ((0, z + r, z + r <= last), (1, z - r, z >= r)):
            at = jnp.clip(t, 0, last)

            @pl.when(here)
            def _():
                o_copy(up, at, j).wait_recv()

            @pl.when(here & (z < last if up else z > 0))
            def _():
                o_copy(up, at, j).start()

    def wy_tick(r):
        wy_copy(r, far).wait_recv()
        wx_copy(r, far, f).start()
        for side in (flag, far):
            wc_copy(r, side, f).start()
        if r == 1:
            wy_copy(last, flag).start()

    near, second = nearest(z, last)
    own_order = (near, second, n_line * last // 2 - near - second)

    def wx_tick(q):
        r, side = (own_order[q], flag) if q < last else (q - last + 1, far)
        wx_copy(r, side, f_x).wait_recv()
        cx_copy(r, side, f_x).start()

    def o_send(j):
        for up in SIDES:
            @pl.when(z < last if up else z > 0)
            def _():
                o_copy(up, z, j, True).start()

    gains = [(k, where, where["fsdp"]) for k, where in enumerate((to_core, to_x, to_diag))]
    for k, where, _ in gains:
        g_copy(k, where, f).start()
    sends = [x_copy(j) for j in range(PIECES)] + [ox_copy(j, f) for j in range(O_PIECES)]
    for copy in sends[:X_LEAD]:
        copy.start()
    own_copy(f).start()
    all_rows = pl.ds(0, o_rows)
    for up in SIDES:
        @pl.when(z < last if up else z > 0)
        def _():
            zw_copy(up, z).start()

    local_w = pltpu.make_async_copy(w_ref, wbuf.at[f], out_sem.at[0])
    local_w.start()
    local_o = pltpu.make_async_copy(wo_ref, wo_out.at[f], out_sem.at[1])
    local_o.start()
    gbuf[f] = gain_ref[...]
    for k, where, slot in gains:
        g_copy(k, where, slot).wait_recv()
    for k in range(gbuf.shape[0]):
        gfull_ref[:, blk(k, feat)] = gbuf[k].astype(F32)

    for tile in range(TILES):
        h_load(tile).wait()
        strip = min(32, tq)

        @pl.loop(0, tq // strip)
        def _(i):
            vals = hbuf[tile % 2, blk(i, strip), :].astype(F32)
            inv = lax.rsqrt(lane_mean(vals * vals) + NORM_EPS)
            nbuf[pl.ds(pl.multiple_of(tile * tq + i * strip, strip), strip), :] = (vals * inv * gfull_ref[...]).astype(BF)

        if tile + 2 < TILES:
            h_load(tile + 2).start()
    put_n = pltpu.make_async_copy(nbuf.at[pl.ds(0, q_len)], n_out, out_sem.at[2])
    put_n.start()

    def project(slot, start, rows, first=False):
        cols = pl.ds(pl.multiple_of(slot * feat + start, 128), rows)

        @pl.loop(0, TILES)
        def _(tile):
            here = blk(tile, tq)
            part = dot(nbuf[here, cols], wbuf[slot, pl.ds(start, rows), :], NN)
            acc[here, :] = part if first else acc[here, :] + part

    def x_tick(j):
        x_in(j).wait_recv()
        y_copy(j, flag).start()
        d_copy(j, flag, f_x).start()
        for copy in sends[j + X_LEAD:j + X_LEAD + 1]:
            copy.start()

    def y_tick(j):
        y_copy(j, far).wait_recv()
        d_copy(j, 1 - flag, f_x).start()

    local_w.wait()
    project(f, 0, feat, first=True)
    x_tick(0)
    x_tick(1)
    own_copy(f_core).wait_recv()
    od_copy(0, wo_ref, f, all_rows).start()
    project(f_core, 0, feat)
    for j in range(2, PIECES):
        x_tick(j)
        y_tick(j - 2)
        if j == PIECES // 2:
            zw_tick(1)
    for j in range(PIECES):
        d_copy(j, flag, f_diag).wait_recv()
    first_half = pl.multiple_of(flag * half, half)
    project(f_x, first_half, half)
    y_tick(PIECES - 2)
    project(f_diag, first_half, half)
    y_tick(PIECES - 1)
    for j in range(PIECES):
        d_copy(j, far, f_diag).wait_recv()
    second_half = pl.multiple_of(far * half, half)
    project(f_x, second_half, half)
    project(f_diag, second_half, half)
    zw_tick(2)
    wx_copy(near, flag, f).start()
    put_w = pltpu.make_async_copy(wbuf, w_out, out_sem.at[3])
    put_w.start()

    @pl.loop(0, TILES)
    def _(tile):
        here = blk(tile, tq)
        cos, sin = cos_ref[here, :], sin_ref[here, :]
        for h in range(kv_heads):
            k_at = q_width // head_dim + h
            kl_ref[here, blk(h, head_dim)] = rope(acc[here, blk(k_at, head_dim)], cos, sin, half_dim).astype(BF)
            vl_ref[here, blk(h, head_dim)] = acc[here, blk(k_at + kv_heads, head_dim)].astype(BF)

    kv_pairs = ((kl_ref, kp_ref), (vl_ref, vp_ref))

    def kv_copies(g):
        return [remote(src.at[:, blk(g, head_dim)], dst.at[:, blk(g, head_dim)], kv_send.at[k, g], kv_recv.at[k, g], {"cp": 1}) for k, (src, dst) in enumerate(kv_pairs)]

    @pl.when(flag == 0)
    def _():
        zero(kp_ref)
        zero(vp_ref)
        for g in range(kv_heads):
            for copy in kv_copies(g):
                copy.start()

    @pl.loop(0, TILES)
    def _(tile):
        here = blk(tile, tq)
        cos, sin = cos_ref[here, :], sin_ref[here, :]
        for h in range(group * kv_heads):
            cols = blk(h, head_dim)
            q_ref[here, cols] = rope(acc[here, cols], cos, sin, half_dim).astype(BF)

    def load_q(item):
        g, tile = item // TILES, lax.rem(item, TILES)
        rows = blk(tile, tq)
        for h in range(group):
            qs[:, blk(h, tq)] = q_ref[rows, blk(g * group + h, head_dim)].T

    def key_piece(item, k_ref, side, start, masked):
        g = item // TILES
        scores = dot(k_ref[start, blk(g, head_dim)], qs[...], NN)
        if masked:
            scores = causal(scores, tq)
        m_old = m_all[item]
        m_new = jnp.maximum(m_old, jnp.max(scores, axis=0, keepdims=True))
        probs = jnp.exp2((scores - m_new) * scale)
        fade = jnp.exp2((m_old - m_new) * scale)
        m_all[item] = m_new
        l_all[item] = l_all[item] * fade + row_sum(probs)
        acc_all[item] = acc_all[item] * fade + dot(vt[g, side, :, start], probs.astype(BF), NN)

    for g in range(kv_heads):
        vt[g, 0] = vl_ref[:, blk(g, head_dim)].T

    @pl.loop(0, kv_heads * TILES)
    def _(item):
        tile = lax.rem(item, TILES)
        load_q(item)
        m_all[item] = jnp.full_like(m_all[item], NEG_BIG)
        l_all[item] = jnp.zeros_like(l_all[item])
        acc_all[item] = jnp.zeros_like(acc_all[item])
        key_piece(item, kl_ref, 0, blk(tile, tq), True)

        @pl.loop(0, tile // 2)
        def _(i):
            key_piece(item, kl_ref, 0, blk(i, 2 * tq), False)

        @pl.when(parity(tile) == 1)
        def _():
            key_piece(item, kl_ref, 0, blk(tile - 1, tq), False)

    for j in range(O_PIECES):
        ox_copy(j, f_x).wait_recv()
        oy_copy(j, flag).start()
        od_copy(1 + j, wo_out.at[f_x, o_span(flag, j)], f_x, o_span(flag, j)).start()

    wx_copy(second, flag, f).start()
    zw_tick(last)

    @pl.loop(0, kv_heads * TILES)
    def _(item):
        g, tile = item // TILES, lax.rem(item, TILES)
        rows = blk(tile, tq)

        @pl.when((flag == 1) & (tile == 0))
        def _():
            for copy in kv_copies(g):
                copy.wait_recv()
            vt[g, 1] = vp_ref[:, blk(g, head_dim)].T

        @pl.when(flag == 1)
        def _():
            load_q(item)

        @pl.loop(0, flag * TILES // 2)
        def _(i):
            key_piece(item, kp_ref, 1, blk(i, 2 * tq), False)

        total = l_all[item]
        lse_ref[item] = m_all[item] * scale + jnp.log2(total)
        out_t = acc_all[item] / total
        for h in range(group):
            o_ref[rows, blk(g * group + h, head_dim)] = out_t[:, h * tq:h * tq + tq].T.astype(BF)

        @pl.when(item > 0)
        def _():
            o_send(item - 1)

        for j in range(O_PIECES):
            @pl.when(item == (j + 1) * kv_heads * TILES // O_PIECES - 1)
            def _():
                oy_copy(j, far).wait_recv()
                od_copy(1 + O_PIECES + j, wo_out.at[f_x, o_span(1 - flag, j)], f_x, o_span(1 - flag, j)).start()

    o_send(o_parts - 1)
    wx_copy(own_order[last - 1], flag, f).start()
    for r in range(1, last):
        wy_copy(r, flag).start()
    od_copy(0, wo_ref, f_core, all_rows).wait_recv()
    for j in range(O_PIECES):
        od_copy(1 + j, wo_out.at[f_x, o_span(flag, j)], f_diag, o_span(flag, j)).wait_recv()
        od_copy(1 + O_PIECES + j, wo_out.at[f_x, o_span(1 - flag, j)], f_diag, o_span(1 - flag, j)).wait_recv()

    put_n.wait()
    local_o.wait()
    n_parts, _, part = wo_out.shape
    loads = [pltpu.make_async_copy(wo_out.at[k], nbuf.at[pl.ds(0, o_rows), blk(k, part)], out_sem.at[4 + k]) for k in range(n_parts)]
    for load in loads:
        load.start()
    keep = pltpu.make_async_copy(o_ref, o_all.at[z], out_sem.at[2])
    keep.start()

    def ct_load(tile):
        slot = parity(tile)
        return pltpu.make_async_copy(ct_ref.at[blk(tile, tq)], hbuf.at[slot], ct_sem.at[slot])

    ct_load(0).start()
    ct_load(1).start()
    zero(dkl_ref)
    zero(dvl_ref)

    @pl.when(flag == 1)
    def _():
        zero(dkp_ref)
        zero(dvp_ref)

    wx_tick(0)
    for k in SIDES:
        o_tick(jnp.int32(k))
    for load in loads:
        load.wait()

    def do_tile(tile):
        ct_load(tile).wait()
        do_ref[tile_rows(tile), :] = dot(hbuf[parity(tile)], nbuf[pl.ds(0, o_rows), :], NT).astype(BF)

        @pl.when(tile + 2 < TILES)
        def _():
            ct_load(tile + 2).start()

    def bwd_item(item):
        g, tile = item // TILES, lax.rem(item, TILES)
        kv_cols = blk(g, head_dim)
        rows = blk(tile, tq)

        @pl.when(tile == 0)
        def _():
            kt_ref[0] = kl_ref[:, kv_cols].T
            kt_ref[1] = kp_ref[:, kv_cols].T

        for h in range(group):
            cols = blk(g * group + h, head_dim)
            stack = blk(h, tq)
            qs_ref[stack, :] = q_ref[rows, cols]
            d_h = do_ref[rows, cols]
            dos_ref[stack, :] = d_h
            prod = d_h.astype(F32) * o_ref[rows, cols].astype(F32)
            delta_ref[:, stack] = row_sum(prod.T)
        zero(dqt_ref)

        def piece(k_ref, v_ref, dk_ref, dv_ref, side, span, masked):
            scores = dot(k_ref[span, kv_cols], qs_ref[...], NT)
            if masked:
                scores = causal(scores, tq)
            probs = jnp.exp2(scores * (score_scale * LOG2E) - lse_ref[item])
            d_probs = dot(v_ref[span, kv_cols], dos_ref[...], NT)
            d_scores = (probs * (d_probs - delta_ref[...])).astype(BF)
            dv_ref[g, span, :] += dot(probs.astype(BF), dos_ref[...], NN)
            dk_ref[g, span, :] += dot(d_scores, qs_ref[...], NN)
            dqt_ref[...] += dot(kt_ref[side, :, span], d_scores, NN)

        piece(kl_ref, vl_ref, dkl_ref, dvl_ref, 0, blk(tile, tq), True)

        @pl.loop(0, tile // 2)
        def _(i):
            piece(kl_ref, vl_ref, dkl_ref, dvl_ref, 0, blk(i, 2 * tq), False)

        @pl.when(parity(tile) == 1)
        def _():
            piece(kl_ref, vl_ref, dkl_ref, dvl_ref, 0, blk(tile - 1, tq), False)

        @pl.loop(0, flag * TILES // 2)
        def _(i):
            piece(kp_ref, vp_ref, dkp_ref, dvp_ref, 1, blk(i, 2 * tq), False)

        for h in range(group):
            dq_h = dqt_ref[:, blk(h, tq)].T * score_scale
            d_ref[rows, blk(g * group + h, head_dim)] = rope(dq_h, cos_ref[rows, :], -sin_ref[rows, :], half_dim).astype(BF)

        @pl.when((tile == TILES - 1) & (flag == 1))
        def _():
            for copy in back(g):
                copy.start()

    def back(g):
        return [remote(ref.at[g], ref.at[g], dk_send.at[k, g], dk_recv.at[k, g], {"cp": 0}) for k, ref in enumerate((dkp_ref, dvp_ref))]

    def kv_done(g):
        @pl.when(flag == 0)
        def _():
            for copy in back(g):
                copy.wait_recv()
            dkl_ref[g] += dkp_ref[g]
            dvl_ref[g] += dvp_ref[g]

        dk = rope(dkl_ref[g] * score_scale, cos_ref[...], -sin_ref[...], half_dim)
        k_at = q_width // head_dim + g
        d_ref[:, blk(k_at, head_dim)] = dk.astype(BF)
        d_ref[:, blk(k_at + kv_heads, head_dim)] = dvl_ref[g].astype(BF)

        @pl.when(flag == 1)
        def _():
            for copy in back(g):
                copy.wait_send()

    items = TILES * (kv_heads + 1)
    plan = {1: [(wx_tick, 1)], 5: [(wy_tick, 1)], 6: [(wx_tick, 2)], 8: [(wy_tick, 2)], 9: [(wx_tick, 3)]}

    @pl.loop(0, items)
    def _(item):
        @pl.when(item < TILES)
        def _():
            do_tile(item)

        @pl.when(item >= TILES)
        def _():
            bwd_item(item - TILES)

        @pl.when(item != 1)
        def _():
            o_tick(jnp.where(item > 1, item + 1, 2))

        for at, jobs in plan.items():
            @pl.when(item == at)
            def _():
                for tick, arg in jobs:
                    tick(arg)

    rest = {1: (wy_tick, 3), 2: (wx_tick, 4), 5: (kv_done, 0), 6: (wx_tick, 5), 9: (kv_done, 1)}
    for k in range(items + 1, o_parts * last):
        o_tick(jnp.int32(k))
        if k - items in rest:
            tick, arg = rest[k - items]
            tick(arg)

    for r in range(1, n_line):
        for side in (flag, far):
            wc_copy(r, side, f_core).wait_recv()
            cx_copy(r, side, f_diag).wait_recv()
            wc_copy(r, side, f).wait_send()
            cx_copy(r, side, f_x).wait_send()
            wx_copy(r, side, f).wait_send()
        wy_copy(r, flag).wait_send()

    @pl.loop(0, n_line)
    def _(t):
        for up in SIDES:
            @pl.when((t <= z) & (z < last) if up else (t >= z) & (z > 0))
            def _():
                for j in range(o_parts):
                    o_copy(up, t, j).wait_send()

    @pl.loop(0, n_line)
    def _(t):
        for up in SIDES:
            @pl.when((t <= z) & (z < last) if up else (t >= z) & (z > 0))
            def _():
                zw_copy(up, t).wait_send()

    for k, where, _ in gains:
        g_copy(k, where, f).wait_send()
    own_copy(f).wait_send()
    od_copy(0, wo_ref, f, all_rows).wait_send()
    for j in range(PIECES):
        x_copy(j).wait_send()
        y_copy(j, flag).wait_send()
        d_copy(j, flag, f_x).wait_send()
        d_copy(j, 1 - flag, f_x).wait_send()
    for j in range(O_PIECES):
        ox_copy(j, f).wait_send()
        oy_copy(j, flag).wait_send()
        od_copy(1 + j, wo_out.at[f_x, o_span(flag, j)], f_x, o_span(flag, j)).wait_send()
        od_copy(1 + O_PIECES + j, wo_out.at[f_x, o_span(1 - flag, j)], f_x, o_span(1 - flag, j)).wait_send()

    @pl.when(flag == 0)
    def _():
        for g in range(kv_heads):
            for copy in kv_copies(g):
                copy.wait_send()

    for local in (keep, put_w):
        local.wait()


def core(hidden, gain, w_qkv, w_out, cosines, sines, cotangent, group, kv_width, n_line, cid):
    q_len, model_dim = hidden.shape
    feat, width = w_qkv.shape
    head_dim = cosines.shape[1]
    q_width = width - 2 * kv_width
    kv_heads = kv_width // head_dim
    o_rows, o_cols = w_out.shape
    n_fsdp = model_dim // feat
    tq = q_len // TILES
    wide = group * tq
    items = kv_heads * TILES
    sds = jax.ShapeDtypeStruct
    line = pltpu.VMEM((items, 1, wide), F32)
    kv = pltpu.VMEM((q_len, kv_width), BF)
    heads = pltpu.VMEM((q_len, q_width), BF)
    sums = pltpu.VMEM((kv_heads, q_len, head_dim), F32)
    stack = pltpu.VMEM((wide, head_dim), BF)
    own, pair, trio = DMA(()), DMA((2,)), DMA((n_fsdp - 1,))
    w_link, w_side, o_link, o_core = DMA((PIECES,)), DMA((2, PIECES)), DMA((O_PIECES,)), DMA((1 + 2 * O_PIECES,))
    hop, side, dkv = DMA((n_line - 1,)), DMA((2, n_line - 1)), DMA((2, kv_heads))
    return pl.pallas_call(
        functools.partial(core_kernel, group, n_line),
        in_specs=[ANY] + [VMEM] * 5 + [ANY],
        out_specs=[VMEM] * 3 + [ANY] * 4,
        out_shape=[sds((q_len, width), BF), sds((q_len, q_width), BF), sds((1, model_dim), F32), sds((q_len, model_dim), BF), sds((n_fsdp, feat, width), BF), sds((n_line, n_fsdp, o_rows, o_cols), BF), sds((n_line, q_len, q_width), BF)],
        scratch_shapes=[
            pltpu.VMEM((n_fsdp, feat, width), BF),
            pltpu.VMEM((max(q_len, o_rows), model_dim), BF),
            pltpu.VMEM((q_len, width), F32),
            pltpu.VMEM((2, tq, model_dim), BF),
            pltpu.VMEM((n_fsdp, 1, feat), BF),
            pltpu.VMEM((head_dim, wide), BF),
            pltpu.VMEM((kv_heads, 2, head_dim, q_len), BF),
            line,
            line,
            pltpu.VMEM((items, head_dim, wide), F32),
            heads,
            line,
            kv, kv, kv, kv,
            heads,
            sums, sums, sums, sums,
            stack,
            stack,
            pltpu.VMEM((1, wide), F32),
            pltpu.VMEM((2, head_dim, q_len), BF),
            pltpu.VMEM((head_dim, wide), F32),
        ] + [pair, trio, trio, own, own, w_link, w_link, w_link, w_link, w_side, w_side, dkv, dkv, o_link, o_link, o_link, o_link, o_core, o_core, DMA((2, n_line)), DMA((n_line,)), DMA((4 + n_fsdp,)), pair, DMA((2, n_line, items)), DMA((n_line, items)), hop, hop, side, side, side, side, side, side, dkv, dkv],
        compiler_params=params(cid),
        name="core",
    )(hidden, gain, w_qkv, w_out, cosines, sines, cotangent)


class Line:
    def __init__(self, n_line, buf_ref, pbuf_ref, send_sem, recv_sem, fill, finish):
        self.last = n_line - 1
        self.z = lax.axis_index("tp")
        self.buf, self.pbuf, self.send_sem, self.recv_sem = buf_ref, pbuf_ref, send_sem, recv_sem
        self.chunks, self.rows = buf_ref.shape[1], buf_ref.shape[2]
        self.block = pbuf_ref.shape[1]
        self.per_block = self.block // self.rows
        self.fill, self.finish = fill, finish
        self.steps = self.chunks + self.last

    def dist(self, side):
        return self.z if side else self.last - self.z

    def toward(self, side, back=False):
        up = bool(side) != back
        return {"tp": jnp.clip(self.z + 1 if up else self.z - 1, 0, self.last)}

    def copy(self, side, chunk):
        spot = self.buf.at[side, chunk]
        return remote(spot, spot, self.send_sem.at[side, chunk], self.recv_sem.at[side, chunk], self.toward(side))

    def live(self, side, step):
        chunk = step - self.dist(side)
        return chunk, (chunk >= 0) & (chunk < self.chunks)

    def prepare(self, step):
        for side in SIDES:
            chunk, ok = self.live(side, step)

            @pl.when(ok & (lax.rem(chunk, self.per_block) == 0))
            def _():
                self.fill(self.pbuf.at[side], blk((side * self.chunks + chunk) // self.per_block, self.block))

    def tick(self, step):
        for side in SIDES:
            chunk, ok = self.live(side, step)
            dist = self.dist(side)
            part = blk(lax.rem(jnp.maximum(chunk, 0), self.per_block), self.rows)

            @pl.when(ok & (dist == 0))
            def _():
                self.buf[side, chunk] = self.pbuf[side, part, :]

            @pl.when(ok & (dist > 0))
            def _():
                self.copy(side, chunk).wait_recv()
                self.buf[side, chunk] += self.pbuf[side, part, :]

            @pl.when(ok & (dist < self.last))
            def _():
                self.copy(side, chunk).start()

            @pl.when(ok & (dist == self.last))
            def _():
                self.finish(chunk, self.buf[side, chunk])

        self.prepare(step + 1)

    def drain(self):
        for side in SIDES:
            @pl.when(self.dist(side) < self.last)
            def _():
                @pl.loop(0, self.chunks)
                def _(chunk):
                    self.copy(side, chunk).wait_send()


def close_kernel(n_line, n_fsdp, d_ref, o_ref, gain_ref, hid_ref, ct_ref, n_ref, w_all, o_all, wo_all, out_ref, blk_ref, gg_ref, ts, yr, dl, xs, ks, xr, buf, gp, ga, gs, gb, gt, gc, ebuf, fb_in, fb_ct, fb_out, send_sem, recv_sem, w_sem, f_sem, ct_sem, fo_sem, lhs_sem, a_send, a_recv, ld_sem, st_sem, x_send, x_recv, e_sem, es_sem, y_send, y_recv, out_send, out_recv, o_sem, wl_sem, h_sem, r_sem, ga_send, ga_recv, gb_send, gb_recv, gc_send, gc_recv):
    last = n_line - 1
    z, flag, f = lax.axis_index("tp"), lax.axis_index("cp"), lax.axis_index("fsdp")
    far = 1 - flag
    f_core, f_x, f_diag = fsdp_peers(f)
    to_core, to_x, to_y = {"fsdp": f_core}, {"fsdp": f_x}, {"cp": far}
    _, feat, width = w_all.shape
    chunks, rows = buf.shape[1], buf.shape[2]
    half = chunks * rows
    g_rows = feat // GRAD_CHUNKS
    owner = (z == 0) | (z == last)
    own_base = jnp.where(z == last, chunks, 0)
    copy = pltpu.make_async_copy

    def own_span(chunk):
        return blk(own_base + chunk, rows)

    def f_loads(chunk):
        slot = parity(chunk)
        return copy(hid_ref.at[own_span(chunk)], fb_in.at[slot], f_sem.at[slot]), copy(ct_ref.at[own_span(chunk)], fb_ct.at[slot], ct_sem.at[slot])

    def f_store(chunk):
        slot = parity(chunk)
        return copy(fb_out.at[slot], out_ref.at[own_span(chunk)], fo_sem.at[slot])

    @pl.when(owner)
    def _():
        for chunk in SIDES:
            for load in f_loads(chunk):
                load.start()

    zero(gp)

    def finish(chunk, total):
        slot = parity(chunk)
        for load in f_loads(chunk):
            load.wait()

        @pl.when(chunk > 1)
        def _():
            f_store(chunk - 2).wait()

        x_in = fb_in[slot].astype(F32)
        inv = lax.rsqrt(lane_mean(x_in * x_in) + NORM_EPS)
        x_hat = x_in * inv
        gp[...] += row_sum(total * x_hat)
        scaled = total * gain_ref[...]
        fb_out[slot] = (fb_ct[slot].astype(F32) + inv * (scaled - x_hat * lane_mean(scaled * x_hat))).astype(BF)
        f_store(chunk).start()

        @pl.when(chunk + 2 < chunks)
        def _():
            for load in f_loads(chunk + 2):
                load.start()

    kinds = range(2)

    def g_at(ref, j):
        return ref.at[blk(j, g_rows)]

    def x_copy(j):
        return remote(g_at(xs, j), g_at(xr, j), x_send.at[j], x_recv.at[j], to_x)

    def y_copy(j):
        return remote(g_at(ts, j), g_at(yr, j), y_send.at[j], y_recv.at[j], to_y)

    def e_store(j):
        return copy(ebuf.at[0], g_at(ts, j), es_sem)

    def meet_x(j):
        x_copy(j).wait_recv()
        loads = [copy(g_at(src, j), ebuf.at[k], e_sem.at[k]) for k, src in enumerate((ks, xr))]
        for load in loads:
            load.start()
        for load in loads:
            load.wait()
        ebuf[0] += ebuf[1]
        e_store(j).start()

    def send_y(j):
        e_store(j).wait()
        y_copy(j).start()

    steps = chunks + last - 1

    def dist(side):
        return z if side else last - z

    def hop(side, chunk):
        span = blk(side * chunks + chunk, rows)
        up = z - 1 if side else z + 1
        return remote(out_ref.at[span], out_ref.at[span], out_send.at[side, chunk], out_recv.at[side, chunk], {"tp": jnp.clip(up, 0, last)})

    ends = [(end, z == (last if end else 0)) for end in SIDES]

    def owner_send(first, stop):
        for end, here in ends:
            @pl.when(here)
            def _():
                @pl.loop(first, stop)
                def _(c):
                    hop(end, c).start()

    def pass_on(step):
        for side in SIDES:
            chunk = step - (last - 1 - dist(side))

            @pl.when((dist(side) < last) & (chunk >= 0) & (chunk < chunks))
            def _():
                hop(side, chunk).wait_recv()

                @pl.when(dist(side) > 0)
                def _():
                    hop(side, chunk).start()

    def sum_phase(wbuf, pbuf, abuf, bbuf, lbuf, lhs):
        w_load = copy(w_all, wbuf, w_sem)
        w_load.start()

        def fill(dst, span):
            for k in range(n_fsdp):
                dst[:, blk(k, feat)] = dot(d_ref[span, :], wbuf[k], NT)

        line = Line(n_line, buf, pbuf, send_sem, recv_sem, fill, finish)
        slots = (f_diag, f_core, f_x, f)

        def lhs_loads(j):
            return [copy(src.at[:, blk(slot * GRAD_CHUNKS + j, g_rows)], lhs.at[m, k], lhs_sem.at[m, k]) for m, src in enumerate((n_ref, ct_ref)) for k, slot in enumerate(slots)]

        def a_copy(kind, j):
            return remote(abuf.at[kind], dl.at[kind, blk(j, g_rows)], a_send.at[kind], a_recv.at[kind, j], to_core)

        def b_stores(j):
            return [copy(bbuf.at[k], g_at(dst, j), st_sem.at[k]) for k, dst in enumerate((xs, ks))]

        def send_x(j):
            for kind in kinds:
                a_copy(kind, j).wait_send()
            for store in b_stores(j):
                store.wait()
            x_copy(j).start()

        def make(j):
            for load in lhs_loads(j):
                load.wait()
            for k in range(len(slots)):
                dst = (abuf, bbuf)[k // 2].at[k % 2]
                dst[:, :width] = dot(lhs[0, k], d_ref[...], TN)
                dst[:, width:] = dot(lhs[1, k], o_ref[...], TN)
            for kind in kinds:
                a_copy(kind, j).start()

            @pl.when(j + 1 < GRAD_CHUNKS)
            def _():
                for load in lhs_loads(j + 1):
                    load.start()

        def meet_core(j):
            loads = [copy(dl.at[kind, blk(j, g_rows)], lbuf.at[kind], ld_sem.at[kind]) for kind in kinds]
            for kind in kinds:
                a_copy(kind, j).wait_recv()
                loads[kind].start()
            for kind in kinds:
                loads[kind].wait()
                bbuf[kind] += lbuf[kind]
            for store in b_stores(j):
                store.start()

        for load in lhs_loads(0):
            load.start()
        w_load.wait()
        line.prepare(0)
        meet([to_core, to_x, to_y] + others("tp", z, n_line) + [{"fsdp": f_diag}])

        @pl.loop(0, line.steps)
        def _(fine):
            line.tick(fine)
            j, odd = fine // 2, parity(fine)

            @pl.when((odd == 0) & (j < GRAD_CHUNKS))
            def _():
                make(j)

            @pl.when((odd == 1) & (j < GRAD_CHUNKS))
            def _():
                meet_core(j)
                send_x(j)

            k = ((fine - FIRST_X) * 2 + 1) // 5

            @pl.when((k >= 0) & (k < EARLY) & (fine == FIRST_X + 5 * k // 2))
            def _():
                meet_x(k)
                send_y(k)

            @pl.when(fine >= chunks)
            def _():
                owner_send((fine - chunks) * LEAD, (fine - chunks + 1) * LEAD)

            @pl.when(fine > chunks)
            def _():
                for k in range(LEAD):
                    pass_on((fine - chunks - 1) * LEAD + k)

        @pl.when(owner)
        def _():
            for chunk in range(chunks - 2, chunks):
                f_store(chunk).wait()

        line.drain()

    pl.run_scoped(
        sum_phase,
        pltpu.VMEM(w_all.shape, BF),
        pltpu.VMEM((2, min(128, half), buf.shape[3]), F32),
        pltpu.VMEM((2, g_rows, ts.shape[1]), F32),
        pltpu.VMEM((2, g_rows, ts.shape[1]), F32),
        pltpu.VMEM((2, g_rows, ts.shape[1]), F32),
        pltpu.VMEM((2, n_fsdp, d_ref.shape[0], g_rows), BF),
    )
    def ga_copy(end, k):
        return remote(gp, ga.at[end], ga_send.at[k], ga_recv.at[end], {"tp": k if end else 1 + k})

    def gb_copy():
        return remote(gs, gb, gb_send, gb_recv, to_y)

    def gc_copy(k, slot):
        to = lax.rem(f + k, n_fsdp)
        return remote(gt.at[to], gc.at[slot], gc_send.at[k - 1], gc_recv.at[k - 1], {"fsdp": to})

    def spread_phase(obuf, wbuf, hbuf, rbuf):
        o_load = copy(o_all, obuf, o_sem)
        o_load.start()
        q_len, n_cols = hbuf.shape[1], hbuf.shape[2]
        per_part = wo_all.shape[3] // n_cols
        items = per_part * n_fsdp

        def item_loads(item):
            slot = parity(item)
            return copy(wo_all.at[:, item // per_part, :, blk(lax.rem(item, per_part), n_cols)], wbuf.at[slot], wl_sem.at[slot]), copy(hid_ref.at[:, blk(item, n_cols)], hbuf.at[slot], h_sem.at[slot])

        def item_store(item):
            slot = parity(item)
            return copy(rbuf.at[slot], blk_ref.at[:, blk(item, n_cols)], r_sem.at[slot])

        for item in SIDES:
            for load in item_loads(item):
                load.start()

        for end, here in ends:
            @pl.when(here)
            def _():
                ga[end] = gp[...]
                for k in range(last):
                    ga_copy(end, k).start()


        def project(quarter):
            item, tile = quarter // TILES, lax.rem(quarter, TILES)
            slot = parity(item)

            @pl.when(tile == 0)
            def _():
                for load in item_loads(item):
                    load.wait()

            @pl.when((tile == 0) & (item > 1))
            def _():
                item_store(item - 2).wait()

            span = blk(tile, q_len // TILES)
            total = sum(dot(obuf[t, span, :], wbuf[slot, t], NN) for t in range(n_line))
            rbuf[slot, span, :] = (hbuf[slot, span, :].astype(F32) + total).astype(BF)

            @pl.when(tile == TILES - 1)
            def _():
                item_store(item).start()

                @pl.when(item + 2 < items)
                def _():
                    for load in item_loads(item + 2):
                        load.start()

        for end, here in ends:
            @pl.when(jnp.logical_not(here))
            def _():
                ga_copy(end, 0).wait_recv()
        gs[...] = ga[0] + ga[1]
        gb_copy().start()

        early = (last - 1) * LEAD

        @pl.loop(0, steps - early)
        def _(step):
            sent = step + last * LEAD
            owner_send(sent, jnp.minimum(sent + 1, chunks))
            pass_on(step + early)

            @pl.when(step == 1)
            def _():
                o_load.wait()

            @pl.when(step > 0)
            def _():
                first = (step - 1) * QUARTERS

                @pl.loop(first, jnp.minimum(first + QUARTERS, items * TILES))
                def _(quarter):
                    project(quarter)

            for k, at in LATE:
                @pl.when(step == at)
                def _():
                    meet_x(k)
                    send_y(k)

        for item in range(items - 2, items):
            item_store(item).wait()

    pl.run_scoped(
        spread_phase,
        pltpu.VMEM(o_all.shape, BF),
        pltpu.VMEM((2, n_line, wo_all.shape[2], min(512, feat)), BF),
        pltpu.VMEM((2, d_ref.shape[0], min(512, feat)), BF),
        pltpu.VMEM((2, d_ref.shape[0], min(512, feat)), BF),
    )

    gb_copy().wait()
    for k in range(n_fsdp):
        gt[k] = gs[:, blk(k, feat)] + gb[:, blk(k, feat)]
    gc[f] = gt[f]
    for side in SIDES:
        @pl.when(dist(side) > 0)
        def _():
            @pl.loop(0, chunks)
            def _(chunk):
                hop(side, chunk).wait_send()

    @pl.loop(0, GRAD_CHUNKS)
    def _(j):
        x_copy(j).wait_send()

    for k in range(1, n_fsdp):
        gc_copy(k, f).start()
    for k in range(1, n_fsdp):
        gc_copy(k, lax.rem(f + n_fsdp - k, n_fsdp)).wait_recv()
    gg_ref[...] = sum(gc[k] for k in range(n_fsdp))
    for k in range(1, n_fsdp):
        gc_copy(k, f).wait_send()
    for end, here in ends:
        @pl.when(here)
        def _():
            for k in range(last):
                ga_copy(end, k).wait_send()

    @pl.loop(0, GRAD_CHUNKS)
    def _(j):
        y_copy(j).wait()


def close(d_lin, attn_out, gain, hidden, cotangent, normed, w_full, o_all, wo_all, cid):
    q_len, model_dim = hidden.shape
    n_line, n_fsdp = wo_all.shape[:2]
    _, feat, width = w_full.shape
    g_width = width + attn_out.shape[1]
    half = q_len // 2
    rows = half // CHUNKS
    sds = jax.ShapeDtypeStruct
    row = pltpu.VMEM((1, model_dim), F32)
    slices = pltpu.VMEM((n_fsdp, 1, feat), F32)
    strip = pltpu.VMEM((2, rows, model_dim), BF)
    own, pair, line, grad, grads = DMA(()), DMA((2,)), DMA((2, CHUNKS)), DMA((GRAD_CHUNKS,)), DMA((2, GRAD_CHUNKS))
    z_trio, f_trio = DMA((n_line - 1,)), DMA((n_fsdp - 1,))
    act, g_part = sds((q_len, model_dim), BF), sds((feat, g_width), F32)
    return pl.pallas_call(
        functools.partial(close_kernel, n_line, n_fsdp),
        in_specs=[VMEM] * 3 + [ANY] * 6,
        out_specs=[ANY, ANY, VMEM] + [ANY] * 6,
        out_shape=[act, act, sds((1, feat), F32), g_part, g_part, sds((2, feat, g_width), F32), g_part, g_part, g_part],
        scratch_shapes=[
            pltpu.VMEM((2, CHUNKS, rows, model_dim), F32),
            row,
            pltpu.VMEM((2, 1, model_dim), F32),
            row,
            row,
            slices,
            slices,
            pltpu.VMEM((2, feat // GRAD_CHUNKS, g_width), F32),
            strip,
            strip,
            strip,
        ] + [line, line, own, pair, pair, pair, DMA((2, n_fsdp)), pair, grads, pair, pair, grad, grad, pair, own, grad, grad, line, line, own, pair, pair, pair, z_trio, pair, own, own, f_trio, f_trio],
        compiler_params=params(cid),
        name="close",
    )(d_lin, attn_out, gain, hidden, cotangent, normed, w_full, o_all, wo_all)


def tail_kernel(head_dim, blk_ref, hid_ref, mine_ref, theirs_ref, blk_out, hid_out, q_out, k_out, v_out, o_out):
    blk_out[...] = blk_ref[...]
    hid_out[...] = hid_ref[...]
    at = 0
    for ref in (q_out, k_out, v_out):
        for h in range(ref.shape[1]):
            cols = blk(at, head_dim)
            ref[:, h, :] = mine_ref[:, cols] + theirs_ref[:, cols]
            at += 1
    rest = slice(at * head_dim, None)
    o_out[...] = (mine_ref[:, rest] + theirs_ref[:, rest]).T


def tail(block_out, grad_hidden, mine, theirs, q_heads, kv_heads, head_dim):
    q_len, model_dim = block_out.shape
    feat = mine.shape[0]
    sds = jax.ShapeDtypeStruct
    act = pl.BlockSpec((q_len // GRAD_CHUNKS, model_dim), lambda i: (i, 0))
    part = pl.BlockSpec((feat // GRAD_CHUNKS, mine.shape[1]), lambda i: (i, 0))

    def heads(n):
        return pl.BlockSpec((feat // GRAD_CHUNKS, n, head_dim), lambda i: (i, 0, 0))

    def like(n):
        return sds((feat, n, head_dim), F32)

    o_rows = q_heads * head_dim
    return pl.pallas_call(
        functools.partial(tail_kernel, head_dim),
        grid=(GRAD_CHUNKS,),
        in_specs=[act, act, part, part],
        out_specs=[act, act, heads(q_heads), heads(kv_heads), heads(kv_heads), pl.BlockSpec((o_rows, feat // GRAD_CHUNKS), lambda i: (0, i))],
        out_shape=[sds(block_out.shape, BF), sds(block_out.shape, BF), like(q_heads), like(kv_heads), like(kv_heads), sds((o_rows, feat), F32)],
        compiler_params=pltpu.CompilerParams(vmem_limit_bytes=VMEM_BYTES),
        name="tail",
    )(block_out, grad_hidden, mine, theirs)


def solution(mesh):
    act_spec = P("fsdp", "cp", None)
    proj_spec = P("fsdp", "tp", None)
    wout_spec = P("tp", None, "fsdp")
    n_line = mesh.shape["tp"]

    def device_step(hidden, cotangent, positions, gain, w_query, w_key, w_value, w_out):
        hidden, cotangent = hidden[0], cotangent[0]
        assert hidden.shape[0] * mesh.shape["cp"] <= WINDOW_LEN
        feat, q_heads, head_dim = w_query.shape
        kv_heads = w_key.shape[1]
        group = q_heads // kv_heads
        q_width, kv_width = q_heads * head_dim, kv_heads * head_dim
        w_qkv = jnp.concatenate([w_query.reshape(feat, q_width), w_key.reshape(feat, kv_width), w_value.reshape(feat, kv_width)], axis=1)
        cosines, sines = rope_tables(positions, head_dim)
        d_lin, attn_out, gain_full, normed, w_full, wo_all, o_all = core(hidden, gain[None], w_qkv, w_out.reshape(q_width, feat), cosines, sines, cotangent, group, kv_width, n_line, 0)
        grad_hidden, block_out, grad_gain, mine, theirs = close(d_lin, attn_out, gain_full, hidden, cotangent, normed, w_full, o_all, wo_all, 1)[:5]
        block_out, grad_hidden, g_query, g_key, g_value, g_out = tail(block_out, grad_hidden, mine, theirs, q_heads, kv_heads, head_dim)
        return block_out[None], grad_hidden[None], grad_gain[0], g_query, g_key, g_value, g_out.reshape(w_out.shape)

    specs = (act_spec, act_spec, P("fsdp"), proj_spec, proj_spec, proj_spec, wout_spec)
    return jax.shard_map(device_step, mesh=mesh, in_specs=specs[:2] + (P("cp"),) + specs[2:], out_specs=specs, check_vma=False)
```

```python
import functools
import math

import jax
import jax.numpy as jnp
from jax import lax
from jax.experimental import pallas as pl
from jax.experimental.pallas import tpu as pltpu
from jax.sharding import PartitionSpec as P

WINDOW_LEN = 4096
ROPE_BASE = 10000.0
NORM_EPS = 1e-5
NEG_BIG = -1e30
LOG2E = math.log2(math.e)
TILES = 4
CHUNKS = 16
LEAD = 2
QUARTERS = 3
PIECES = 8
O_PIECES = 2
GRAD_CHUNKS = 8
FIRST_X = 6
EARLY = 6
GAIN_AT = 10
LATE = ((6, 4), (7, 9))
VMEM_BYTES = 67043328
SIDES = range(2)

MESH = pl.DeviceIdType.MESH
ANY = pl.BlockSpec(memory_space=pl.ANY)
VMEM = pl.BlockSpec(memory_space=pltpu.VMEM)
DMA = pltpu.SemaphoreType.DMA
BF, F32 = jnp.bfloat16, jnp.float32

NT = (((1,), (1,)), ((), ()))
NN = (((1,), (0,)), ((), ()))
TN = (((0,), (0,)), ((), ()))


def dot(a, b, dims):
    return lax.dot_general(a, b, dims, preferred_element_type=F32)


def parity(k):
    return lax.rem(k, 2)


def blk(k, n):
    return pl.ds(k * n if isinstance(k, int) else pl.multiple_of(k * n, n), n)


def lane_mean(vals):
    return jnp.mean(vals, axis=1, keepdims=True)


def row_sum(vals):
    return jnp.sum(vals, axis=0, keepdims=True)


def zero(ref):
    ref[...] = jnp.zeros_like(ref)


def remote(src, dst, send, recv, where):
    return pltpu.make_async_remote_copy(src_ref=src, dst_ref=dst, send_sem=send, recv_sem=recv, device_id=where, device_id_type=MESH)


def meet(peers):
    barrier = pltpu.get_barrier_semaphore()
    for where in peers:
        pl.semaphore_signal(barrier, inc=1, device_id=where, device_id_type=MESH)
    pl.semaphore_wait(barrier, len(peers))


def fsdp_peers(f):
    core = parity(f)
    other = f + 1 - 2 * core
    far = lax.rem(f + 2, 4)
    return other, far, lax.rem(other + 2, 4)


def others(axis, index, count):
    return [{axis: lax.rem(index + k, count)} for k in range(1, count)]


def nearest(z, last):
    near = jnp.where(z > 0, last, 1)
    second = jnp.where(z == 0, 2, jnp.where(z == last, last - 1, 1))
    return near, second


def rope(vals, cos, sin, half_dim):
    return vals * cos + pltpu.roll(vals, half_dim, 1) * sin


def causal(scores, tq):
    key_idx = lax.broadcasted_iota(jnp.int32, scores.shape, 0)
    q_idx = lax.rem(lax.broadcasted_iota(jnp.int32, scores.shape, 1), tq)
    return jnp.where(key_idx <= q_idx, scores, NEG_BIG)


def params(cid):
    return pltpu.CompilerParams(collective_id=cid, has_side_effects=True, vmem_limit_bytes=VMEM_BYTES)


def rope_tables(positions, head_dim):
    inv_freq = ROPE_BASE ** (-jnp.arange(0, head_dim, 2).astype(F32) / head_dim)
    angles = positions.astype(F32)[:, None] * inv_freq[None, :]
    cosines, sines = jnp.cos(angles), jnp.sin(angles)
    return jnp.concatenate([cosines, cosines], axis=1), jnp.concatenate([-sines, sines], axis=1)


def core_kernel(group, n_line, hid_ref, gain_ref, w_ref, wo_ref, cos_ref, sin_ref, ct_ref, d_ref, o_ref, gfull_ref, n_out, w_out, wo_all, o_all, wbuf, nbuf, acc, hbuf, gbuf, qs, vt, m_all, l_all, acc_all, q_ref, lse_ref, kl_ref, vl_ref, kp_ref, vp_ref, do_ref, dkl_ref, dvl_ref, dkp_ref, dvp_ref, qs_ref, dos_ref, delta_ref, kt_ref, dqt_ref, h_sem, g_send, g_recv, own_send, own_recv, x_send, x_recv, y_send, y_recv, d_send, d_recv, kv_send, kv_recv, ox_send, ox_recv, oy_send, oy_recv, od_send, od_recv, zw_send, zw_recv, out_sem, ct_sem, o_sems, o_recv, wy_send, wy_recv, wx_send, wx_recv, wc_send, wc_recv, cx_send, cx_recv, dk_send, dk_recv):
    q_len, feat = hid_ref.shape[0], w_ref.shape[0]
    head_dim = cos_ref.shape[1]
    half_dim = head_dim // 2
    kv_width = kl_ref.shape[1]
    kv_heads = kv_width // head_dim
    q_width = q_ref.shape[1]
    tq = q_len // TILES
    wide = group * tq
    score_scale = head_dim ** -0.5
    scale = head_dim ** -0.5 * LOG2E
    half = feat // 2
    piece = half // PIECES
    o_rows = wo_ref.shape[0]
    o_half = o_rows // 2
    o_piece = o_half // O_PIECES
    flag, f, z = lax.axis_index("cp"), lax.axis_index("fsdp"), lax.axis_index("tp")
    wo_out = wo_all.at[z]
    last = n_line - 1
    far = 1 - flag
    f_core, f_x, f_diag = fsdp_peers(f)
    to_core, to_x, to_diag, to_y = {"fsdp": f_core}, {"fsdp": f_x}, {"fsdp": f_diag}, {"cp": far}

    def h_load(tile):
        slot = parity(tile)
        return pltpu.make_async_copy(hid_ref.at[blk(tile, tq)], hbuf.at[slot], h_sem.at[slot])

    h_load(0).start()
    h_load(1).start()
    meet([to_core, to_x, to_diag, to_y] + others("tp", z, n_line))

    def span(side, j):
        return blk(side * PIECES + j, piece)

    def x_copy(j):
        return remote(w_ref.at[span(flag, j)], wbuf.at[f, span(flag, j)], x_send.at[j], x_recv.at[j], to_x)

    def x_in(j):
        return remote(w_ref.at[span(flag, j)], wbuf.at[f_x, span(flag, j)], x_send.at[j], x_recv.at[j], to_x)

    def y_copy(j, side):
        return remote(wbuf.at[f_x, span(side, j)], wbuf.at[f_x, span(side, j)], y_send.at[j], y_recv.at[j], to_y)

    def d_copy(j, side, slot):
        return remote(wbuf.at[slot, span(side, j)], wbuf.at[slot, span(side, j)], d_send.at[side, j], d_recv.at[side, j], to_core)

    def g_copy(k, where, slot):
        return remote(gain_ref, gbuf.at[slot], g_send.at[k], g_recv.at[k], where)

    def own_copy(slot):
        return remote(w_ref, wbuf.at[slot], own_send, own_recv, to_core)

    def o_span(side, j):
        return blk(side * O_PIECES + j, o_piece)

    def ox_copy(j, slot):
        return remote(wo_ref.at[o_span(flag, j)], wo_out.at[slot, o_span(flag, j)], ox_send.at[j], ox_recv.at[j], to_x)

    def oy_copy(j, side):
        return remote(wo_out.at[f_x, o_span(side, j)], wo_out.at[f_x, o_span(side, j)], oy_send.at[j], oy_recv.at[j], to_y)

    def od_copy(k, src, slot, where):
        return remote(src, wo_out.at[slot, where], od_send.at[k], od_recv.at[k], to_core)

    def zw_copy(up, t):
        spot = wo_all.at[t, f, blk(flag, o_half)]
        where = jnp.minimum(z + 1, last) if up else jnp.maximum(z - 1, 0)
        src = spot if t is not z else wo_ref.at[blk(flag, o_half)]
        return remote(src, spot, zw_send.at[up, t], zw_recv.at[t], {"tp": where})

    def zw_tick(r):
        for up, t, here in ((0, z + r, z + r <= last), (1, z - r, z >= r)):
            at = jnp.clip(t, 0, last)

            @pl.when(here)
            def _():
                zw_copy(up, at).wait_recv()

            @pl.when(here & (z < last if up else z > 0))
            def _():
                zw_copy(up, at).start()

    def tile_rows(j):
        return blk(j, tq)

    o_parts = kv_heads * TILES

    def o_piece_at(ref, j):
        return ref.at[tile_rows(lax.rem(j, TILES)), blk(j // TILES, group * head_dim)]

    def o_copy(up, t, j, own=False):
        spot = o_piece_at(o_all.at[t], j)
        src = o_piece_at(o_ref, j) if own else spot
        where = jnp.minimum(z + 1, last) if up else jnp.maximum(z - 1, 0)
        return remote(src, spot, o_sems.at[up, t, j], o_recv.at[t, j], {"tp": where})

    def wo_half(r, slot, side):
        return wo_all.at[lax.rem(z + r, n_line), slot, blk(side, o_half)]

    def wy_copy(r, side):
        return remote(wo_half(r, f, side), wo_half(r, f, side), wy_send.at[r - 1], wy_recv.at[r - 1], to_y)

    def wx_copy(r, side, slot):
        return remote(wo_half(r, slot, side), wo_half(r, slot, side), wx_send.at[side, r - 1], wx_recv.at[side, r - 1], to_x)

    def wc_copy(r, side, slot):
        return remote(wo_half(r, slot, side), wo_half(r, slot, side), wc_send.at[side, r - 1], wc_recv.at[side, r - 1], to_core)

    def cx_copy(r, side, slot):
        return remote(wo_half(r, slot, side), wo_half(r, slot, side), cx_send.at[side, r - 1], cx_recv.at[side, r - 1], to_core)

    def o_tick(k):
        r, j = k // o_parts + 1, lax.rem(k, o_parts)
        for up, t, here in ((0, z + r, z + r <= last), (1, z - r, z >= r)):
            at = jnp.clip(t, 0, last)

            @pl.when(here)
            def _():
                o_copy(up, at, j).wait_recv()

            @pl.when(here & (z < last if up else z > 0))
            def _():
                o_copy(up, at, j).start()

    def wy_tick(r):
        wy_copy(r, far).wait_recv()
        wx_copy(r, far, f).start()
        for side in (flag, far):
            wc_copy(r, side, f).start()
        if r == 1:
            wy_copy(last, flag).start()

    near, second = nearest(z, last)
    own_order = (near, second, n_line * last // 2 - near - second)

    def wx_tick(q):
        r, side = (own_order[q], flag) if q < last else (q - last + 1, far)
        wx_copy(r, side, f_x).wait_recv()
        cx_copy(r, side, f_x).start()

    def o_send(j):
        for up in SIDES:
            @pl.when(z < last if up else z > 0)
            def _():
                o_copy(up, z, j, True).start()

    gains = [(k, where, where["fsdp"]) for k, where in enumerate((to_core, to_x, to_diag))]
    for k, where, _ in gains:
        g_copy(k, where, f).start()
    sends = [x_copy(j) for j in range(PIECES)] + [ox_copy(j, f) for j in range(O_PIECES)]
    for j in range(LEAD):
        sends[j].start()
    own_copy(f).start()
    all_rows = pl.ds(0, o_rows)
    for up in SIDES:
        @pl.when(z < last if up else z > 0)
        def _():
            zw_copy(up, z).start()

    local_w = pltpu.make_async_copy(w_ref, wbuf.at[f], out_sem.at[0])
    local_w.start()
    local_o = pltpu.make_async_copy(wo_ref, wo_out.at[f], out_sem.at[1])
    local_o.start()
    gbuf[f] = gain_ref[...]
    for k, where, slot in gains:
        g_copy(k, where, slot).wait_recv()
    for k in range(gbuf.shape[0]):
        gfull_ref[:, blk(k, feat)] = gbuf[k].astype(F32)

    for tile in range(TILES):
        h_load(tile).wait()
        strip = min(32, tq)

        @pl.loop(0, tq // strip)
        def _(i):
            vals = hbuf[tile % 2, blk(i, strip), :].astype(F32)
            inv = lax.rsqrt(lane_mean(vals * vals) + NORM_EPS)
            nbuf[pl.ds(pl.multiple_of(tile * tq + i * strip, strip), strip), :] = (vals * inv * gfull_ref[...]).astype(BF)

        if tile + 2 < TILES:
            h_load(tile + 2).start()
    put_n = pltpu.make_async_copy(nbuf.at[pl.ds(0, q_len)], n_out, out_sem.at[2])
    put_n.start()

    def project(slot, start, rows, first=False):
        cols = pl.ds(pl.multiple_of(slot * feat + start, 128), rows)

        @pl.loop(0, TILES)
        def _(tile):
            here = blk(tile, tq)
            part = dot(nbuf[here, cols], wbuf[slot, pl.ds(start, rows), :], NN)
            acc[here, :] = part if first else acc[here, :] + part

    def x_tick(j):
        x_in(j).wait_recv()
        y_copy(j, flag).start()
        d_copy(j, flag, f_x).start()
        sends[j + LEAD].start()

    def y_tick(j):
        y_copy(j, far).wait_recv()
        d_copy(j, 1 - flag, f_x).start()

    local_w.wait()
    project(f, 0, feat, first=True)
    x_tick(0)
    x_tick(1)
    own_copy(f_core).wait_recv()
    od_copy(0, wo_ref, f, all_rows).start()
    project(f_core, 0, feat)
    for j in range(2, PIECES):
        x_tick(j)
        y_tick(j - 2)
        if j == PIECES // 2:
            zw_tick(1)
    for j in range(PIECES):
        d_copy(j, flag, f_diag).wait_recv()
    first_half = pl.multiple_of(flag * half, half)
    project(f_x, first_half, half)
    y_tick(PIECES - 2)
    project(f_diag, first_half, half)
    y_tick(PIECES - 1)
    for j in range(PIECES):
        d_copy(j, far, f_diag).wait_recv()
    second_half = pl.multiple_of(far * half, half)
    project(f_x, second_half, half)
    project(f_diag, second_half, half)
    zw_tick(2)
    wx_copy(near, flag, f).start()
    put_w = pltpu.make_async_copy(wbuf, w_out, out_sem.at[3])
    put_w.start()

    @pl.loop(0, TILES)
    def _(tile):
        here = blk(tile, tq)
        cos, sin = cos_ref[here, :], sin_ref[here, :]
        for h in range(kv_heads):
            k_at = q_width // head_dim + h
            kl_ref[here, blk(h, head_dim)] = rope(acc[here, blk(k_at, head_dim)], cos, sin, half_dim).astype(BF)
            vl_ref[here, blk(h, head_dim)] = acc[here, blk(k_at + kv_heads, head_dim)].astype(BF)

    kv_pairs = ((kl_ref, kp_ref), (vl_ref, vp_ref))

    def kv_copies(g):
        return [remote(src.at[:, blk(g, head_dim)], dst.at[:, blk(g, head_dim)], kv_send.at[k, g], kv_recv.at[k, g], {"cp": 1}) for k, (src, dst) in enumerate(kv_pairs)]

    @pl.when(flag == 0)
    def _():
        zero(kp_ref)
        zero(vp_ref)
        for g in range(kv_heads):
            for copy in kv_copies(g):
                copy.start()

    @pl.loop(0, TILES)
    def _(tile):
        here = blk(tile, tq)
        cos, sin = cos_ref[here, :], sin_ref[here, :]
        for h in range(group * kv_heads):
            cols = blk(h, head_dim)
            q_ref[here, cols] = rope(acc[here, cols], cos, sin, half_dim).astype(BF)

    def load_q(item):
        g, tile = item // TILES, lax.rem(item, TILES)
        rows = blk(tile, tq)
        for h in range(group):
            qs[:, blk(h, tq)] = q_ref[rows, blk(g * group + h, head_dim)].T

    def key_piece(item, k_ref, side, start, masked):
        g = item // TILES
        scores = dot(k_ref[start, blk(g, head_dim)], qs[...], NN)
        if masked:
            scores = causal(scores, tq)
        m_old = m_all[item]
        m_new = jnp.maximum(m_old, jnp.max(scores, axis=0, keepdims=True))
        probs = jnp.exp2((scores - m_new) * scale)
        fade = jnp.exp2((m_old - m_new) * scale)
        m_all[item] = m_new
        l_all[item] = l_all[item] * fade + row_sum(probs)
        acc_all[item] = acc_all[item] * fade + dot(vt[g, side, :, start], probs.astype(BF), NN)

    for g in range(kv_heads):
        vt[g, 0] = vl_ref[:, blk(g, head_dim)].T

    @pl.loop(0, kv_heads * TILES)
    def _(item):
        tile = lax.rem(item, TILES)
        load_q(item)
        m_all[item] = jnp.full_like(m_all[item], NEG_BIG)
        l_all[item] = jnp.zeros_like(l_all[item])
        acc_all[item] = jnp.zeros_like(acc_all[item])
        key_piece(item, kl_ref, 0, blk(tile, tq), True)

        @pl.loop(0, tile // 2)
        def _(i):
            key_piece(item, kl_ref, 0, blk(i, 2 * tq), False)

        @pl.when(parity(tile) == 1)
        def _():
            key_piece(item, kl_ref, 0, blk(tile - 1, tq), False)

    for j in range(O_PIECES):
        ox_copy(j, f_x).wait_recv()
        oy_copy(j, flag).start()
        od_copy(1 + j, wo_out.at[f_x, o_span(flag, j)], f_x, o_span(flag, j)).start()

    wx_copy(second, flag, f).start()
    zw_tick(last)

    @pl.loop(0, kv_heads * TILES)
    def _(item):
        g, tile = item // TILES, lax.rem(item, TILES)
        rows = blk(tile, tq)

        @pl.when((flag == 1) & (tile == 0))
        def _():
            for copy in kv_copies(g):
                copy.wait_recv()
            vt[g, 1] = vp_ref[:, blk(g, head_dim)].T

        @pl.when(flag == 1)
        def _():
            load_q(item)

        @pl.loop(0, flag * TILES // 2)
        def _(i):
            key_piece(item, kp_ref, 1, blk(i, 2 * tq), False)

        total = l_all[item]
        lse_ref[item] = m_all[item] * scale + jnp.log2(total)
        out_t = acc_all[item] / total
        for h in range(group):
            o_ref[rows, blk(g * group + h, head_dim)] = out_t[:, h * tq:h * tq + tq].T.astype(BF)

        @pl.when(item > 0)
        def _():
            o_send(item - 1)

        for j in range(O_PIECES):
            @pl.when(item == (j + 1) * kv_heads * TILES // O_PIECES - 1)
            def _():
                oy_copy(j, far).wait_recv()
                od_copy(1 + O_PIECES + j, wo_out.at[f_x, o_span(1 - flag, j)], f_x, o_span(1 - flag, j)).start()

    o_send(o_parts - 1)
    wx_copy(own_order[last - 1], flag, f).start()
    for r in range(1, last):
        wy_copy(r, flag).start()
    od_copy(0, wo_ref, f_core, all_rows).wait_recv()
    for j in range(O_PIECES):
        od_copy(1 + j, wo_out.at[f_x, o_span(flag, j)], f_diag, o_span(flag, j)).wait_recv()
        od_copy(1 + O_PIECES + j, wo_out.at[f_x, o_span(1 - flag, j)], f_diag, o_span(1 - flag, j)).wait_recv()

    put_n.wait()
    local_o.wait()
    n_parts, _, part = wo_out.shape
    loads = [pltpu.make_async_copy(wo_out.at[k], nbuf.at[pl.ds(0, o_rows), blk(k, part)], out_sem.at[4 + k]) for k in range(n_parts)]
    for load in loads:
        load.start()
    keep = pltpu.make_async_copy(o_ref, o_all.at[z], out_sem.at[2])
    keep.start()

    def ct_load(tile):
        slot = parity(tile)
        return pltpu.make_async_copy(ct_ref.at[blk(tile, tq)], hbuf.at[slot], ct_sem.at[slot])

    ct_load(0).start()
    ct_load(1).start()
    zero(dkl_ref)
    zero(dvl_ref)

    @pl.when(flag == 1)
    def _():
        zero(dkp_ref)
        zero(dvp_ref)

    wx_tick(0)
    for k in SIDES:
        o_tick(jnp.int32(k))
    for load in loads:
        load.wait()

    def do_tile(tile):
        ct_load(tile).wait()
        do_ref[tile_rows(tile), :] = dot(hbuf[parity(tile)], nbuf[pl.ds(0, o_rows), :], NT).astype(BF)

        @pl.when(tile + 2 < TILES)
        def _():
            ct_load(tile + 2).start()

    def bwd_item(item):
        g, tile = item // TILES, lax.rem(item, TILES)
        kv_cols = blk(g, head_dim)
        rows = blk(tile, tq)

        @pl.when(tile == 0)
        def _():
            kt_ref[0] = kl_ref[:, kv_cols].T
            kt_ref[1] = kp_ref[:, kv_cols].T

        for h in range(group):
            cols = blk(g * group + h, head_dim)
            stack = blk(h, tq)
            qs_ref[stack, :] = q_ref[rows, cols]
            d_h = do_ref[rows, cols]
            dos_ref[stack, :] = d_h
            prod = d_h.astype(F32) * o_ref[rows, cols].astype(F32)
            delta_ref[:, stack] = row_sum(prod.T)
        zero(dqt_ref)

        def piece(k_ref, v_ref, dk_ref, dv_ref, side, span, masked):
            scores = dot(k_ref[span, kv_cols], qs_ref[...], NT)
            if masked:
                scores = causal(scores, tq)
            probs = jnp.exp2(scores * (score_scale * LOG2E) - lse_ref[item])
            d_probs = dot(v_ref[span, kv_cols], dos_ref[...], NT)
            d_scores = (probs * (d_probs - delta_ref[...])).astype(BF)
            dv_ref[g, span, :] += dot(probs.astype(BF), dos_ref[...], NN)
            dk_ref[g, span, :] += dot(d_scores, qs_ref[...], NN)
            dqt_ref[...] += dot(kt_ref[side, :, span], d_scores, NN)

        piece(kl_ref, vl_ref, dkl_ref, dvl_ref, 0, blk(tile, tq), True)

        @pl.loop(0, tile // 2)
        def _(i):
            piece(kl_ref, vl_ref, dkl_ref, dvl_ref, 0, blk(i, 2 * tq), False)

        @pl.when(parity(tile) == 1)
        def _():
            piece(kl_ref, vl_ref, dkl_ref, dvl_ref, 0, blk(tile - 1, tq), False)

        @pl.loop(0, flag * TILES // 2)
        def _(i):
            piece(kp_ref, vp_ref, dkp_ref, dvp_ref, 1, blk(i, 2 * tq), False)

        for h in range(group):
            dq_h = dqt_ref[:, blk(h, tq)].T * score_scale
            d_ref[rows, blk(g * group + h, head_dim)] = rope(dq_h, cos_ref[rows, :], -sin_ref[rows, :], half_dim).astype(BF)

        @pl.when((tile == TILES - 1) & (flag == 1))
        def _():
            for copy in back(g):
                copy.start()

    def back(g):
        return [remote(ref.at[g], ref.at[g], dk_send.at[k, g], dk_recv.at[k, g], {"cp": 0}) for k, ref in enumerate((dkp_ref, dvp_ref))]

    def kv_done(g):
        @pl.when(flag == 0)
        def _():
            for copy in back(g):
                copy.wait_recv()
            dkl_ref[g] += dkp_ref[g]
            dvl_ref[g] += dvp_ref[g]

        dk = rope(dkl_ref[g] * score_scale, cos_ref[...], -sin_ref[...], half_dim)
        k_at = q_width // head_dim + g
        d_ref[:, blk(k_at, head_dim)] = dk.astype(BF)
        d_ref[:, blk(k_at + kv_heads, head_dim)] = dvl_ref[g].astype(BF)

        @pl.when(flag == 1)
        def _():
            for copy in back(g):
                copy.wait_send()

    items = TILES * (kv_heads + 1)
    plan = {1: [(wx_tick, 1)], 5: [(wy_tick, 1)], 6: [(wx_tick, 2)], 8: [(wy_tick, 2)], 9: [(wx_tick, 3)]}

    @pl.loop(0, items)
    def _(item):
        @pl.when(item < TILES)
        def _():
            do_tile(item)

        @pl.when(item >= TILES)
        def _():
            bwd_item(item - TILES)

        @pl.when(item != 1)
        def _():
            o_tick(jnp.where(item > 1, item + 1, 2))

        for at, jobs in plan.items():
            @pl.when(item == at)
            def _():
                for tick, arg in jobs:
                    tick(arg)

    rest = {1: (wy_tick, 3), 2: (wx_tick, 4), 5: (kv_done, 0), 6: (wx_tick, 5), 9: (kv_done, 1)}
    for k in range(items + 1, o_parts * last):
        o_tick(jnp.int32(k))
        if k - items in rest:
            tick, arg = rest[k - items]
            tick(arg)

    for r in range(1, n_line):
        for side in (flag, far):
            wc_copy(r, side, f_core).wait_recv()
            cx_copy(r, side, f_diag).wait_recv()
            wc_copy(r, side, f).wait_send()
            cx_copy(r, side, f_x).wait_send()
            wx_copy(r, side, f).wait_send()
        wy_copy(r, flag).wait_send()

    @pl.loop(0, n_line)
    def _(t):
        for up in SIDES:
            @pl.when((t <= z) & (z < last) if up else (t >= z) & (z > 0))
            def _():
                for j in range(o_parts):
                    o_copy(up, t, j).wait_send()

    @pl.loop(0, n_line)
    def _(t):
        for up in SIDES:
            @pl.when((t <= z) & (z < last) if up else (t >= z) & (z > 0))
            def _():
                zw_copy(up, t).wait_send()

    for k, where, _ in gains:
        g_copy(k, where, f).wait_send()
    own_copy(f).wait_send()
    od_copy(0, wo_ref, f, all_rows).wait_send()
    for j in range(PIECES):
        x_copy(j).wait_send()
        y_copy(j, flag).wait_send()
        d_copy(j, flag, f_x).wait_send()
        d_copy(j, 1 - flag, f_x).wait_send()
    for j in range(O_PIECES):
        ox_copy(j, f).wait_send()
        oy_copy(j, flag).wait_send()
        od_copy(1 + j, wo_out.at[f_x, o_span(flag, j)], f_x, o_span(flag, j)).wait_send()
        od_copy(1 + O_PIECES + j, wo_out.at[f_x, o_span(1 - flag, j)], f_x, o_span(1 - flag, j)).wait_send()

    @pl.when(flag == 0)
    def _():
        for g in range(kv_heads):
            for copy in kv_copies(g):
                copy.wait_send()

    for local in (keep, put_w):
        local.wait()


def core(hidden, gain, w_qkv, w_out, cosines, sines, cotangent, group, kv_width, n_line, cid):
    q_len, model_dim = hidden.shape
    feat, width = w_qkv.shape
    head_dim = cosines.shape[1]
    q_width = width - 2 * kv_width
    kv_heads = kv_width // head_dim
    o_rows, o_cols = w_out.shape
    n_fsdp = model_dim // feat
    tq = q_len // TILES
    wide = group * tq
    items = kv_heads * TILES
    sds = jax.ShapeDtypeStruct
    line = pltpu.VMEM((items, 1, wide), F32)
    kv = pltpu.VMEM((q_len, kv_width), BF)
    heads = pltpu.VMEM((q_len, q_width), BF)
    sums = pltpu.VMEM((kv_heads, q_len, head_dim), F32)
    stack = pltpu.VMEM((wide, head_dim), BF)
    own, pair, trio = DMA(()), DMA((2,)), DMA((n_fsdp - 1,))
    w_link, w_side, o_link, o_core = DMA((PIECES,)), DMA((2, PIECES)), DMA((O_PIECES,)), DMA((1 + 2 * O_PIECES,))
    hop, side, dkv = DMA((n_line - 1,)), DMA((2, n_line - 1)), DMA((2, kv_heads))
    return pl.pallas_call(
        functools.partial(core_kernel, group, n_line),
        in_specs=[ANY] + [VMEM] * 5 + [ANY],
        out_specs=[VMEM] * 3 + [ANY] * 4,
        out_shape=[sds((q_len, width), BF), sds((q_len, q_width), BF), sds((1, model_dim), F32), sds((q_len, model_dim), BF), sds((n_fsdp, feat, width), BF), sds((n_line, n_fsdp, o_rows, o_cols), BF), sds((n_line, q_len, q_width), BF)],
        scratch_shapes=[
            pltpu.VMEM((n_fsdp, feat, width), BF),
            pltpu.VMEM((max(q_len, o_rows), model_dim), BF),
            pltpu.VMEM((q_len, width), F32),
            pltpu.VMEM((2, tq, model_dim), BF),
            pltpu.VMEM((n_fsdp, 1, feat), BF),
            pltpu.VMEM((head_dim, wide), BF),
            pltpu.VMEM((kv_heads, 2, head_dim, q_len), BF),
            line,
            line,
            pltpu.VMEM((items, head_dim, wide), F32),
            heads,
            line,
            kv, kv, kv, kv,
            heads,
            sums, sums, sums, sums,
            stack,
            stack,
            pltpu.VMEM((1, wide), F32),
            pltpu.VMEM((2, head_dim, q_len), BF),
            pltpu.VMEM((head_dim, wide), F32),
        ] + [pair, trio, trio, own, own, w_link, w_link, w_link, w_link, w_side, w_side, dkv, dkv, o_link, o_link, o_link, o_link, o_core, o_core, DMA((2, n_line)), DMA((n_line,)), DMA((4 + n_fsdp,)), pair, DMA((2, n_line, items)), DMA((n_line, items)), hop, hop, side, side, side, side, side, side, dkv, dkv],
        compiler_params=params(cid),
        name="core",
    )(hidden, gain, w_qkv, w_out, cosines, sines, cotangent)


class Line:
    def __init__(self, n_line, buf_ref, pbuf_ref, send_sem, recv_sem, fill, finish):
        self.last = n_line - 1
        self.z = lax.axis_index("tp")
        self.buf, self.pbuf, self.send_sem, self.recv_sem = buf_ref, pbuf_ref, send_sem, recv_sem
        self.chunks, self.rows = buf_ref.shape[1], buf_ref.shape[2]
        self.block = pbuf_ref.shape[1]
        self.per_block = self.block // self.rows
        self.fill, self.finish = fill, finish
        self.steps = self.chunks + self.last

    def dist(self, side):
        return self.z if side else self.last - self.z

    def toward(self, side, back=False):
        up = bool(side) != back
        return {"tp": jnp.clip(self.z + 1 if up else self.z - 1, 0, self.last)}

    def copy(self, side, chunk):
        spot = self.buf.at[side, chunk]
        return remote(spot, spot, self.send_sem.at[side, chunk], self.recv_sem.at[side, chunk], self.toward(side))

    def live(self, side, step):
        chunk = step - self.dist(side)
        return chunk, (chunk >= 0) & (chunk < self.chunks)

    def prepare(self, step):
        for side in SIDES:
            chunk, ok = self.live(side, step)

            @pl.when(ok & (lax.rem(chunk, self.per_block) == 0))
            def _():
                self.fill(self.pbuf.at[side], blk((side * self.chunks + chunk) // self.per_block, self.block))

    def tick(self, step):
        for side in SIDES:
            chunk, ok = self.live(side, step)
            dist = self.dist(side)
            part = blk(lax.rem(jnp.maximum(chunk, 0), self.per_block), self.rows)

            @pl.when(ok & (dist == 0))
            def _():
                self.buf[side, chunk] = self.pbuf[side, part, :]

            @pl.when(ok & (dist > 0))
            def _():
                self.copy(side, chunk).wait_recv()
                self.buf[side, chunk] += self.pbuf[side, part, :]

            @pl.when(ok & (dist < self.last))
            def _():
                self.copy(side, chunk).start()

            @pl.when(ok & (dist == self.last))
            def _():
                self.finish(chunk, self.buf[side, chunk])

        self.prepare(step + 1)

    def drain(self):
        for side in SIDES:
            @pl.when(self.dist(side) < self.last)
            def _():
                @pl.loop(0, self.chunks)
                def _(chunk):
                    self.copy(side, chunk).wait_send()


def close_kernel(n_line, n_fsdp, d_ref, o_ref, gain_ref, hid_ref, ct_ref, n_ref, w_all, o_all, wo_all, out_ref, blk_ref, gg_ref, ts, yr, dl, xs, ks, xr, buf, gp, ga, gs, gb, gt, gc, ebuf, fb_in, fb_ct, fb_out, send_sem, recv_sem, w_sem, f_sem, ct_sem, fo_sem, lhs_sem, a_send, a_recv, ld_sem, st_sem, x_send, x_recv, e_sem, es_sem, y_send, y_recv, out_send, out_recv, o_sem, wl_sem, h_sem, r_sem, ga_send, ga_recv, gb_send, gb_recv, gc_send, gc_recv):
    last = n_line - 1
    z, flag, f = lax.axis_index("tp"), lax.axis_index("cp"), lax.axis_index("fsdp")
    far = 1 - flag
    f_core, f_x, f_diag = fsdp_peers(f)
    to_core, to_x, to_y = {"fsdp": f_core}, {"fsdp": f_x}, {"cp": far}
    _, feat, width = w_all.shape
    chunks, rows = buf.shape[1], buf.shape[2]
    half = chunks * rows
    g_rows = feat // GRAD_CHUNKS
    owner = (z == 0) | (z == last)
    own_base = jnp.where(z == last, chunks, 0)
    copy = pltpu.make_async_copy

    def own_span(chunk):
        return blk(own_base + chunk, rows)

    def f_loads(chunk):
        slot = parity(chunk)
        return copy(hid_ref.at[own_span(chunk)], fb_in.at[slot], f_sem.at[slot]), copy(ct_ref.at[own_span(chunk)], fb_ct.at[slot], ct_sem.at[slot])

    def f_store(chunk):
        slot = parity(chunk)
        return copy(fb_out.at[slot], out_ref.at[own_span(chunk)], fo_sem.at[slot])

    @pl.when(owner)
    def _():
        for chunk in SIDES:
            for load in f_loads(chunk):
                load.start()

    zero(gp)

    def finish(chunk, total):
        slot = parity(chunk)
        for load in f_loads(chunk):
            load.wait()

        @pl.when(chunk > 1)
        def _():
            f_store(chunk - 2).wait()

        x_in = fb_in[slot].astype(F32)
        inv = lax.rsqrt(lane_mean(x_in * x_in) + NORM_EPS)
        x_hat = x_in * inv
        gp[...] += row_sum(total * x_hat)
        scaled = total * gain_ref[...]
        fb_out[slot] = (fb_ct[slot].astype(F32) + inv * (scaled - x_hat * lane_mean(scaled * x_hat))).astype(BF)
        f_store(chunk).start()

        @pl.when(chunk + 2 < chunks)
        def _():
            for load in f_loads(chunk + 2):
                load.start()

    kinds = range(2)

    def g_at(ref, j):
        return ref.at[blk(j, g_rows)]

    def x_copy(j):
        return remote(g_at(xs, j), g_at(xr, j), x_send.at[j], x_recv.at[j], to_x)

    def y_copy(j):
        return remote(g_at(ts, j), g_at(yr, j), y_send.at[j], y_recv.at[j], to_y)

    def e_store(j):
        return copy(ebuf.at[0], g_at(ts, j), es_sem)

    def meet_x(j):
        x_copy(j).wait_recv()
        loads = [copy(g_at(src, j), ebuf.at[k], e_sem.at[k]) for k, src in enumerate((ks, xr))]
        for load in loads:
            load.start()
        for load in loads:
            load.wait()
        ebuf[0] += ebuf[1]
        e_store(j).start()

    def send_y(j):
        e_store(j).wait()
        y_copy(j).start()

    steps = chunks + last - 1

    def dist(side):
        return z if side else last - z

    def hop(side, chunk):
        span = blk(side * chunks + chunk, rows)
        up = z - 1 if side else z + 1
        return remote(out_ref.at[span], out_ref.at[span], out_send.at[side, chunk], out_recv.at[side, chunk], {"tp": jnp.clip(up, 0, last)})

    ends = [(end, z == (last if end else 0)) for end in SIDES]

    def owner_send(first, stop):
        for end, here in ends:
            @pl.when(here)
            def _():
                @pl.loop(first, stop)
                def _(c):
                    hop(end, c).start()

    def pass_on(step):
        for side in SIDES:
            chunk = step - (last - 1 - dist(side))

            @pl.when((dist(side) < last) & (chunk >= 0) & (chunk < chunks))
            def _():
                hop(side, chunk).wait_recv()

                @pl.when(dist(side) > 0)
                def _():
                    hop(side, chunk).start()

    def sum_phase(wbuf, pbuf, abuf, bbuf, lbuf, lhs):
        w_load = copy(w_all, wbuf, w_sem)
        w_load.start()

        def fill(dst, span):
            for k in range(n_fsdp):
                dst[:, blk(k, feat)] = dot(d_ref[span, :], wbuf[k], NT)

        line = Line(n_line, buf, pbuf, send_sem, recv_sem, fill, finish)
        slots = (f_diag, f_core, f_x, f)

        def lhs_loads(j):
            return [copy(src.at[:, blk(slot * GRAD_CHUNKS + j, g_rows)], lhs.at[m, k], lhs_sem.at[m, k]) for m, src in enumerate((n_ref, ct_ref)) for k, slot in enumerate(slots)]

        def a_copy(kind, j):
            return remote(abuf.at[kind], dl.at[kind, blk(j, g_rows)], a_send.at[kind], a_recv.at[kind, j], to_core)

        def b_stores(j):
            return [copy(bbuf.at[k], g_at(dst, j), st_sem.at[k]) for k, dst in enumerate((xs, ks))]

        def send_x(j):
            for kind in kinds:
                a_copy(kind, j).wait_send()
            for store in b_stores(j):
                store.wait()
            x_copy(j).start()

        def make(j):
            for load in lhs_loads(j):
                load.wait()
            for k in range(len(slots)):
                dst = (abuf, bbuf)[k // 2].at[k % 2]
                dst[:, :width] = dot(lhs[0, k], d_ref[...], TN)
                dst[:, width:] = dot(lhs[1, k], o_ref[...], TN)
            for kind in kinds:
                a_copy(kind, j).start()

            @pl.when(j + 1 < GRAD_CHUNKS)
            def _():
                for load in lhs_loads(j + 1):
                    load.start()

        def meet_core(j):
            loads = [copy(dl.at[kind, blk(j, g_rows)], lbuf.at[kind], ld_sem.at[kind]) for kind in kinds]
            for kind in kinds:
                a_copy(kind, j).wait_recv()
                loads[kind].start()
            for kind in kinds:
                loads[kind].wait()
                bbuf[kind] += lbuf[kind]
            for store in b_stores(j):
                store.start()

        for load in lhs_loads(0):
            load.start()
        w_load.wait()
        line.prepare(0)
        meet([to_core, to_x, to_y] + others("tp", z, n_line) + [{"fsdp": f_diag}])

        @pl.loop(0, line.steps)
        def _(fine):
            line.tick(fine)
            j, odd = fine // 2, parity(fine)

            @pl.when((odd == 0) & (j < GRAD_CHUNKS))
            def _():
                make(j)

            @pl.when((odd == 1) & (j < GRAD_CHUNKS))
            def _():
                meet_core(j)
                send_x(j)

            k = ((fine - FIRST_X) * 2 + 1) // 5

            @pl.when((k >= 0) & (k < EARLY) & (fine == FIRST_X + 5 * k // 2))
            def _():
                meet_x(k)
                send_y(k)

            @pl.when(fine >= chunks)
            def _():
                owner_send((fine - chunks) * LEAD, (fine - chunks + 1) * LEAD)

            @pl.when(fine > chunks)
            def _():
                for k in range(LEAD):
                    pass_on((fine - chunks - 1) * LEAD + k)

        @pl.when(owner)
        def _():
            for chunk in range(chunks - 2, chunks):
                f_store(chunk).wait()

        line.drain()

    pl.run_scoped(
        sum_phase,
        pltpu.VMEM(w_all.shape, BF),
        pltpu.VMEM((2, min(128, half), buf.shape[3]), F32),
        pltpu.VMEM((2, g_rows, ts.shape[1]), F32),
        pltpu.VMEM((2, g_rows, ts.shape[1]), F32),
        pltpu.VMEM((2, g_rows, ts.shape[1]), F32),
        pltpu.VMEM((2, n_fsdp, d_ref.shape[0], g_rows), BF),
    )
    def ga_copy(end, k):
        return remote(gp, ga.at[end], ga_send.at[k], ga_recv.at[end], {"tp": k if end else 1 + k})

    def gb_copy():
        return remote(gs, gb, gb_send, gb_recv, to_y)

    def gc_copy(k, slot):
        to = lax.rem(f + k, n_fsdp)
        return remote(gt.at[to], gc.at[slot], gc_send.at[k - 1], gc_recv.at[k - 1], {"fsdp": to})

    def spread_phase(obuf, wbuf, hbuf, rbuf):
        o_load = copy(o_all, obuf, o_sem)
        o_load.start()
        q_len, n_cols = hbuf.shape[1], hbuf.shape[2]
        per_part = wo_all.shape[3] // n_cols
        items = per_part * n_fsdp

        def item_loads(item):
            slot = parity(item)
            return copy(wo_all.at[:, item // per_part, :, blk(lax.rem(item, per_part), n_cols)], wbuf.at[slot], wl_sem.at[slot]), copy(hid_ref.at[:, blk(item, n_cols)], hbuf.at[slot], h_sem.at[slot])

        def item_store(item):
            slot = parity(item)
            return copy(rbuf.at[slot], blk_ref.at[:, blk(item, n_cols)], r_sem.at[slot])

        for item in SIDES:
            for load in item_loads(item):
                load.start()

        for end, here in ends:
            @pl.when(here)
            def _():
                ga[end] = gp[...]
                for k in range(last):
                    ga_copy(end, k).start()


        def project(quarter):
            item, tile = quarter // TILES, lax.rem(quarter, TILES)
            slot = parity(item)

            @pl.when(tile == 0)
            def _():
                for load in item_loads(item):
                    load.wait()

            @pl.when((tile == 0) & (item > 1))
            def _():
                item_store(item - 2).wait()

            span = blk(tile, q_len // TILES)
            total = sum(dot(obuf[t, span, :], wbuf[slot, t], NN) for t in range(n_line))
            rbuf[slot, span, :] = (hbuf[slot, span, :].astype(F32) + total).astype(BF)

            @pl.when(tile == TILES - 1)
            def _():
                item_store(item).start()

                @pl.when(item + 2 < items)
                def _():
                    for load in item_loads(item + 2):
                        load.start()

        for end, here in ends:
            @pl.when(jnp.logical_not(here))
            def _():
                ga_copy(end, 0).wait_recv()
        gs[...] = ga[0] + ga[1]
        gb_copy().start()

        early = (last - 1) * LEAD

        @pl.loop(0, steps - early)
        def _(step):
            sent = step + last * LEAD
            owner_send(sent, jnp.minimum(sent + 1, chunks))
            pass_on(step + early)

            @pl.when(step == 1)
            def _():
                o_load.wait()

            @pl.when(step == GAIN_AT)
            def _():
                gb_copy().wait()
                for k in range(n_fsdp):
                    gt[k] = gs[:, blk(k, feat)] + gb[:, blk(k, feat)]
                gc[f] = gt[f]

            @pl.when(step == GAIN_AT + 1)
            def _():
                for k in range(1, n_fsdp):
                    gc_copy(k, f).start()

            @pl.when(step > 0)
            def _():
                first = (step - 1) * QUARTERS

                @pl.loop(first, jnp.minimum(first + QUARTERS, items * TILES))
                def _(quarter):
                    project(quarter)

            for k, at in LATE:
                @pl.when(step == at)
                def _():
                    meet_x(k)
                    send_y(k)

        for item in range(items - 2, items):
            item_store(item).wait()

    pl.run_scoped(
        spread_phase,
        pltpu.VMEM(o_all.shape, BF),
        pltpu.VMEM((2, n_line, wo_all.shape[2], min(512, feat)), BF),
        pltpu.VMEM((2, d_ref.shape[0], min(512, feat)), BF),
        pltpu.VMEM((2, d_ref.shape[0], min(512, feat)), BF),
    )

    for side in SIDES:
        @pl.when(dist(side) > 0)
        def _():
            @pl.loop(0, chunks)
            def _(chunk):
                hop(side, chunk).wait_send()

    @pl.loop(0, GRAD_CHUNKS)
    def _(j):
        x_copy(j).wait_send()

    for k in range(1, n_fsdp):
        gc_copy(k, lax.rem(f + n_fsdp - k, n_fsdp)).wait_recv()
    gg_ref[...] = sum(gc[k] for k in range(n_fsdp))
    for k in range(1, n_fsdp):
        gc_copy(k, f).wait_send()
    for end, here in ends:
        @pl.when(here)
        def _():
            for k in range(last):
                ga_copy(end, k).wait_send()

    @pl.loop(0, GRAD_CHUNKS)
    def _(j):
        y_copy(j).wait()


def close(d_lin, attn_out, gain, hidden, cotangent, normed, w_full, o_all, wo_all, cid):
    q_len, model_dim = hidden.shape
    n_line, n_fsdp = wo_all.shape[:2]
    _, feat, width = w_full.shape
    g_width = width + attn_out.shape[1]
    half = q_len // 2
    rows = half // CHUNKS
    sds = jax.ShapeDtypeStruct
    row = pltpu.VMEM((1, model_dim), F32)
    slices = pltpu.VMEM((n_fsdp, 1, feat), F32)
    strip = pltpu.VMEM((2, rows, model_dim), BF)
    own, pair, line, grad, grads = DMA(()), DMA((2,)), DMA((2, CHUNKS)), DMA((GRAD_CHUNKS,)), DMA((2, GRAD_CHUNKS))
    z_trio, f_trio = DMA((n_line - 1,)), DMA((n_fsdp - 1,))
    act, g_part = sds((q_len, model_dim), BF), sds((feat, g_width), F32)
    return pl.pallas_call(
        functools.partial(close_kernel, n_line, n_fsdp),
        in_specs=[VMEM] * 3 + [ANY] * 6,
        out_specs=[ANY, ANY, VMEM] + [ANY] * 6,
        out_shape=[act, act, sds((1, feat), F32), g_part, g_part, sds((2, feat, g_width), F32), g_part, g_part, g_part],
        scratch_shapes=[
            pltpu.VMEM((2, CHUNKS, rows, model_dim), F32),
            row,
            pltpu.VMEM((2, 1, model_dim), F32),
            row,
            row,
            slices,
            slices,
            pltpu.VMEM((2, feat // GRAD_CHUNKS, g_width), F32),
            strip,
            strip,
            strip,
        ] + [line, line, own, pair, pair, pair, DMA((2, n_fsdp)), pair, grads, pair, pair, grad, grad, pair, own, grad, grad, line, line, own, pair, pair, pair, z_trio, pair, own, own, f_trio, f_trio],
        compiler_params=params(cid),
        name="close",
    )(d_lin, attn_out, gain, hidden, cotangent, normed, w_full, o_all, wo_all)


def tail_kernel(head_dim, blk_ref, hid_ref, mine_ref, theirs_ref, blk_out, hid_out, q_out, k_out, v_out, o_out):
    blk_out[...] = blk_ref[...]
    hid_out[...] = hid_ref[...]
    at = 0
    for ref in (q_out, k_out, v_out):
        for h in range(ref.shape[1]):
            cols = blk(at, head_dim)
            ref[:, h, :] = mine_ref[:, cols] + theirs_ref[:, cols]
            at += 1
    rest = slice(at * head_dim, None)
    o_out[...] = (mine_ref[:, rest] + theirs_ref[:, rest]).T


def tail(block_out, grad_hidden, mine, theirs, q_heads, kv_heads, head_dim):
    q_len, model_dim = block_out.shape
    feat = mine.shape[0]
    sds = jax.ShapeDtypeStruct
    act = pl.BlockSpec((q_len // GRAD_CHUNKS, model_dim), lambda i: (i, 0))
    part = pl.BlockSpec((feat // GRAD_CHUNKS, mine.shape[1]), lambda i: (i, 0))

    def heads(n):
        return pl.BlockSpec((feat // GRAD_CHUNKS, n, head_dim), lambda i: (i, 0, 0))

    def like(n):
        return sds((feat, n, head_dim), F32)

    o_rows = q_heads * head_dim
    return pl.pallas_call(
        functools.partial(tail_kernel, head_dim),
        grid=(GRAD_CHUNKS,),
        in_specs=[act, act, part, part],
        out_specs=[act, act, heads(q_heads), heads(kv_heads), heads(kv_heads), pl.BlockSpec((o_rows, feat // GRAD_CHUNKS), lambda i: (0, i))],
        out_shape=[sds(block_out.shape, BF), sds(block_out.shape, BF), like(q_heads), like(kv_heads), like(kv_heads), sds((o_rows, feat), F32)],
        compiler_params=pltpu.CompilerParams(vmem_limit_bytes=VMEM_BYTES),
        name="tail",
    )(block_out, grad_hidden, mine, theirs)


def solution(mesh):
    act_spec = P("fsdp", "cp", None)
    proj_spec = P("fsdp", "tp", None)
    wout_spec = P("tp", None, "fsdp")
    n_line = mesh.shape["tp"]

    def device_step(hidden, cotangent, positions, gain, w_query, w_key, w_value, w_out):
        hidden, cotangent = hidden[0], cotangent[0]
        assert hidden.shape[0] * mesh.shape["cp"] <= WINDOW_LEN
        feat, q_heads, head_dim = w_query.shape
        kv_heads = w_key.shape[1]
        group = q_heads // kv_heads
        q_width, kv_width = q_heads * head_dim, kv_heads * head_dim
        w_qkv = jnp.concatenate([w_query.reshape(feat, q_width), w_key.reshape(feat, kv_width), w_value.reshape(feat, kv_width)], axis=1)
        cosines, sines = rope_tables(positions, head_dim)
        d_lin, attn_out, gain_full, normed, w_full, wo_all, o_all = core(hidden, gain[None], w_qkv, w_out.reshape(q_width, feat), cosines, sines, cotangent, group, kv_width, n_line, 0)
        grad_hidden, block_out, grad_gain, mine, theirs = close(d_lin, attn_out, gain_full, hidden, cotangent, normed, w_full, o_all, wo_all, 1)[:5]
        block_out, grad_hidden, g_query, g_key, g_value, g_out = tail(block_out, grad_hidden, mine, theirs, q_heads, kv_heads, head_dim)
        return block_out[None], grad_hidden[None], grad_gain[0], g_query, g_key, g_value, g_out.reshape(w_out.shape)

    specs = (act_spec, act_spec, P("fsdp"), proj_spec, proj_spec, proj_spec, wout_spec)
    return jax.shard_map(device_step, mesh=mesh, in_specs=specs[:2] + (P("cp"),) + specs[2:], out_specs=specs, check_vma=False)
```
